32 devices in a mesh: ctx: 8 (over y, x, core), fsdp: 4 (over z).
Axes of the slice: x: 2, y: 2, z: 4, core: 2. Of those that a mesh axis runs over, the one named last changes fastest.
Arguments:
- tokens: bfloat16 [4, 1536, 1536], P('fsdp', 'ctx'), may hold values from -6 to 6
- positions: int32 [4, 1536], P('fsdp', 'ctx'), may hold values from 0 to 1535, as said below
- qkv_weight: bfloat16 [1, 1536, 3072], P(None, 'fsdp'), as said below
- out_weight: bfloat16 [1, 1536, 1536], P(None, 'fsdp'), may hold values from -2.5 to 2.5
- gate_up_weight: bfloat16 [1, 1536, 2, 4096], P(None, 'fsdp'), may hold values from -0.15625 to 0.15625
- down_weight: bfloat16 [1, 4096, 1536], P(None, 'fsdp'), may hold values from -0.09375 to 0.09375
- attn_gain: bfloat16 [1, 1536], P(None, 'fsdp'), may hold values from 0.5 to 1.5
- ffn_gain: bfloat16 [1, 1536], P(None, 'fsdp'), may hold values from 0.5 to 1.5
- cotangent: float32 [4, 1536, 1536], P('fsdp', 'ctx'), may hold values from -6 to 6
Outputs:
- activations: bfloat16 [4, 1536, 1536], P('fsdp', 'ctx')
- input_grad: float32 [4, 1536, 1536], P('fsdp', 'ctx')
- qkv_grad: float32 [1, 1536, 3072], P(None, 'fsdp')
- out_grad: float32 [1, 1536, 1536], P(None, 'fsdp')
- gate_up_grad: float32 [1, 1536, 2, 4096], P(None, 'fsdp')
- down_grad: float32 [1, 4096, 1536], P(None, 'fsdp')
- attn_gain_grad: float32 [1, 1536], P(None, 'fsdp')
- ffn_gain_grad: float32 [1, 1536], P(None, 'fsdp')
The draws below stay inside these ranges and needn't reach their ends.
Inputs may be any that keep to these rules, and one draw needn't show every extreme that they name: Each sequence holds every position of 0 to 1535 once. Its rows form aligned blocks of 192 rows; a block holds span c (the 96 positions from c * 96 on, in order) and then span 2 * 8 - 1 - c likewise; c differs between the blocks of a sequence. `qkv_weight`: projection weights of mean zero.
All inputs are finite; a program needn't handle non-finite values.
Results may differ from the reference program's by a relative error of at most 0.017.
The reference program's roundings to bfloat16 on the way count: a program that leaves them out, or rounds other values in their place, can miss the bound.
Values may be sent and summed in bfloat16 or wider, within the bound.
A program may use at most 320 MiB of HBM per device.

```python
import math
import jax
import jax.numpy as jnp
from jax import lax

D = 1536
HEADS = 16
KV_HEADS = 8
HEAD_DIM = 96
FF = 4096
LAYERS = 1
SPAN = 96
SEQS = 4
LENGTH = 1536


def draw_positions(key, part):
    devices = LENGTH // (2 * SPAN)

    def one_sequence(sequence_id):
        dealing = jax.random.permutation(jax.random.fold_in(key, sequence_id), devices).astype(jnp.int32)
        offsets = jnp.arange(SPAN, dtype=jnp.int32)
        early_rows = dealing[:, None] * SPAN + offsets[None, :]
        late_rows = (2 * devices - 1 - dealing)[:, None] * SPAN + offsets[None, :]
        return jnp.concatenate([early_rows, late_rows], axis=1).reshape(LENGTH)
    return jax.vmap(one_sequence)(jnp.arange(SEQS, dtype=jnp.int32))


def draw_qkv_weight(key, part):
    columns = (HEADS + 2 * KV_HEADS) * HEAD_DIM
    values = jax.random.normal(jax.random.fold_in(key, 3), (LAYERS, D, columns), jnp.float32) * D ** (-0.5)
    return values.astype(jnp.bfloat16)


def block_scale(own_key, dims, split, smallest, largest):
    factor_of, own = 1.0, jax.random.fold_in(own_key, 6)
    for axis_at, shards_of in split:
        heights = jnp.exp(jax.random.uniform(jax.random.fold_in(own, axis_at), (shards_of,), jnp.float32, smallest / len(split), largest / len(split)))
        factor_of = factor_of * jnp.repeat(heights, dims[axis_at] // shards_of).reshape([-1 if axis == axis_at else 1 for axis in range(len(dims))])
    return factor_of


def gaussian(rng, shape, width, reach, pieces=(), kind=jnp.bfloat16):
    level = block_scale(rng, shape, pieces, -0.22, 0.18) if pieces else 1.0
    drawn = jax.random.normal(rng, shape, jnp.float32) * width * level
    return jnp.minimum(jnp.maximum(drawn, -reach), reach).astype(kind)


def setup_inputs(seed: int = 0) -> dict:
    streams_of = jax.random.split(jax.random.key(seed), 10)
    return {
        "tokens": gaussian(streams_of[0], (SEQS, LENGTH, D), 1.0, 6.0, ((0, 4), (1, 8))),
        "positions": draw_positions(jax.random.fold_in(streams_of[9], 71), 0),
        "qkv_weight": draw_qkv_weight(jax.random.fold_in(streams_of[9], 71), 0),
        "out_weight": gaussian(streams_of[3], (LAYERS, HEADS * HEAD_DIM, D), (max(1, D // 256)) ** -0.5, 2.5, ((1, 4),)),
        "gate_up_weight": gaussian(streams_of[4], (LAYERS, D, 2, FF), D ** -0.5, 0.15625, ((1, 4),)),
        "down_weight": gaussian(streams_of[5], (LAYERS, FF, D), FF ** -0.5, 0.09375, ((1, 4),)),
        "attn_gain": jnp.clip(1.0 + 0.1 * jax.random.normal(streams_of[6], (LAYERS, D), jnp.float32), 0.5, 1.5).astype(jnp.bfloat16),
        "ffn_gain": jnp.clip(1.0 + 0.1 * jax.random.normal(streams_of[7], (LAYERS, D), jnp.float32), 0.5, 1.5).astype(jnp.bfloat16),
        "cotangent": gaussian(streams_of[8], (SEQS, LENGTH, D), 1.0, 6.0, ((0, 4), (1, 8)), jnp.float32),
    }


@jax.custom_vjp
def low(v):
    return lax.optimization_barrier(v.astype(jnp.bfloat16)).astype(jnp.float32)

@jax.custom_vjp
def low_back(v):
    return v

def low_keep(v):
    return (low(v), None)

def low_pass(kept, grad):
    return (grad,)

def back_keep(v):
    return (v, None)

def back_low(kept, grad):
    return (low(grad),)
low.defvjp(low_keep, low_pass)
low_back.defvjp(back_keep, back_low)
epsilon = 1e-05
rope_base = 100000.0

def product(left, right):
    return jnp.dot(left, right, preferred_element_type=jnp.float32, precision=lax.Precision.HIGHEST)

def normalize(rows, gain):
    factor = lax.rsqrt(lax.optimization_barrier(jnp.mean(rows * rows, axis=-1, keepdims=True)) + epsilon)
    return rows * factor * gain

def angles(place):
    halfway = HEAD_DIM // 2
    frequency = rope_base ** (-(jnp.arange(halfway, dtype=jnp.float32) * 2.0 / HEAD_DIM))
    phases = place.astype(jnp.float32)[:, None] * frequency[None, :]
    phases = jnp.concatenate([phases, phases], axis=-1)
    return (jnp.cos(phases)[:, None, :], jnp.sin(phases)[:, None, :])

def rotate(vectors, cosine, sine):
    halfway = vectors.shape[-1] // 2
    turned = jnp.concatenate([-vectors[..., halfway:], vectors[..., :halfway]], axis=-1)
    return vectors * cosine + turned * sine

def attend(queries, keys, values, place):
    groups = HEADS // KV_HEADS
    scaling = HEAD_DIM ** (-0.5)
    query_rows = math.gcd(LENGTH, 512)
    count = LENGTH // query_rows
    grouped = queries.reshape(count, query_rows, KV_HEADS, groups, HEAD_DIM)
    place_blocks = place.reshape(count, query_rows)

    def query_block(inputs):
        query_part, place_part = inputs
        scores = jnp.einsum('rkgd,skd->kgrs', query_part, keys, precision=lax.Precision.HIGHEST) * scaling
        scores = low_back(scores)
        allowed = place[None, None, None, :] <= place_part[None, None, :, None]
        scores = jnp.where(allowed, scores, -1e+30)
        softmax_rows = low(jax.nn.softmax(scores, axis=-1))
        return jnp.einsum('kgrs,skd->rkgd', softmax_rows, values, precision=lax.Precision.HIGHEST)
    result = lax.map(jax.checkpoint(query_block), (grouped, place_blocks))
    return result.reshape(LENGTH, HEADS * HEAD_DIM)

def layer(stream, place, qkv_full, out_full, gate_up_full, down_full, attn_full, ffn_full):
    cosine, sine = angles(place)
    query_width = HEADS * HEAD_DIM
    key_width = KV_HEADS * HEAD_DIM
    normed = low(normalize(stream, attn_full))
    projected = low_back(product(normed, qkv_full))
    queries = low(rotate(projected[:, :query_width].reshape(LENGTH, HEADS, HEAD_DIM), cosine, sine))
    keys = low(rotate(projected[:, query_width:query_width + key_width].reshape(LENGTH, KV_HEADS, HEAD_DIM), cosine, sine))
    values = low(projected[:, query_width + key_width:].reshape(LENGTH, KV_HEADS, HEAD_DIM))
    attended = low(low_back(attend(queries, keys, values, place)))
    middle = stream + low_back(product(attended, out_full))
    second = low(normalize(middle, ffn_full))
    gate_up = low_back(jnp.einsum('rd,dcf->rcf', second, gate_up_full, precision=lax.Precision.HIGHEST))
    hidden = low(jax.nn.silu(gate_up[:, 0]) * gate_up[:, 1])
    return middle + low_back(product(hidden, down_full))

def reference(tokens, positions, qkv_weight, out_weight, gate_up_weight, down_weight, attn_gain, ffn_gain, cotangent):
    params = (qkv_weight.astype(jnp.float32), out_weight.astype(jnp.float32), gate_up_weight.astype(jnp.float32), down_weight.astype(jnp.float32), attn_gain.astype(jnp.float32), ffn_gain.astype(jnp.float32))
    inputs = tokens.astype(jnp.float32)

    def forward(streams, weights):

        def single(pair):
            stream, place = pair
            for layer_id in range(LAYERS):
                stream = layer(stream, place, weights[0][layer_id], weights[1][layer_id], weights[2][layer_id], weights[3][layer_id], weights[4][layer_id], weights[5][layer_id])
            return stream
        return lax.map(single, (streams, positions))
    result, pullback = jax.vjp(forward, inputs, params)
    input_grad, grads = pullback(cotangent.astype(jnp.float32))
    return (result.astype(jnp.bfloat16), input_grad, grads[0], grads[1], grads[2], grads[3], grads[4], grads[5])
```

```python
import functools
import jax
import jax.numpy as jnp
from jax import lax
from jax.experimental import pallas as pl
from jax.experimental.pallas import tpu as pltpu
from jax.sharding import PartitionSpec as P

HEADS = 16
KV_HEADS = 8
HEAD_DIM = 96
LAYERS = 1


epsilon = 1e-05
rope_base = 100000.0


def angles(place):
    halfway = HEAD_DIM // 2
    frequency = rope_base ** (-(jnp.arange(halfway, dtype=jnp.float32) * 2.0 / HEAD_DIM))
    phases = place.astype(jnp.float32)[:, None] * frequency[None, :]
    phases = jnp.concatenate([phases, phases], axis=-1)
    return (jnp.cos(phases)[:, None, :], jnp.sin(phases)[:, None, :])


def rotate(vectors, cosine, sine):
    halfway = vectors.shape[-1] // 2
    turned = jnp.concatenate([-vectors[..., halfway:], vectors[..., :halfway]], axis=-1)
    return vectors * cosine + turned * sine


def rotate_back(grads, cosine, sine):
    halfway = grads.shape[-1] // 2
    scaled = grads * sine
    return grads * cosine + jnp.concatenate(
        [scaled[..., halfway:], -scaled[..., :halfway]], axis=-1
    )


def normalize(rows, gain):
    factor = lax.rsqrt(jnp.mean(rows * rows, axis=-1, keepdims=True) + epsilon)
    return (rows * factor * gain, factor)


def normalize_back(upstream, rows, factor, gain):
    unit_rows = rows * factor
    gain_grad = jnp.sum(upstream * unit_rows, axis=0)
    scaled = upstream * gain
    row_inner = jnp.mean(scaled * unit_rows, axis=-1, keepdims=True)
    return (factor * (scaled - unit_rows * row_inner), gain_grad)


def split_blocks(queries, keys_all, values_all, key_place):
    rows = queries.shape[0]
    half = rows // 2
    shards = key_place.shape[0] // rows
    key_blocks = keys_all.reshape(shards, 2, half, KV_HEADS, HEAD_DIM)
    value_blocks = values_all.reshape(shards, 2, half, KV_HEADS, HEAD_DIM)
    place_blocks = key_place.reshape(shards, 2, half)
    return (key_blocks, value_blocks, place_blocks)


def scores_of(queries, key_block, place_block, query_place):
    scaling = HEAD_DIM ** (-0.5)
    scores = (
        jnp.einsum("rkgd,skd->kgrs", queries, key_block, preferred_element_type=jnp.float32)
        * scaling
    )
    allowed = place_block[None, None, None, :] <= query_place[None, None, :, None]
    return (scores, allowed)


def reachable(place_block, query_place):
    return jnp.min(place_block) <= jnp.max(query_place)


def attention_forward(queries, keys_all, values_all, query_place, key_place):
    key_blocks, value_blocks, place_blocks = split_blocks(queries, keys_all, values_all, key_place)
    rows = queries.shape[0]
    half = rows // 2
    groups = HEADS // KV_HEADS
    query_spans = queries.reshape(2, half, KV_HEADS, groups, HEAD_DIM)
    place_spans = query_place.reshape(2, half)

    def sweep_max(carry, inputs):
        key_block, place_block = inputs
        updated_all = []
        for span in range(2):
            state = carry[span]
            for part in range(2):

                def live(current, span=span, part=part):
                    maximum, total = current
                    scores, allowed = scores_of(
                        query_spans[span], key_block[part], place_block[part], place_spans[span]
                    )
                    masked = jnp.where(allowed, scores, -1e30)
                    updated = jnp.maximum(maximum, jnp.max(masked, axis=-1))
                    weights_now = jnp.where(allowed, jnp.exp(masked - updated[..., None]), 0.0)
                    return (
                        updated,
                        total * jnp.exp(maximum - updated) + jnp.sum(weights_now, axis=-1),
                    )

                state = lax.cond(
                    reachable(place_block[part], place_spans[span]),
                    live,
                    lambda current: current,
                    state,
                )
            updated_all.append(state)
        return (tuple(updated_all), None)

    start_max = jnp.full((KV_HEADS, groups, half), -1e30, jnp.float32)
    start_total = jnp.zeros((KV_HEADS, groups, half), jnp.float32)
    start = ((start_max, start_total), (start_max, start_total))
    finals, unused = lax.scan(sweep_max, start, (key_blocks, place_blocks))
    logsum_spans = [finals[span][0] + jnp.log(finals[span][1]) for span in range(2)]

    def sweep_out(results, inputs):
        key_block, value_block, place_block = inputs
        updated_all = []
        for span in range(2):
            result = results[span]
            for part in range(2):

                def live(current, span=span, part=part):
                    scores, allowed = scores_of(
                        query_spans[span], key_block[part], place_block[part], place_spans[span]
                    )
                    softmax_rows = jnp.where(
                        allowed, jnp.exp(scores - logsum_spans[span][..., None]), 0.0
                    ).astype(jnp.bfloat16)
                    return current + jnp.einsum(
                        "kgrs,skd->rkgd",
                        softmax_rows,
                        value_block[part],
                        preferred_element_type=jnp.float32,
                    )

                result = lax.cond(
                    reachable(place_block[part], place_spans[span]),
                    live,
                    lambda current: current,
                    result,
                )
            updated_all.append(result)
        return (tuple(updated_all), None)

    start_out = jnp.zeros((half, KV_HEADS, groups, HEAD_DIM), jnp.float32)
    outs, unused_out = lax.scan(
        sweep_out, (start_out, start_out), (key_blocks, value_blocks, place_blocks)
    )
    logsum = jnp.concatenate(logsum_spans, axis=-1)
    attended = jnp.concatenate([outs[0], outs[1]], axis=0)
    return (logsum, attended)


def attention_backward(
    queries, keys_all, values_all, query_place, key_place, logsum, attended_grad, row_inner
):
    key_blocks, value_blocks, place_blocks = split_blocks(queries, keys_all, values_all, key_place)
    rows = queries.shape[0]
    half = rows // 2
    groups = HEADS // KV_HEADS
    scaling = HEAD_DIM ** (-0.5)
    query_spans = queries.reshape(2, half, KV_HEADS, groups, HEAD_DIM)
    place_spans = query_place.reshape(2, half)
    grad_spans = attended_grad.reshape(2, half, KV_HEADS, groups, HEAD_DIM)
    logsum_spans = logsum.reshape(KV_HEADS, groups, 2, half)
    inner_spans = row_inner.reshape(KV_HEADS, groups, 2, half)

    def sweep_back(query_grads, inputs):
        key_block, value_block, place_block = inputs
        query_grads = list(query_grads)
        key_parts = []
        value_parts = []
        for part in range(2):
            key_acc = jnp.zeros((half, KV_HEADS, HEAD_DIM), jnp.float32)
            value_acc = jnp.zeros((half, KV_HEADS, HEAD_DIM), jnp.float32)
            for span in range(2):

                def live(current, span=span, part=part):
                    query_grad, key_grad, value_grad = current
                    scores, allowed = scores_of(
                        query_spans[span], key_block[part], place_block[part], place_spans[span]
                    )
                    softmax_rows = jnp.where(
                        allowed, jnp.exp(scores - logsum_spans[:, :, span][..., None]), 0.0
                    )
                    rounded = softmax_rows.astype(jnp.bfloat16)
                    weight_grad = jnp.einsum(
                        "rkgd,skd->kgrs",
                        grad_spans[span],
                        value_block[part],
                        preferred_element_type=jnp.float32,
                    )
                    score_grad = (
                        softmax_rows * (weight_grad - inner_spans[:, :, span][..., None])
                    ).astype(jnp.bfloat16)
                    query_grad = (
                        query_grad
                        + jnp.einsum(
                            "kgrs,skd->rkgd",
                            score_grad,
                            key_block[part],
                            preferred_element_type=jnp.float32,
                        )
                        * scaling
                    )
                    key_grad = (
                        key_grad
                        + jnp.einsum(
                            "kgrs,rkgd->skd",
                            score_grad,
                            query_spans[span],
                            preferred_element_type=jnp.float32,
                        )
                        * scaling
                    )
                    value_grad = value_grad + jnp.einsum(
                        "kgrs,rkgd->skd",
                        rounded,
                        grad_spans[span],
                        preferred_element_type=jnp.float32,
                    )
                    return (query_grad, key_grad, value_grad)

                state = (query_grads[span], key_acc, value_acc)
                state = lax.cond(
                    reachable(place_block[part], place_spans[span]),
                    live,
                    lambda current: current,
                    state,
                )
                query_grads[span], key_acc, value_acc = state
            key_parts.append(key_acc)
            value_parts.append(value_acc)
        key_out = jnp.concatenate(key_parts, axis=0)
        value_out = jnp.concatenate(value_parts, axis=0)
        return (tuple(query_grads), (key_out, value_out))

    start_grad = jnp.zeros((half, KV_HEADS, groups, HEAD_DIM), jnp.float32)
    query_pair, (key_grads, value_grads) = lax.scan(
        sweep_back, (start_grad, start_grad), (key_blocks, value_blocks, place_blocks)
    )
    query_grad = jnp.concatenate([query_pair[0], query_pair[1]], axis=0)
    return (
        query_grad,
        key_grads.reshape(-1, KV_HEADS, HEAD_DIM),
        value_grads.reshape(-1, KV_HEADS, HEAD_DIM),
    )


def fetch_layer(qkv_weight, out_weight, gate_up_weight, down_weight, attn_gain, ffn_gain, layer_id):
    return (
        lax.all_gather(qkv_weight[layer_id], "fsdp", axis=0, tiled=True),
        lax.all_gather(out_weight[layer_id], "fsdp", axis=0, tiled=True),
        lax.all_gather(gate_up_weight[layer_id], "fsdp", axis=0, tiled=True),
        lax.all_gather(down_weight[layer_id], "fsdp", axis=0, tiled=True),
        lax.all_gather(attn_gain[layer_id], "fsdp", axis=0, tiled=True),
        lax.all_gather(ffn_gain[layer_id], "fsdp", axis=0, tiled=True),
    )


def fetch_again(qkv_weight, out_weight, gate_up_weight, down_weight, attn_gain, ffn_gain, layer_id):
    return (
        lax.all_gather(qkv_weight[layer_id], "fsdp", axis=0, tiled=True),
        lax.all_gather(out_weight[layer_id], "fsdp", axis=0, tiled=True),
        lax.all_gather(gate_up_weight[layer_id], "fsdp", axis=0, tiled=True),
        lax.all_gather(down_weight[layer_id], "fsdp", axis=0, tiled=True),
        lax.all_gather(attn_gain[layer_id], "fsdp", axis=0, tiled=True),
        lax.all_gather(ffn_gain[layer_id], "fsdp", axis=0, tiled=True),
    )


def forward_layer(stream, query_place, key_place, gathered):
    qkv_full, out_full, gate_up_full, down_full, attn_full, ffn_full = gathered
    rows = stream.shape[0]
    groups = HEADS // KV_HEADS
    query_width = HEADS * HEAD_DIM
    key_width = KV_HEADS * HEAD_DIM
    cosine, sine = angles(query_place)
    normed, first_factor = normalize(stream, attn_full.astype(jnp.float32))
    normed = normed.astype(jnp.bfloat16)
    projected = jnp.dot(normed, qkv_full, preferred_element_type=jnp.float32)
    queries = rotate(projected[:, :query_width].reshape(rows, HEADS, HEAD_DIM), cosine, sine)
    queries = queries.reshape(rows, KV_HEADS, groups, HEAD_DIM).astype(jnp.bfloat16)
    keys_local = rotate(
        projected[:, query_width : query_width + key_width].reshape(rows, KV_HEADS, HEAD_DIM),
        cosine,
        sine,
    ).astype(jnp.bfloat16)
    values_local = (
        projected[:, query_width + key_width :]
        .reshape(rows, KV_HEADS, HEAD_DIM)
        .astype(jnp.bfloat16)
    )
    keys_all, values_all = (
        lax.all_gather(keys_local, "ctx", axis=0, tiled=True),
        lax.all_gather(values_local, "ctx", axis=0, tiled=True),
    )
    logsum, attended = attention_forward(queries, keys_all, values_all, query_place, key_place)
    attended_low = attended.reshape(rows, query_width).astype(jnp.bfloat16)
    middle = stream + jnp.dot(attended_low, out_full, preferred_element_type=jnp.float32)
    second, second_factor = normalize(middle, ffn_full.astype(jnp.float32))
    second = second.astype(jnp.bfloat16)
    gate_up = jnp.einsum("rd,dcf->rcf", second, gate_up_full, preferred_element_type=jnp.float32)
    hidden = (jax.nn.silu(gate_up[:, 0]) * gate_up[:, 1]).astype(jnp.bfloat16)
    result = middle + jnp.dot(hidden, down_full, preferred_element_type=jnp.float32)
    stored = (
        stream,
        first_factor,
        normed,
        queries,
        keys_local,
        values_local,
        keys_all,
        values_all,
        logsum,
        attended,
        attended_low,
        middle,
        second_factor,
        second,
        gate_up,
        hidden,
    )
    return (result, stored)


def backward_layer(upstream, stored, gathered, query_place, key_place, keys_all, values_all):
    (
        stream,
        first_factor,
        normed,
        queries,
        keys_local,
        values_local,
        kept_keys,
        kept_values,
        logsum,
        attended,
        attended_low,
        middle,
        second_factor,
        second,
        gate_up,
        hidden,
    ) = stored
    qkv_full, out_full, gate_up_full, down_full, attn_full, ffn_full = gathered
    rows = stream.shape[0]
    groups = HEADS // KV_HEADS
    cosine, sine = angles(query_place)
    upstream_low = upstream.astype(jnp.bfloat16)
    hidden_grad = jnp.einsum(
        "rd,fd->rf", upstream_low, down_full, preferred_element_type=jnp.float32
    )
    gate_part = gate_up[:, 0]
    up_part = gate_up[:, 1]
    sigmoid = jax.nn.sigmoid(gate_part)
    gate_grad = hidden_grad * up_part * sigmoid * (1.0 + gate_part * (1.0 - sigmoid))
    up_grad = hidden_grad * gate_part * sigmoid
    gate_up_low = jnp.stack([gate_grad, up_grad], axis=1).astype(jnp.bfloat16)
    second_grad = jnp.einsum(
        "rcf,dcf->rd", gate_up_low, gate_up_full, preferred_element_type=jnp.float32
    )
    middle_grad, ffn_gain_grad = normalize_back(
        second_grad, middle, second_factor, ffn_full.astype(jnp.float32)
    )
    middle_grad = middle_grad + upstream
    middle_low = middle_grad.astype(jnp.bfloat16)
    attended_grad = jnp.einsum(
        "rd,od->ro", middle_low, out_full, preferred_element_type=jnp.float32
    )
    attended_grad = attended_grad.astype(jnp.bfloat16).reshape(rows, KV_HEADS, groups, HEAD_DIM)
    row_inner = jnp.einsum("rkgd,rkgd->kgr", attended_grad.astype(jnp.float32), attended)
    query_grad, key_grads, value_grads = attention_backward(
        queries, keys_all, values_all, query_place, key_place, logsum, attended_grad, row_inner
    )
    key_grad, value_grad = (
        lax.psum_scatter(key_grads, "ctx", scatter_dimension=0, tiled=True),
        lax.psum_scatter(value_grads, "ctx", scatter_dimension=0, tiled=True),
    )
    query_grad = rotate_back(query_grad.reshape(rows, HEADS, HEAD_DIM), cosine, sine)
    key_grad = rotate_back(key_grad, cosine, sine)
    projected_grad = jnp.concatenate(
        [query_grad.reshape(rows, -1), key_grad.reshape(rows, -1), value_grad.reshape(rows, -1)],
        axis=1,
    ).astype(jnp.bfloat16)
    normed_grad = jnp.einsum(
        "re,de->rd", projected_grad, qkv_full, preferred_element_type=jnp.float32
    )
    stream_grad, attn_gain_grad = normalize_back(
        normed_grad, stream, first_factor, attn_full.astype(jnp.float32)
    )
    stream_grad = stream_grad + middle_grad
    qkv_grad = jnp.einsum("rd,re->de", normed, projected_grad, preferred_element_type=jnp.float32)
    out_grad = jnp.einsum("ro,rd->od", attended_low, middle_low, preferred_element_type=jnp.float32)
    gate_up_grad = jnp.einsum(
        "rd,rcf->dcf", second, gate_up_low, preferred_element_type=jnp.float32
    )
    down_grad = jnp.einsum("rf,rd->fd", hidden, upstream_low, preferred_element_type=jnp.float32)
    sharded = (
        lax.psum_scatter(qkv_grad, "fsdp", scatter_dimension=0, tiled=True),
        lax.psum_scatter(out_grad, "fsdp", scatter_dimension=0, tiled=True),
        lax.psum_scatter(gate_up_grad, "fsdp", scatter_dimension=0, tiled=True),
        lax.psum_scatter(down_grad, "fsdp", scatter_dimension=0, tiled=True),
        lax.psum_scatter(attn_gain_grad, "fsdp", scatter_dimension=0, tiled=True),
        lax.psum_scatter(ffn_gain_grad, "fsdp", scatter_dimension=0, tiled=True),
    )
    totals = lax.psum(
        (sharded[0], sharded[1], sharded[2], sharded[3], sharded[4], sharded[5]), "ctx"
    )
    return (stream_grad, totals)


def body(
    tokens,
    positions,
    qkv_weight,
    out_weight,
    gate_up_weight,
    down_weight,
    attn_gain,
    ffn_gain,
    cotangent,
):
    query_place = positions[0]
    key_place = lax.all_gather(query_place, "ctx", axis=0, tiled=True)
    stream = tokens[0].astype(jnp.float32)
    gathered_list = []
    layer_id = 0
    gathered = fetch_layer(
        qkv_weight, out_weight, gate_up_weight, down_weight, attn_gain, ffn_gain, layer_id
    )
    stream, stored = forward_layer(stream, query_place, key_place, gathered)
    saved = [stored]
    gathered_list.append(gathered)
    activations = stream.astype(jnp.bfloat16)[None]
    upstream = cotangent[0]
    layer_grads = [None] * LAYERS
    for layer_id in reversed(range(LAYERS)):
        stored = saved[layer_id]
        gathered = fetch_again(
            qkv_weight, out_weight, gate_up_weight, down_weight, attn_gain, ffn_gain, layer_id
        )
        keys_all, values_all = (stored[6], stored[7])
        upstream, totals = backward_layer(
            upstream, stored, gathered, query_place, key_place, keys_all, values_all
        )
        layer_grads[layer_id] = totals
    outputs = [jnp.stack([entry[slot] for entry in layer_grads], axis=0) for slot in range(6)]
    return (
        activations,
        upstream[None],
        outputs[0],
        outputs[1],
        outputs[2],
        outputs[3],
        outputs[4],
        outputs[5],
    )


LANES = 128


def spread(heads):
    half = HEAD_DIM // 2
    pad = ((0, 0), (0, 0), (0, 64 - half))
    return jnp.concatenate([jnp.pad(heads[..., :half], pad), jnp.pad(heads[..., half:], pad)], axis=-1)


def gathered_spread(padded):
    half = HEAD_DIM // 2
    return jnp.concatenate([padded[..., :half], padded[..., 64 : 64 + half]], axis=-1)


def tables(length):
    half = HEAD_DIM // 2
    frequency = rope_base ** (-(jnp.arange(half, dtype=jnp.float32) * 2.0 / HEAD_DIM))
    phases = jnp.arange(length, dtype=jnp.float32)[:, None] * frequency[None, :]
    pad = ((0, 0), (0, 64 - half))
    cosine = jnp.pad(jnp.cos(phases), pad)
    sine = jnp.pad(jnp.sin(phases), pad)
    return (
        jnp.concatenate([cosine, cosine], axis=1),
        jnp.concatenate([-sine, sine], axis=1),
    )


def nt(left, right):
    return lax.dot_general(left, right, (((1,), (1,)), ((), ())), preferred_element_type=jnp.float32)


def nn(left, right):
    return lax.dot_general(left, right, (((1,), (0,)), ((), ())), preferred_element_type=jnp.float32)


def tn(left, right):
    return lax.dot_general(left, right, (((0,), (0,)), ((), ())), preferred_element_type=jnp.float32)


def causal(width):
    key_at = lax.broadcasted_iota(jnp.int32, (width, 2 * width), 0)
    query_at = lax.broadcasted_iota(jnp.int32, (width, 2 * width), 1)
    query_at = jnp.where(query_at >= width, query_at - width, query_at)
    return key_at <= query_at


def attend_kernel(
    span, tok_ref, gain_ref, w_ref, cos_ref, sin_ref,
    normed_ref, q_ref, k_ref, v_ref, att_ref, low_ref, lse_ref,
):
    length = tok_ref.shape[0]
    half = 96
    pairs = length // (2 * half)
    step = 2 * 2 * half
    lane = lax.broadcasted_iota(jnp.int32, (half, LANES), 1)
    for chunk in range(length // step):
        rows = pl.ds(chunk * step, step)
        x = tok_ref[rows, :].astype(jnp.float32)
        factor = lax.rsqrt(jnp.mean(x * x, axis=-1, keepdims=True) + epsilon)
        normed = (x * factor * gain_ref[...]).astype(jnp.bfloat16)
        normed_ref[rows, :] = normed
        proj = nn(normed, w_ref[...])
        for piece in range(step // half):
            at = span[chunk * (step // half) + piece]
            spot = pl.multiple_of(at * half, half)
            cosine = cos_ref[pl.ds(spot, half), :]
            sine = sin_ref[pl.ds(spot, half), :]
            mine = proj[piece * half : (piece + 1) * half]

            def turned(part):
                z = mine[:, part * LANES : (part + 1) * LANES]
                return (z * cosine + pltpu.roll(z, 64, 1) * sine).astype(jnp.bfloat16)

            base = (at // 2) * (4 * half) + (at % 2) * half
            q_ref[pl.ds(pl.multiple_of(base, half), half), :] = turned(0)
            q_ref[pl.ds(pl.multiple_of(base + 2 * half, half), half), :] = turned(1)
            k_ref[pl.ds(spot, half), :] = turned(2)
            v_ref[pl.ds(spot, half), :] = mine[:, 3 * LANES :].astype(jnp.bfloat16)
    scaling = HEAD_DIM ** (-0.5)
    mask = causal(2 * half)
    values_t = v_ref[...].astype(jnp.float32).T.astype(jnp.bfloat16)
    for pair in range(pairs):
        width = (pair + 1) * 2 * half
        q = q_ref[pl.ds(pair * 4 * half, 4 * half), :]
        scores = nt(k_ref[pl.ds(0, width), :], q) * scaling
        last = jnp.where(mask, scores[width - 2 * half :], -1e30)
        scores = last if pair == 0 else jnp.concatenate([scores[: width - 2 * half], last], axis=0)
        top = jnp.max(scores, axis=0, keepdims=True)
        e = jnp.exp(scores - top)
        total = jnp.sum(e, axis=0, keepdims=True)
        weights = (e * (1.0 / total)).astype(jnp.bfloat16)
        lse_ref[pl.ds(pair, 1), :] = top + jnp.log(total)
        out_t = nn(values_t[:, :width], weights)
        att_ref[pl.ds(pair * LANES, LANES), :] = out_t
        out = out_t.T.astype(jnp.bfloat16).astype(jnp.float32)
        for part in range(2):
            at = span[2 * pairs + 2 * pair + part]
            first = out[part * half : (part + 1) * half]
            second = pltpu.roll(out[(2 + part) * half : (3 + part) * half], half, 1)
            spot = pl.ds(pl.multiple_of(at * half, half), half)
            low_ref[spot, 0:LANES] = jnp.where(lane < half, first, second).astype(jnp.bfloat16)
            low_ref[spot, LANES : 2 * half] = second[:, : 2 * half - LANES].astype(jnp.bfloat16)


def back_kernel(
    span, grad_ref, q_ref, k_ref, v_ref, att_ref, lse_ref, cos_ref, sin_ref,
    out_ref, dk_ref, dv_ref,
):
    length = k_ref.shape[0]
    half = 96
    pairs = length // (2 * half)
    scaling = HEAD_DIM ** (-0.5)
    mask = causal(2 * half)
    lane = lax.broadcasted_iota(jnp.int32, (half, LANES), 1)
    keys_t = k_ref[...].astype(jnp.float32).T.astype(jnp.bfloat16)
    for pair in reversed(range(pairs)):
        width = (pair + 1) * 2 * half
        q = q_ref[pl.ds(pair * 4 * half, 4 * half), :]
        firsts, seconds = [], []
        for part in range(2):
            at = span[2 * pairs + 2 * pair + part]
            rows = pl.ds(pl.multiple_of(at * half, half), half)
            left = grad_ref[rows, 0:LANES].astype(jnp.float32)
            right = jnp.concatenate(
                [grad_ref[rows, LANES : 2 * half].astype(jnp.float32), jnp.zeros((half, 64), jnp.float32)], axis=1
            )
            firsts.append(jnp.where(lane < half, left, 0.0))
            seconds.append(pltpu.roll(jnp.where(lane < half, right, left), LANES - half, 1))
        seconds = [jnp.where(lane < half, s, 0.0) for s in seconds]
        grads = jnp.concatenate(firsts + seconds, axis=0)
        delta = jnp.sum(grads.T * att_ref[pl.ds(pair * LANES, LANES), :], axis=0, keepdims=True)
        grads = grads.astype(jnp.bfloat16)
        keys = k_ref[pl.ds(0, width), :]
        weights = jnp.exp(nt(keys, q) * scaling - lse_ref[pl.ds(pair, 1), :])
        last = jnp.where(mask, weights[width - 2 * half :], 0.0)
        weights = last if pair == 0 else jnp.concatenate([weights[: width - 2 * half], last], axis=0)
        dp = nt(v_ref[pl.ds(0, width), :], grads)
        ds = (weights * (dp - delta)).astype(jnp.bfloat16)
        dk = nn(ds, q) * scaling
        dv = nn(weights.astype(jnp.bfloat16), grads)
        if pair == pairs - 1:
            dk_ref[...] = dk
            dv_ref[...] = dv
        else:
            dk_ref[pl.ds(0, width), :] += dk
            dv_ref[pl.ds(0, width), :] += dv
        dq = nn(keys_t[:, :width], ds).T * scaling
        for part in range(2):
            at = span[2 * pairs + 2 * pair + part]
            rows = pl.ds(pl.multiple_of(at * half, half), half)
            spot = pl.ds((2 * pair + part) * half, half)
            cosine, sine = cos_ref[spot, :], sin_ref[spot, :]
            for head in range(2):
                z = dq[(2 * head + part) * half : (2 * head + part + 1) * half]
                out_ref[rows, head * LANES : (head + 1) * LANES] = (
                    z * cosine - pltpu.roll(z, 64, 1) * sine
                ).astype(jnp.bfloat16)
    for block in range(2 * pairs):
        at = span[2 * pairs + block]
        rows = pl.ds(pl.multiple_of(at * half, half), half)
        spot = pl.ds(block * half, half)
        z = dk_ref[spot, :]
        out_ref[rows, 2 * LANES : 3 * LANES] = (
            z * cos_ref[spot, :] - pltpu.roll(z, 64, 1) * sin_ref[spot, :]
        ).astype(jnp.bfloat16)
        out_ref[rows, 3 * LANES :] = dv_ref[spot, :].astype(jnp.bfloat16)


def vm(count):
    return [pl.BlockSpec(memory_space=pltpu.VMEM)] * count


MESH = pl.DeviceIdType.MESH


class Place:
    def __init__(self):
        self.me = lax.axis_index("ctx")
        core, x, y = self.me % 2, (self.me // 2) % 2, self.me // 4
        self.dp, self.dx, self.dy = 1 - 2 * core, 2 - 4 * x, 4 - 8 * y
        self.p, self.x, self.y = self.me + self.dp, self.me + self.dx, self.me + self.dy
        self.d = self.x + self.dy
        self.z = lax.axis_index("fsdp")
        self.planes = lax.axis_size("fsdp")
        self.n = lax.axis_size("ctx")


def greet(place, ctx=True, planes=False):
    barrier = pltpu.get_barrier_semaphore()
    count = 0
    if ctx:
        for step in range(1, place.n):
            pl.semaphore_signal(
                barrier, inc=1, device_id={"ctx": lax.rem(place.me + step, place.n)}, device_id_type=MESH
            )
            count += 1
    if planes:
        for step in range(1, place.planes):
            pl.semaphore_signal(
                barrier, inc=1, device_id={"fsdp": lax.rem(place.z + step, place.planes)}, device_id_type=MESH
            )
            count += 1
    pl.semaphore_wait(barrier, count)


def send(source, target, send_sem, recv_sem, **where):
    return pltpu.make_async_remote_copy(
        src_ref=source, dst_ref=target, send_sem=send_sem, recv_sem=recv_sem,
        device_id=where, device_id_type=MESH,
    )


class Gather:
    sems = 14

    def __init__(self, place, own, out, sem):
        self.place, self.own, self.out, self.sem = place, own, out, sem
        self.half = out.shape[1] // 2
        self.started = []
        self.met = False

    def go(self, source, target, index, rank):
        copy = send(source, target, self.sem.at[0, index], self.sem.at[1, index], ctx=rank)
        copy.start()
        self.started.append(copy)

    def part(self, rank, half):
        return self.out.at[rank, pl.ds(half * self.half, self.half)]

    def start(self):
        p = self.place
        keep = pltpu.make_async_copy(self.own, self.out.at[p.me], self.sem.at[0, 13])
        keep.start()
        self.keep = keep
        halves = [self.own.at[pl.ds(h * self.half, self.half)] for h in range(2)]
        self.go(halves[0], self.part(p.me, 0), 0, p.x)
        self.go(halves[1], self.part(p.me, 1), 3, p.y)
        self.go(self.own, self.out.at[p.me], 6, p.p)
        self.go(halves[1], self.part(p.me, 1), 1, p.x)
        self.go(halves[0], self.part(p.me, 0), 2, p.y)

    def arrived(self, rank, half, index):
        part = self.part(rank, half)
        pltpu.make_async_copy(part, part, self.sem.at[1, index]).wait()
        return part

    def relay(self):
        p = self.place
        part = self.arrived(p.x, 0, 0)
        self.go(part, part, 4, p.y)
        self.go(part, part, 7, p.p)
        part = self.arrived(p.y, 1, 3)
        self.go(part, part, 5, p.x)
        self.go(part, part, 10, p.p)

    def rest(self):
        p = self.place
        for rank, half, index, onward in ((p.x, 1, 1, 8), (p.y, 0, 2, 9), (p.d, 0, 4, 11), (p.d, 1, 5, 12)):
            part = self.arrived(rank, half, index)
            self.go(part, part, onward, p.p)

    def first_partner(self):
        part = self.out.at[self.place.p]
        pltpu.make_async_copy(part, part, self.sem.at[1, 6]).wait()
        self.met = True

    def partner(self):
        p = self.place
        if not self.met:
            self.first_partner()
        for rank, half, index in (
            (p.x, 0, 7), (p.y, 1, 10), (p.x, 1, 8), (p.y, 0, 9), (p.d, 0, 11), (p.d, 1, 12),
        ):
            self.arrived(rank + p.dp, half, index)

    def finish(self, kept=False):
        if not kept:
            self.keep.wait()
        for copy in self.started:
            copy.wait_send()


class PlaneGather:
    def __init__(self, place, own, out, sem):
        self.place, self.own, self.out, self.sem = place, own, out, sem

    def hop(self, step, up):
        p = self.place
        sign = 1 if up else -1
        source = p.z - sign * step
        target = p.z + sign
        ok = jnp.logical_and(
            jnp.logical_and(source >= 0, source < p.planes),
            jnp.logical_and(target >= 0, target < p.planes),
        )
        source = jnp.clip(source, 0, p.planes - 1)
        target = jnp.clip(target, 0, p.planes - 1)
        block = self.own if step == 0 else self.out.at[source]
        return ok, send(
            block, self.out.at[source], self.sem.at[0 if up else 1, source], self.sem.at[2, source], fsdp=target
        )

    def start(self):
        p = self.place
        self.keep = pltpu.make_async_copy(self.own, self.out.at[p.z], self.sem.at[2, p.z])
        self.keep.start()
        for up in (True, False):
            ok, copy = self.hop(0, up)
            pl.when(ok)(copy.start)

    def got(self, step, up):
        p = self.place
        source = p.z - step if up else p.z + step
        ok = jnp.logical_and(source >= 0, source < p.planes)
        source = jnp.clip(source, 0, p.planes - 1)
        part = self.out.at[source]
        return ok, pltpu.make_async_copy(part, part, self.sem.at[2, source])

    def step(self, number):
        for up in (True, False):
            ok, copy = self.got(number, up)
            pl.when(ok)(copy.wait)
            if number < self.place.planes - 1:
                ok, copy = self.hop(number, up)
                pl.when(ok)(copy.start)

    def finish(self):
        self.keep.wait()
        for number in range(self.place.planes - 1):
            for up in (True, False):
                ok, copy = self.hop(number, up)
                pl.when(ok)(copy.wait_send)


class Exchange:
    def __init__(self, place, blocks, out, sem):
        self.place, self.blocks, self.out, self.sem = place, blocks, out, sem

    def pick(self, rank):
        return self.blocks.at[rank]

    def copy(self, step):
        p = self.place
        rank = lax.rem(p.me + step, p.n)
        return send(self.pick(rank), self.out.at[p.me], self.sem.at[0, step], self.sem.at[1, step], ctx=rank)

    def start(self):
        p = self.place
        for step in range(1, p.n):
            self.copy(step).start()
        self.keep = pltpu.make_async_copy(self.pick(p.me), self.out.at[p.me], self.sem.at[0, 0])
        self.keep.start()

    def finish(self):
        p = self.place
        self.keep.wait()
        for step in range(1, p.n):
            self.copy(step).wait_send()
        for step in range(1, p.n):
            part = self.out.at[lax.rem(p.me + p.n - step, p.n)]
            pltpu.make_async_copy(part, part, self.sem.at[1, step]).wait()


class Share(Exchange):
    def pick(self, rank):
        return self.blocks


class PlaneShare:
    def __init__(self, place, block, out, sem):
        self.place, self.block, self.out, self.sem = place, block, out, sem

    def copy(self, step):
        p = self.place
        plane = lax.rem(p.z + step, p.planes)
        return send(self.block, self.out.at[p.z], self.sem.at[0, step], self.sem.at[1, step], fsdp=plane)

    def start(self):
        p = self.place
        for step in range(1, p.planes):
            self.copy(step).start()
        self.keep = pltpu.make_async_copy(self.block, self.out.at[p.z], self.sem.at[0, 0])
        self.keep.start()

    def finish(self):
        p = self.place
        self.keep.wait()
        for step in range(1, p.planes):
            self.copy(step).wait_send()
        for step in range(1, p.planes):
            part = self.out.at[lax.rem(p.z + p.planes - step, p.planes)]
            pltpu.make_async_copy(part, part, self.sem.at[1, step]).wait()


def anywhere(count):
    return [pl.BlockSpec(memory_space=pl.ANY)] * count


def first_kernel(tok, up, qkv, out_block, spot, gains, tok_all, up_all, qkv_all, out_all, spots, gain_all, *sems):
    place = Place()
    greet(place, planes=True)
    tokens = Gather(place, tok, tok_all, sems[0])
    cots = Gather(place, up, up_all, sems[1])
    qkvs = PlaneGather(place, qkv, qkv_all, sems[2])
    outs = PlaneGather(place, out_block, out_all, sems[3])
    spans = Share(place, spot, spots, sems[4])
    scales = PlaneShare(place, gains, gain_all, sems[5])
    spans.start()
    scales.start()
    qkvs.start()
    tokens.start()
    tokens.relay()
    qkvs.step(1)
    cots.start()
    qkvs.step(2)
    outs.start()
    tokens.rest()
    qkvs.step(3)
    tokens.partner()
    outs.step(1)
    cots.relay()
    outs.step(2)
    cots.rest()
    outs.step(3)
    cots.partner()
    for move in (spans, scales, qkvs, tokens, cots, outs):
        move.finish()


def first_moves(tok, up, qkv, out_block, spot, gains):
    n, planes = lax.axis_size("ctx"), lax.axis_size("fsdp")
    shape = lambda count, x: jax.ShapeDtypeStruct((count,) + x.shape, x.dtype)
    dma = pltpu.SemaphoreType.DMA
    return pl.pallas_call(
        first_kernel,
        out_shape=(
            shape(n, tok), shape(n, up), shape(planes, qkv), shape(planes, out_block), shape(n, spot), shape(planes, gains)
        ),
        in_specs=vm(6),
        out_specs=anywhere(6),
        scratch_shapes=[
            dma((2, Gather.sems)), dma((2, Gather.sems)), dma((3, planes)), dma((3, planes)), dma((2, n)), dma((2, planes)),
        ],
        compiler_params=pltpu.CompilerParams(collective_id=1, has_side_effects=True),
        name="first_moves",
    )(tok, up, qkv, out_block, spot, gains)


class Reduce:
    sems = 10

    def __init__(self, place, mine, theirs, first, out, second, sem):
        self.place, self.mine, self.theirs, self.first, self.out, self.second, self.sem = (
            place, mine, theirs, first, out, second, sem
        )
        self.half = out.shape[1]
        self.started = []

    def push(self, slot):
        copy = send(
            self.theirs.at[slot], self.first.at[slot], self.sem.at[0, slot], self.sem.at[1, slot], ctx=self.place.p
        )
        copy.start()
        return copy

    def pushed(self):
        for slot in range(4):
            send(
                self.theirs.at[slot], self.first.at[slot], self.sem.at[0, slot], self.sem.at[1, slot],
                ctx=self.place.p,
            ).wait_send()

    def add(self, slot):
        part = self.first.at[slot]
        pltpu.make_async_copy(part, part, self.sem.at[1, slot]).wait()
        self.mine[slot] = self.mine[slot] + self.first[slot].astype(jnp.float32)

    def go(self, index, value, rank):
        self.out[index] = value.astype(jnp.bfloat16)
        copy = send(
            self.out.at[index], self.second.at[index], self.sem.at[0, 4 + index], self.sem.at[1, 4 + index], ctx=rank
        )
        copy.start()
        self.started.append(copy)

    def top(self, slot):
        return self.mine[slot, pl.ds(0, self.half), :]

    def low(self, slot):
        return self.mine[slot, pl.ds(self.half, self.half), :]

    def got(self, index):
        part = self.second.at[index]
        pltpu.make_async_copy(part, part, self.sem.at[1, 4 + index]).wait()
        return self.second[index].astype(jnp.float32)

    def across(self):
        self.add(3)
        self.go(1, self.top(3), self.place.x)
        self.go(3, self.low(3), self.place.y)

    def beside(self):
        self.add(1)
        self.go(0, self.top(1), self.place.x)
        self.add(2)
        self.go(2, self.low(2), self.place.y)

    def turn(self):
        self.go(4, self.top(2) + self.got(1), self.place.y)
        self.go(5, self.low(1) + self.got(3), self.place.x)

    def total(self):
        self.add(0)
        upper = self.top(0) + self.got(0) + self.got(4)
        lower = self.low(0) + self.got(2) + self.got(5)
        return jnp.concatenate([upper, lower], axis=0)

    def finish(self):
        self.pushed()
        for copy in self.started:
            copy.wait_send()


def flip(place, i):
    return place.me + (i % 2) * place.dp + ((i // 2) % 2) * place.dx + (i // 4) * place.dy


def middle_kernel(
    low, tok, up, up_all, out_w, gu_w, down_w, gain,
    second_all, hidden, gul, agrad, mcols, middle_grad, result, gain_grad,
    attended, own, middle, agrad_send, mcols_send, mine, theirs, first, out, second, theirs2, first2, out2, second2,
    low_sem, gather_sem, reduce_sem, reduce_sem2, agrad_sem, mcols_sem,
):
    place = Place()
    n = place.n
    rows = tok.shape[0]
    heads = rows
    greet(place)
    moved = Exchange(place, low, attended, low_sem)
    moved.start()
    moved.finish()
    total = tok[...].astype(jnp.float32)
    for q in range(8):
        total = total + nn(attended[q], out_w[pl.ds(q * heads, heads), :])
    middle[...] = total
    factor = lax.rsqrt(jnp.mean(total * total, axis=-1, keepdims=True) + epsilon)
    own[...] = (total * factor * gain[...]).astype(jnp.bfloat16)
    seconds = Gather(place, own, second_all, gather_sem)
    seconds.start()
    grads = Reduce(place, mine, theirs, first, out, second, reduce_sem)
    wide = hidden.shape[2]

    def block(i, block_of):
        rank = flip(place, i)
        gate_up = nn(block_of(rank), gu_w[...])
        gate, raised = gate_up[:, :wide], gate_up[:, wide:]
        sigmoid = 1.0 / (1.0 + jnp.exp(-gate))
        silu = gate * sigmoid
        hidden[rank] = (silu * raised).astype(jnp.bfloat16)
        hidden_grad = nt(up_all[rank], down_w[...])
        gul[rank, :, pl.ds(0, wide)] = (hidden_grad * raised * sigmoid * (1.0 + gate * (1.0 - sigmoid))).astype(jnp.bfloat16)
        gul[rank, :, pl.ds(wide, wide)] = (hidden_grad * silu).astype(jnp.bfloat16)
        return nt(gul[rank], gu_w[...])

    def pair(k, carry):
        theirs[k] = block(2 * k + 1, lambda rank: second_all[rank]).astype(jnp.bfloat16)
        grads.push(k)
        mine[k] = block(2 * k, lambda rank: second_all[rank])
        return carry

    seconds.relay()
    seconds.keep.wait()
    seconds.first_partner()
    pair(0, 0)
    seconds.rest()
    seconds.partner()
    lax.fori_loop(1, 3, pair, 0)
    grads.beside()
    pair(3, 0)
    grads.across()

    sums = Reduce(place, mine, theirs2, first2, out2, second2, reduce_sem2)

    def other(k, carry):
        theirs2[k] = nn(hidden[flip(place, 2 * k + 1)], down_w[...]).astype(jnp.bfloat16)
        sums.push(k)
        return carry

    lax.fori_loop(0, 2, other, 0)
    grads.turn()
    lax.fori_loop(2, 4, other, 0)
    second_grad = grads.total()
    x = middle[...]
    factor = lax.rsqrt(jnp.mean(x * x, axis=-1, keepdims=True) + epsilon)
    unit = x * factor
    gain_grad[...] = jnp.sum(second_grad * unit, axis=0, keepdims=True)
    scaled = second_grad * gain[...]
    inner = jnp.mean(scaled * unit, axis=-1, keepdims=True)
    grad = up[...] + factor * (scaled - unit * inner)
    middle_grad[...] = grad
    rounded = grad.astype(jnp.bfloat16)
    seconds.finish(kept=True)
    own[...] = rounded
    for q in range(8):
        mcols_send[q] = rounded[:, q * heads : (q + 1) * heads]

    def head_grads(q, carry):
        agrad_send[q] = nt(own[...], out_w[pl.ds(pl.multiple_of(q * heads, heads), heads), :]).astype(jnp.bfloat16)
        return carry

    lax.fori_loop(0, n, head_grads, 0)
    heads_back = Exchange(place, agrad_send, agrad, agrad_sem)
    heads_back.start()
    columns = Exchange(place, mcols_send, mcols, mcols_sem)
    columns.start()

    def ours(k, carry):
        mine[k] = nn(hidden[flip(place, 2 * k)], down_w[...])
        return carry

    lax.fori_loop(0, 4, ours, 0)
    sums.across()
    sums.beside()
    sums.turn()
    result[...] = (middle[...] + sums.total()).astype(jnp.bfloat16)
    heads_back.finish()
    columns.finish()
    grads.finish()
    sums.finish()


def middle_moves(low, tok, up, up_all, out_w, gu_w, down_w, gain):
    n = lax.axis_size("ctx")
    rows, width = tok.shape
    wide = down_w.shape[0]
    bf, f32 = jnp.bfloat16, jnp.float32
    shape = jax.ShapeDtypeStruct
    dma = pltpu.SemaphoreType.DMA
    halves = pltpu.VMEM((6, rows // 2, width), bf)
    quads = pltpu.VMEM((4, rows, width), bf)
    blocks = pltpu.VMEM((n, rows, rows), bf)
    return pl.pallas_call(
        middle_kernel,
        out_shape=(
            shape((n, rows, width), bf), shape((n, rows, wide), bf), shape((n, rows, 2 * wide), bf),
            shape((n, rows, rows), bf), shape((n, rows, rows), bf), shape((rows, width), f32), shape((rows, width), bf),
            shape((1, width), f32),
        ),
        in_specs=vm(8),
        out_specs=vm(8),
        scratch_shapes=[
            blocks, pltpu.VMEM((rows, width), bf), pltpu.VMEM((rows, width), f32), blocks, blocks,
            pltpu.VMEM((4, rows, width), f32), quads, quads, halves, halves, quads, quads, halves, halves,
            dma((2, n)), dma((2, Gather.sems)), dma((2, Reduce.sems)), dma((2, Reduce.sems)), dma((2, n)), dma((2, n)),
        ],
        compiler_params=pltpu.CompilerParams(collective_id=5, has_side_effects=True, vmem_limit_bytes=67043328),
        name="middle_moves",
    )(low, tok, up, up_all, out_w, gu_w, down_w, gain)


def last_kernel(
    pgrad, qkv_w, tok, middle_grad, gain, ffn_gain, low, down_part, gu_part,
    grad, gains, low_all, down_all, gu_all,
    mine, theirs, first, out, second, mine_gain, ctx_gain, plane_sum, plane_gain,
    reduce_sem, gather_sem, down_sem, gu_sem, gain_sem, plane_sem,
):
    place = Place()
    greet(place, planes=True)
    grads = Reduce(place, mine, theirs, first, out, second, reduce_sem)

    def push(k, carry):
        theirs[k] = nt(pgrad[flip(place, 2 * k + 1)], qkv_w[...]).astype(jnp.bfloat16)
        grads.push(k)
        return carry

    def keep(k, carry):
        mine[k] = nt(pgrad[flip(place, 2 * k)], qkv_w[...])
        return carry

    lax.fori_loop(0, 4, push, 0)
    lax.fori_loop(0, 4, keep, 0)
    grads.across()
    grads.beside()
    grads.turn()
    moves = [
        Gather(place, low, low_all, gather_sem),
        Gather(place, down_part, down_all, down_sem),
        Gather(place, gu_part, gu_all, gu_sem),
    ]
    moves[0].start()
    normed_grad = grads.total()
    x = tok[...].astype(jnp.float32)
    factor = lax.rsqrt(jnp.mean(x * x, axis=-1, keepdims=True) + epsilon)
    unit = x * factor
    gain_grad = jnp.sum(normed_grad * unit, axis=0, keepdims=True)
    scaled = normed_grad * gain[...]
    inner = jnp.mean(scaled * unit, axis=-1, keepdims=True)
    grad[...] = middle_grad[...] + factor * (scaled - unit * inner)
    shard = mine_gain.shape[1]
    count = mine_gain.shape[0] // 2
    for at in range(count):
        mine_gain[pl.ds(at, 1), :] = gain_grad[:, at * shard : (at + 1) * shard]
        mine_gain[pl.ds(count + at, 1), :] = ffn_gain[:, at * shard : (at + 1) * shard]
    ctx_sum = Share(place, mine_gain, ctx_gain, gain_sem)
    ctx_sum.start()
    for at, move in enumerate(moves):
        if at:
            move.start()
        move.relay()
        move.rest()
    ctx_sum.finish()
    plane_sum[...] = jnp.sum(ctx_gain[...], axis=0)
    planes = PlaneShare(place, plane_sum, plane_gain, plane_sem)
    planes.start()
    for move in moves:
        move.partner()
    planes.finish()
    gains[...] = jnp.sum(plane_gain[...], axis=0)
    for move in moves:
        move.finish()
    grads.finish()


def last_moves(pgrad, qkv_w, tok, middle_grad, gain, ffn_gain, low, down_part, gu_part):
    n, planes = lax.axis_size("ctx"), lax.axis_size("fsdp")
    rows, width = tok.shape
    bf, f32 = jnp.bfloat16, jnp.float32
    shape = jax.ShapeDtypeStruct
    dma = pltpu.SemaphoreType.DMA
    halves = pltpu.VMEM((6, rows // 2, width), bf)
    quads = pltpu.VMEM((4, rows, width), bf)
    small = (2 * planes, width // planes)
    many = lambda x: shape((n,) + x.shape, x.dtype)
    return pl.pallas_call(
        last_kernel,
        out_shape=(
            shape((rows, width), f32), shape(small, f32), many(low), many(down_part), many(gu_part),
        ),
        in_specs=vm(9),
        out_specs=vm(2) + anywhere(3),
        scratch_shapes=[
            pltpu.VMEM((4, rows, width), f32), quads, quads, halves, halves,
            pltpu.VMEM(small, f32), pltpu.VMEM((n,) + small, f32), pltpu.VMEM(small, f32), pltpu.VMEM((planes,) + small, f32),
            dma((2, Reduce.sems)), dma((2, Gather.sems)), dma((2, Gather.sems)), dma((2, Gather.sems)), dma((2, n)), dma((2, planes)),
        ],
        compiler_params=pltpu.CompilerParams(collective_id=6, has_side_effects=True, vmem_limit_bytes=67043328),
        name="last_moves",
    )(pgrad, qkv_w, tok, middle_grad, gain, ffn_gain, low, down_part, gu_part)


def gathers_kernel(count, *refs):
    place = Place()
    greet(place)
    moves = [Gather(place, refs[at], refs[count + at], refs[2 * count + at]) for at in range(count)]
    for move in moves:
        move.start()
        move.relay()
        move.rest()
    for move in moves:
        move.partner()
    for move in moves:
        move.finish()


def gathers(number, *arrays):
    n = lax.axis_size("ctx")
    count = len(arrays)
    return pl.pallas_call(
        functools.partial(gathers_kernel, count),
        out_shape=tuple(jax.ShapeDtypeStruct((n,) + x.shape, x.dtype) for x in arrays),
        in_specs=vm(count),
        out_specs=anywhere(count),
        scratch_shapes=[pltpu.SemaphoreType.DMA((2, Gather.sems))] * count,
        compiler_params=pltpu.CompilerParams(collective_id=number, has_side_effects=True),
        name="gathers",
    )(*arrays)


def attend(spans, tokens_all, gain, weight, cosine, sine):
    length = tokens_all.shape[0]
    pairs = length // 192
    shapes = (
        jax.ShapeDtypeStruct(tokens_all.shape, jnp.bfloat16),
        jax.ShapeDtypeStruct((2 * length, LANES), jnp.bfloat16),
        jax.ShapeDtypeStruct((length, LANES), jnp.bfloat16),
        jax.ShapeDtypeStruct((length, LANES), jnp.bfloat16),
        jax.ShapeDtypeStruct((pairs * LANES, 384), jnp.float32),
        jax.ShapeDtypeStruct((length, 192), jnp.bfloat16),
        jax.ShapeDtypeStruct((pairs, 384), jnp.float32),
    )
    return pl.pallas_call(
        attend_kernel,
        out_shape=shapes,
        in_specs=[pl.BlockSpec(memory_space=pltpu.SMEM)] + vm(5),
        out_specs=vm(7),
        name="attend",
    )(spans, tokens_all, gain, weight, cosine, sine)


def attend_back(spans, grad, q, k, v, att, lse, cosine, sine):
    length = k.shape[0]
    return pl.pallas_call(
        back_kernel,
        out_shape=jax.ShapeDtypeStruct((length, 4 * LANES), jnp.bfloat16),
        in_specs=[pl.BlockSpec(memory_space=pltpu.SMEM)] + vm(8),
        out_specs=pl.BlockSpec(memory_space=pltpu.VMEM),
        scratch_shapes=[pltpu.VMEM((length, LANES), jnp.float32)] * 2,
        name="attend_back",
    )(spans, grad, q, k, v, att, lse, cosine, sine)


def fast_body(
    tokens, positions, qkv_weight, out_weight, gate_up_weight, down_weight, attn_gain, ffn_gain, cotangent
):
    me = lax.axis_index("ctx")
    n = lax.axis_size("ctx")
    planes = lax.axis_size("fsdp")
    rows = tokens.shape[1]
    length = n * rows
    width = tokens.shape[2]
    wide = down_weight.shape[1] * planes
    shard = qkv_weight.shape[1]
    query_width = HEADS * HEAD_DIM
    key_width = KV_HEADS * HEAD_DIM

    def pick(x, axis):
        return lax.dynamic_index_in_dim(x, me, axis, keepdims=False)

    qkv = qkv_weight[0]
    q_part = pick(qkv[:, :query_width].reshape(shard, n, 2, HEAD_DIM), 1)
    k_part = pick(qkv[:, query_width : query_width + key_width].reshape(shard, n, 1, HEAD_DIM), 1)
    v_part = pick(qkv[:, query_width + key_width :].reshape(shard, n, HEAD_DIM), 1)
    qk = spread(jnp.concatenate([q_part, k_part], axis=1)).reshape(shard, 3 * LANES)
    qkv_block = jnp.concatenate([qk, jnp.pad(v_part, ((0, 0), (0, LANES - HEAD_DIM)))], axis=1)
    out_rows = shard // n
    out_block = pick(out_weight[0].reshape(n, out_rows, width), 0)
    gate_up_block = pick(gate_up_weight[0].reshape(shard, 2, planes, n, wide // planes // n), 3)
    gate_up_block = lax.all_gather(gate_up_block, "fsdp", axis=0, tiled=True)
    gate_up_block = gate_up_block.reshape(planes * shard, 2 * wide // n)
    down_block = pick(down_weight[0].reshape(n, -1, width), 0)
    down_block = lax.all_gather(down_block, "fsdp", axis=0, tiled=True)
    upstream = cotangent[0]
    gains = jnp.concatenate([attn_gain, ffn_gain, jnp.zeros((6, shard), attn_gain.dtype)], axis=0).astype(jnp.float32)
    spot = jnp.full((8, LANES), positions[0, 0], jnp.int32)
    tokens_all, upstream_all, qkv_block, out_block, spots, gains = first_moves(
        tokens[0], upstream.astype(jnp.bfloat16), qkv_block, out_block.reshape(out_rows, width), spot, gains
    )
    tokens_all = tokens_all.reshape(length, width)
    qkv_block = qkv_block.reshape(width, -1)
    gains = gains[:, :2].transpose(1, 0, 2).reshape(2, width)
    attn_full, ffn_full = gains[0], gains[1]
    (out_full,) = gathers(2, out_block.reshape(planes * out_rows, width))
    out_full = out_full.reshape(n, planes, out_rows, width).transpose(1, 0, 2, 3).reshape(planes * shard, width)

    early = spots[:, 0, 0] // (rows // 2)
    span = jnp.stack([early, 2 * n - 1 - early], axis=1).reshape(2 * n)
    order = jnp.sum(
        jnp.where(span[None, :] == jnp.arange(2 * n)[:, None], jnp.arange(2 * n)[None, :], 0), axis=1
    )
    spans = jnp.concatenate([span, order]).astype(jnp.int32)
    cosine, sine = tables(length)

    normed, q, k, v, att, low, lse = attend(spans, tokens_all, attn_full[None], qkv_block, cosine, sine)

    second_all, hidden, gate_up_low, attended_grad, middle_cols, middle_grad, result, ffn_partial = middle_moves(
        low.reshape(n, rows, -1), tokens[0], upstream, upstream_all, out_full, gate_up_block, down_block, ffn_full[None]
    )
    own = wide // n
    second_all = second_all.reshape(length, width)
    hidden = hidden.reshape(length, own)
    gate_up_low = gate_up_low.reshape(length, 2 * own)

    def reduce_planes(block):
        return lax.psum_scatter(block.astype(jnp.bfloat16), "fsdp", scatter_dimension=0, tiled=True)

    down_grad = reduce_planes(tn(hidden, upstream_all.reshape(length, width)))
    gate_up_grad = reduce_planes(tn(second_all, gate_up_low))
    projected_grad = attend_back(
        spans, attended_grad.reshape(length, -1), q, k, v, att, lse, cosine, sine
    )
    stream_grad, gains, low_all, down_grad, gate_up_grad = last_moves(
        projected_grad.reshape(n, rows, -1), qkv_block, tokens[0], middle_grad, attn_full[None], ffn_partial,
        low, down_grad, gate_up_grad,
    )
    low_all = low_all.transpose(1, 0, 2).reshape(length, query_width)
    gains = gains.reshape(2, planes, shard)
    gains = lax.dynamic_index_in_dim(gains, lax.axis_index("fsdp"), 1, keepdims=False)
    qkv_grad = reduce_planes(tn(normed, projected_grad))
    out_grad = reduce_planes(tn(low_all, middle_cols.reshape(length, -1)))
    qkv_grad, out_grad = gathers(7, qkv_grad, out_grad)
    pieces = qkv_grad.reshape(n, shard, 4, LANES).transpose(1, 0, 2, 3)
    qkv_grad = jnp.concatenate(
        [
            gathered_spread(pieces[:, :, 0:2]).reshape(shard, query_width),
            gathered_spread(pieces[:, :, 2]).reshape(shard, key_width),
            pieces[:, :, 3, :HEAD_DIM].reshape(shard, key_width),
        ],
        axis=1,
    ).astype(jnp.float32)
    out_grad = out_grad.transpose(1, 0, 2).reshape(shard, width).astype(jnp.float32)
    gate_up_grad = gate_up_grad.reshape(n, shard, 2, planes, -1).transpose(1, 2, 3, 0, 4)
    gate_up_grad = gate_up_grad.reshape(shard, 2, wide).astype(jnp.float32)
    down_grad = down_grad.reshape(-1, width).astype(jnp.float32)
    return (
        result[None],
        stream_grad[None],
        qkv_grad[None],
        out_grad[None],
        gate_up_grad[None],
        down_grad[None],
        gains[0][None],
        gains[1][None],
    )


def solution(mesh):
    split = mesh.shape["ctx"] == KV_HEADS
    placed = (
        P("fsdp", "ctx", None),
        P("fsdp", "ctx"),
        P(None, "fsdp", None),
        P(None, "fsdp", None),
        P(None, "fsdp", None, None),
        P(None, "fsdp", None),
        P(None, "fsdp"),
        P(None, "fsdp"),
        P("fsdp", "ctx", None),
    )
    return jax.shard_map(
        fast_body if split else body,
        mesh=mesh,
        in_specs=placed,
        out_specs=(
            P("fsdp", "ctx", None),
            P("fsdp", "ctx", None),
            P(None, "fsdp", None),
            P(None, "fsdp", None),
            P(None, "fsdp", None, None),
            P(None, "fsdp", None),
            P(None, "fsdp"),
            P(None, "fsdp"),
        ),
        check_vma=False,
    )
```

```python
import functools
import jax
import jax.numpy as jnp
from jax import lax
from jax.experimental import pallas as pl
from jax.experimental.pallas import tpu as pltpu
from jax.sharding import PartitionSpec as P

HEADS = 16
KV_HEADS = 8
HEAD_DIM = 96
LAYERS = 1


epsilon = 1e-05
rope_base = 100000.0


def angles(place):
    halfway = HEAD_DIM // 2
    frequency = rope_base ** (-(jnp.arange(halfway, dtype=jnp.float32) * 2.0 / HEAD_DIM))
    phases = place.astype(jnp.float32)[:, None] * frequency[None, :]
    phases = jnp.concatenate([phases, phases], axis=-1)
    return (jnp.cos(phases)[:, None, :], jnp.sin(phases)[:, None, :])


def rotate(vectors, cosine, sine):
    halfway = vectors.shape[-1] // 2
    turned = jnp.concatenate([-vectors[..., halfway:], vectors[..., :halfway]], axis=-1)
    return vectors * cosine + turned * sine


def rotate_back(grads, cosine, sine):
    halfway = grads.shape[-1] // 2
    scaled = grads * sine
    return grads * cosine + jnp.concatenate(
        [scaled[..., halfway:], -scaled[..., :halfway]], axis=-1
    )


def normalize(rows, gain):
    factor = lax.rsqrt(jnp.mean(rows * rows, axis=-1, keepdims=True) + epsilon)
    return (rows * factor * gain, factor)


def normalize_back(upstream, rows, factor, gain):
    unit_rows = rows * factor
    gain_grad = jnp.sum(upstream * unit_rows, axis=0)
    scaled = upstream * gain
    row_inner = jnp.mean(scaled * unit_rows, axis=-1, keepdims=True)
    return (factor * (scaled - unit_rows * row_inner), gain_grad)


def split_blocks(queries, keys_all, values_all, key_place):
    rows = queries.shape[0]
    half = rows // 2
    shards = key_place.shape[0] // rows
    key_blocks = keys_all.reshape(shards, 2, half, KV_HEADS, HEAD_DIM)
    value_blocks = values_all.reshape(shards, 2, half, KV_HEADS, HEAD_DIM)
    place_blocks = key_place.reshape(shards, 2, half)
    return (key_blocks, value_blocks, place_blocks)


def scores_of(queries, key_block, place_block, query_place):
    scaling = HEAD_DIM ** (-0.5)
    scores = (
        jnp.einsum("rkgd,skd->kgrs", queries, key_block, preferred_element_type=jnp.float32)
        * scaling
    )
    allowed = place_block[None, None, None, :] <= query_place[None, None, :, None]
    return (scores, allowed)


def reachable(place_block, query_place):
    return jnp.min(place_block) <= jnp.max(query_place)


def attention_forward(queries, keys_all, values_all, query_place, key_place):
    key_blocks, value_blocks, place_blocks = split_blocks(queries, keys_all, values_all, key_place)
    rows = queries.shape[0]
    half = rows // 2
    groups = HEADS // KV_HEADS
    query_spans = queries.reshape(2, half, KV_HEADS, groups, HEAD_DIM)
    place_spans = query_place.reshape(2, half)

    def sweep_max(carry, inputs):
        key_block, place_block = inputs
        updated_all = []
        for span in range(2):
            state = carry[span]
            for part in range(2):

                def live(current, span=span, part=part):
                    maximum, total = current
                    scores, allowed = scores_of(
                        query_spans[span], key_block[part], place_block[part], place_spans[span]
                    )
                    masked = jnp.where(allowed, scores, -1e30)
                    updated = jnp.maximum(maximum, jnp.max(masked, axis=-1))
                    weights_now = jnp.where(allowed, jnp.exp(masked - updated[..., None]), 0.0)
                    return (
                        updated,
                        total * jnp.exp(maximum - updated) + jnp.sum(weights_now, axis=-1),
                    )

                state = lax.cond(
                    reachable(place_block[part], place_spans[span]),
                    live,
                    lambda current: current,
                    state,
                )
            updated_all.append(state)
        return (tuple(updated_all), None)

    start_max = jnp.full((KV_HEADS, groups, half), -1e30, jnp.float32)
    start_total = jnp.zeros((KV_HEADS, groups, half), jnp.float32)
    start = ((start_max, start_total), (start_max, start_total))
    finals, unused = lax.scan(sweep_max, start, (key_blocks, place_blocks))
    logsum_spans = [finals[span][0] + jnp.log(finals[span][1]) for span in range(2)]

    def sweep_out(results, inputs):
        key_block, value_block, place_block = inputs
        updated_all = []
        for span in range(2):
            result = results[span]
            for part in range(2):

                def live(current, span=span, part=part):
                    scores, allowed = scores_of(
                        query_spans[span], key_block[part], place_block[part], place_spans[span]
                    )
                    softmax_rows = jnp.where(
                        allowed, jnp.exp(scores - logsum_spans[span][..., None]), 0.0
                    ).astype(jnp.bfloat16)
                    return current + jnp.einsum(
                        "kgrs,skd->rkgd",
                        softmax_rows,
                        value_block[part],
                        preferred_element_type=jnp.float32,
                    )

                result = lax.cond(
                    reachable(place_block[part], place_spans[span]),
                    live,
                    lambda current: current,
                    result,
                )
            updated_all.append(result)
        return (tuple(updated_all), None)

    start_out = jnp.zeros((half, KV_HEADS, groups, HEAD_DIM), jnp.float32)
    outs, unused_out = lax.scan(
        sweep_out, (start_out, start_out), (key_blocks, value_blocks, place_blocks)
    )
    logsum = jnp.concatenate(logsum_spans, axis=-1)
    attended = jnp.concatenate([outs[0], outs[1]], axis=0)
    return (logsum, attended)


def attention_backward(
    queries, keys_all, values_all, query_place, key_place, logsum, attended_grad, row_inner
):
    key_blocks, value_blocks, place_blocks = split_blocks(queries, keys_all, values_all, key_place)
    rows = queries.shape[0]
    half = rows // 2
    groups = HEADS // KV_HEADS
    scaling = HEAD_DIM ** (-0.5)
    query_spans = queries.reshape(2, half, KV_HEADS, groups, HEAD_DIM)
    place_spans = query_place.reshape(2, half)
    grad_spans = attended_grad.reshape(2, half, KV_HEADS, groups, HEAD_DIM)
    logsum_spans = logsum.reshape(KV_HEADS, groups, 2, half)
    inner_spans = row_inner.reshape(KV_HEADS, groups, 2, half)

    def sweep_back(query_grads, inputs):
        key_block, value_block, place_block = inputs
        query_grads = list(query_grads)
        key_parts = []
        value_parts = []
        for part in range(2):
            key_acc = jnp.zeros((half, KV_HEADS, HEAD_DIM), jnp.float32)
            value_acc = jnp.zeros((half, KV_HEADS, HEAD_DIM), jnp.float32)
            for span in range(2):

                def live(current, span=span, part=part):
                    query_grad, key_grad, value_grad = current
                    scores, allowed = scores_of(
                        query_spans[span], key_block[part], place_block[part], place_spans[span]
                    )
                    softmax_rows = jnp.where(
                        allowed, jnp.exp(scores - logsum_spans[:, :, span][..., None]), 0.0
                    )
                    rounded = softmax_rows.astype(jnp.bfloat16)
                    weight_grad = jnp.einsum(
                        "rkgd,skd->kgrs",
                        grad_spans[span],
                        value_block[part],
                        preferred_element_type=jnp.float32,
                    )
                    score_grad = (
                        softmax_rows * (weight_grad - inner_spans[:, :, span][..., None])
                    ).astype(jnp.bfloat16)
                    query_grad = (
                        query_grad
                        + jnp.einsum(
                            "kgrs,skd->rkgd",
                            score_grad,
                            key_block[part],
                            preferred_element_type=jnp.float32,
                        )
                        * scaling
                    )
                    key_grad = (
                        key_grad
                        + jnp.einsum(
                            "kgrs,rkgd->skd",
                            score_grad,
                            query_spans[span],
                            preferred_element_type=jnp.float32,
                        )
                        * scaling
                    )
                    value_grad = value_grad + jnp.einsum(
                        "kgrs,rkgd->skd",
                        rounded,
                        grad_spans[span],
                        preferred_element_type=jnp.float32,
                    )
                    return (query_grad, key_grad, value_grad)

                state = (query_grads[span], key_acc, value_acc)
                state = lax.cond(
                    reachable(place_block[part], place_spans[span]),
                    live,
                    lambda current: current,
                    state,
                )
                query_grads[span], key_acc, value_acc = state
            key_parts.append(key_acc)
            value_parts.append(value_acc)
        key_out = jnp.concatenate(key_parts, axis=0)
        value_out = jnp.concatenate(value_parts, axis=0)
        return (tuple(query_grads), (key_out, value_out))

    start_grad = jnp.zeros((half, KV_HEADS, groups, HEAD_DIM), jnp.float32)
    query_pair, (key_grads, value_grads) = lax.scan(
        sweep_back, (start_grad, start_grad), (key_blocks, value_blocks, place_blocks)
    )
    query_grad = jnp.concatenate([query_pair[0], query_pair[1]], axis=0)
    return (
        query_grad,
        key_grads.reshape(-1, KV_HEADS, HEAD_DIM),
        value_grads.reshape(-1, KV_HEADS, HEAD_DIM),
    )


def fetch_layer(qkv_weight, out_weight, gate_up_weight, down_weight, attn_gain, ffn_gain, layer_id):
    return (
        lax.all_gather(qkv_weight[layer_id], "fsdp", axis=0, tiled=True),
        lax.all_gather(out_weight[layer_id], "fsdp", axis=0, tiled=True),
        lax.all_gather(gate_up_weight[layer_id], "fsdp", axis=0, tiled=True),
        lax.all_gather(down_weight[layer_id], "fsdp", axis=0, tiled=True),
        lax.all_gather(attn_gain[layer_id], "fsdp", axis=0, tiled=True),
        lax.all_gather(ffn_gain[layer_id], "fsdp", axis=0, tiled=True),
    )


def fetch_again(qkv_weight, out_weight, gate_up_weight, down_weight, attn_gain, ffn_gain, layer_id):
    return (
        lax.all_gather(qkv_weight[layer_id], "fsdp", axis=0, tiled=True),
        lax.all_gather(out_weight[layer_id], "fsdp", axis=0, tiled=True),
        lax.all_gather(gate_up_weight[layer_id], "fsdp", axis=0, tiled=True),
        lax.all_gather(down_weight[layer_id], "fsdp", axis=0, tiled=True),
        lax.all_gather(attn_gain[layer_id], "fsdp", axis=0, tiled=True),
        lax.all_gather(ffn_gain[layer_id], "fsdp", axis=0, tiled=True),
    )


def forward_layer(stream, query_place, key_place, gathered):
    qkv_full, out_full, gate_up_full, down_full, attn_full, ffn_full = gathered
    rows = stream.shape[0]
    groups = HEADS // KV_HEADS
    query_width = HEADS * HEAD_DIM
    key_width = KV_HEADS * HEAD_DIM
    cosine, sine = angles(query_place)
    normed, first_factor = normalize(stream, attn_full.astype(jnp.float32))
    normed = normed.astype(jnp.bfloat16)
    projected = jnp.dot(normed, qkv_full, preferred_element_type=jnp.float32)
    queries = rotate(projected[:, :query_width].reshape(rows, HEADS, HEAD_DIM), cosine, sine)
    queries = queries.reshape(rows, KV_HEADS, groups, HEAD_DIM).astype(jnp.bfloat16)
    keys_local = rotate(
        projected[:, query_width : query_width + key_width].reshape(rows, KV_HEADS, HEAD_DIM),
        cosine,
        sine,
    ).astype(jnp.bfloat16)
    values_local = (
        projected[:, query_width + key_width :]
        .reshape(rows, KV_HEADS, HEAD_DIM)
        .astype(jnp.bfloat16)
    )
    keys_all, values_all = (
        lax.all_gather(keys_local, "ctx", axis=0, tiled=True),
        lax.all_gather(values_local, "ctx", axis=0, tiled=True),
    )
    logsum, attended = attention_forward(queries, keys_all, values_all, query_place, key_place)
    attended_low = attended.reshape(rows, query_width).astype(jnp.bfloat16)
    middle = stream + jnp.dot(attended_low, out_full, preferred_element_type=jnp.float32)
    second, second_factor = normalize(middle, ffn_full.astype(jnp.float32))
    second = second.astype(jnp.bfloat16)
    gate_up = jnp.einsum("rd,dcf->rcf", second, gate_up_full, preferred_element_type=jnp.float32)
    hidden = (jax.nn.silu(gate_up[:, 0]) * gate_up[:, 1]).astype(jnp.bfloat16)
    result = middle + jnp.dot(hidden, down_full, preferred_element_type=jnp.float32)
    stored = (
        stream,
        first_factor,
        normed,
        queries,
        keys_local,
        values_local,
        keys_all,
        values_all,
        logsum,
        attended,
        attended_low,
        middle,
        second_factor,
        second,
        gate_up,
        hidden,
    )
    return (result, stored)


def backward_layer(upstream, stored, gathered, query_place, key_place, keys_all, values_all):
    (
        stream,
        first_factor,
        normed,
        queries,
        keys_local,
        values_local,
        kept_keys,
        kept_values,
        logsum,
        attended,
        attended_low,
        middle,
        second_factor,
        second,
        gate_up,
        hidden,
    ) = stored
    qkv_full, out_full, gate_up_full, down_full, attn_full, ffn_full = gathered
    rows = stream.shape[0]
    groups = HEADS // KV_HEADS
    cosine, sine = angles(query_place)
    upstream_low = upstream.astype(jnp.bfloat16)
    hidden_grad = jnp.einsum(
        "rd,fd->rf", upstream_low, down_full, preferred_element_type=jnp.float32
    )
    gate_part = gate_up[:, 0]
    up_part = gate_up[:, 1]
    sigmoid = jax.nn.sigmoid(gate_part)
    gate_grad = hidden_grad * up_part * sigmoid * (1.0 + gate_part * (1.0 - sigmoid))
    up_grad = hidden_grad * gate_part * sigmoid
    gate_up_low = jnp.stack([gate_grad, up_grad], axis=1).astype(jnp.bfloat16)
    second_grad = jnp.einsum(
        "rcf,dcf->rd", gate_up_low, gate_up_full, preferred_element_type=jnp.float32
    )
    middle_grad, ffn_gain_grad = normalize_back(
        second_grad, middle, second_factor, ffn_full.astype(jnp.float32)
    )
    middle_grad = middle_grad + upstream
    middle_low = middle_grad.astype(jnp.bfloat16)
    attended_grad = jnp.einsum(
        "rd,od->ro", middle_low, out_full, preferred_element_type=jnp.float32
    )
    attended_grad = attended_grad.astype(jnp.bfloat16).reshape(rows, KV_HEADS, groups, HEAD_DIM)
    row_inner = jnp.einsum("rkgd,rkgd->kgr", attended_grad.astype(jnp.float32), attended)
    query_grad, key_grads, value_grads = attention_backward(
        queries, keys_all, values_all, query_place, key_place, logsum, attended_grad, row_inner
    )
    key_grad, value_grad = (
        lax.psum_scatter(key_grads, "ctx", scatter_dimension=0, tiled=True),
        lax.psum_scatter(value_grads, "ctx", scatter_dimension=0, tiled=True),
    )
    query_grad = rotate_back(query_grad.reshape(rows, HEADS, HEAD_DIM), cosine, sine)
    key_grad = rotate_back(key_grad, cosine, sine)
    projected_grad = jnp.concatenate(
        [query_grad.reshape(rows, -1), key_grad.reshape(rows, -1), value_grad.reshape(rows, -1)],
        axis=1,
    ).astype(jnp.bfloat16)
    normed_grad = jnp.einsum(
        "re,de->rd", projected_grad, qkv_full, preferred_element_type=jnp.float32
    )
    stream_grad, attn_gain_grad = normalize_back(
        normed_grad, stream, first_factor, attn_full.astype(jnp.float32)
    )
    stream_grad = stream_grad + middle_grad
    qkv_grad = jnp.einsum("rd,re->de", normed, projected_grad, preferred_element_type=jnp.float32)
    out_grad = jnp.einsum("ro,rd->od", attended_low, middle_low, preferred_element_type=jnp.float32)
    gate_up_grad = jnp.einsum(
        "rd,rcf->dcf", second, gate_up_low, preferred_element_type=jnp.float32
    )
    down_grad = jnp.einsum("rf,rd->fd", hidden, upstream_low, preferred_element_type=jnp.float32)
    sharded = (
        lax.psum_scatter(qkv_grad, "fsdp", scatter_dimension=0, tiled=True),
        lax.psum_scatter(out_grad, "fsdp", scatter_dimension=0, tiled=True),
        lax.psum_scatter(gate_up_grad, "fsdp", scatter_dimension=0, tiled=True),
        lax.psum_scatter(down_grad, "fsdp", scatter_dimension=0, tiled=True),
        lax.psum_scatter(attn_gain_grad, "fsdp", scatter_dimension=0, tiled=True),
        lax.psum_scatter(ffn_gain_grad, "fsdp", scatter_dimension=0, tiled=True),
    )
    totals = lax.psum(
        (sharded[0], sharded[1], sharded[2], sharded[3], sharded[4], sharded[5]), "ctx"
    )
    return (stream_grad, totals)


def body(
    tokens,
    positions,
    qkv_weight,
    out_weight,
    gate_up_weight,
    down_weight,
    attn_gain,
    ffn_gain,
    cotangent,
):
    query_place = positions[0]
    key_place = lax.all_gather(query_place, "ctx", axis=0, tiled=True)
    stream = tokens[0].astype(jnp.float32)
    gathered_list = []
    layer_id = 0
    gathered = fetch_layer(
        qkv_weight, out_weight, gate_up_weight, down_weight, attn_gain, ffn_gain, layer_id
    )
    stream, stored = forward_layer(stream, query_place, key_place, gathered)
    saved = [stored]
    gathered_list.append(gathered)
    activations = stream.astype(jnp.bfloat16)[None]
    upstream = cotangent[0]
    layer_grads = [None] * LAYERS
    for layer_id in reversed(range(LAYERS)):
        stored = saved[layer_id]
        gathered = fetch_again(
            qkv_weight, out_weight, gate_up_weight, down_weight, attn_gain, ffn_gain, layer_id
        )
        keys_all, values_all = (stored[6], stored[7])
        upstream, totals = backward_layer(
            upstream, stored, gathered, query_place, key_place, keys_all, values_all
        )
        layer_grads[layer_id] = totals
    outputs = [jnp.stack([entry[slot] for entry in layer_grads], axis=0) for slot in range(6)]
    return (
        activations,
        upstream[None],
        outputs[0],
        outputs[1],
        outputs[2],
        outputs[3],
        outputs[4],
        outputs[5],
    )


LANES = 128


def spread(heads):
    half = HEAD_DIM // 2
    pad = ((0, 0), (0, 0), (0, 64 - half))
    return jnp.concatenate([jnp.pad(heads[..., :half], pad), jnp.pad(heads[..., half:], pad)], axis=-1)


def gathered_spread(padded):
    half = HEAD_DIM // 2
    return jnp.concatenate([padded[..., :half], padded[..., 64 : 64 + half]], axis=-1)


def table(length):
    half = HEAD_DIM // 2
    frequency = rope_base ** (-(jnp.arange(half, dtype=jnp.float32) * 2.0 / HEAD_DIM))
    phases = jnp.arange(length, dtype=jnp.float32)[:, None] * frequency[None, :]
    pad = ((0, 0), (0, 64 - half))
    return jnp.concatenate([jnp.pad(jnp.cos(phases), pad), jnp.pad(jnp.sin(phases), pad)], axis=1)


def wave(rows):
    first = lax.broadcasted_iota(jnp.int32, rows.shape, 1) < 64
    other = pltpu.roll(rows, 64, 1)
    return jnp.where(first, rows, other), jnp.where(first, -other, rows)


def nt(left, right):
    return lax.dot_general(left, right, (((1,), (1,)), ((), ())), preferred_element_type=jnp.float32)


def nn(left, right):
    return lax.dot_general(left, right, (((1,), (0,)), ((), ())), preferred_element_type=jnp.float32)


def tn(left, right):
    return lax.dot_general(left, right, (((0,), (0,)), ((), ())), preferred_element_type=jnp.float32)


def causal(width):
    key_at = lax.broadcasted_iota(jnp.int32, (width, 2 * width), 0)
    query_at = lax.broadcasted_iota(jnp.int32, (width, 2 * width), 1)
    query_at = jnp.where(query_at >= width, query_at - width, query_at)
    return key_at <= query_at


def back_kernel(
    span, grad_ref, q_ref, k_ref, v_ref, att_ref, lse_ref, turn_ref,
    out_ref, dk_ref, dv_ref,
):
    length = k_ref.shape[0]
    half = 96
    pairs = length // (2 * half)
    scaling = HEAD_DIM ** (-0.5)
    mask = causal(2 * half)
    lane = lax.broadcasted_iota(jnp.int32, (half, LANES), 1)
    keys_t = k_ref[...].astype(jnp.float32).T.astype(jnp.bfloat16)
    for pair in reversed(range(pairs)):
        width = (pair + 1) * 2 * half
        q = q_ref[pl.ds(pair * 4 * half, 4 * half), :]
        firsts, seconds = [], []
        for part in range(2):
            at = span[2 * pairs + 2 * pair + part]
            rows = pl.ds(pl.multiple_of(at * half, half), half)
            left = grad_ref[rows, 0:LANES].astype(jnp.float32)
            right = jnp.concatenate(
                [grad_ref[rows, LANES : 2 * half].astype(jnp.float32), jnp.zeros((half, 64), jnp.float32)], axis=1
            )
            firsts.append(jnp.where(lane < half, left, 0.0))
            seconds.append(pltpu.roll(jnp.where(lane < half, right, left), LANES - half, 1))
        seconds = [jnp.where(lane < half, s, 0.0) for s in seconds]
        grads = jnp.concatenate(firsts + seconds, axis=0)
        delta = jnp.sum(grads.T * att_ref[pl.ds(pair * LANES, LANES), :], axis=0, keepdims=True)
        grads = grads.astype(jnp.bfloat16)
        keys = k_ref[pl.ds(0, width), :]
        weights = jnp.exp(nt(keys, q) * scaling - lse_ref[pl.ds(pair, 1), :])
        last = jnp.where(mask, weights[width - 2 * half :], 0.0)
        weights = last if pair == 0 else jnp.concatenate([weights[: width - 2 * half], last], axis=0)
        dp = nt(v_ref[pl.ds(0, width), :], grads)
        ds = (weights * (dp - delta)).astype(jnp.bfloat16)
        dk = nn(ds, q) * scaling
        dv = nn(weights.astype(jnp.bfloat16), grads)
        if pair == pairs - 1:
            dk_ref[...] = dk
            dv_ref[...] = dv
        else:
            dk_ref[pl.ds(0, width), :] += dk
            dv_ref[pl.ds(0, width), :] += dv
        dq = nn(keys_t[:, :width], ds).T * scaling
        for part in range(2):
            at = span[2 * pairs + 2 * pair + part]
            rows = pl.ds(pl.multiple_of(at * half, half), half)
            spot = pl.ds((2 * pair + part) * half, half)
            cosine, sine = wave(turn_ref[spot, :])
            for head in range(2):
                z = dq[(2 * head + part) * half : (2 * head + part + 1) * half]
                out_ref[rows, head * LANES : (head + 1) * LANES] = (
                    z * cosine - pltpu.roll(z, 64, 1) * sine
                ).astype(jnp.bfloat16)
    for block in range(2 * pairs):
        at = span[2 * pairs + block]
        rows = pl.ds(pl.multiple_of(at * half, half), half)
        spot = pl.ds(block * half, half)
        z = dk_ref[spot, :]
        cosine, sine = wave(turn_ref[spot, :])
        out_ref[rows, 2 * LANES : 3 * LANES] = (
            z * cosine - pltpu.roll(z, 64, 1) * sine
        ).astype(jnp.bfloat16)
        out_ref[rows, 3 * LANES :] = dv_ref[spot, :].astype(jnp.bfloat16)


def vm(count):
    return [pl.BlockSpec(memory_space=pltpu.VMEM)] * count


MESH = pl.DeviceIdType.MESH


class Place:
    def __init__(self):
        self.me = lax.axis_index("ctx")
        core, x, y = self.me % 2, (self.me // 2) % 2, self.me // 4
        self.dp, self.dx, self.dy = 1 - 2 * core, 2 - 4 * x, 4 - 8 * y
        self.p, self.x, self.y = self.me + self.dp, self.me + self.dx, self.me + self.dy
        self.d = self.x + self.dy
        self.z = lax.axis_index("fsdp")
        self.planes = lax.axis_size("fsdp")
        self.n = lax.axis_size("ctx")


def greet(place, ctx=True, planes=False):
    barrier = pltpu.get_barrier_semaphore()
    count = 0
    if ctx:
        for step in range(1, place.n):
            pl.semaphore_signal(
                barrier, inc=1, device_id={"ctx": lax.rem(place.me + step, place.n)}, device_id_type=MESH
            )
            count += 1
    if planes:
        for step in range(1, place.planes):
            pl.semaphore_signal(
                barrier, inc=1, device_id={"fsdp": lax.rem(place.z + step, place.planes)}, device_id_type=MESH
            )
            count += 1
    pl.semaphore_wait(barrier, count)


def send(source, target, send_sem, recv_sem, **where):
    return pltpu.make_async_remote_copy(
        src_ref=source, dst_ref=target, send_sem=send_sem, recv_sem=recv_sem,
        device_id=where, device_id_type=MESH,
    )


class Gather:
    sems = 14

    def __init__(self, place, own, out, sem):
        self.place, self.own, self.out, self.sem = place, own, out, sem
        self.half = out.shape[1] // 2
        self.started = []
        self.met = False

    def go(self, source, target, index, rank):
        copy = send(source, target, self.sem.at[0, index], self.sem.at[1, index], ctx=rank)
        copy.start()
        self.started.append(copy)

    def part(self, rank, half):
        return self.out.at[rank, pl.ds(half * self.half, self.half)]

    def whole(self, rank):
        return self.out.at[rank]

    def start(self):
        p = self.place
        keep = pltpu.make_async_copy(self.own, self.whole(p.me), self.sem.at[0, 13])
        keep.start()
        self.keep = keep
        halves = [self.own.at[pl.ds(h * self.half, self.half)] for h in range(2)]
        self.go(halves[0], self.part(p.me, 0), 0, p.x)
        self.go(halves[1], self.part(p.me, 1), 3, p.y)
        self.go(self.own, self.whole(p.me), 6, p.p)
        self.go(halves[1], self.part(p.me, 1), 1, p.x)
        self.go(halves[0], self.part(p.me, 0), 2, p.y)

    def arrived(self, rank, half, index):
        part = self.part(rank, half)
        pltpu.make_async_copy(part, part, self.sem.at[1, index]).wait()
        return part

    def relay(self):
        p = self.place
        part = self.arrived(p.x, 0, 0)
        self.go(part, part, 4, p.y)
        self.go(part, part, 7, p.p)
        part = self.arrived(p.y, 1, 3)
        self.go(part, part, 5, p.x)
        self.go(part, part, 10, p.p)

    def rest(self):
        p = self.place
        for rank, half, index, onward in ((p.x, 1, 1, 8), (p.y, 0, 2, 9), (p.d, 0, 4, 11), (p.d, 1, 5, 12)):
            part = self.arrived(rank, half, index)
            self.go(part, part, onward, p.p)

    def first_partner(self):
        part = self.whole(self.place.p)
        pltpu.make_async_copy(part, part, self.sem.at[1, 6]).wait()
        self.met = True

    def partner(self):
        p = self.place
        if not self.met:
            self.first_partner()
        for rank, half, index in (
            (p.x, 0, 7), (p.y, 1, 10), (p.x, 1, 8), (p.y, 0, 9), (p.d, 0, 11), (p.d, 1, 12),
        ):
            self.arrived(rank + p.dp, half, index)

    def finish(self, kept=False):
        if not kept:
            self.keep.wait()
        for copy in self.started:
            copy.wait_send()


class PlaneGather:
    def __init__(self, place, own, out, sem):
        self.place, self.own, self.out, self.sem = place, own, out, sem

    def hop(self, step, up):
        p = self.place
        sign = 1 if up else -1
        source = p.z - sign * step
        target = p.z + sign
        ok = jnp.logical_and(
            jnp.logical_and(source >= 0, source < p.planes),
            jnp.logical_and(target >= 0, target < p.planes),
        )
        source = jnp.clip(source, 0, p.planes - 1)
        target = jnp.clip(target, 0, p.planes - 1)
        block = self.own if step == 0 else self.out.at[source]
        return ok, send(
            block, self.out.at[source], self.sem.at[0 if up else 1, source], self.sem.at[2, source], fsdp=target
        )

    def start(self):
        p = self.place
        self.keep = pltpu.make_async_copy(self.own, self.out.at[p.z], self.sem.at[2, p.z])
        self.keep.start()
        for up in (True, False):
            ok, copy = self.hop(0, up)
            pl.when(ok)(copy.start)

    def got(self, step, up):
        p = self.place
        source = p.z - step if up else p.z + step
        ok = jnp.logical_and(source >= 0, source < p.planes)
        source = jnp.clip(source, 0, p.planes - 1)
        part = self.out.at[source]
        return ok, pltpu.make_async_copy(part, part, self.sem.at[2, source])

    def step(self, number):
        for up in (True, False):
            ok, copy = self.got(number, up)
            pl.when(ok)(copy.wait)
            if number < self.place.planes - 1:
                ok, copy = self.hop(number, up)
                pl.when(ok)(copy.start)

    def finish(self, kept=False):
        if not kept:
            self.keep.wait()
        for number in range(self.place.planes - 1):
            for up in (True, False):
                ok, copy = self.hop(number, up)
                pl.when(ok)(copy.wait_send)


class Exchange:
    def __init__(self, place, blocks, out, sem):
        self.place, self.blocks, self.out, self.sem = place, blocks, out, sem

    def pick(self, rank):
        return self.blocks.at[rank]

    def copy(self, step):
        p = self.place
        rank = lax.rem(p.me + step, p.n)
        return send(self.pick(rank), self.out.at[p.me], self.sem.at[0, step], self.sem.at[1, step], ctx=rank)

    def start(self):
        p = self.place
        for step in range(1, p.n):
            self.copy(step).start()
        self.keep = pltpu.make_async_copy(self.pick(p.me), self.out.at[p.me], self.sem.at[0, 0])
        self.keep.start()

    def finish(self):
        p = self.place
        self.keep.wait()
        for step in range(1, p.n):
            self.copy(step).wait_send()
        for step in range(1, p.n):
            part = self.out.at[lax.rem(p.me + p.n - step, p.n)]
            pltpu.make_async_copy(part, part, self.sem.at[1, step]).wait()


class Share(Exchange):
    def pick(self, rank):
        return self.blocks


class PlaneShare:
    def __init__(self, place, block, out, sem):
        self.place, self.block, self.out, self.sem = place, block, out, sem

    def copy(self, step):
        p = self.place
        plane = lax.rem(p.z + step, p.planes)
        return send(self.block, self.out.at[p.z], self.sem.at[0, step], self.sem.at[1, step], fsdp=plane)

    def start(self):
        p = self.place
        for step in range(1, p.planes):
            self.copy(step).start()
        self.keep = pltpu.make_async_copy(self.block, self.out.at[p.z], self.sem.at[0, 0])
        self.keep.start()

    def finish(self):
        p = self.place
        self.keep.wait()
        for step in range(1, p.planes):
            self.copy(step).wait_send()
        for step in range(1, p.planes):
            part = self.out.at[lax.rem(p.z + p.planes - step, p.planes)]
            pltpu.make_async_copy(part, part, self.sem.at[1, step]).wait()


def anywhere(count):
    return [pl.BlockSpec(memory_space=pl.ANY)] * count


class Reduce:
    sems = 10

    def __init__(self, place, mine, theirs, first, out, second, sem):
        self.place, self.mine, self.theirs, self.first, self.out, self.second, self.sem = (
            place, mine, theirs, first, out, second, sem
        )
        self.half = out.shape[1]
        self.started = []

    def push(self, slot):
        copy = send(
            self.theirs.at[slot], self.first.at[slot], self.sem.at[0, slot], self.sem.at[1, slot], ctx=self.place.p
        )
        copy.start()
        return copy

    def pushed(self):
        for slot in range(4):
            send(
                self.theirs.at[slot], self.first.at[slot], self.sem.at[0, slot], self.sem.at[1, slot],
                ctx=self.place.p,
            ).wait_send()

    def add(self, slot):
        part = self.first.at[slot]
        pltpu.make_async_copy(part, part, self.sem.at[1, slot]).wait()
        self.mine[slot] = self.mine[slot] + self.first[slot].astype(jnp.float32)

    def go(self, index, value, rank):
        self.out[index] = value.astype(jnp.bfloat16)
        copy = send(
            self.out.at[index], self.second.at[index], self.sem.at[0, 4 + index], self.sem.at[1, 4 + index], ctx=rank
        )
        copy.start()
        self.started.append(copy)

    def top(self, slot):
        return self.mine[slot, pl.ds(0, self.half), :]

    def low(self, slot):
        return self.mine[slot, pl.ds(self.half, self.half), :]

    def got(self, index):
        part = self.second.at[index]
        pltpu.make_async_copy(part, part, self.sem.at[1, 4 + index]).wait()
        return self.second[index].astype(jnp.float32)

    def across(self):
        self.add(3)
        self.go(1, self.top(3), self.place.x)
        self.go(3, self.low(3), self.place.y)

    def beside(self):
        self.add(1)
        self.go(0, self.top(1), self.place.x)
        self.add(2)
        self.go(2, self.low(2), self.place.y)

    def turn(self):
        self.go(4, self.top(2) + self.got(1), self.place.y)
        self.go(5, self.low(1) + self.got(3), self.place.x)

    def total(self, use):
        self.add(0)
        use(pl.ds(0, self.half), self.top(0) + self.got(0) + self.got(4))
        use(pl.ds(self.half, self.half), self.low(0) + self.got(2) + self.got(5))

    def finish(self):
        self.pushed()
        for copy in self.started:
            copy.wait_send()


def flip(place, i):
    return place.me + (i % 2) * place.dp + ((i // 2) % 2) * place.dx + (i // 4) * place.dy


def last_kernel(
    pgrad, qkv_w, tok, middle_grad, gain, ffn_gain, low, down_part, gu_part, hidden, down_w, middle,
    grad, result, gains, low_all, down_all, gu_all,
    mine, theirs, first, out, second, theirs2, first2, out2, second2, gain_sum, mine_gain, ctx_gain, plane_sum, plane_gain,
    reduce_sem, reduce_sem2, gather_sem, down_sem, gu_sem, gain_sem, plane_sem,
):
    place = Place()
    greet(place, planes=True)
    grads = Reduce(place, mine, theirs, first, out, second, reduce_sem)
    pgrad_width = tok.shape[1]

    def push(k, carry):
        theirs[k] = nt(pgrad[flip(place, 2 * k + 1)], qkv_w[...].reshape(pgrad_width, -1)).astype(jnp.bfloat16)
        grads.push(k)
        return carry

    def keep(k, carry):
        mine[k] = nt(pgrad[flip(place, 2 * k)], qkv_w[...].reshape(pgrad_width, -1))
        return carry

    lax.fori_loop(0, 4, push, 0)
    lax.fori_loop(0, 4, keep, 0)
    grads.across()
    grads.beside()
    sums = Reduce(place, mine, theirs2, first2, out2, second2, reduce_sem2)

    def other(k, carry):
        theirs2[k] = nn(hidden[flip(place, 2 * k + 1)], down_w[...].reshape(-1, pgrad_width)).astype(jnp.bfloat16)
        sums.push(k)
        return carry

    def ours(k, carry):
        mine[k] = nn(hidden[flip(place, 2 * k)], down_w[...].reshape(-1, pgrad_width))
        return carry

    lax.fori_loop(0, 4, other, 0)
    grads.turn()
    moves = [
        Gather(place, low, low_all, gather_sem),
        Gather(place, down_part, down_all, down_sem),
        Gather(place, gu_part, gu_all, gu_sem),
    ]
    moves[0].start()
    gain_sum[...] = jnp.zeros_like(gain_sum)

    def norm_back(part, normed_grad):
        x = tok[part, :].astype(jnp.float32)
        factor = lax.rsqrt(jnp.mean(x * x, axis=-1, keepdims=True) + epsilon)
        unit = x * factor
        gain_sum[...] += jnp.sum(normed_grad * unit, axis=0, keepdims=True)
        scaled = normed_grad * gain[...]
        inner = jnp.mean(scaled * unit, axis=-1, keepdims=True)
        grad[part, :] = middle_grad[part, :] + factor * (scaled - unit * inner)

    grads.total(norm_back)
    gain_grad = gain_sum[...]
    shard = mine_gain.shape[1]
    count = mine_gain.shape[0] // 2
    for at in range(count):
        mine_gain[pl.ds(at, 1), :] = gain_grad[:, at * shard : (at + 1) * shard]
        mine_gain[pl.ds(count + at, 1), :] = ffn_gain[:, at * shard : (at + 1) * shard]
    ctx_sum = Share(place, mine_gain, ctx_gain, gain_sem)
    ctx_sum.start()
    for at, move in enumerate(moves):
        if at:
            move.start()
        move.relay()
        move.rest()
    lax.fori_loop(0, 4, ours, 0)
    sums.across()
    sums.beside()
    sums.turn()

    def finish_rows(part, down_sum):
        result[part, :] = (middle[part, :] + down_sum).astype(jnp.bfloat16)

    sums.total(finish_rows)
    ctx_sum.finish()
    plane_sum[...] = jnp.sum(ctx_gain[...], axis=0)
    planes = PlaneShare(place, plane_sum, plane_gain, plane_sem)
    planes.start()
    for move in moves:
        move.partner()
    planes.finish()
    gains[...] = jnp.sum(plane_gain[...], axis=0)
    for move in moves:
        move.finish()
    grads.finish()
    sums.finish()


def last_moves(pgrad, qkv_w, tok, middle_grad, gain, ffn_gain, low, down_part, gu_part, hidden, down_w, middle):
    n, planes = lax.axis_size("ctx"), lax.axis_size("fsdp")
    rows, width = tok.shape
    bf, f32 = jnp.bfloat16, jnp.float32
    shape = jax.ShapeDtypeStruct
    dma = pltpu.SemaphoreType.DMA
    halves = pltpu.VMEM((6, rows // 2, width), bf)
    quads = pltpu.VMEM((4, rows, width), bf)
    small = (2 * planes, width // planes)
    many = lambda x: shape((n,) + x.shape, x.dtype)
    return pl.pallas_call(
        last_kernel,
        out_shape=(
            shape((rows, width), f32), shape((rows, width), bf), shape(small, f32), many(low), many(down_part), many(gu_part),
        ),
        in_specs=vm(12),
        out_specs=vm(3) + anywhere(3),
        scratch_shapes=[
            pltpu.VMEM((4, rows, width), f32), quads, quads, halves, halves, quads, quads, halves, halves, pltpu.VMEM((1, width), f32),
            pltpu.VMEM(small, f32), pltpu.VMEM((n,) + small, f32), pltpu.VMEM(small, f32), pltpu.VMEM((planes,) + small, f32),
            dma((2, Reduce.sems)), dma((2, Reduce.sems)), dma((2, Gather.sems)), dma((2, Gather.sems)), dma((2, Gather.sems)), dma((2, n)), dma((2, planes)),
        ],
        compiler_params=pltpu.CompilerParams(collective_id=6, has_side_effects=True, vmem_limit_bytes=67043328),
        name="last_moves",
    )(pgrad, qkv_w, tok, middle_grad, gain, ffn_gain, low, down_part, gu_part, hidden, down_w, middle)


def gathers_kernel(count, *refs):
    place = Place()
    greet(place)
    moves = [Gather(place, refs[at], refs[count + at], refs[2 * count + at]) for at in range(count)]
    for move in moves:
        move.start()
        move.relay()
        move.rest()
    for move in moves:
        move.partner()
    for move in moves:
        move.finish()


def gathers(number, *arrays):
    n = lax.axis_size("ctx")
    count = len(arrays)
    return pl.pallas_call(
        functools.partial(gathers_kernel, count),
        out_shape=tuple(jax.ShapeDtypeStruct((n,) + x.shape, x.dtype) for x in arrays),
        in_specs=vm(count),
        out_specs=anywhere(count),
        scratch_shapes=[pltpu.SemaphoreType.DMA((2, Gather.sems))] * count,
        compiler_params=pltpu.CompilerParams(collective_id=number, has_side_effects=True),
        name="gathers",
    )(*arrays)


class Steps:
    def __init__(self, *steps):
        self.steps = list(steps)

    def next(self, count=1):
        for step in self.steps[:count]:
            step()
        self.steps = self.steps[count:]

    def rest(self):
        self.next(len(self.steps))


class OutGather(Gather):
    def __init__(self, place, own, out, sem):
        self.place, self.own, self.out, self.sem = place, own, out, sem
        self.half = out.shape[0] // 2
        self.started = []
        self.met = False

    def part(self, rank, half):
        return self.out.at[pl.ds(half * self.half, self.half), rank]

    def whole(self, rank):
        return self.out.at[:, rank]


def front_kernel(
    tok, up_low, spot, gain_own, qkv_own, out_own, gu_own, down_own, turn_ref, up,
    normed, up_all, second_all, hidden, gul, qkv_w, down_w, q_ref, k_ref, v_ref, att_ref, lse_ref, low,
    middle_grad, middle, gain_grad, spots, gains, agrad, mcols,
    gu_w, out_block, out_w, qr, kr, vr, low_sorted, gain_all, spots_s,
    attended, mcols_send, own, mine, theirs, first, out, second,
    tok_sem, up_sem, spot_sem, gain_sem, qkv_sem, out_sem, outc_sem, gu_sem, down_sem, local_sem,
    low_sem, gather_sem, reduce_sem, agrad_sem, mcols_sem,
):
    place = Place()
    n = place.n
    rows = tok.shape[0]
    half = rows // 2
    pairs = 8
    heads = rows
    greet(place, planes=True)
    spans = Share(place, spot, spots, spot_sem)
    scales = PlaneShare(place, gain_own, gain_all, gain_sem)
    tokens = Gather(place, tok, normed, tok_sem)
    cots = Gather(place, up_low, up_all, up_sem)
    qkvs = PlaneGather(place, qkv_own, qkv_w, qkv_sem)
    outs = PlaneGather(place, out_own, out_block, out_sem)
    outc = OutGather(place, out_block, out_w, outc_sem)
    gus = PlaneGather(place, gu_own, gu_w, gu_sem)
    downs = PlaneGather(place, down_own, down_w, down_sem)
    fetch = pltpu.make_async_copy(up, middle_grad, local_sem.at[0])
    fetch.start()
    spans.start()
    scales.start()
    qkvs.start()
    tokens.start()
    tokens.relay()
    qkvs.step(1)
    outs.start()
    qkvs.step(2)
    downs.start()
    tokens.rest()
    qkvs.step(3)
    cots.start()
    tokens.partner()
    tokens.finish()
    spans.finish()
    scales.finish()
    qkvs.keep.wait()
    table = pltpu.make_async_copy(spots, spots_s, local_sem.at[1])
    table.start()
    for g in range(2):
        gains[pl.ds(g, 1), :] = jnp.concatenate([gain_all[z, pl.ds(g, 1), :] for z in range(4)], axis=1)
    table.wait()
    early = [spots_s[j, 0, 0] for j in range(pairs)]
    holder = []
    for t in range(pairs):
        at = 0
        for j in range(pairs):
            at = jnp.where(early[j] == t, j, at)
        holder.append(at)

    def block_of(s):
        return 2 * holder[s] if s < pairs else 2 * holder[2 * pairs - 1 - s] + 1

    def span_of(b):
        return early[b // 2] if b % 2 == 0 else 2 * pairs - 1 - early[b // 2]

    def project(j, carry):
        x = normed[pl.ds(2 * j, 2)].reshape(2 * rows, -1).astype(jnp.float32)
        factor = lax.rsqrt(jnp.mean(x * x, axis=-1, keepdims=True) + epsilon)
        scaled = (x * factor * gains[pl.ds(0, 1), :]).astype(jnp.bfloat16)
        normed[pl.ds(2 * j, 2)] = scaled.reshape(2, rows, -1)
        proj = nn(scaled, qkv_w[...].reshape(-1, 4 * LANES))
        for piece in range(4):
            c = spots_s[2 * j + piece // 2, 0, 0]
            cosine, sine = wave(turn_ref[c if piece % 2 == 0 else 2 * pairs - 1 - c])
            mine_rows = proj[piece * half : (piece + 1) * half]

            def turned(part):
                z = mine_rows[:, part * LANES : (part + 1) * LANES]
                return (z * cosine + pltpu.roll(z, 64, 1) * sine).astype(jnp.bfloat16)

            qr[4 * j + piece, 0] = turned(0)
            qr[4 * j + piece, 1] = turned(1)
            kr[4 * j + piece] = turned(2)
            vr[4 * j + piece] = mine_rows[:, 3 * LANES :].astype(jnp.bfloat16)
        return carry

    lax.fori_loop(0, 4, project, 0)
    for s in range(2 * pairs):
        b = block_of(s)
        base = (s // 2) * 4 * half + (s % 2) * half
        both = qr[b]
        q_ref[pl.ds(base, half), :] = both[0]
        q_ref[pl.ds(base + 2 * half, half), :] = both[1]
        k_ref[pl.ds(s * half, half), :] = kr[b]
        v_ref[pl.ds(s * half, half), :] = vr[b]

    steps = Steps(
        lambda: outs.step(1), cots.relay, lambda: outs.step(2), lambda: outs.step(3),
        lambda: (outs.keep.wait(), outc.start(), downs.step(1), gus.start()), cots.rest, outc.relay,
        lambda: (downs.step(2), outc.rest()), lambda: (cots.partner(), outc.partner()),
    )
    scaling = HEAD_DIM ** (-0.5)
    mask = causal(2 * half)
    lane = lax.broadcasted_iota(jnp.int32, (half, LANES), 1)
    values_t = v_ref[...].astype(jnp.float32).T.astype(jnp.bfloat16)
    for pair in range(pairs):
        width = (pair + 1) * 2 * half
        q = q_ref[pl.ds(pair * 4 * half, 4 * half), :]
        before = width - 2 * half
        parts = [jnp.where(mask, nt(k_ref[pl.ds(before, 2 * half), :], q) * scaling, -1e30)]
        if pair:
            parts.append(nt(k_ref[pl.ds(0, before), :], q) * scaling)
        tops = [jnp.max(part, axis=0, keepdims=True) for part in parts]
        top = jnp.maximum(tops[0], tops[-1])
        parts = [jnp.exp(part - top) for part in parts]
        total = sum(jnp.sum(part, axis=0, keepdims=True) for part in parts)
        parts = [(part * (1.0 / total)).astype(jnp.bfloat16) for part in parts]
        lse_ref[pl.ds(pair, 1), :] = top + jnp.log(total)
        out_t = nn(values_t[:, before:width], parts[0])
        if pair:
            out_t = out_t + nn(values_t[:, :before], parts[1])
        att_ref[pl.ds(pair * LANES, LANES), :] = out_t
        result = out_t.T.astype(jnp.bfloat16).astype(jnp.float32)
        for part in range(2):
            left = result[part * half : (part + 1) * half]
            right = pltpu.roll(result[(2 + part) * half : (3 + part) * half], half, 1)
            low_sorted[2 * pair + part, :, 0:LANES] = jnp.where(lane < half, left, right).astype(jnp.bfloat16)
            low_sorted[2 * pair + part, :, LANES : 2 * half] = right[:, : 2 * half - LANES].astype(jnp.bfloat16)
        steps.next()
    for b in range(2 * pairs):
        low[b // 2, pl.ds((b % 2) * half, half), :] = low_sorted[span_of(b)]
    moved = Exchange(place, low, attended, low_sem)
    moved.start()
    steps.rest()
    outc.keep.wait()
    moved.finish()
    total = tok[...].astype(jnp.float32)
    for q in range(8):
        total = total + nn(attended[q], out_w[q // 2, pl.ds(4 * (q % 2), 4)].reshape(heads, -1))
    middle[...] = total
    factor = lax.rsqrt(jnp.mean(total * total, axis=-1, keepdims=True) + epsilon)
    own[...] = (total * factor * gains[pl.ds(1, 1), :]).astype(jnp.bfloat16)
    seconds = Gather(place, own, second_all, gather_sem)
    seconds.start()
    downs.step(3)
    gus.step(1)
    seconds.relay()
    gus.step(2)
    seconds.rest()
    gus.step(3)
    seconds.partner()
    gus.keep.wait()
    downs.keep.wait()
    seconds.keep.wait()
    cots.keep.wait()
    grads = Reduce(place, mine, theirs, first, out, second, reduce_sem)
    wide = hidden.shape[2]

    def block(i):
        rank = flip(place, i)
        gate_up = nn(second_all[rank], gu_w[...].reshape(-1, 2 * wide))
        gate, raised = gate_up[:, :wide], gate_up[:, wide:]
        sigmoid = 1.0 / (1.0 + jnp.exp(-gate))
        silu = gate * sigmoid
        hidden[rank] = (silu * raised).astype(jnp.bfloat16)
        hidden_grad = nt(up_all[rank], down_w[...].reshape(wide, -1))
        gul[rank, :, pl.ds(0, wide)] = (hidden_grad * raised * sigmoid * (1.0 + gate * (1.0 - sigmoid))).astype(jnp.bfloat16)
        gul[rank, :, pl.ds(wide, wide)] = (hidden_grad * silu).astype(jnp.bfloat16)
        return nt(gul[rank], gu_w[...].reshape(-1, 2 * wide))

    def pair_of(k, carry):
        theirs[k] = block(2 * k + 1).astype(jnp.bfloat16)
        grads.push(k)
        mine[k] = block(2 * k)
        return carry

    lax.fori_loop(1, 4, pair_of, 0)
    grads.across()
    grads.beside()
    lax.fori_loop(0, 1, pair_of, 0)
    grads.turn()
    fetch.wait()
    seconds.finish(kept=True)
    gain_grad[...] = jnp.zeros_like(gain_grad)

    def norm_back(part, second_grad):
        x = middle[part, :]
        factor = lax.rsqrt(jnp.mean(x * x, axis=-1, keepdims=True) + epsilon)
        unit = x * factor
        gain_grad[...] += jnp.sum(second_grad * unit, axis=0, keepdims=True)
        scaled = second_grad * gains[pl.ds(1, 1), :]
        inner = jnp.mean(scaled * unit, axis=-1, keepdims=True)
        grad = middle_grad[part, :] + factor * (scaled - unit * inner)
        middle_grad[part, :] = grad
        own[part, :] = grad.astype(jnp.bfloat16)

    grads.total(norm_back)

    def head_grads(q, carry):
        weight = out_w[q // 2, pl.ds(4 * (q % 2), 4)].reshape(heads, -1)
        attended[q] = nt(own[...], weight).astype(jnp.bfloat16)
        return carry

    lax.fori_loop(0, n, head_grads, 0)
    heads_back = Exchange(place, attended, agrad, agrad_sem)
    heads_back.start()
    for q in range(8):
        mcols_send[q] = own[:, q * heads : (q + 1) * heads]
    columns = Exchange(place, mcols_send, mcols, mcols_sem)
    columns.start()
    for move in (qkvs, outs, gus, downs):
        move.finish(kept=True)
    for move in (cots, outc):
        move.finish(kept=True)
    heads_back.finish()
    columns.finish()
    grads.finish()


def front_moves(tok, up_low, spot, gain_own, qkv_own, out_own, gu_own, down_own, turns, up):
    n, planes = lax.axis_size("ctx"), lax.axis_size("fsdp")
    rows, width = tok.shape
    length = n * rows
    wide = planes * down_own.shape[0]
    bf, f32 = jnp.bfloat16, jnp.float32
    shape = jax.ShapeDtypeStruct
    dma = pltpu.SemaphoreType.DMA
    pairs = length // 192
    halves = pltpu.VMEM((6, rows // 2, width), bf)
    quads = pltpu.VMEM((4, rows, width), bf)
    blocks = pltpu.VMEM((n, rows, rows), bf)
    all_of = lambda x: shape((planes,) + x.shape, x.dtype)
    gathered = lambda x: pltpu.VMEM((planes,) + x.shape, x.dtype)
    ring = dma((2, Gather.sems))
    line = dma((3, planes))
    swap = dma((2, n))
    return pl.pallas_call(
        front_kernel,
        out_shape=(
            shape((n, rows, width), bf), shape((n, rows, width), bf), shape((n, rows, width), bf),
            shape((n, rows, wide), bf), shape((n, rows, 2 * wide), bf), all_of(qkv_own), all_of(down_own),
            shape((2 * length, LANES), bf), shape((length, LANES), bf), shape((length, LANES), bf),
            shape((pairs * LANES, 384), f32), shape((pairs, 384), f32), shape((n, rows, rows), bf),
            shape((rows, width), f32), shape((rows, width), f32), shape((1, width), f32), shape((n,) + spot.shape, spot.dtype),
            shape((2, width), f32), shape((n, rows, rows), bf), shape((n, rows, rows), bf),
        ),
        in_specs=vm(9) + anywhere(1),
        out_specs=vm(18) + anywhere(2),
        scratch_shapes=[
            gathered(gu_own), gathered(out_own), pltpu.VMEM((planes, n) + out_own.shape, bf),
            pltpu.VMEM((16, 2, 96, LANES), bf), pltpu.VMEM((16, 96, LANES), bf), pltpu.VMEM((16, 96, LANES), bf),
            pltpu.VMEM((16, 96, 192), bf), gathered(gain_own), pltpu.SMEM((n,) + spot.shape, jnp.int32),
            blocks, blocks, pltpu.VMEM((rows, width), bf),
            pltpu.VMEM((4, rows, width), f32), quads, quads, halves, halves,
            ring, ring, swap, dma((2, planes)), line, line, ring, line, line, dma((2,)),
            swap, ring, dma((2, Reduce.sems)), swap, swap,
        ],
        compiler_params=pltpu.CompilerParams(collective_id=1, has_side_effects=True, vmem_limit_bytes=67043328),
        name="front_moves",
    )(tok, up_low, spot, gain_own, qkv_own, out_own, gu_own, down_own, turns, up)


def attend_back(spans, grad, q, k, v, att, lse, turns):
    length = k.shape[0]
    return pl.pallas_call(
        back_kernel,
        out_shape=jax.ShapeDtypeStruct((length, 4 * LANES), jnp.bfloat16),
        in_specs=[pl.BlockSpec(memory_space=pltpu.SMEM)] + vm(7),
        out_specs=pl.BlockSpec(memory_space=pltpu.VMEM),
        scratch_shapes=[pltpu.VMEM((length, LANES), jnp.float32)] * 2,
        name="attend_back",
    )(spans, grad, q, k, v, att, lse, turns)


def fast_body(
    tokens, positions, qkv_weight, out_weight, gate_up_weight, down_weight, attn_gain, ffn_gain, cotangent
):
    me = lax.axis_index("ctx")
    n = lax.axis_size("ctx")
    planes = lax.axis_size("fsdp")
    rows = tokens.shape[1]
    length = n * rows
    width = tokens.shape[2]
    wide = down_weight.shape[1] * planes
    own = wide // n
    piece = own // planes
    shard = qkv_weight.shape[1]
    query_width = HEADS * HEAD_DIM
    key_width = KV_HEADS * HEAD_DIM
    cut = lax.dynamic_slice_in_dim

    qkv = qkv_weight[0]
    q_part = cut(qkv, me * 2 * HEAD_DIM, 2 * HEAD_DIM, 1)
    k_part = cut(qkv, query_width + me * HEAD_DIM, HEAD_DIM, 1)
    v_part = cut(qkv, query_width + key_width + me * HEAD_DIM, HEAD_DIM, 1)
    half = HEAD_DIM // 2
    gap = jnp.zeros((shard, 64 - half), qkv.dtype)
    columns = []
    for part in (q_part[:, :HEAD_DIM], q_part[:, HEAD_DIM:], k_part):
        columns += [part[:, :half], gap, part[:, half:], gap]
    qkv_own = jnp.concatenate(columns + [v_part, gap, gap], axis=1)
    out_own = cut(out_weight[0], me * (shard // n), shard // n, 0)
    pieces = [cut(gate_up_weight[0], at * (wide // planes) + me * piece, piece, 2) for at in range(planes)]
    gate_up_own = jnp.concatenate([x[:, s] for s in range(2) for x in pieces], axis=1)
    down_own = cut(down_weight[0], me * piece, piece, 0)
    gains = jnp.concatenate([attn_gain, ffn_gain, jnp.zeros((6, shard), attn_gain.dtype)], axis=0).astype(jnp.float32)
    spot = jnp.full((8, LANES), positions[0, 0] // (rows // 2), jnp.int32)
    turns = table(length)
    (
        normed, upstream_all, second_all, hidden, gate_up_low, qkv_block, down_block, q, k, v, att, lse, low,
        middle_grad, middle, ffn_partial, spots, gains, attended_grad, middle_cols,
    ) = front_moves(
        tokens[0], cotangent[0].astype(jnp.bfloat16), spot, gains, qkv_own, out_own, gate_up_own, down_own,
        turns.reshape(2 * n, rows // 2, LANES), cotangent[0],
    )
    early = spots[:, 0, 0]
    span = jnp.stack([early, 2 * n - 1 - early], axis=1).reshape(2 * n)
    order = jnp.max(
        jnp.where(span[None, :] == jnp.arange(2 * n)[:, None], jnp.arange(2 * n)[None, :], 0), axis=1
    )
    spans = jnp.concatenate([span, order]).astype(jnp.int32)

    def flat(x):
        return x.reshape(length, -1)

    def reduce_planes(block):
        return lax.psum_scatter(block.astype(jnp.bfloat16), "fsdp", scatter_dimension=0, tiled=True)

    down_grad = reduce_planes(tn(flat(hidden), flat(upstream_all)))
    gate_up_grad = reduce_planes(tn(flat(second_all), flat(gate_up_low)))
    projected_grad = attend_back(spans, flat(attended_grad), q, k, v, att, lse, turns)
    stream_grad, result, gain_grads, low_all, down_grad, gate_up_grad = last_moves(
        projected_grad.reshape(n, rows, -1), qkv_block, tokens[0], middle_grad, gains[0:1], ffn_partial,
        flat(low), down_grad, gate_up_grad, hidden, down_block, middle,
    )
    low_all = low_all.transpose(1, 0, 2).reshape(length, query_width)
    gain_grads = gain_grads.reshape(2, planes, shard)
    gain_grads = lax.dynamic_index_in_dim(gain_grads, lax.axis_index("fsdp"), 1, keepdims=False)
    qkv_grad = reduce_planes(tn(flat(normed), projected_grad))
    out_grad = reduce_planes(tn(low_all, flat(middle_cols)))
    qkv_grad, out_grad = gathers(7, qkv_grad, out_grad)
    pieces = qkv_grad.reshape(n, shard, 4, LANES).transpose(1, 0, 2, 3)
    qkv_grad = jnp.concatenate(
        [
            gathered_spread(pieces[:, :, 0:2]).reshape(shard, query_width),
            gathered_spread(pieces[:, :, 2]).reshape(shard, key_width),
            pieces[:, :, 3, :HEAD_DIM].reshape(shard, key_width),
        ],
        axis=1,
    ).astype(jnp.float32)
    out_grad = out_grad.transpose(1, 0, 2).reshape(shard, width).astype(jnp.float32)
    gate_up_grad = gate_up_grad.reshape(n, shard, 2, planes, -1).transpose(1, 2, 3, 0, 4)
    gate_up_grad = gate_up_grad.reshape(shard, 2, wide).astype(jnp.float32)
    down_grad = down_grad.reshape(-1, width).astype(jnp.float32)
    return (
        result[None],
        stream_grad[None],
        qkv_grad[None],
        out_grad[None],
        gate_up_grad[None],
        down_grad[None],
        gain_grads[0][None],
        gain_grads[1][None],
    )


def solution(mesh):
    split = mesh.shape["ctx"] == KV_HEADS
    placed = (
        P("fsdp", "ctx", None),
        P("fsdp", "ctx"),
        P(None, "fsdp", None),
        P(None, "fsdp", None),
        P(None, "fsdp", None, None),
        P(None, "fsdp", None),
        P(None, "fsdp"),
        P(None, "fsdp"),
        P("fsdp", "ctx", None),
    )
    return jax.shard_map(
        fast_body if split else body,
        mesh=mesh,
        in_specs=placed,
        out_specs=(
            P("fsdp", "ctx", None),
            P("fsdp", "ctx", None),
            P(None, "fsdp", None),
            P(None, "fsdp", None),
            P(None, "fsdp", None, None),
            P(None, "fsdp", None),
            P(None, "fsdp"),
            P(None, "fsdp"),
        ),
        check_vma=False,
    )
```

```python
import functools
import jax
import jax.numpy as jnp
from jax import lax
from jax.experimental import pallas as pl
from jax.experimental.pallas import tpu as pltpu
from jax.sharding import PartitionSpec as P

HEADS = 16
KV_HEADS = 8
HEAD_DIM = 96
LAYERS = 1


epsilon = 1e-05
rope_base = 100000.0


def angles(place):
    halfway = HEAD_DIM // 2
    frequency = rope_base ** (-(jnp.arange(halfway, dtype=jnp.float32) * 2.0 / HEAD_DIM))
    phases = place.astype(jnp.float32)[:, None] * frequency[None, :]
    phases = jnp.concatenate([phases, phases], axis=-1)
    return (jnp.cos(phases)[:, None, :], jnp.sin(phases)[:, None, :])


def rotate(vectors, cosine, sine):
    halfway = vectors.shape[-1] // 2
    turned = jnp.concatenate([-vectors[..., halfway:], vectors[..., :halfway]], axis=-1)
    return vectors * cosine + turned * sine


def rotate_back(grads, cosine, sine):
    halfway = grads.shape[-1] // 2
    scaled = grads * sine
    return grads * cosine + jnp.concatenate(
        [scaled[..., halfway:], -scaled[..., :halfway]], axis=-1
    )


def normalize(rows, gain):
    factor = lax.rsqrt(jnp.mean(rows * rows, axis=-1, keepdims=True) + epsilon)
    return (rows * factor * gain, factor)


def normalize_back(upstream, rows, factor, gain):
    unit_rows = rows * factor
    gain_grad = jnp.sum(upstream * unit_rows, axis=0)
    scaled = upstream * gain
    row_inner = jnp.mean(scaled * unit_rows, axis=-1, keepdims=True)
    return (factor * (scaled - unit_rows * row_inner), gain_grad)


def split_blocks(queries, keys_all, values_all, key_place):
    rows = queries.shape[0]
    half = rows // 2
    shards = key_place.shape[0] // rows
    key_blocks = keys_all.reshape(shards, 2, half, KV_HEADS, HEAD_DIM)
    value_blocks = values_all.reshape(shards, 2, half, KV_HEADS, HEAD_DIM)
    place_blocks = key_place.reshape(shards, 2, half)
    return (key_blocks, value_blocks, place_blocks)


def scores_of(queries, key_block, place_block, query_place):
    scaling = HEAD_DIM ** (-0.5)
    scores = (
        jnp.einsum("rkgd,skd->kgrs", queries, key_block, preferred_element_type=jnp.float32)
        * scaling
    )
    allowed = place_block[None, None, None, :] <= query_place[None, None, :, None]
    return (scores, allowed)


def reachable(place_block, query_place):
    return jnp.min(place_block) <= jnp.max(query_place)


def attention_forward(queries, keys_all, values_all, query_place, key_place):
    key_blocks, value_blocks, place_blocks = split_blocks(queries, keys_all, values_all, key_place)
    rows = queries.shape[0]
    half = rows // 2
    groups = HEADS // KV_HEADS
    query_spans = queries.reshape(2, half, KV_HEADS, groups, HEAD_DIM)
    place_spans = query_place.reshape(2, half)

    def sweep_max(carry, inputs):
        key_block, place_block = inputs
        updated_all = []
        for span in range(2):
            state = carry[span]
            for part in range(2):

                def live(current, span=span, part=part):
                    maximum, total = current
                    scores, allowed = scores_of(
                        query_spans[span], key_block[part], place_block[part], place_spans[span]
                    )
                    masked = jnp.where(allowed, scores, -1e30)
                    updated = jnp.maximum(maximum, jnp.max(masked, axis=-1))
                    weights_now = jnp.where(allowed, jnp.exp(masked - updated[..., None]), 0.0)
                    return (
                        updated,
                        total * jnp.exp(maximum - updated) + jnp.sum(weights_now, axis=-1),
                    )

                state = lax.cond(
                    reachable(place_block[part], place_spans[span]),
                    live,
                    lambda current: current,
                    state,
                )
            updated_all.append(state)
        return (tuple(updated_all), None)

    start_max = jnp.full((KV_HEADS, groups, half), -1e30, jnp.float32)
    start_total = jnp.zeros((KV_HEADS, groups, half), jnp.float32)
    start = ((start_max, start_total), (start_max, start_total))
    finals, unused = lax.scan(sweep_max, start, (key_blocks, place_blocks))
    logsum_spans = [finals[span][0] + jnp.log(finals[span][1]) for span in range(2)]

    def sweep_out(results, inputs):
        key_block, value_block, place_block = inputs
        updated_all = []
        for span in range(2):
            result = results[span]
            for part in range(2):

                def live(current, span=span, part=part):
                    scores, allowed = scores_of(
                        query_spans[span], key_block[part], place_block[part], place_spans[span]
                    )
                    softmax_rows = jnp.where(
                        allowed, jnp.exp(scores - logsum_spans[span][..., None]), 0.0
                    ).astype(jnp.bfloat16)
                    return current + jnp.einsum(
                        "kgrs,skd->rkgd",
                        softmax_rows,
                        value_block[part],
                        preferred_element_type=jnp.float32,
                    )

                result = lax.cond(
                    reachable(place_block[part], place_spans[span]),
                    live,
                    lambda current: current,
                    result,
                )
            updated_all.append(result)
        return (tuple(updated_all), None)

    start_out = jnp.zeros((half, KV_HEADS, groups, HEAD_DIM), jnp.float32)
    outs, unused_out = lax.scan(
        sweep_out, (start_out, start_out), (key_blocks, value_blocks, place_blocks)
    )
    logsum = jnp.concatenate(logsum_spans, axis=-1)
    attended = jnp.concatenate([outs[0], outs[1]], axis=0)
    return (logsum, attended)


def attention_backward(
    queries, keys_all, values_all, query_place, key_place, logsum, attended_grad, row_inner
):
    key_blocks, value_blocks, place_blocks = split_blocks(queries, keys_all, values_all, key_place)
    rows = queries.shape[0]
    half = rows // 2
    groups = HEADS // KV_HEADS
    scaling = HEAD_DIM ** (-0.5)
    query_spans = queries.reshape(2, half, KV_HEADS, groups, HEAD_DIM)
    place_spans = query_place.reshape(2, half)
    grad_spans = attended_grad.reshape(2, half, KV_HEADS, groups, HEAD_DIM)
    logsum_spans = logsum.reshape(KV_HEADS, groups, 2, half)
    inner_spans = row_inner.reshape(KV_HEADS, groups, 2, half)

    def sweep_back(query_grads, inputs):
        key_block, value_block, place_block = inputs
        query_grads = list(query_grads)
        key_parts = []
        value_parts = []
        for part in range(2):
            key_acc = jnp.zeros((half, KV_HEADS, HEAD_DIM), jnp.float32)
            value_acc = jnp.zeros((half, KV_HEADS, HEAD_DIM), jnp.float32)
            for span in range(2):

                def live(current, span=span, part=part):
                    query_grad, key_grad, value_grad = current
                    scores, allowed = scores_of(
                        query_spans[span], key_block[part], place_block[part], place_spans[span]
                    )
                    softmax_rows = jnp.where(
                        allowed, jnp.exp(scores - logsum_spans[:, :, span][..., None]), 0.0
                    )
                    rounded = softmax_rows.astype(jnp.bfloat16)
                    weight_grad = jnp.einsum(
                        "rkgd,skd->kgrs",
                        grad_spans[span],
                        value_block[part],
                        preferred_element_type=jnp.float32,
                    )
                    score_grad = (
                        softmax_rows * (weight_grad - inner_spans[:, :, span][..., None])
                    ).astype(jnp.bfloat16)
                    query_grad = (
                        query_grad
                        + jnp.einsum(
                            "kgrs,skd->rkgd",
                            score_grad,
                            key_block[part],
                            preferred_element_type=jnp.float32,
                        )
                        * scaling
                    )
                    key_grad = (
                        key_grad
                        + jnp.einsum(
                            "kgrs,rkgd->skd",
                            score_grad,
                            query_spans[span],
                            preferred_element_type=jnp.float32,
                        )
                        * scaling
                    )
                    value_grad = value_grad + jnp.einsum(
                        "kgrs,rkgd->skd",
                        rounded,
                        grad_spans[span],
                        preferred_element_type=jnp.float32,
                    )
                    return (query_grad, key_grad, value_grad)

                state = (query_grads[span], key_acc, value_acc)
                state = lax.cond(
                    reachable(place_block[part], place_spans[span]),
                    live,
                    lambda current: current,
                    state,
                )
                query_grads[span], key_acc, value_acc = state
            key_parts.append(key_acc)
            value_parts.append(value_acc)
        key_out = jnp.concatenate(key_parts, axis=0)
        value_out = jnp.concatenate(value_parts, axis=0)
        return (tuple(query_grads), (key_out, value_out))

    start_grad = jnp.zeros((half, KV_HEADS, groups, HEAD_DIM), jnp.float32)
    query_pair, (key_grads, value_grads) = lax.scan(
        sweep_back, (start_grad, start_grad), (key_blocks, value_blocks, place_blocks)
    )
    query_grad = jnp.concatenate([query_pair[0], query_pair[1]], axis=0)
    return (
        query_grad,
        key_grads.reshape(-1, KV_HEADS, HEAD_DIM),
        value_grads.reshape(-1, KV_HEADS, HEAD_DIM),
    )


def fetch_layer(qkv_weight, out_weight, gate_up_weight, down_weight, attn_gain, ffn_gain, layer_id):
    return (
        lax.all_gather(qkv_weight[layer_id], "fsdp", axis=0, tiled=True),
        lax.all_gather(out_weight[layer_id], "fsdp", axis=0, tiled=True),
        lax.all_gather(gate_up_weight[layer_id], "fsdp", axis=0, tiled=True),
        lax.all_gather(down_weight[layer_id], "fsdp", axis=0, tiled=True),
        lax.all_gather(attn_gain[layer_id], "fsdp", axis=0, tiled=True),
        lax.all_gather(ffn_gain[layer_id], "fsdp", axis=0, tiled=True),
    )


def fetch_again(qkv_weight, out_weight, gate_up_weight, down_weight, attn_gain, ffn_gain, layer_id):
    return (
        lax.all_gather(qkv_weight[layer_id], "fsdp", axis=0, tiled=True),
        lax.all_gather(out_weight[layer_id], "fsdp", axis=0, tiled=True),
        lax.all_gather(gate_up_weight[layer_id], "fsdp", axis=0, tiled=True),
        lax.all_gather(down_weight[layer_id], "fsdp", axis=0, tiled=True),
        lax.all_gather(attn_gain[layer_id], "fsdp", axis=0, tiled=True),
        lax.all_gather(ffn_gain[layer_id], "fsdp", axis=0, tiled=True),
    )


def forward_layer(stream, query_place, key_place, gathered):
    qkv_full, out_full, gate_up_full, down_full, attn_full, ffn_full = gathered
    rows = stream.shape[0]
    groups = HEADS // KV_HEADS
    query_width = HEADS * HEAD_DIM
    key_width = KV_HEADS * HEAD_DIM
    cosine, sine = angles(query_place)
    normed, first_factor = normalize(stream, attn_full.astype(jnp.float32))
    normed = normed.astype(jnp.bfloat16)
    projected = jnp.dot(normed, qkv_full, preferred_element_type=jnp.float32)
    queries = rotate(projected[:, :query_width].reshape(rows, HEADS, HEAD_DIM), cosine, sine)
    queries = queries.reshape(rows, KV_HEADS, groups, HEAD_DIM).astype(jnp.bfloat16)
    keys_local = rotate(
        projected[:, query_width : query_width + key_width].reshape(rows, KV_HEADS, HEAD_DIM),
        cosine,
        sine,
    ).astype(jnp.bfloat16)
    values_local = (
        projected[:, query_width + key_width :]
        .reshape(rows, KV_HEADS, HEAD_DIM)
        .astype(jnp.bfloat16)
    )
    keys_all, values_all = (
        lax.all_gather(keys_local, "ctx", axis=0, tiled=True),
        lax.all_gather(values_local, "ctx", axis=0, tiled=True),
    )
    logsum, attended = attention_forward(queries, keys_all, values_all, query_place, key_place)
    attended_low = attended.reshape(rows, query_width).astype(jnp.bfloat16)
    middle = stream + jnp.dot(attended_low, out_full, preferred_element_type=jnp.float32)
    second, second_factor = normalize(middle, ffn_full.astype(jnp.float32))
    second = second.astype(jnp.bfloat16)
    gate_up = jnp.einsum("rd,dcf->rcf", second, gate_up_full, preferred_element_type=jnp.float32)
    hidden = (jax.nn.silu(gate_up[:, 0]) * gate_up[:, 1]).astype(jnp.bfloat16)
    result = middle + jnp.dot(hidden, down_full, preferred_element_type=jnp.float32)
    stored = (
        stream,
        first_factor,
        normed,
        queries,
        keys_local,
        values_local,
        keys_all,
        values_all,
        logsum,
        attended,
        attended_low,
        middle,
        second_factor,
        second,
        gate_up,
        hidden,
    )
    return (result, stored)


def backward_layer(upstream, stored, gathered, query_place, key_place, keys_all, values_all):
    (
        stream,
        first_factor,
        normed,
        queries,
        keys_local,
        values_local,
        kept_keys,
        kept_values,
        logsum,
        attended,
        attended_low,
        middle,
        second_factor,
        second,
        gate_up,
        hidden,
    ) = stored
    qkv_full, out_full, gate_up_full, down_full, attn_full, ffn_full = gathered
    rows = stream.shape[0]
    groups = HEADS // KV_HEADS
    cosine, sine = angles(query_place)
    upstream_low = upstream.astype(jnp.bfloat16)
    hidden_grad = jnp.einsum(
        "rd,fd->rf", upstream_low, down_full, preferred_element_type=jnp.float32
    )
    gate_part = gate_up[:, 0]
    up_part = gate_up[:, 1]
    sigmoid = jax.nn.sigmoid(gate_part)
    gate_grad = hidden_grad * up_part * sigmoid * (1.0 + gate_part * (1.0 - sigmoid))
    up_grad = hidden_grad * gate_part * sigmoid
    gate_up_low = jnp.stack([gate_grad, up_grad], axis=1).astype(jnp.bfloat16)
    second_grad = jnp.einsum(
        "rcf,dcf->rd", gate_up_low, gate_up_full, preferred_element_type=jnp.float32
    )
    middle_grad, ffn_gain_grad = normalize_back(
        second_grad, middle, second_factor, ffn_full.astype(jnp.float32)
    )
    middle_grad = middle_grad + upstream
    middle_low = middle_grad.astype(jnp.bfloat16)
    attended_grad = jnp.einsum(
        "rd,od->ro", middle_low, out_full, preferred_element_type=jnp.float32
    )
    attended_grad = attended_grad.astype(jnp.bfloat16).reshape(rows, KV_HEADS, groups, HEAD_DIM)
    row_inner = jnp.einsum("rkgd,rkgd->kgr", attended_grad.astype(jnp.float32), attended)
    query_grad, key_grads, value_grads = attention_backward(
        queries, keys_all, values_all, query_place, key_place, logsum, attended_grad, row_inner
    )
    key_grad, value_grad = (
        lax.psum_scatter(key_grads, "ctx", scatter_dimension=0, tiled=True),
        lax.psum_scatter(value_grads, "ctx", scatter_dimension=0, tiled=True),
    )
    query_grad = rotate_back(query_grad.reshape(rows, HEADS, HEAD_DIM), cosine, sine)
    key_grad = rotate_back(key_grad, cosine, sine)
    projected_grad = jnp.concatenate(
        [query_grad.reshape(rows, -1), key_grad.reshape(rows, -1), value_grad.reshape(rows, -1)],
        axis=1,
    ).astype(jnp.bfloat16)
    normed_grad = jnp.einsum(
        "re,de->rd", projected_grad, qkv_full, preferred_element_type=jnp.float32
    )
    stream_grad, attn_gain_grad = normalize_back(
        normed_grad, stream, first_factor, attn_full.astype(jnp.float32)
    )
    stream_grad = stream_grad + middle_grad
    qkv_grad = jnp.einsum("rd,re->de", normed, projected_grad, preferred_element_type=jnp.float32)
    out_grad = jnp.einsum("ro,rd->od", attended_low, middle_low, preferred_element_type=jnp.float32)
    gate_up_grad = jnp.einsum(
        "rd,rcf->dcf", second, gate_up_low, preferred_element_type=jnp.float32
    )
    down_grad = jnp.einsum("rf,rd->fd", hidden, upstream_low, preferred_element_type=jnp.float32)
    sharded = (
        lax.psum_scatter(qkv_grad, "fsdp", scatter_dimension=0, tiled=True),
        lax.psum_scatter(out_grad, "fsdp", scatter_dimension=0, tiled=True),
        lax.psum_scatter(gate_up_grad, "fsdp", scatter_dimension=0, tiled=True),
        lax.psum_scatter(down_grad, "fsdp", scatter_dimension=0, tiled=True),
        lax.psum_scatter(attn_gain_grad, "fsdp", scatter_dimension=0, tiled=True),
        lax.psum_scatter(ffn_gain_grad, "fsdp", scatter_dimension=0, tiled=True),
    )
    totals = lax.psum(
        (sharded[0], sharded[1], sharded[2], sharded[3], sharded[4], sharded[5]), "ctx"
    )
    return (stream_grad, totals)


def body(
    tokens,
    positions,
    qkv_weight,
    out_weight,
    gate_up_weight,
    down_weight,
    attn_gain,
    ffn_gain,
    cotangent,
):
    query_place = positions[0]
    key_place = lax.all_gather(query_place, "ctx", axis=0, tiled=True)
    stream = tokens[0].astype(jnp.float32)
    gathered_list = []
    layer_id = 0
    gathered = fetch_layer(
        qkv_weight, out_weight, gate_up_weight, down_weight, attn_gain, ffn_gain, layer_id
    )
    stream, stored = forward_layer(stream, query_place, key_place, gathered)
    saved = [stored]
    gathered_list.append(gathered)
    activations = stream.astype(jnp.bfloat16)[None]
    upstream = cotangent[0]
    layer_grads = [None] * LAYERS
    for layer_id in reversed(range(LAYERS)):
        stored = saved[layer_id]
        gathered = fetch_again(
            qkv_weight, out_weight, gate_up_weight, down_weight, attn_gain, ffn_gain, layer_id
        )
        keys_all, values_all = (stored[6], stored[7])
        upstream, totals = backward_layer(
            upstream, stored, gathered, query_place, key_place, keys_all, values_all
        )
        layer_grads[layer_id] = totals
    outputs = [jnp.stack([entry[slot] for entry in layer_grads], axis=0) for slot in range(6)]
    return (
        activations,
        upstream[None],
        outputs[0],
        outputs[1],
        outputs[2],
        outputs[3],
        outputs[4],
        outputs[5],
    )


LANES = 128


def spread(heads):
    half = HEAD_DIM // 2
    pad = ((0, 0), (0, 0), (0, 64 - half))
    return jnp.concatenate([jnp.pad(heads[..., :half], pad), jnp.pad(heads[..., half:], pad)], axis=-1)


def gathered_spread(padded):
    half = HEAD_DIM // 2
    return jnp.concatenate([padded[..., :half], padded[..., 64 : 64 + half]], axis=-1)


def table(length):
    half = HEAD_DIM // 2
    frequency = rope_base ** (-(jnp.arange(half, dtype=jnp.float32) * 2.0 / HEAD_DIM))
    phases = jnp.arange(length, dtype=jnp.float32)[:, None] * frequency[None, :]
    pad = ((0, 0), (0, 64 - half))
    return jnp.concatenate([jnp.pad(jnp.cos(phases), pad), jnp.pad(jnp.sin(phases), pad)], axis=1)


def wave(rows):
    first = lax.broadcasted_iota(jnp.int32, rows.shape, 1) < 64
    other = pltpu.roll(rows, 64, 1)
    return jnp.where(first, rows, other), jnp.where(first, -other, rows)


def nt(left, right):
    return lax.dot_general(left, right, (((1,), (1,)), ((), ())), preferred_element_type=jnp.float32)


def nn(left, right):
    return lax.dot_general(left, right, (((1,), (0,)), ((), ())), preferred_element_type=jnp.float32)


def tn(left, right):
    return lax.dot_general(left, right, (((0,), (0,)), ((), ())), preferred_element_type=jnp.float32)


def causal(width):
    key_at = lax.broadcasted_iota(jnp.int32, (width, 2 * width), 0)
    query_at = lax.broadcasted_iota(jnp.int32, (width, 2 * width), 1)
    query_at = jnp.where(query_at >= width, query_at - width, query_at)
    return key_at <= query_at


def vm(count):
    return [pl.BlockSpec(memory_space=pltpu.VMEM)] * count


MESH = pl.DeviceIdType.MESH


class Place:
    def __init__(self):
        self.me = lax.axis_index("ctx")
        core, x, y = self.me % 2, (self.me // 2) % 2, self.me // 4
        self.dp, self.dx, self.dy = 1 - 2 * core, 2 - 4 * x, 4 - 8 * y
        self.p, self.x, self.y = self.me + self.dp, self.me + self.dx, self.me + self.dy
        self.d = self.x + self.dy
        self.z = lax.axis_index("fsdp")
        self.planes = lax.axis_size("fsdp")
        self.n = lax.axis_size("ctx")


def greet(place, ctx=True, planes=False):
    barrier = pltpu.get_barrier_semaphore()
    count = 0
    if ctx:
        for step in range(1, place.n):
            pl.semaphore_signal(
                barrier, inc=1, device_id={"ctx": lax.rem(place.me + step, place.n)}, device_id_type=MESH
            )
            count += 1
    if planes:
        for step in range(1, place.planes):
            pl.semaphore_signal(
                barrier, inc=1, device_id={"fsdp": lax.rem(place.z + step, place.planes)}, device_id_type=MESH
            )
            count += 1
    pl.semaphore_wait(barrier, count)


def send(source, target, send_sem, recv_sem, **where):
    return pltpu.make_async_remote_copy(
        src_ref=source, dst_ref=target, send_sem=send_sem, recv_sem=recv_sem,
        device_id=where, device_id_type=MESH,
    )


class Gather:
    sems = 14

    def __init__(self, place, own, out, sem):
        self.place, self.own, self.out, self.sem = place, own, out, sem
        self.half = out.shape[1] // 2
        self.started = []
        self.met = False

    def go(self, source, target, index, rank):
        copy = send(source, target, self.sem.at[0, index], self.sem.at[1, index], ctx=rank)
        copy.start()
        self.started.append(copy)

    def part(self, rank, half):
        return self.out.at[rank, pl.ds(half * self.half, self.half)]

    def whole(self, rank):
        return self.out.at[rank]

    def start(self):
        p = self.place
        keep = pltpu.make_async_copy(self.own, self.whole(p.me), self.sem.at[0, 13])
        keep.start()
        self.keep = keep
        halves = [self.own.at[pl.ds(h * self.half, self.half)] for h in range(2)]
        self.go(halves[0], self.part(p.me, 0), 0, p.x)
        self.go(halves[1], self.part(p.me, 1), 3, p.y)
        self.go(self.own, self.whole(p.me), 6, p.p)
        self.go(halves[1], self.part(p.me, 1), 1, p.x)
        self.go(halves[0], self.part(p.me, 0), 2, p.y)

    def arrived(self, rank, half, index):
        part = self.part(rank, half)
        pltpu.make_async_copy(part, part, self.sem.at[1, index]).wait()
        return part

    def relay(self):
        p = self.place
        part = self.arrived(p.x, 0, 0)
        self.go(part, part, 4, p.y)
        self.go(part, part, 7, p.p)
        part = self.arrived(p.y, 1, 3)
        self.go(part, part, 5, p.x)
        self.go(part, part, 10, p.p)

    def rest(self):
        p = self.place
        for rank, half, index, onward in ((p.x, 1, 1, 8), (p.y, 0, 2, 9), (p.d, 0, 4, 11), (p.d, 1, 5, 12)):
            part = self.arrived(rank, half, index)
            self.go(part, part, onward, p.p)

    def first_partner(self):
        part = self.whole(self.place.p)
        pltpu.make_async_copy(part, part, self.sem.at[1, 6]).wait()
        self.met = True

    def partner(self):
        p = self.place
        if not self.met:
            self.first_partner()
        for rank, half, index in (
            (p.x, 0, 7), (p.y, 1, 10), (p.x, 1, 8), (p.y, 0, 9), (p.d, 0, 11), (p.d, 1, 12),
        ):
            self.arrived(rank + p.dp, half, index)

    def finish(self, kept=False):
        if not kept:
            self.keep.wait()
        for copy in self.started:
            copy.wait_send()


class PlaneGather:
    def __init__(self, place, own, out, sem):
        self.place, self.own, self.out, self.sem = place, own, out, sem

    def hop(self, step, up):
        p = self.place
        sign = 1 if up else -1
        source = p.z - sign * step
        target = p.z + sign
        ok = jnp.logical_and(
            jnp.logical_and(source >= 0, source < p.planes),
            jnp.logical_and(target >= 0, target < p.planes),
        )
        source = jnp.clip(source, 0, p.planes - 1)
        target = jnp.clip(target, 0, p.planes - 1)
        block = self.own if step == 0 else self.out.at[source]
        return ok, send(
            block, self.out.at[source], self.sem.at[0 if up else 1, source], self.sem.at[2, source], fsdp=target
        )

    def start(self):
        p = self.place
        self.keep = pltpu.make_async_copy(self.own, self.out.at[p.z], self.sem.at[2, p.z])
        self.keep.start()
        for up in (True, False):
            ok, copy = self.hop(0, up)
            pl.when(ok)(copy.start)

    def got(self, step, up):
        p = self.place
        source = p.z - step if up else p.z + step
        ok = jnp.logical_and(source >= 0, source < p.planes)
        source = jnp.clip(source, 0, p.planes - 1)
        part = self.out.at[source]
        return ok, pltpu.make_async_copy(part, part, self.sem.at[2, source])

    def step(self, number):
        for up in (True, False):
            ok, copy = self.got(number, up)
            pl.when(ok)(copy.wait)
            if number < self.place.planes - 1:
                ok, copy = self.hop(number, up)
                pl.when(ok)(copy.start)

    def finish(self, kept=False):
        if not kept:
            self.keep.wait()
        for number in range(self.place.planes - 1):
            for up in (True, False):
                ok, copy = self.hop(number, up)
                pl.when(ok)(copy.wait_send)


class Exchange:
    def __init__(self, place, blocks, out, sem):
        self.place, self.blocks, self.out, self.sem = place, blocks, out, sem

    def pick(self, rank):
        return self.blocks.at[rank]

    def copy(self, step):
        p = self.place
        rank = lax.rem(p.me + step, p.n)
        return send(self.pick(rank), self.out.at[p.me], self.sem.at[0, step], self.sem.at[1, step], ctx=rank)

    def start(self):
        p = self.place
        for step in range(1, p.n):
            self.copy(step).start()
        self.keep = pltpu.make_async_copy(self.pick(p.me), self.out.at[p.me], self.sem.at[0, 0])
        self.keep.start()

    def finish(self):
        p = self.place
        self.keep.wait()
        for step in range(1, p.n):
            self.copy(step).wait_send()
        for step in range(1, p.n):
            part = self.out.at[lax.rem(p.me + p.n - step, p.n)]
            pltpu.make_async_copy(part, part, self.sem.at[1, step]).wait()


class Share(Exchange):
    def pick(self, rank):
        return self.blocks


class PlaneShare:
    def __init__(self, place, block, out, sem):
        self.place, self.block, self.out, self.sem = place, block, out, sem

    def copy(self, step):
        p = self.place
        plane = lax.rem(p.z + step, p.planes)
        return send(self.block, self.out.at[p.z], self.sem.at[0, step], self.sem.at[1, step], fsdp=plane)

    def start(self):
        p = self.place
        for step in range(1, p.planes):
            self.copy(step).start()
        self.keep = pltpu.make_async_copy(self.block, self.out.at[p.z], self.sem.at[0, 0])
        self.keep.start()

    def finish(self):
        p = self.place
        self.keep.wait()
        for step in range(1, p.planes):
            self.copy(step).wait_send()
        for step in range(1, p.planes):
            part = self.out.at[lax.rem(p.z + p.planes - step, p.planes)]
            pltpu.make_async_copy(part, part, self.sem.at[1, step]).wait()


def anywhere(count):
    return [pl.BlockSpec(memory_space=pl.ANY)] * count


class Reduce:
    sems = 10

    def __init__(self, place, mine, theirs, first, out, second, sem):
        self.place, self.mine, self.theirs, self.first, self.out, self.second, self.sem = (
            place, mine, theirs, first, out, second, sem
        )
        self.half = out.shape[1]
        self.started = []

    def push(self, slot):
        copy = send(
            self.theirs.at[slot], self.first.at[slot], self.sem.at[0, slot], self.sem.at[1, slot], ctx=self.place.p
        )
        copy.start()
        return copy

    def pushed(self):
        for slot in range(4):
            send(
                self.theirs.at[slot], self.first.at[slot], self.sem.at[0, slot], self.sem.at[1, slot],
                ctx=self.place.p,
            ).wait_send()

    def add(self, slot):
        part = self.first.at[slot]
        pltpu.make_async_copy(part, part, self.sem.at[1, slot]).wait()
        self.mine[slot] = self.mine[slot] + self.first[slot].astype(jnp.float32)

    def go(self, index, value, rank):
        self.out[index] = value.astype(jnp.bfloat16)
        copy = send(
            self.out.at[index], self.second.at[index], self.sem.at[0, 4 + index], self.sem.at[1, 4 + index], ctx=rank
        )
        copy.start()
        self.started.append(copy)

    def top(self, slot):
        return self.mine[slot, pl.ds(0, self.half), :]

    def low(self, slot):
        return self.mine[slot, pl.ds(self.half, self.half), :]

    def got(self, index):
        part = self.second.at[index]
        pltpu.make_async_copy(part, part, self.sem.at[1, 4 + index]).wait()
        return self.second[index].astype(jnp.float32)

    def across(self):
        self.add(3)
        self.go(1, self.top(3), self.place.x)
        self.go(3, self.low(3), self.place.y)

    def beside(self):
        self.add(1)
        self.go(0, self.top(1), self.place.x)
        self.add(2)
        self.go(2, self.low(2), self.place.y)

    def turn(self):
        self.go(4, self.top(2) + self.got(1), self.place.y)
        self.go(5, self.low(1) + self.got(3), self.place.x)

    def total(self, use):
        self.add(0)
        use(pl.ds(0, self.half), self.top(0) + self.got(0) + self.got(4))
        use(pl.ds(self.half, self.half), self.low(0) + self.got(2) + self.got(5))

    def finish(self):
        self.pushed()
        for copy in self.started:
            copy.wait_send()


def flip(place, i):
    return place.me + (i % 2) * place.dp + ((i // 2) % 2) * place.dx + (i // 4) * place.dy


class Steps:
    def __init__(self, *steps):
        self.steps = list(steps)

    def next(self, count=1):
        for step in self.steps[:count]:
            step()
        self.steps = self.steps[count:]

    def rest(self):
        self.next(len(self.steps))


class OutGather(Gather):
    def __init__(self, place, own, out, sem):
        self.place, self.own, self.out, self.sem = place, own, out, sem
        self.half = out.shape[0] // 2
        self.started = []
        self.met = False

    def part(self, rank, half):
        return self.out.at[pl.ds(half * self.half, self.half), rank]

    def whole(self, rank):
        return self.out.at[:, rank]


def front_kernel(
    tok, up_low, spot, gain_own, qkv_own, out_own, gu_own, down_own, turn_ref, up,
    normed, up_all, second_all, hidden, gul, qkv_w, down_w, q_ref, k_ref, v_ref, att_ref, lse_ref, low,
    middle_grad, middle, gain_grad, spots, gains, agrad, mcols,
    gu_w, out_block, out_w, qr, kr, vr, low_sorted, gain_all, spots_s,
    attended, mcols_send, own, mine, theirs, first, out, second,
    tok_sem, up_sem, spot_sem, gain_sem, qkv_sem, out_sem, outc_sem, gu_sem, down_sem, local_sem,
    low_sem, gather_sem, reduce_sem, agrad_sem, mcols_sem,
):
    place = Place()
    n = place.n
    rows = tok.shape[0]
    half = rows // 2
    pairs = 8
    heads = rows
    greet(place, planes=True)
    spans = Share(place, spot, spots, spot_sem)
    scales = PlaneShare(place, gain_own, gain_all, gain_sem)
    tokens = Gather(place, tok, normed, tok_sem)
    cots = Gather(place, up_low, up_all, up_sem)
    qkvs = PlaneGather(place, qkv_own, qkv_w, qkv_sem)
    outs = PlaneGather(place, out_own, out_block, out_sem)
    outc = OutGather(place, out_block, out_w, outc_sem)
    gus = PlaneGather(place, gu_own, gu_w, gu_sem)
    downs = PlaneGather(place, down_own, down_w, down_sem)
    fetch = pltpu.make_async_copy(up, middle_grad, local_sem.at[0])
    fetch.start()
    spans.start()
    scales.start()
    qkvs.start()
    tokens.start()
    tokens.relay()
    qkvs.step(1)
    outs.start()
    qkvs.step(2)
    downs.start()
    tokens.rest()
    qkvs.step(3)
    cots.start()
    tokens.partner()
    tokens.finish()
    spans.finish()
    scales.finish()
    qkvs.keep.wait()
    table = pltpu.make_async_copy(spots, spots_s, local_sem.at[1])
    table.start()
    for g in range(2):
        gains[pl.ds(g, 1), :] = jnp.concatenate([gain_all[z, pl.ds(g, 1), :] for z in range(4)], axis=1)
    table.wait()
    early = [spots_s[j, 0, 0] for j in range(pairs)]
    holder = []
    for t in range(pairs):
        at = 0
        for j in range(pairs):
            at = jnp.where(early[j] == t, j, at)
        holder.append(at)

    def block_of(s):
        return 2 * holder[s] if s < pairs else 2 * holder[2 * pairs - 1 - s] + 1

    def span_of(b):
        return early[b // 2] if b % 2 == 0 else 2 * pairs - 1 - early[b // 2]

    def project(j, carry):
        x = normed[pl.ds(2 * j, 2)].reshape(2 * rows, -1).astype(jnp.float32)
        factor = lax.rsqrt(jnp.mean(x * x, axis=-1, keepdims=True) + epsilon)
        scaled = (x * factor * gains[pl.ds(0, 1), :]).astype(jnp.bfloat16)
        normed[pl.ds(2 * j, 2)] = scaled.reshape(2, rows, -1)
        proj = nn(scaled, qkv_w[...].reshape(-1, 4 * LANES))
        for piece in range(4):
            c = spots_s[2 * j + piece // 2, 0, 0]
            cosine, sine = wave(turn_ref[c if piece % 2 == 0 else 2 * pairs - 1 - c])
            mine_rows = proj[piece * half : (piece + 1) * half]

            def turned(part):
                z = mine_rows[:, part * LANES : (part + 1) * LANES]
                return (z * cosine + pltpu.roll(z, 64, 1) * sine).astype(jnp.bfloat16)

            qr[4 * j + piece, 0] = turned(0)
            qr[4 * j + piece, 1] = turned(1)
            kr[4 * j + piece] = turned(2)
            vr[4 * j + piece] = mine_rows[:, 3 * LANES :].astype(jnp.bfloat16)
        return carry

    lax.fori_loop(0, 4, project, 0)
    for s in range(2 * pairs):
        b = block_of(s)
        base = (s // 2) * 4 * half + (s % 2) * half
        both = qr[b]
        q_ref[pl.ds(base, half), :] = both[0]
        q_ref[pl.ds(base + 2 * half, half), :] = both[1]
        k_ref[pl.ds(s * half, half), :] = kr[b]
        v_ref[pl.ds(s * half, half), :] = vr[b]

    steps = Steps(
        lambda: outs.step(1), cots.relay, lambda: outs.step(2), lambda: outs.step(3),
        lambda: (outs.keep.wait(), outc.start(), downs.step(1), gus.start()), cots.rest, outc.relay,
        lambda: (downs.step(2), outc.rest()), lambda: (cots.partner(), outc.partner()),
    )
    scaling = HEAD_DIM ** (-0.5)
    mask = causal(2 * half)
    lane = lax.broadcasted_iota(jnp.int32, (half, LANES), 1)
    values_t = v_ref[...].astype(jnp.float32).T.astype(jnp.bfloat16)
    for pair in range(pairs):
        width = (pair + 1) * 2 * half
        q = q_ref[pl.ds(pair * 4 * half, 4 * half), :]
        before = width - 2 * half
        parts = [jnp.where(mask, nt(k_ref[pl.ds(before, 2 * half), :], q) * scaling, -1e30)]
        if pair:
            parts.append(nt(k_ref[pl.ds(0, before), :], q) * scaling)
        tops = [jnp.max(part, axis=0, keepdims=True) for part in parts]
        top = jnp.maximum(tops[0], tops[-1])
        parts = [jnp.exp(part - top) for part in parts]
        total = sum(jnp.sum(part, axis=0, keepdims=True) for part in parts)
        parts = [(part * (1.0 / total)).astype(jnp.bfloat16) for part in parts]
        lse_ref[pl.ds(pair, 1), :] = top + jnp.log(total)
        out_t = nn(values_t[:, before:width], parts[0])
        if pair:
            out_t = out_t + nn(values_t[:, :before], parts[1])
        att_ref[pl.ds(pair * LANES, LANES), :] = out_t
        result = out_t.T.astype(jnp.bfloat16).astype(jnp.float32)
        for part in range(2):
            left = result[part * half : (part + 1) * half]
            right = pltpu.roll(result[(2 + part) * half : (3 + part) * half], half, 1)
            low_sorted[2 * pair + part, :, 0:LANES] = jnp.where(lane < half, left, right).astype(jnp.bfloat16)
            low_sorted[2 * pair + part, :, LANES : 2 * half] = right[:, : 2 * half - LANES].astype(jnp.bfloat16)
        steps.next()
    for b in range(2 * pairs):
        low[b // 2, pl.ds((b % 2) * half, half), :] = low_sorted[span_of(b)]
    moved = Exchange(place, low, attended, low_sem)
    moved.start()
    steps.rest()
    outc.keep.wait()
    moved.finish()
    total = tok[...].astype(jnp.float32)
    for q in range(8):
        total = total + nn(attended[q], out_w[q // 2, pl.ds(4 * (q % 2), 4)].reshape(heads, -1))
    middle[...] = total
    factor = lax.rsqrt(jnp.mean(total * total, axis=-1, keepdims=True) + epsilon)
    own[...] = (total * factor * gains[pl.ds(1, 1), :]).astype(jnp.bfloat16)
    seconds = Gather(place, own, second_all, gather_sem)
    seconds.start()
    downs.step(3)
    gus.step(1)
    seconds.relay()
    gus.step(2)
    seconds.rest()
    gus.step(3)
    seconds.partner()
    gus.keep.wait()
    downs.keep.wait()
    seconds.keep.wait()
    cots.keep.wait()
    grads = Reduce(place, mine, theirs, first, out, second, reduce_sem)
    wide = hidden.shape[2]

    def block(i):
        rank = flip(place, i)
        gate_up = nn(second_all[rank], gu_w[...].reshape(-1, 2 * wide))
        gate, raised = gate_up[:, :wide], gate_up[:, wide:]
        sigmoid = 1.0 / (1.0 + jnp.exp(-gate))
        silu = gate * sigmoid
        hidden[rank] = (silu * raised).astype(jnp.bfloat16)
        hidden_grad = nt(up_all[rank], down_w[...].reshape(wide, -1))
        gul[rank, :, pl.ds(0, wide)] = (hidden_grad * raised * sigmoid * (1.0 + gate * (1.0 - sigmoid))).astype(jnp.bfloat16)
        gul[rank, :, pl.ds(wide, wide)] = (hidden_grad * silu).astype(jnp.bfloat16)
        return nt(gul[rank], gu_w[...].reshape(-1, 2 * wide))

    def pair_of(k, carry):
        theirs[k] = block(2 * k + 1).astype(jnp.bfloat16)
        grads.push(k)
        mine[k] = block(2 * k)
        return carry

    lax.fori_loop(1, 4, pair_of, 0)
    grads.across()
    grads.beside()
    lax.fori_loop(0, 1, pair_of, 0)
    grads.turn()
    fetch.wait()
    seconds.finish(kept=True)
    gain_grad[...] = jnp.zeros_like(gain_grad)

    def norm_back(part, second_grad):
        x = middle[part, :]
        factor = lax.rsqrt(jnp.mean(x * x, axis=-1, keepdims=True) + epsilon)
        unit = x * factor
        gain_grad[...] += jnp.sum(second_grad * unit, axis=0, keepdims=True)
        scaled = second_grad * gains[pl.ds(1, 1), :]
        inner = jnp.mean(scaled * unit, axis=-1, keepdims=True)
        grad = middle_grad[part, :] + factor * (scaled - unit * inner)
        middle_grad[part, :] = grad
        own[part, :] = grad.astype(jnp.bfloat16)

    grads.total(norm_back)

    def head_grads(q, carry):
        weight = out_w[q // 2, pl.ds(4 * (q % 2), 4)].reshape(heads, -1)
        attended[q] = nt(own[...], weight).astype(jnp.bfloat16)
        return carry

    lax.fori_loop(0, n, head_grads, 0)
    heads_back = Exchange(place, attended, agrad, agrad_sem)
    heads_back.start()
    for q in range(8):
        mcols_send[q] = own[:, q * heads : (q + 1) * heads]
    columns = Exchange(place, mcols_send, mcols, mcols_sem)
    columns.start()
    for move in (qkvs, outs, gus, downs):
        move.finish(kept=True)
    for move in (cots, outc):
        move.finish(kept=True)
    heads_back.finish()
    columns.finish()
    grads.finish()


def front_moves(tok, up_low, spot, gain_own, qkv_own, out_own, gu_own, down_own, turns, up):
    n, planes = lax.axis_size("ctx"), lax.axis_size("fsdp")
    rows, width = tok.shape
    length = n * rows
    wide = planes * down_own.shape[0]
    bf, f32 = jnp.bfloat16, jnp.float32
    shape = jax.ShapeDtypeStruct
    dma = pltpu.SemaphoreType.DMA
    pairs = length // 192
    halves = pltpu.VMEM((6, rows // 2, width), bf)
    quads = pltpu.VMEM((4, rows, width), bf)
    blocks = pltpu.VMEM((n, rows, rows), bf)
    all_of = lambda x: shape((planes,) + x.shape, x.dtype)
    gathered = lambda x: pltpu.VMEM((planes,) + x.shape, x.dtype)
    ring = dma((2, Gather.sems))
    line = dma((3, planes))
    swap = dma((2, n))
    return pl.pallas_call(
        front_kernel,
        out_shape=(
            shape((n, rows, width), bf), shape((n, rows, width), bf), shape((n, rows, width), bf),
            shape((n, rows, wide), bf), shape((n, rows, 2 * wide), bf), all_of(qkv_own), all_of(down_own),
            shape((2 * length, LANES), bf), shape((length, LANES), bf), shape((length, LANES), bf),
            shape((pairs * LANES, 384), f32), shape((pairs, 384), f32), shape((n, rows, rows), bf),
            shape((rows, width), f32), shape((rows, width), f32), shape((1, width), f32), shape((n,) + spot.shape, spot.dtype),
            shape((2, width), f32), shape((n, rows, rows), bf), shape((n, rows, rows), bf),
        ),
        in_specs=vm(9) + anywhere(1),
        out_specs=vm(18) + anywhere(2),
        scratch_shapes=[
            gathered(gu_own), gathered(out_own), pltpu.VMEM((planes, n) + out_own.shape, bf),
            pltpu.VMEM((16, 2, 96, LANES), bf), pltpu.VMEM((16, 96, LANES), bf), pltpu.VMEM((16, 96, LANES), bf),
            pltpu.VMEM((16, 96, 192), bf), gathered(gain_own), pltpu.SMEM((n,) + spot.shape, jnp.int32),
            blocks, blocks, pltpu.VMEM((rows, width), bf),
            pltpu.VMEM((4, rows, width), f32), quads, quads, halves, halves,
            ring, ring, swap, dma((2, planes)), line, line, ring, line, line, dma((2,)),
            swap, ring, dma((2, Reduce.sems)), swap, swap,
        ],
        compiler_params=pltpu.CompilerParams(collective_id=1, has_side_effects=True, vmem_limit_bytes=67043328),
        name="front_moves",
    )(tok, up_low, spot, gain_own, qkv_own, out_own, gu_own, down_own, turns, up)


class PlaneReduce:
    def __init__(self, place, block, recv, sem):
        self.place, self.block, self.recv, self.sem = place, block, recv, sem

    def hop(self, ok, part, slot, target, first, wait):
        copy = send(
            self.block.at[part], self.recv.at[slot], self.sem.at[0, part], self.sem.at[1, slot], fsdp=target
        )

        @pl.when(ok)
        def _():
            if wait:
                copy.wait_send()
                return
            if not first:
                self.merge(part, part)
            copy.start()

    def merge(self, part, slot):
        piece = self.recv.at[slot]
        pltpu.make_async_copy(piece, piece, self.sem.at[1, slot]).wait()
        total = self.block[part].astype(jnp.float32) + self.recv[slot].astype(jnp.float32)
        self.block[part] = total.astype(jnp.bfloat16)

    def ends(self, i, wait=False):
        z = self.place.z
        low = z == 0
        part = jnp.where(low, 3 - i, i)
        slot = part if i < 2 else jnp.where(low, part, 4)
        self.hop(jnp.logical_or(low, z == 3), part, slot, jnp.where(low, 1, 2), True, wait)

    def inner(self, up, down, slot_up, slot_down, to_up, to_down, wait=False):
        z = self.place.z
        low = z == 1
        part = jnp.where(low, up, down)
        slot = jnp.where(low, slot_up, slot_down)
        self.hop(jnp.logical_or(low, z == 2), part, slot, jnp.where(low, to_up, to_down), False, wait)

    def start(self, wait=False):
        for i in range(3):
            self.ends(i, wait)

    def step1(self, wait=False):
        self.inner(3, 0, 3, 0, 2, 1, wait)

    def step2(self, wait=False):
        self.inner(2, 1, 2, 4, 2, 1, wait)
        self.inner(0, 3, 4, 3, 0, 3, wait)

    def total(self):
        z = self.place.z

        @pl.when(z > 0)
        def _():
            self.merge(z, z)

        @pl.when(z < 3)
        def _():
            self.merge(z, 4)

    def own(self):
        return self.block.at[self.place.z]

    def finish(self):
        self.start(True)
        self.step1(True)
        self.step2(True)


def back_moves_kernel(
    early_ref, hidden, agrad, mcols, low, q_ref, k_ref, v_ref, att_ref, lse_ref, turn_ref, qkv_w, down_w, tok, gain,
    ffn_gain, middle, second_all, gul, up_all, normed, middle_grad,
    grad, result, gains, low_all, down_all, gu_all, out_all, qkv_all,
    wide_a, wide_b, low_buf, down_g, gu_g, out_g, qkv_g, down_r, gu_r, out_r, qkv_r,
    mine, theirs, first, out, second, dk_ref, dv_ref, pg_sorted, pgrad,
    gain_sum, mine_gain, ctx_gain, plane_sum, plane_gain,
    free, local_sem, sum_sem, reduce_sem, low_sem, down_zs, gu_zs, out_zs, qkv_zs, down_cs, gu_cs, out_cs, qkv_cs,
    gain_sem, plane_sem,
):
    place = Place()
    n = place.n
    rows = tok.shape[0]
    half = rows // 2
    pairs = 8
    width = tok.shape[1]
    length = n * rows
    loads = [
        pltpu.make_async_copy(source, target, local_sem.at[at])
        for at, (source, target) in enumerate((
            (up_all, wide_b), (second_all, wide_a), (gul, wide_b.at[:, :, pl.ds(0, gul.shape[2])]),
            (normed, wide_a), (middle_grad, grad),
        ))
    ]
    loads[0].start()
    loads[1].start()
    loads[4].start()
    greet(place, planes=True)
    early = [early_ref[j] for j in range(pairs)]
    holder = []
    for t in range(pairs):
        at = 0
        for j in range(pairs):
            at = jnp.where(early[j] == t, j, at)
        holder.append(at)

    def block_of(s):
        return 2 * holder[s] if s < pairs else 2 * holder[2 * pairs - 1 - s] + 1

    def span_of(b):
        return early[b // 2] if b % 2 == 0 else 2 * pairs - 1 - early[b // 2]

    down_z = PlaneReduce(place, down_g, down_r, down_zs)
    gu_z = PlaneReduce(place, gu_g, gu_r, gu_zs)
    out_z = PlaneReduce(place, out_g, out_r, out_zs)
    qkv_z = PlaneReduce(place, qkv_g, qkv_r, qkv_zs)
    sums = Reduce(place, mine, theirs, first, out, second, sum_sem)
    lows = Gather(place, low, low_all, low_sem)

    loads[0].wait()
    piece = down_g.shape[1]

    def down_block(t, carry):
        left = hidden[:, :, pl.ds(pl.multiple_of(t * piece, piece), piece)].reshape(length, piece)
        down_g[t] = tn(left, wide_b[...].reshape(length, width)).astype(jnp.bfloat16)
        return carry

    lax.fori_loop(0, 4, down_block, 0)
    down_z.start()
    loads[2].start()

    def other(k, carry):
        theirs[k] = nn(hidden[flip(place, 2 * k + 1)], down_w[...].reshape(-1, width)).astype(jnp.bfloat16)
        sums.push(k)
        return carry

    def ours(k, carry):
        mine[k] = nn(hidden[flip(place, 2 * k)], down_w[...].reshape(-1, width))
        return carry

    lax.fori_loop(0, 4, other, 0)
    lax.fori_loop(0, 4, ours, 0)
    sums.across()
    sums.beside()
    loads[1].wait()
    loads[2].wait()
    shard = gu_g.shape[1]

    def gu_block(t, carry):
        left = wide_a[:, :, pl.ds(pl.multiple_of(t * shard, shard), shard)].reshape(length, shard)
        right = wide_b[:, :, pl.ds(0, gul.shape[2])].reshape(length, gul.shape[2])
        gu_g[t] = tn(left, right).astype(jnp.bfloat16)
        return carry

    lax.fori_loop(0, 4, gu_block, 0)
    gu_z.start()
    loads[3].start()
    down_z.step1()
    sums.turn()
    lows.start()

    def finish_rows(part, down_sum):
        result[part, :] = (middle[part, :] + down_sum).astype(jnp.bfloat16)

    def sums_done():
        sums.total(finish_rows)
        sums.finish()
        for rank in (place.p, place.x, place.y):
            pl.semaphore_signal(free, inc=1, device_id={"ctx": rank}, device_id_type=MESH)

    downs = Gather(place, down_z.own(), down_all, down_cs)
    gus = Gather(place, gu_z.own(), gu_all, gu_cs)
    steps = Steps(
        sums_done, down_z.step2, lows.relay, lambda: (down_z.total(), gu_z.step1()), lows.rest,
        downs.start, downs.relay, lambda: (lows.partner(), downs.rest()),
    )
    scaling = HEAD_DIM ** (-0.5)
    mask = causal(2 * half)
    lane = lax.broadcasted_iota(jnp.int32, (half, LANES), 1)
    keys_t = k_ref[...].astype(jnp.float32).T.astype(jnp.bfloat16)
    for pair in reversed(range(pairs)):
        q = q_ref[pl.ds(pair * 4 * half, 4 * half), :]
        firsts, seconds = [], []
        for part in range(2):
            piece_of = agrad[block_of(2 * pair + part)].astype(jnp.float32)
            left = piece_of[:, 0:LANES]
            right = jnp.concatenate([piece_of[:, LANES : 2 * half], jnp.zeros((half, 64), jnp.float32)], axis=1)
            firsts.append(jnp.where(lane < half, left, 0.0))
            seconds.append(pltpu.roll(jnp.where(lane < half, right, left), LANES - half, 1))
        seconds = [jnp.where(lane < half, s, 0.0) for s in seconds]
        grads = jnp.concatenate(firsts + seconds, axis=0)
        delta = jnp.sum(grads.T * att_ref[pl.ds(pair * LANES, LANES), :], axis=0, keepdims=True)
        grads = grads.astype(jnp.bfloat16)
        before = pair * 2 * half
        cuts = [(before, 2 * half)] + [(at, min(768, before - at)) for at in range(0, before, 768)]
        dq_t = None
        for at, count in cuts:
            keys = pl.ds(at, count)
            weights = jnp.exp(nt(k_ref[keys, :], q) * scaling - lse_ref[pl.ds(pair, 1), :])
            if at == before:
                weights = jnp.where(mask, weights, 0.0)
            dp = nt(v_ref[keys, :], grads)
            ds = (weights * (dp - delta)).astype(jnp.bfloat16)
            dk = nn(ds, q) * scaling
            dv = nn(weights.astype(jnp.bfloat16), grads)
            if pair == pairs - 1:
                dk_ref[keys, :] = dk
                dv_ref[keys, :] = dv
            else:
                dk_ref[keys, :] += dk
                dv_ref[keys, :] += dv
            term = nn(keys_t[:, at : at + count], ds)
            dq_t = term if dq_t is None else dq_t + term
        dq = dq_t.T * scaling
        for part in range(2):
            cosine, sine = wave(turn_ref[2 * pair + part])
            for head in range(2):
                z = dq[(2 * head + part) * half : (2 * head + part + 1) * half]
                pg_sorted[2 * pair + part, :, head * LANES : (head + 1) * LANES] = (
                    z * cosine - pltpu.roll(z, 64, 1) * sine
                ).astype(jnp.bfloat16)
        steps.next()
    for s in range(2 * pairs):
        spot = pl.ds(s * half, half)
        cosine, sine = wave(turn_ref[s])
        z = dk_ref[spot, :]
        pg_sorted[s, :, 2 * LANES : 3 * LANES] = (z * cosine - pltpu.roll(z, 64, 1) * sine).astype(jnp.bfloat16)
        pg_sorted[s, :, 3 * LANES :] = dv_ref[spot, :].astype(jnp.bfloat16)
    for b in range(2 * pairs):
        pgrad[b // 2, pl.ds((b % 2) * half, half), :] = pg_sorted[span_of(b)]
    steps.rest()

    loads[3].wait()

    def qkv_block(t, carry):
        left = wide_a[:, :, pl.ds(pl.multiple_of(t * shard, shard), shard)].reshape(length, shard)
        qkv_g[t] = tn(left, pgrad[...].reshape(length, 4 * LANES)).astype(jnp.bfloat16)
        return carry

    lax.fori_loop(0, 4, qkv_block, 0)
    qkv_z.start()
    pl.semaphore_wait(free, 3)
    grads = Reduce(place, mine, theirs, first, out, second, reduce_sem)

    def push(k, carry):
        theirs[k] = nt(pgrad[flip(place, 2 * k + 1)], qkv_w[...].reshape(width, -1)).astype(jnp.bfloat16)
        grads.push(k)
        return carry

    def keep(k, carry):
        mine[k] = nt(pgrad[flip(place, 2 * k)], qkv_w[...].reshape(width, -1))
        return carry

    lax.fori_loop(0, 4, push, 0)
    lax.fori_loop(0, 4, keep, 0)
    grads.across()
    grads.beside()
    lows.keep.wait()
    for t in range(4):
        for side in range(2):
            src = 2 * t + side
            fetch = pltpu.make_async_copy(low_all.at[src], low_buf, local_sem.at[5 + src])
            fetch.start()
            fetch.wait()
            out_g[t, pl.ds(side * rows, rows), :] = tn(
                low_buf[...].reshape(length, rows), mcols[...].reshape(length, rows)
            ).astype(jnp.bfloat16)
    out_z.start()
    gu_z.step2()
    downs.partner()
    grads.turn()
    gain_sum[...] = jnp.zeros_like(gain_sum)
    loads[4].wait()

    def norm_back(part, normed_grad):
        x = tok[part, :].astype(jnp.float32)
        factor = lax.rsqrt(jnp.mean(x * x, axis=-1, keepdims=True) + epsilon)
        unit = x * factor
        gain_sum[...] += jnp.sum(normed_grad * unit, axis=0, keepdims=True)
        scaled = normed_grad * gain[...]
        inner = jnp.mean(scaled * unit, axis=-1, keepdims=True)
        grad[part, :] = grad[part, :] + factor * (scaled - unit * inner)

    grads.total(norm_back)
    gain_grad = gain_sum[...]
    count = mine_gain.shape[0] // 2
    for at in range(count):
        mine_gain[pl.ds(at, 1), :] = gain_grad[:, at * shard : (at + 1) * shard]
        mine_gain[pl.ds(count + at, 1), :] = ffn_gain[:, at * shard : (at + 1) * shard]
    ctx_sum = Share(place, mine_gain, ctx_gain, gain_sem)
    ctx_sum.start()
    qkv_z.step1()
    gu_z.total()
    gus.start()
    out_z.step1()
    ctx_sum.finish()
    plane_sum[...] = jnp.sum(ctx_gain[...], axis=0)
    planes = PlaneShare(place, plane_sum, plane_gain, plane_sem)
    planes.start()
    gus.relay()
    qkv_z.step2()
    gus.rest()
    out_z.step2()
    planes.finish()
    gains[...] = jnp.sum(plane_gain[...], axis=0)
    qkv_z.total()
    qkvs = Gather(place, qkv_z.own(), qkv_all, qkv_cs)
    qkvs.start()
    gus.partner()
    out_z.total()
    outs = Gather(place, out_z.own(), out_all, out_cs)
    qkvs.relay()
    outs.start()
    qkvs.rest()
    outs.relay()
    outs.rest()
    qkvs.partner()
    outs.partner()
    for move in (down_z, gu_z, out_z, qkv_z, downs, gus, outs, qkvs, grads):
        move.finish()
    lows.finish(kept=True)


def back_moves(early, hidden, agrad, mcols, low, q, k, v, att, lse, turns, qkv_w, down_w, tok, gain, ffn_gain, middle,
               second_all, gul, up_all, normed, middle_grad):
    n, planes = lax.axis_size("ctx"), lax.axis_size("fsdp")
    rows, width = tok.shape
    length = n * rows
    wide = hidden.shape[2]
    shard = width // planes
    bf, f32 = jnp.bfloat16, jnp.float32
    shape = jax.ShapeDtypeStruct
    dma = pltpu.SemaphoreType.DMA
    halves = pltpu.VMEM((6, rows // 2, width), bf)
    quads = pltpu.VMEM((4, rows, width), bf)
    small = (2 * planes, shard)
    parts = ((wide // planes, width), (shard, 2 * wide), (shard, rows), (shard, 4 * LANES))
    ring = dma((2, Gather.sems))
    return pl.pallas_call(
        back_moves_kernel,
        out_shape=(
            shape((rows, width), f32), shape((rows, width), bf), shape(small, f32), shape((n,) + low.shape, bf),
        ) + tuple(shape((n,) + part, bf) for part in parts),
        in_specs=[pl.BlockSpec(memory_space=pltpu.SMEM)] + vm(16) + anywhere(5),
        out_specs=vm(3) + anywhere(5),
        scratch_shapes=[pltpu.VMEM((n, rows, width), bf)] * 2 + [pltpu.VMEM(low.shape, bf)]
        + [pltpu.VMEM((planes,) + part, bf) for part in parts]
        + [pltpu.VMEM((planes + 1,) + part, bf) for part in parts]
        + [
            pltpu.VMEM((4, rows, width), f32), quads, quads, halves, halves,
            pltpu.VMEM((length, LANES), f32), pltpu.VMEM((length, LANES), f32),
            pltpu.VMEM((16, 96, 4 * LANES), bf), pltpu.VMEM((n, rows, 4 * LANES), bf),
            pltpu.VMEM((1, width), f32), pltpu.VMEM(small, f32), pltpu.VMEM((n,) + small, f32),
            pltpu.VMEM(small, f32), pltpu.VMEM((planes,) + small, f32),
            pltpu.SemaphoreType.REGULAR, dma((13,)), dma((2, Reduce.sems)), dma((2, Reduce.sems)), ring,
            dma((2, 5)), dma((2, 5)), dma((2, 5)), dma((2, 5)), ring, ring, ring, ring, dma((2, n)), dma((2, planes)),
        ],
        compiler_params=pltpu.CompilerParams(collective_id=6, has_side_effects=True, vmem_limit_bytes=67043328),
        name="back_moves",
    )(early, hidden, agrad, mcols, low, q, k, v, att, lse, turns, qkv_w, down_w, tok, gain, ffn_gain, middle,
      second_all, gul, up_all, normed, middle_grad)


def fast_body(
    tokens, positions, qkv_weight, out_weight, gate_up_weight, down_weight, attn_gain, ffn_gain, cotangent
):
    me = lax.axis_index("ctx")
    n = lax.axis_size("ctx")
    planes = lax.axis_size("fsdp")
    rows = tokens.shape[1]
    length = n * rows
    width = tokens.shape[2]
    wide = down_weight.shape[1] * planes
    own = wide // n
    piece = own // planes
    shard = qkv_weight.shape[1]
    query_width = HEADS * HEAD_DIM
    key_width = KV_HEADS * HEAD_DIM
    cut = lax.dynamic_slice_in_dim

    qkv = qkv_weight[0]
    q_part = cut(qkv, me * 2 * HEAD_DIM, 2 * HEAD_DIM, 1)
    k_part = cut(qkv, query_width + me * HEAD_DIM, HEAD_DIM, 1)
    v_part = cut(qkv, query_width + key_width + me * HEAD_DIM, HEAD_DIM, 1)
    half = HEAD_DIM // 2
    gap = jnp.zeros((shard, 64 - half), qkv.dtype)
    columns = []
    for part in (q_part[:, :HEAD_DIM], q_part[:, HEAD_DIM:], k_part):
        columns += [part[:, :half], gap, part[:, half:], gap]
    qkv_own = jnp.concatenate(columns + [v_part, gap, gap], axis=1)
    out_own = cut(out_weight[0], me * (shard // n), shard // n, 0)
    pieces = [cut(gate_up_weight[0], at * (wide // planes) + me * piece, piece, 2) for at in range(planes)]
    gate_up_own = jnp.concatenate([x[:, s] for s in range(2) for x in pieces], axis=1)
    down_own = cut(down_weight[0], me * piece, piece, 0)
    gains = jnp.concatenate([attn_gain, ffn_gain, jnp.zeros((6, shard), attn_gain.dtype)], axis=0).astype(jnp.float32)
    spot = jnp.full((8, LANES), positions[0, 0] // (rows // 2), jnp.int32)
    turns = table(length)
    (
        normed, upstream_all, second_all, hidden, gate_up_low, qkv_block, down_block, q, k, v, att, lse, low,
        middle_grad, middle, ffn_partial, spots, gains, attended_grad, middle_cols,
    ) = front_moves(
        tokens[0], cotangent[0].astype(jnp.bfloat16), spot, gains, qkv_own, out_own, gate_up_own, down_own,
        turns.reshape(2 * n, rows // 2, LANES), cotangent[0],
    )
    stream_grad, result, gain_grads, _, down_grad, gate_up_grad, out_grad, qkv_grad = back_moves(
        spots[:, 0, 0], hidden, attended_grad.reshape(2 * n, rows // 2, -1), middle_cols, low, q, k, v, att, lse,
        turns.reshape(2 * n, rows // 2, LANES), qkv_block, down_block, tokens[0], gains[0:1], ffn_partial, middle,
        second_all, gate_up_low, upstream_all, normed, middle_grad,
    )
    gain_grads = gain_grads.reshape(2, planes, shard)
    gain_grads = lax.dynamic_index_in_dim(gain_grads, lax.axis_index("fsdp"), 1, keepdims=False)
    pieces = qkv_grad.reshape(n, shard, 4, LANES).transpose(1, 0, 2, 3)
    qkv_grad = jnp.concatenate(
        [
            gathered_spread(pieces[:, :, 0:2]).reshape(shard, query_width),
            gathered_spread(pieces[:, :, 2]).reshape(shard, key_width),
            pieces[:, :, 3, :HEAD_DIM].reshape(shard, key_width),
        ],
        axis=1,
    ).astype(jnp.float32)
    out_grad = out_grad.transpose(1, 0, 2).reshape(shard, width).astype(jnp.float32)
    gate_up_grad = gate_up_grad.reshape(n, shard, 2, planes, -1).transpose(1, 2, 3, 0, 4)
    gate_up_grad = gate_up_grad.reshape(shard, 2, wide).astype(jnp.float32)
    down_grad = down_grad.reshape(-1, width).astype(jnp.float32)
    return (
        result[None],
        stream_grad[None],
        qkv_grad[None],
        out_grad[None],
        gate_up_grad[None],
        down_grad[None],
        gain_grads[0][None],
        gain_grads[1][None],
    )


def solution(mesh):
    split = mesh.shape["ctx"] == KV_HEADS and mesh.shape["fsdp"] == 4
    placed = (
        P("fsdp", "ctx", None),
        P("fsdp", "ctx"),
        P(None, "fsdp", None),
        P(None, "fsdp", None),
        P(None, "fsdp", None, None),
        P(None, "fsdp", None),
        P(None, "fsdp"),
        P(None, "fsdp"),
        P("fsdp", "ctx", None),
    )
    return jax.shard_map(
        fast_body if split else body,
        mesh=mesh,
        in_specs=placed,
        out_specs=(
            P("fsdp", "ctx", None),
            P("fsdp", "ctx", None),
            P(None, "fsdp", None),
            P(None, "fsdp", None),
            P(None, "fsdp", None, None),
            P(None, "fsdp", None),
            P(None, "fsdp"),
            P(None, "fsdp"),
        ),
        check_vma=False,
    )
```

```python
import functools
import jax
import jax.numpy as jnp
from jax import lax
from jax.experimental import pallas as pl
from jax.experimental.pallas import tpu as pltpu
from jax.sharding import PartitionSpec as P

HEADS = 16
KV_HEADS = 8
HEAD_DIM = 96
LAYERS = 1


epsilon = 1e-05
rope_base = 100000.0


def angles(place):
    halfway = HEAD_DIM // 2
    frequency = rope_base ** (-(jnp.arange(halfway, dtype=jnp.float32) * 2.0 / HEAD_DIM))
    phases = place.astype(jnp.float32)[:, None] * frequency[None, :]
    phases = jnp.concatenate([phases, phases], axis=-1)
    return (jnp.cos(phases)[:, None, :], jnp.sin(phases)[:, None, :])


def rotate(vectors, cosine, sine):
    halfway = vectors.shape[-1] // 2
    turned = jnp.concatenate([-vectors[..., halfway:], vectors[..., :halfway]], axis=-1)
    return vectors * cosine + turned * sine


def rotate_back(grads, cosine, sine):
    halfway = grads.shape[-1] // 2
    scaled = grads * sine
    return grads * cosine + jnp.concatenate(
        [scaled[..., halfway:], -scaled[..., :halfway]], axis=-1
    )


def normalize(rows, gain):
    factor = lax.rsqrt(jnp.mean(rows * rows, axis=-1, keepdims=True) + epsilon)
    return (rows * factor * gain, factor)


def normalize_back(upstream, rows, factor, gain):
    unit_rows = rows * factor
    gain_grad = jnp.sum(upstream * unit_rows, axis=0)
    scaled = upstream * gain
    row_inner = jnp.mean(scaled * unit_rows, axis=-1, keepdims=True)
    return (factor * (scaled - unit_rows * row_inner), gain_grad)


def split_blocks(queries, keys_all, values_all, key_place):
    rows = queries.shape[0]
    half = rows // 2
    shards = key_place.shape[0] // rows
    key_blocks = keys_all.reshape(shards, 2, half, KV_HEADS, HEAD_DIM)
    value_blocks = values_all.reshape(shards, 2, half, KV_HEADS, HEAD_DIM)
    place_blocks = key_place.reshape(shards, 2, half)
    return (key_blocks, value_blocks, place_blocks)


def scores_of(queries, key_block, place_block, query_place):
    scaling = HEAD_DIM ** (-0.5)
    scores = (
        jnp.einsum("rkgd,skd->kgrs", queries, key_block, preferred_element_type=jnp.float32)
        * scaling
    )
    allowed = place_block[None, None, None, :] <= query_place[None, None, :, None]
    return (scores, allowed)


def reachable(place_block, query_place):
    return jnp.min(place_block) <= jnp.max(query_place)


def attention_forward(queries, keys_all, values_all, query_place, key_place):
    key_blocks, value_blocks, place_blocks = split_blocks(queries, keys_all, values_all, key_place)
    rows = queries.shape[0]
    half = rows // 2
    groups = HEADS // KV_HEADS
    query_spans = queries.reshape(2, half, KV_HEADS, groups, HEAD_DIM)
    place_spans = query_place.reshape(2, half)

    def sweep_max(carry, inputs):
        key_block, place_block = inputs
        updated_all = []
        for span in range(2):
            state = carry[span]
            for part in range(2):

                def live(current, span=span, part=part):
                    maximum, total = current
                    scores, allowed = scores_of(
                        query_spans[span], key_block[part], place_block[part], place_spans[span]
                    )
                    masked = jnp.where(allowed, scores, -1e30)
                    updated = jnp.maximum(maximum, jnp.max(masked, axis=-1))
                    weights_now = jnp.where(allowed, jnp.exp(masked - updated[..., None]), 0.0)
                    return (
                        updated,
                        total * jnp.exp(maximum - updated) + jnp.sum(weights_now, axis=-1),
                    )

                state = lax.cond(
                    reachable(place_block[part], place_spans[span]),
                    live,
                    lambda current: current,
                    state,
                )
            updated_all.append(state)
        return (tuple(updated_all), None)

    start_max = jnp.full((KV_HEADS, groups, half), -1e30, jnp.float32)
    start_total = jnp.zeros((KV_HEADS, groups, half), jnp.float32)
    start = ((start_max, start_total), (start_max, start_total))
    finals, unused = lax.scan(sweep_max, start, (key_blocks, place_blocks))
    logsum_spans = [finals[span][0] + jnp.log(finals[span][1]) for span in range(2)]

    def sweep_out(results, inputs):
        key_block, value_block, place_block = inputs
        updated_all = []
        for span in range(2):
            result = results[span]
            for part in range(2):

                def live(current, span=span, part=part):
                    scores, allowed = scores_of(
                        query_spans[span], key_block[part], place_block[part], place_spans[span]
                    )
                    softmax_rows = jnp.where(
                        allowed, jnp.exp(scores - logsum_spans[span][..., None]), 0.0
                    ).astype(jnp.bfloat16)
                    return current + jnp.einsum(
                        "kgrs,skd->rkgd",
                        softmax_rows,
                        value_block[part],
                        preferred_element_type=jnp.float32,
                    )

                result = lax.cond(
                    reachable(place_block[part], place_spans[span]),
                    live,
                    lambda current: current,
                    result,
                )
            updated_all.append(result)
        return (tuple(updated_all), None)

    start_out = jnp.zeros((half, KV_HEADS, groups, HEAD_DIM), jnp.float32)
    outs, unused_out = lax.scan(
        sweep_out, (start_out, start_out), (key_blocks, value_blocks, place_blocks)
    )
    logsum = jnp.concatenate(logsum_spans, axis=-1)
    attended = jnp.concatenate([outs[0], outs[1]], axis=0)
    return (logsum, attended)


def attention_backward(
    queries, keys_all, values_all, query_place, key_place, logsum, attended_grad, row_inner
):
    key_blocks, value_blocks, place_blocks = split_blocks(queries, keys_all, values_all, key_place)
    rows = queries.shape[0]
    half = rows // 2
    groups = HEADS // KV_HEADS
    scaling = HEAD_DIM ** (-0.5)
    query_spans = queries.reshape(2, half, KV_HEADS, groups, HEAD_DIM)
    place_spans = query_place.reshape(2, half)
    grad_spans = attended_grad.reshape(2, half, KV_HEADS, groups, HEAD_DIM)
    logsum_spans = logsum.reshape(KV_HEADS, groups, 2, half)
    inner_spans = row_inner.reshape(KV_HEADS, groups, 2, half)

    def sweep_back(query_grads, inputs):
        key_block, value_block, place_block = inputs
        query_grads = list(query_grads)
        key_parts = []
        value_parts = []
        for part in range(2):
            key_acc = jnp.zeros((half, KV_HEADS, HEAD_DIM), jnp.float32)
            value_acc = jnp.zeros((half, KV_HEADS, HEAD_DIM), jnp.float32)
            for span in range(2):

                def live(current, span=span, part=part):
                    query_grad, key_grad, value_grad = current
                    scores, allowed = scores_of(
                        query_spans[span], key_block[part], place_block[part], place_spans[span]
                    )
                    softmax_rows = jnp.where(
                        allowed, jnp.exp(scores - logsum_spans[:, :, span][..., None]), 0.0
                    )
                    rounded = softmax_rows.astype(jnp.bfloat16)
                    weight_grad = jnp.einsum(
                        "rkgd,skd->kgrs",
                        grad_spans[span],
                        value_block[part],
                        preferred_element_type=jnp.float32,
                    )
                    score_grad = (
                        softmax_rows * (weight_grad - inner_spans[:, :, span][..., None])
                    ).astype(jnp.bfloat16)
                    query_grad = (
                        query_grad
                        + jnp.einsum(
                            "kgrs,skd->rkgd",
                            score_grad,
                            key_block[part],
                            preferred_element_type=jnp.float32,
                        )
                        * scaling
                    )
                    key_grad = (
                        key_grad
                        + jnp.einsum(
                            "kgrs,rkgd->skd",
                            score_grad,
                            query_spans[span],
                            preferred_element_type=jnp.float32,
                        )
                        * scaling
                    )
                    value_grad = value_grad + jnp.einsum(
                        "kgrs,rkgd->skd",
                        rounded,
                        grad_spans[span],
                        preferred_element_type=jnp.float32,
                    )
                    return (query_grad, key_grad, value_grad)

                state = (query_grads[span], key_acc, value_acc)
                state = lax.cond(
                    reachable(place_block[part], place_spans[span]),
                    live,
                    lambda current: current,
                    state,
                )
                query_grads[span], key_acc, value_acc = state
            key_parts.append(key_acc)
            value_parts.append(value_acc)
        key_out = jnp.concatenate(key_parts, axis=0)
        value_out = jnp.concatenate(value_parts, axis=0)
        return (tuple(query_grads), (key_out, value_out))

    start_grad = jnp.zeros((half, KV_HEADS, groups, HEAD_DIM), jnp.float32)
    query_pair, (key_grads, value_grads) = lax.scan(
        sweep_back, (start_grad, start_grad), (key_blocks, value_blocks, place_blocks)
    )
    query_grad = jnp.concatenate([query_pair[0], query_pair[1]], axis=0)
    return (
        query_grad,
        key_grads.reshape(-1, KV_HEADS, HEAD_DIM),
        value_grads.reshape(-1, KV_HEADS, HEAD_DIM),
    )


def fetch_layer(qkv_weight, out_weight, gate_up_weight, down_weight, attn_gain, ffn_gain, layer_id):
    return (
        lax.all_gather(qkv_weight[layer_id], "fsdp", axis=0, tiled=True),
        lax.all_gather(out_weight[layer_id], "fsdp", axis=0, tiled=True),
        lax.all_gather(gate_up_weight[layer_id], "fsdp", axis=0, tiled=True),
        lax.all_gather(down_weight[layer_id], "fsdp", axis=0, tiled=True),
        lax.all_gather(attn_gain[layer_id], "fsdp", axis=0, tiled=True),
        lax.all_gather(ffn_gain[layer_id], "fsdp", axis=0, tiled=True),
    )


def fetch_again(qkv_weight, out_weight, gate_up_weight, down_weight, attn_gain, ffn_gain, layer_id):
    return (
        lax.all_gather(qkv_weight[layer_id], "fsdp", axis=0, tiled=True),
        lax.all_gather(out_weight[layer_id], "fsdp", axis=0, tiled=True),
        lax.all_gather(gate_up_weight[layer_id], "fsdp", axis=0, tiled=True),
        lax.all_gather(down_weight[layer_id], "fsdp", axis=0, tiled=True),
        lax.all_gather(attn_gain[layer_id], "fsdp", axis=0, tiled=True),
        lax.all_gather(ffn_gain[layer_id], "fsdp", axis=0, tiled=True),
    )


def forward_layer(stream, query_place, key_place, gathered):
    qkv_full, out_full, gate_up_full, down_full, attn_full, ffn_full = gathered
    rows = stream.shape[0]
    groups = HEADS // KV_HEADS
    query_width = HEADS * HEAD_DIM
    key_width = KV_HEADS * HEAD_DIM
    cosine, sine = angles(query_place)
    normed, first_factor = normalize(stream, attn_full.astype(jnp.float32))
    normed = normed.astype(jnp.bfloat16)
    projected = jnp.dot(normed, qkv_full, preferred_element_type=jnp.float32)
    queries = rotate(projected[:, :query_width].reshape(rows, HEADS, HEAD_DIM), cosine, sine)
    queries = queries.reshape(rows, KV_HEADS, groups, HEAD_DIM).astype(jnp.bfloat16)
    keys_local = rotate(
        projected[:, query_width : query_width + key_width].reshape(rows, KV_HEADS, HEAD_DIM),
        cosine,
        sine,
    ).astype(jnp.bfloat16)
    values_local = (
        projected[:, query_width + key_width :]
        .reshape(rows, KV_HEADS, HEAD_DIM)
        .astype(jnp.bfloat16)
    )
    keys_all, values_all = (
        lax.all_gather(keys_local, "ctx", axis=0, tiled=True),
        lax.all_gather(values_local, "ctx", axis=0, tiled=True),
    )
    logsum, attended = attention_forward(queries, keys_all, values_all, query_place, key_place)
    attended_low = attended.reshape(rows, query_width).astype(jnp.bfloat16)
    middle = stream + jnp.dot(attended_low, out_full, preferred_element_type=jnp.float32)
    second, second_factor = normalize(middle, ffn_full.astype(jnp.float32))
    second = second.astype(jnp.bfloat16)
    gate_up = jnp.einsum("rd,dcf->rcf", second, gate_up_full, preferred_element_type=jnp.float32)
    hidden = (jax.nn.silu(gate_up[:, 0]) * gate_up[:, 1]).astype(jnp.bfloat16)
    result = middle + jnp.dot(hidden, down_full, preferred_element_type=jnp.float32)
    stored = (
        stream,
        first_factor,
        normed,
        queries,
        keys_local,
        values_local,
        keys_all,
        values_all,
        logsum,
        attended,
        attended_low,
        middle,
        second_factor,
        second,
        gate_up,
        hidden,
    )
    return (result, stored)


def backward_layer(upstream, stored, gathered, query_place, key_place, keys_all, values_all):
    (
        stream,
        first_factor,
        normed,
        queries,
        keys_local,
        values_local,
        kept_keys,
        kept_values,
        logsum,
        attended,
        attended_low,
        middle,
        second_factor,
        second,
        gate_up,
        hidden,
    ) = stored
    qkv_full, out_full, gate_up_full, down_full, attn_full, ffn_full = gathered
    rows = stream.shape[0]
    groups = HEADS // KV_HEADS
    cosine, sine = angles(query_place)
    upstream_low = upstream.astype(jnp.bfloat16)
    hidden_grad = jnp.einsum(
        "rd,fd->rf", upstream_low, down_full, preferred_element_type=jnp.float32
    )
    gate_part = gate_up[:, 0]
    up_part = gate_up[:, 1]
    sigmoid = jax.nn.sigmoid(gate_part)
    gate_grad = hidden_grad * up_part * sigmoid * (1.0 + gate_part * (1.0 - sigmoid))
    up_grad = hidden_grad * gate_part * sigmoid
    gate_up_low = jnp.stack([gate_grad, up_grad], axis=1).astype(jnp.bfloat16)
    second_grad = jnp.einsum(
        "rcf,dcf->rd", gate_up_low, gate_up_full, preferred_element_type=jnp.float32
    )
    middle_grad, ffn_gain_grad = normalize_back(
        second_grad, middle, second_factor, ffn_full.astype(jnp.float32)
    )
    middle_grad = middle_grad + upstream
    middle_low = middle_grad.astype(jnp.bfloat16)
    attended_grad = jnp.einsum(
        "rd,od->ro", middle_low, out_full, preferred_element_type=jnp.float32
    )
    attended_grad = attended_grad.astype(jnp.bfloat16).reshape(rows, KV_HEADS, groups, HEAD_DIM)
    row_inner = jnp.einsum("rkgd,rkgd->kgr", attended_grad.astype(jnp.float32), attended)
    query_grad, key_grads, value_grads = attention_backward(
        queries, keys_all, values_all, query_place, key_place, logsum, attended_grad, row_inner
    )
    key_grad, value_grad = (
        lax.psum_scatter(key_grads, "ctx", scatter_dimension=0, tiled=True),
        lax.psum_scatter(value_grads, "ctx", scatter_dimension=0, tiled=True),
    )
    query_grad = rotate_back(query_grad.reshape(rows, HEADS, HEAD_DIM), cosine, sine)
    key_grad = rotate_back(key_grad, cosine, sine)
    projected_grad = jnp.concatenate(
        [query_grad.reshape(rows, -1), key_grad.reshape(rows, -1), value_grad.reshape(rows, -1)],
        axis=1,
    ).astype(jnp.bfloat16)
    normed_grad = jnp.einsum(
        "re,de->rd", projected_grad, qkv_full, preferred_element_type=jnp.float32
    )
    stream_grad, attn_gain_grad = normalize_back(
        normed_grad, stream, first_factor, attn_full.astype(jnp.float32)
    )
    stream_grad = stream_grad + middle_grad
    qkv_grad = jnp.einsum("rd,re->de", normed, projected_grad, preferred_element_type=jnp.float32)
    out_grad = jnp.einsum("ro,rd->od", attended_low, middle_low, preferred_element_type=jnp.float32)
    gate_up_grad = jnp.einsum(
        "rd,rcf->dcf", second, gate_up_low, preferred_element_type=jnp.float32
    )
    down_grad = jnp.einsum("rf,rd->fd", hidden, upstream_low, preferred_element_type=jnp.float32)
    sharded = (
        lax.psum_scatter(qkv_grad, "fsdp", scatter_dimension=0, tiled=True),
        lax.psum_scatter(out_grad, "fsdp", scatter_dimension=0, tiled=True),
        lax.psum_scatter(gate_up_grad, "fsdp", scatter_dimension=0, tiled=True),
        lax.psum_scatter(down_grad, "fsdp", scatter_dimension=0, tiled=True),
        lax.psum_scatter(attn_gain_grad, "fsdp", scatter_dimension=0, tiled=True),
        lax.psum_scatter(ffn_gain_grad, "fsdp", scatter_dimension=0, tiled=True),
    )
    totals = lax.psum(
        (sharded[0], sharded[1], sharded[2], sharded[3], sharded[4], sharded[5]), "ctx"
    )
    return (stream_grad, totals)


def body(
    tokens,
    positions,
    qkv_weight,
    out_weight,
    gate_up_weight,
    down_weight,
    attn_gain,
    ffn_gain,
    cotangent,
):
    query_place = positions[0]
    key_place = lax.all_gather(query_place, "ctx", axis=0, tiled=True)
    stream = tokens[0].astype(jnp.float32)
    gathered_list = []
    layer_id = 0
    gathered = fetch_layer(
        qkv_weight, out_weight, gate_up_weight, down_weight, attn_gain, ffn_gain, layer_id
    )
    stream, stored = forward_layer(stream, query_place, key_place, gathered)
    saved = [stored]
    gathered_list.append(gathered)
    activations = stream.astype(jnp.bfloat16)[None]
    upstream = cotangent[0]
    layer_grads = [None] * LAYERS
    for layer_id in reversed(range(LAYERS)):
        stored = saved[layer_id]
        gathered = fetch_again(
            qkv_weight, out_weight, gate_up_weight, down_weight, attn_gain, ffn_gain, layer_id
        )
        keys_all, values_all = (stored[6], stored[7])
        upstream, totals = backward_layer(
            upstream, stored, gathered, query_place, key_place, keys_all, values_all
        )
        layer_grads[layer_id] = totals
    outputs = [jnp.stack([entry[slot] for entry in layer_grads], axis=0) for slot in range(6)]
    return (
        activations,
        upstream[None],
        outputs[0],
        outputs[1],
        outputs[2],
        outputs[3],
        outputs[4],
        outputs[5],
    )


LANES = 128


def spread(heads):
    half = HEAD_DIM // 2
    pad = ((0, 0), (0, 0), (0, 64 - half))
    return jnp.concatenate([jnp.pad(heads[..., :half], pad), jnp.pad(heads[..., half:], pad)], axis=-1)


def gathered_spread(padded):
    half = HEAD_DIM // 2
    return jnp.concatenate([padded[..., :half], padded[..., 64 : 64 + half]], axis=-1)


def table(length):
    half = HEAD_DIM // 2
    frequency = rope_base ** (-(jnp.arange(half, dtype=jnp.float32) * 2.0 / HEAD_DIM))
    phases = jnp.arange(length, dtype=jnp.float32)[:, None] * frequency[None, :]
    pad = ((0, 0), (0, 64 - half))
    return jnp.concatenate([jnp.pad(jnp.cos(phases), pad), jnp.pad(jnp.sin(phases), pad)], axis=1)


def wave(rows):
    first = lax.broadcasted_iota(jnp.int32, rows.shape, 1) < 64
    other = pltpu.roll(rows, 64, 1)
    return jnp.where(first, rows, other), jnp.where(first, -other, rows)


def nt(left, right):
    return lax.dot_general(left, right, (((1,), (1,)), ((), ())), preferred_element_type=jnp.float32)


def nn(left, right):
    return lax.dot_general(left, right, (((1,), (0,)), ((), ())), preferred_element_type=jnp.float32)


def tn(left, right):
    return lax.dot_general(left, right, (((0,), (0,)), ((), ())), preferred_element_type=jnp.float32)


def causal(width):
    key_at = lax.broadcasted_iota(jnp.int32, (width, 2 * width), 0)
    query_at = lax.broadcasted_iota(jnp.int32, (width, 2 * width), 1)
    query_at = jnp.where(query_at >= width, query_at - width, query_at)
    return key_at <= query_at


def vm(count):
    return [pl.BlockSpec(memory_space=pltpu.VMEM)] * count


MESH = pl.DeviceIdType.MESH


class Place:
    def __init__(self):
        self.me = lax.axis_index("ctx")
        core, x, y = self.me % 2, (self.me // 2) % 2, self.me // 4
        self.dp, self.dx, self.dy = 1 - 2 * core, 2 - 4 * x, 4 - 8 * y
        self.p, self.x, self.y = self.me + self.dp, self.me + self.dx, self.me + self.dy
        self.d = self.x + self.dy
        self.z = lax.axis_index("fsdp")
        self.planes = lax.axis_size("fsdp")
        self.n = lax.axis_size("ctx")


def greet(place, ctx=True, planes=False):
    barrier = pltpu.get_barrier_semaphore()
    count = 0
    if ctx:
        for step in range(1, place.n):
            pl.semaphore_signal(
                barrier, inc=1, device_id={"ctx": lax.rem(place.me + step, place.n)}, device_id_type=MESH
            )
            count += 1
    if planes:
        for step in range(1, place.planes):
            pl.semaphore_signal(
                barrier, inc=1, device_id={"fsdp": lax.rem(place.z + step, place.planes)}, device_id_type=MESH
            )
            count += 1
    pl.semaphore_wait(barrier, count)


def send(source, target, send_sem, recv_sem, **where):
    return pltpu.make_async_remote_copy(
        src_ref=source, dst_ref=target, send_sem=send_sem, recv_sem=recv_sem,
        device_id=where, device_id_type=MESH,
    )


class Gather:
    sems = 14

    def __init__(self, place, own, out, sem):
        self.place, self.own, self.out, self.sem = place, own, out, sem
        self.half = out.shape[1] // 2
        self.started = []
        self.met = False

    def go(self, source, target, index, rank):
        copy = send(source, target, self.sem.at[0, index], self.sem.at[1, index], ctx=rank)
        copy.start()
        self.started.append(copy)

    def part(self, rank, half):
        return self.out.at[rank, pl.ds(half * self.half, self.half)]

    def whole(self, rank):
        return self.out.at[rank]

    def start(self):
        p = self.place
        keep = pltpu.make_async_copy(self.own, self.whole(p.me), self.sem.at[0, 13])
        keep.start()
        self.keep = keep
        halves = [self.own.at[pl.ds(h * self.half, self.half)] for h in range(2)]
        self.go(halves[0], self.part(p.me, 0), 0, p.x)
        self.go(halves[1], self.part(p.me, 1), 3, p.y)
        self.go(self.own, self.whole(p.me), 6, p.p)
        self.go(halves[1], self.part(p.me, 1), 1, p.x)
        self.go(halves[0], self.part(p.me, 0), 2, p.y)

    def arrived(self, rank, half, index):
        part = self.part(rank, half)
        pltpu.make_async_copy(part, part, self.sem.at[1, index]).wait()
        return part

    def relay(self):
        p = self.place
        part = self.arrived(p.x, 0, 0)
        self.go(part, part, 4, p.y)
        self.go(part, part, 7, p.p)
        part = self.arrived(p.y, 1, 3)
        self.go(part, part, 5, p.x)
        self.go(part, part, 10, p.p)

    def rest(self):
        p = self.place
        for rank, half, index, onward in ((p.x, 1, 1, 8), (p.y, 0, 2, 9), (p.d, 0, 4, 11), (p.d, 1, 5, 12)):
            part = self.arrived(rank, half, index)
            self.go(part, part, onward, p.p)

    def first_partner(self):
        part = self.whole(self.place.p)
        pltpu.make_async_copy(part, part, self.sem.at[1, 6]).wait()
        self.met = True

    def partner(self):
        p = self.place
        if not self.met:
            self.first_partner()
        for rank, half, index in (
            (p.x, 0, 7), (p.y, 1, 10), (p.x, 1, 8), (p.y, 0, 9), (p.d, 0, 11), (p.d, 1, 12),
        ):
            self.arrived(rank + p.dp, half, index)

    def finish(self, kept=False):
        if not kept:
            self.keep.wait()
        for copy in self.started:
            copy.wait_send()


class PlaneGather:
    def __init__(self, place, own, out, sem):
        self.place, self.own, self.out, self.sem = place, own, out, sem

    def hop(self, step, up):
        p = self.place
        sign = 1 if up else -1
        source = p.z - sign * step
        target = p.z + sign
        ok = jnp.logical_and(
            jnp.logical_and(source >= 0, source < p.planes),
            jnp.logical_and(target >= 0, target < p.planes),
        )
        source = jnp.clip(source, 0, p.planes - 1)
        target = jnp.clip(target, 0, p.planes - 1)
        block = self.own if step == 0 else self.out.at[source]
        return ok, send(
            block, self.out.at[source], self.sem.at[0 if up else 1, source], self.sem.at[2, source], fsdp=target
        )

    def start(self):
        p = self.place
        self.keep = pltpu.make_async_copy(self.own, self.out.at[p.z], self.sem.at[2, p.z])
        self.keep.start()
        for up in (True, False):
            ok, copy = self.hop(0, up)
            pl.when(ok)(copy.start)

    def got(self, step, up):
        p = self.place
        source = p.z - step if up else p.z + step
        ok = jnp.logical_and(source >= 0, source < p.planes)
        source = jnp.clip(source, 0, p.planes - 1)
        part = self.out.at[source]
        return ok, pltpu.make_async_copy(part, part, self.sem.at[2, source])

    def step(self, number):
        for up in (True, False):
            ok, copy = self.got(number, up)
            pl.when(ok)(copy.wait)
            if number < self.place.planes - 1:
                ok, copy = self.hop(number, up)
                pl.when(ok)(copy.start)

    def finish(self, kept=False):
        if not kept:
            self.keep.wait()
        for number in range(self.place.planes - 1):
            for up in (True, False):
                ok, copy = self.hop(number, up)
                pl.when(ok)(copy.wait_send)


class Exchange:
    def __init__(self, place, blocks, out, sem):
        self.place, self.blocks, self.out, self.sem = place, blocks, out, sem

    def pick(self, rank):
        return self.blocks.at[rank]

    def copy(self, step):
        p = self.place
        rank = lax.rem(p.me + step, p.n)
        return send(self.pick(rank), self.out.at[p.me], self.sem.at[0, step], self.sem.at[1, step], ctx=rank)

    def start(self):
        p = self.place
        for step in range(1, p.n):
            self.copy(step).start()
        self.keep = pltpu.make_async_copy(self.pick(p.me), self.out.at[p.me], self.sem.at[0, 0])
        self.keep.start()

    def finish(self):
        p = self.place
        self.keep.wait()
        for step in range(1, p.n):
            self.copy(step).wait_send()
        for step in range(1, p.n):
            part = self.out.at[lax.rem(p.me + p.n - step, p.n)]
            pltpu.make_async_copy(part, part, self.sem.at[1, step]).wait()


class Share(Exchange):
    def pick(self, rank):
        return self.blocks


class PlaneShare:
    def __init__(self, place, block, out, sem):
        self.place, self.block, self.out, self.sem = place, block, out, sem

    def copy(self, step):
        p = self.place
        plane = lax.rem(p.z + step, p.planes)
        return send(self.block, self.out.at[p.z], self.sem.at[0, step], self.sem.at[1, step], fsdp=plane)

    def start(self):
        p = self.place
        for step in range(1, p.planes):
            self.copy(step).start()
        self.keep = pltpu.make_async_copy(self.block, self.out.at[p.z], self.sem.at[0, 0])
        self.keep.start()

    def finish(self):
        p = self.place
        self.keep.wait()
        for step in range(1, p.planes):
            self.copy(step).wait_send()
        for step in range(1, p.planes):
            part = self.out.at[lax.rem(p.z + p.planes - step, p.planes)]
            pltpu.make_async_copy(part, part, self.sem.at[1, step]).wait()


def anywhere(count):
    return [pl.BlockSpec(memory_space=pl.ANY)] * count


class Reduce:
    sems = 10

    def __init__(self, place, mine, theirs, first, out, second, sem):
        self.place, self.mine, self.theirs, self.first, self.out, self.second, self.sem = (
            place, mine, theirs, first, out, second, sem
        )
        self.half = out.shape[1]
        self.started = []

    def push(self, slot):
        copy = send(
            self.theirs.at[slot], self.first.at[slot], self.sem.at[0, slot], self.sem.at[1, slot], ctx=self.place.p
        )
        copy.start()
        return copy

    def pushed(self):
        for slot in range(4):
            send(
                self.theirs.at[slot], self.first.at[slot], self.sem.at[0, slot], self.sem.at[1, slot],
                ctx=self.place.p,
            ).wait_send()

    def add(self, slot):
        part = self.first.at[slot]
        pltpu.make_async_copy(part, part, self.sem.at[1, slot]).wait()
        self.mine[slot] = self.mine[slot] + self.first[slot].astype(jnp.float32)

    def go(self, index, value, rank):
        self.out[index] = value.astype(jnp.bfloat16)
        copy = send(
            self.out.at[index], self.second.at[index], self.sem.at[0, 4 + index], self.sem.at[1, 4 + index], ctx=rank
        )
        copy.start()
        self.started.append(copy)

    def top(self, slot):
        return self.mine[slot, pl.ds(0, self.half), :]

    def low(self, slot):
        return self.mine[slot, pl.ds(self.half, self.half), :]

    def got(self, index):
        part = self.second.at[index]
        pltpu.make_async_copy(part, part, self.sem.at[1, 4 + index]).wait()
        return self.second[index].astype(jnp.float32)

    def across(self):
        self.add(3)
        self.go(1, self.top(3), self.place.x)
        self.go(3, self.low(3), self.place.y)

    def beside(self):
        self.add(1)
        self.go(0, self.top(1), self.place.x)
        self.add(2)
        self.go(2, self.low(2), self.place.y)

    def turn(self):
        self.go(4, self.top(2) + self.got(1), self.place.y)
        self.go(5, self.low(1) + self.got(3), self.place.x)

    def total(self, use):
        self.add(0)
        use(pl.ds(0, self.half), self.top(0) + self.got(0) + self.got(4))
        use(pl.ds(self.half, self.half), self.low(0) + self.got(2) + self.got(5))

    def finish(self):
        self.pushed()
        for copy in self.started:
            copy.wait_send()


def flip(place, i):
    return place.me + (i % 2) * place.dp + ((i // 2) % 2) * place.dx + (i // 4) * place.dy


class Steps:
    def __init__(self, *steps):
        self.steps = list(steps)

    def next(self, count=1):
        for step in self.steps[:count]:
            step()
        self.steps = self.steps[count:]

    def rest(self):
        self.next(len(self.steps))


class OutGather(Gather):
    def __init__(self, place, own, out, sem):
        self.place, self.own, self.out, self.sem = place, own, out, sem
        self.half = out.shape[0] // 2
        self.started = []
        self.met = False

    def part(self, rank, half):
        return self.out.at[pl.ds(half * self.half, self.half), rank]

    def whole(self, rank):
        return self.out.at[:, rank]


def front_kernel(
    tok, up_low, spot, gain_own, qkv_own, out_own, gu_own, down_own, turn_ref, up,
    normed, up_all, second_all, hidden, gul, qkv_w, down_w, q_ref, k_ref, v_ref, att_ref, lse_ref, low,
    middle_grad, middle, gain_grad, spots, gains, agrad, mcols,
    gu_w, out_block, out_w, qr, kr, vr, low_sorted, gain_all, spots_s,
    attended, mcols_send, own, mine, theirs, first, out, second,
    tok_sem, up_sem, spot_sem, gain_sem, qkv_sem, out_sem, outc_sem, gu_sem, down_sem, local_sem,
    low_sem, gather_sem, reduce_sem, agrad_sem, mcols_sem,
):
    place = Place()
    n = place.n
    rows = tok.shape[0]
    half = rows // 2
    pairs = 8
    heads = rows
    greet(place, planes=True)
    spans = Share(place, spot, spots, spot_sem)
    scales = PlaneShare(place, gain_own, gain_all, gain_sem)
    tokens = Gather(place, tok, normed, tok_sem)
    cots = Gather(place, up_low, up_all, up_sem)
    qkvs = PlaneGather(place, qkv_own, qkv_w, qkv_sem)
    outs = PlaneGather(place, out_own, out_block, out_sem)
    outc = OutGather(place, out_block, out_w, outc_sem)
    gus = PlaneGather(place, gu_own, gu_w, gu_sem)
    downs = PlaneGather(place, down_own, down_w, down_sem)
    fetch = pltpu.make_async_copy(up, middle_grad, local_sem.at[0])
    fetch.start()
    spans.start()
    scales.start()
    qkvs.start()
    tokens.start()
    tokens.relay()
    qkvs.step(1)
    outs.start()
    qkvs.step(2)
    downs.start()
    tokens.rest()
    qkvs.step(3)
    cots.start()
    tokens.partner()
    tokens.finish()
    spans.finish()
    scales.finish()
    qkvs.keep.wait()
    table = pltpu.make_async_copy(spots, spots_s, local_sem.at[1])
    table.start()
    for g in range(2):
        gains[pl.ds(g, 1), :] = jnp.concatenate([gain_all[z, pl.ds(g, 1), :] for z in range(4)], axis=1)
    table.wait()
    early = [spots_s[j, 0, 0] for j in range(pairs)]
    holder = []
    for t in range(pairs):
        at = 0
        for j in range(pairs):
            at = jnp.where(early[j] == t, j, at)
        holder.append(at)

    def block_of(s):
        return 2 * holder[s] if s < pairs else 2 * holder[2 * pairs - 1 - s] + 1

    def span_of(b):
        return early[b // 2] if b % 2 == 0 else 2 * pairs - 1 - early[b // 2]

    def project(j, carry):
        x = normed[pl.ds(2 * j, 2)].reshape(2 * rows, -1).astype(jnp.float32)
        factor = lax.rsqrt(jnp.mean(x * x, axis=-1, keepdims=True) + epsilon)
        scaled = (x * factor * gains[pl.ds(0, 1), :]).astype(jnp.bfloat16)
        normed[pl.ds(2 * j, 2)] = scaled.reshape(2, rows, -1)
        proj = nn(scaled, qkv_w[...].reshape(-1, 4 * LANES))
        for piece in range(4):
            c = spots_s[2 * j + piece // 2, 0, 0]
            cosine, sine = wave(turn_ref[c if piece % 2 == 0 else 2 * pairs - 1 - c])
            mine_rows = proj[piece * half : (piece + 1) * half]

            def turned(part):
                z = mine_rows[:, part * LANES : (part + 1) * LANES]
                return (z * cosine + pltpu.roll(z, 64, 1) * sine).astype(jnp.bfloat16)

            qr[4 * j + piece, 0] = turned(0)
            qr[4 * j + piece, 1] = turned(1)
            kr[4 * j + piece] = turned(2)
            vr[4 * j + piece] = mine_rows[:, 3 * LANES :].astype(jnp.bfloat16)
        return carry

    lax.fori_loop(0, 4, project, 0)
    for s in range(2 * pairs):
        b = block_of(s)
        base = (s // 2) * 4 * half + (s % 2) * half
        both = qr[b]
        q_ref[pl.ds(base, half), :] = both[0]
        q_ref[pl.ds(base + 2 * half, half), :] = both[1]
        k_ref[pl.ds(s * half, half), :] = kr[b]
        v_ref[pl.ds(s * half, half), :] = vr[b]

    steps = Steps(
        lambda: outs.step(1), cots.relay, lambda: outs.step(2), lambda: outs.step(3),
        lambda: (outs.keep.wait(), outc.start(), downs.step(1), gus.start()), cots.rest, outc.relay,
        lambda: (downs.step(2), outc.rest()), lambda: (cots.partner(), outc.partner()),
    )
    scaling = HEAD_DIM ** (-0.5)
    mask = causal(2 * half)
    lane = lax.broadcasted_iota(jnp.int32, (half, LANES), 1)
    values_t = v_ref[...].astype(jnp.float32).T.astype(jnp.bfloat16)
    for pair in range(pairs):
        width = (pair + 1) * 2 * half
        q = q_ref[pl.ds(pair * 4 * half, 4 * half), :]
        before = width - 2 * half
        parts = [jnp.where(mask, nt(k_ref[pl.ds(before, 2 * half), :], q) * scaling, -1e30)]
        if pair:
            parts.append(nt(k_ref[pl.ds(0, before), :], q) * scaling)
        tops = [jnp.max(part, axis=0, keepdims=True) for part in parts]
        top = jnp.maximum(tops[0], tops[-1])
        parts = [jnp.exp(part - top) for part in parts]
        total = sum(jnp.sum(part, axis=0, keepdims=True) for part in parts)
        parts = [(part * (1.0 / total)).astype(jnp.bfloat16) for part in parts]
        lse_ref[pl.ds(pair, 1), :] = top + jnp.log(total)
        out_t = nn(values_t[:, before:width], parts[0])
        if pair:
            out_t = out_t + nn(values_t[:, :before], parts[1])
        att_ref[pl.ds(pair * LANES, LANES), :] = out_t
        result = out_t.T.astype(jnp.bfloat16).astype(jnp.float32)
        for part in range(2):
            left = result[part * half : (part + 1) * half]
            right = pltpu.roll(result[(2 + part) * half : (3 + part) * half], half, 1)
            low_sorted[2 * pair + part, :, 0:LANES] = jnp.where(lane < half, left, right).astype(jnp.bfloat16)
            low_sorted[2 * pair + part, :, LANES : 2 * half] = right[:, : 2 * half - LANES].astype(jnp.bfloat16)
        steps.next()
    for b in range(2 * pairs):
        low[b // 2, pl.ds((b % 2) * half, half), :] = low_sorted[span_of(b)]
    moved = Exchange(place, low, attended, low_sem)
    moved.start()
    steps.rest()
    outc.keep.wait()
    moved.finish()
    total = tok[...].astype(jnp.float32)
    for q in range(8):
        total = total + nn(attended[q], out_w[q // 2, pl.ds(4 * (q % 2), 4)].reshape(heads, -1))
    middle[...] = total
    factor = lax.rsqrt(jnp.mean(total * total, axis=-1, keepdims=True) + epsilon)
    own[...] = (total * factor * gains[pl.ds(1, 1), :]).astype(jnp.bfloat16)
    seconds = Gather(place, own, second_all, gather_sem)
    seconds.start()
    downs.step(3)
    gus.step(1)
    seconds.relay()
    gus.step(2)
    seconds.rest()
    gus.step(3)
    seconds.partner()
    gus.keep.wait()
    downs.keep.wait()
    seconds.keep.wait()
    cots.keep.wait()
    grads = Reduce(place, mine, theirs, first, out, second, reduce_sem)
    wide = hidden.shape[2]

    def block(i):
        rank = flip(place, i)
        gate_up = nn(second_all[rank], gu_w[...].reshape(-1, 2 * wide))
        gate, raised = gate_up[:, :wide], gate_up[:, wide:]
        sigmoid = 1.0 / (1.0 + jnp.exp(-gate))
        silu = gate * sigmoid
        hidden[rank] = (silu * raised).astype(jnp.bfloat16)
        hidden_grad = nt(up_all[rank], down_w[...].reshape(wide, -1))
        gul[rank, :, pl.ds(0, wide)] = (hidden_grad * raised * sigmoid * (1.0 + gate * (1.0 - sigmoid))).astype(jnp.bfloat16)
        gul[rank, :, pl.ds(wide, wide)] = (hidden_grad * silu).astype(jnp.bfloat16)
        return nt(gul[rank], gu_w[...].reshape(-1, 2 * wide))

    def pair_of(k, carry):
        theirs[k] = block(2 * k + 1).astype(jnp.bfloat16)
        grads.push(k)
        mine[k] = block(2 * k)
        return carry

    lax.fori_loop(1, 4, pair_of, 0)
    grads.across()
    grads.beside()
    lax.fori_loop(0, 1, pair_of, 0)
    grads.turn()
    fetch.wait()
    seconds.finish(kept=True)
    gain_grad[...] = jnp.zeros_like(gain_grad)

    def norm_back(part, second_grad):
        x = middle[part, :]
        factor = lax.rsqrt(jnp.mean(x * x, axis=-1, keepdims=True) + epsilon)
        unit = x * factor
        gain_grad[...] += jnp.sum(second_grad * unit, axis=0, keepdims=True)
        scaled = second_grad * gains[pl.ds(1, 1), :]
        inner = jnp.mean(scaled * unit, axis=-1, keepdims=True)
        grad = middle_grad[part, :] + factor * (scaled - unit * inner)
        middle_grad[part, :] = grad
        own[part, :] = grad.astype(jnp.bfloat16)

    grads.total(norm_back)

    def head_grads(q, carry):
        weight = out_w[q // 2, pl.ds(4 * (q % 2), 4)].reshape(heads, -1)
        attended[q] = nt(own[...], weight).astype(jnp.bfloat16)
        return carry

    lax.fori_loop(0, n, head_grads, 0)
    heads_back = Exchange(place, attended, agrad, agrad_sem)
    heads_back.start()
    for q in range(8):
        mcols_send[q] = own[:, q * heads : (q + 1) * heads]
    columns = Exchange(place, mcols_send, mcols, mcols_sem)
    columns.start()
    for move in (qkvs, outs, gus, downs):
        move.finish(kept=True)
    for move in (cots, outc):
        move.finish(kept=True)
    heads_back.finish()
    columns.finish()
    grads.finish()


def front_moves(tok, up_low, spot, gain_own, qkv_own, out_own, gu_own, down_own, turns, up):
    n, planes = lax.axis_size("ctx"), lax.axis_size("fsdp")
    rows, width = tok.shape
    length = n * rows
    wide = planes * down_own.shape[0]
    bf, f32 = jnp.bfloat16, jnp.float32
    shape = jax.ShapeDtypeStruct
    dma = pltpu.SemaphoreType.DMA
    pairs = length // 192
    halves = pltpu.VMEM((6, rows // 2, width), bf)
    quads = pltpu.VMEM((4, rows, width), bf)
    blocks = pltpu.VMEM((n, rows, rows), bf)
    all_of = lambda x: shape((planes,) + x.shape, x.dtype)
    gathered = lambda x: pltpu.VMEM((planes,) + x.shape, x.dtype)
    ring = dma((2, Gather.sems))
    line = dma((3, planes))
    swap = dma((2, n))
    return pl.pallas_call(
        front_kernel,
        out_shape=(
            shape((n, rows, width), bf), shape((n, rows, width), bf), shape((n, rows, width), bf),
            shape((n, rows, wide), bf), shape((n, rows, 2 * wide), bf), all_of(qkv_own), all_of(down_own),
            shape((2 * length, LANES), bf), shape((length, LANES), bf), shape((length, LANES), bf),
            shape((pairs * LANES, 384), f32), shape((pairs, 384), f32), shape((n, rows, rows), bf),
            shape((rows, width), f32), shape((rows, width), f32), shape((1, width), f32), shape((n,) + spot.shape, spot.dtype),
            shape((2, width), f32), shape((n, rows, rows), bf), shape((n, rows, rows), bf),
        ),
        in_specs=vm(9) + anywhere(1),
        out_specs=vm(18) + anywhere(2),
        scratch_shapes=[
            gathered(gu_own), gathered(out_own), pltpu.VMEM((planes, n) + out_own.shape, bf),
            pltpu.VMEM((16, 2, 96, LANES), bf), pltpu.VMEM((16, 96, LANES), bf), pltpu.VMEM((16, 96, LANES), bf),
            pltpu.VMEM((16, 96, 192), bf), gathered(gain_own), pltpu.SMEM((n,) + spot.shape, jnp.int32),
            blocks, blocks, pltpu.VMEM((rows, width), bf),
            pltpu.VMEM((4, rows, width), f32), quads, quads, halves, halves,
            ring, ring, swap, dma((2, planes)), line, line, ring, line, line, dma((2,)),
            swap, ring, dma((2, Reduce.sems)), swap, swap,
        ],
        compiler_params=pltpu.CompilerParams(collective_id=1, has_side_effects=True, vmem_limit_bytes=67043328),
        name="front_moves",
    )(tok, up_low, spot, gain_own, qkv_own, out_own, gu_own, down_own, turns, up)


class PlaneReduce:
    def __init__(self, place, block, recv, sem):
        self.place, self.block, self.recv, self.sem = place, block, recv, sem

    def hop(self, ok, part, slot, target, first, wait):
        copy = send(
            self.block.at[part], self.recv.at[slot], self.sem.at[0, part], self.sem.at[1, slot], fsdp=target
        )

        @pl.when(ok)
        def _():
            if wait:
                copy.wait_send()
                return
            if not first:
                self.merge(part, part)
            copy.start()

    def merge(self, part, slot):
        piece = self.recv.at[slot]
        pltpu.make_async_copy(piece, piece, self.sem.at[1, slot]).wait()
        total = self.block[part].astype(jnp.float32) + self.recv[slot].astype(jnp.float32)
        self.block[part] = total.astype(jnp.bfloat16)

    def ends(self, i, wait=False):
        z = self.place.z
        low = z == 0
        part = jnp.where(low, 3 - i, i)
        slot = part if i < 2 else jnp.where(low, part, 4)
        self.hop(jnp.logical_or(low, z == 3), part, slot, jnp.where(low, 1, 2), True, wait)

    def inner(self, up, down, slot_up, slot_down, to_up, to_down, wait=False):
        z = self.place.z
        low = z == 1
        part = jnp.where(low, up, down)
        slot = jnp.where(low, slot_up, slot_down)
        self.hop(jnp.logical_or(low, z == 2), part, slot, jnp.where(low, to_up, to_down), False, wait)

    def start(self, wait=False):
        for i in range(3):
            self.ends(i, wait)

    def step1(self, wait=False):
        self.inner(3, 0, 3, 0, 2, 1, wait)

    def step2(self, wait=False):
        self.inner(2, 1, 2, 4, 2, 1, wait)
        self.inner(0, 3, 4, 3, 0, 3, wait)

    def total(self):
        z = self.place.z

        @pl.when(z > 0)
        def _():
            self.merge(z, z)

        @pl.when(z < 3)
        def _():
            self.merge(z, 4)

    def own(self):
        return self.block.at[self.place.z]

    def finish(self):
        self.start(True)
        self.step1(True)
        self.step2(True)


def back_moves_kernel(
    early_ref, hidden, agrad, mcols, low, q_ref, k_ref, v_ref, att_ref, lse_ref, turn_ref, qkv_w, down_w, tok, gain,
    ffn_gain, middle, second_all, gul, up_all, normed, middle_grad,
    grad, result, gains, low_all, down_all, gu_all, out_all, qkv_all,
    wide_a, wide_b, low_buf, down_g, gu_g, out_g, qkv_g, down_r, gu_r, out_r, qkv_r,
    mine, theirs, first, out, second, dk_ref, dv_ref, pg_sorted, pgrad,
    gain_sum, mine_gain, ctx_gain, plane_sum, plane_gain,
    free, local_sem, sum_sem, reduce_sem, low_sem, down_zs, gu_zs, out_zs, qkv_zs, down_cs, gu_cs, out_cs, qkv_cs,
    gain_sem, plane_sem,
):
    place = Place()
    n = place.n
    rows = tok.shape[0]
    half = rows // 2
    pairs = 8
    width = tok.shape[1]
    length = n * rows
    loads = [
        pltpu.make_async_copy(source, target, local_sem.at[at])
        for at, (source, target) in enumerate((
            (up_all, wide_b), (second_all, wide_a), (gul, wide_b.at[:, :, pl.ds(0, gul.shape[2])]),
            (normed, wide_a), (middle_grad, grad),
        ))
    ]
    loads[0].start()
    loads[1].start()
    loads[4].start()
    greet(place, planes=True)
    early = [early_ref[j] for j in range(pairs)]
    holder = []
    for t in range(pairs):
        at = 0
        for j in range(pairs):
            at = jnp.where(early[j] == t, j, at)
        holder.append(at)

    def block_of(s):
        return 2 * holder[s] if s < pairs else 2 * holder[2 * pairs - 1 - s] + 1

    def span_of(b):
        return early[b // 2] if b % 2 == 0 else 2 * pairs - 1 - early[b // 2]

    down_z = PlaneReduce(place, down_g, down_r, down_zs)
    gu_z = PlaneReduce(place, gu_g, gu_r, gu_zs)
    out_z = PlaneReduce(place, out_g, out_r, out_zs)
    qkv_z = PlaneReduce(place, qkv_g, qkv_r, qkv_zs)
    sums = Reduce(place, mine, theirs, first, out, second, sum_sem)
    lows = Gather(place, low, low_all, low_sem)

    loads[0].wait()
    piece = down_g.shape[1]

    def down_block(t, carry):
        left = hidden[:, :, pl.ds(pl.multiple_of(t * piece, piece), piece)].reshape(length, piece)
        down_g[t] = tn(left, wide_b[...].reshape(length, width)).astype(jnp.bfloat16)
        return carry

    lax.fori_loop(0, 4, down_block, 0)
    down_z.start()
    loads[2].start()

    def other(k, carry):
        theirs[k] = nn(hidden[flip(place, 2 * k + 1)], down_w[...].reshape(-1, width)).astype(jnp.bfloat16)
        sums.push(k)
        return carry

    def ours(k, carry):
        mine[k] = nn(hidden[flip(place, 2 * k)], down_w[...].reshape(-1, width))
        return carry

    lax.fori_loop(0, 4, other, 0)
    lax.fori_loop(0, 4, ours, 0)
    sums.across()
    sums.beside()
    loads[1].wait()
    loads[2].wait()
    shard = gu_g.shape[1]

    def gu_block(t, carry):
        left = wide_a[:, :, pl.ds(pl.multiple_of(t * shard, shard), shard)].reshape(length, shard)
        right = wide_b[:, :, pl.ds(0, gul.shape[2])].reshape(length, gul.shape[2])
        gu_g[t] = tn(left, right).astype(jnp.bfloat16)
        return carry

    lax.fori_loop(0, 4, gu_block, 0)
    gu_z.start()
    loads[3].start()
    down_z.step1()
    sums.turn()
    lows.start()

    def finish_rows(part, down_sum):
        result[part, :] = (middle[part, :] + down_sum).astype(jnp.bfloat16)

    def sums_done():
        sums.total(finish_rows)
        sums.finish()
        for rank in (place.p, place.x, place.y):
            pl.semaphore_signal(free, inc=1, device_id={"ctx": rank}, device_id_type=MESH)

    downs = Gather(place, down_z.own(), down_all, down_cs)
    gus = Gather(place, gu_z.own(), gu_all, gu_cs)
    steps = Steps(
        sums_done, down_z.step2, lows.relay, lambda: (down_z.total(), gu_z.step1()), lows.rest,
        downs.start, downs.relay, lambda: (lows.partner(), downs.rest()),
    )
    scaling = HEAD_DIM ** (-0.5)
    mask = causal(2 * half)
    lane = lax.broadcasted_iota(jnp.int32, (half, LANES), 1)
    keys_t = k_ref[...].astype(jnp.float32).T.astype(jnp.bfloat16)
    for pair in reversed(range(pairs)):
        q = q_ref[pl.ds(pair * 4 * half, 4 * half), :]
        firsts, seconds = [], []
        for part in range(2):
            piece_of = agrad[block_of(2 * pair + part)].astype(jnp.float32)
            left = piece_of[:, 0:LANES]
            right = jnp.concatenate([piece_of[:, LANES : 2 * half], jnp.zeros((half, 64), jnp.float32)], axis=1)
            firsts.append(jnp.where(lane < half, left, 0.0))
            seconds.append(pltpu.roll(jnp.where(lane < half, right, left), LANES - half, 1))
        seconds = [jnp.where(lane < half, s, 0.0) for s in seconds]
        grads = jnp.concatenate(firsts + seconds, axis=0)
        delta = jnp.sum(grads.T * att_ref[pl.ds(pair * LANES, LANES), :], axis=0, keepdims=True)
        grads = grads.astype(jnp.bfloat16)
        before = pair * 2 * half
        cuts = [(before, 2 * half)] + [(at, min(768, before - at)) for at in range(0, before, 768)]
        dq_t = None
        for at, count in cuts:
            keys = pl.ds(at, count)
            weights = jnp.exp(nt(k_ref[keys, :], q) * scaling - lse_ref[pl.ds(pair, 1), :])
            if at == before:
                weights = jnp.where(mask, weights, 0.0)
            dp = nt(v_ref[keys, :], grads)
            ds = (weights * (dp - delta)).astype(jnp.bfloat16)
            dk = nn(ds, q) * scaling
            dv = nn(weights.astype(jnp.bfloat16), grads)
            if pair == pairs - 1:
                dk_ref[keys, :] = dk
                dv_ref[keys, :] = dv
            else:
                dk_ref[keys, :] += dk
                dv_ref[keys, :] += dv
            term = nn(keys_t[:, at : at + count], ds)
            dq_t = term if dq_t is None else dq_t + term
        dq = dq_t.T * scaling
        for part in range(2):
            cosine, sine = wave(turn_ref[2 * pair + part])
            for head in range(2):
                z = dq[(2 * head + part) * half : (2 * head + part + 1) * half]
                pg_sorted[2 * pair + part, :, head * LANES : (head + 1) * LANES] = (
                    z * cosine - pltpu.roll(z, 64, 1) * sine
                ).astype(jnp.bfloat16)
        steps.next()
    for s in range(2 * pairs):
        spot = pl.ds(s * half, half)
        cosine, sine = wave(turn_ref[s])
        z = dk_ref[spot, :]
        pg_sorted[s, :, 2 * LANES : 3 * LANES] = (z * cosine - pltpu.roll(z, 64, 1) * sine).astype(jnp.bfloat16)
        pg_sorted[s, :, 3 * LANES :] = dv_ref[spot, :].astype(jnp.bfloat16)
    for b in range(2 * pairs):
        pgrad[b // 2, pl.ds((b % 2) * half, half), :] = pg_sorted[span_of(b)]
    steps.rest()

    loads[3].wait()

    def qkv_block(t, carry):
        left = wide_a[:, :, pl.ds(pl.multiple_of(t * shard, shard), shard)].reshape(length, shard)
        qkv_g[t] = tn(left, pgrad[...].reshape(length, 4 * LANES)).astype(jnp.bfloat16)
        return carry

    lax.fori_loop(0, 4, qkv_block, 0)
    qkv_z.start()
    pl.semaphore_wait(free, 3)
    grads = Reduce(place, mine, theirs, first, out, second, reduce_sem)

    def push(k, carry):
        theirs[k] = nt(pgrad[flip(place, 2 * k + 1)], qkv_w[...].reshape(width, -1)).astype(jnp.bfloat16)
        grads.push(k)
        return carry

    def keep(k, carry):
        mine[k] = nt(pgrad[flip(place, 2 * k)], qkv_w[...].reshape(width, -1))
        return carry

    lax.fori_loop(0, 4, push, 0)
    lax.fori_loop(0, 4, keep, 0)
    grads.across()
    grads.beside()
    lows.keep.wait()
    for t in range(4):
        for side in range(2):
            src = 2 * t + side
            fetch = pltpu.make_async_copy(low_all.at[src], low_buf, local_sem.at[5 + src])
            fetch.start()
            fetch.wait()
            out_g[t, pl.ds(side * rows, rows), :] = tn(
                low_buf[...].reshape(length, rows), mcols[...].reshape(length, rows)
            ).astype(jnp.bfloat16)
    out_z.start()
    gu_z.step2()
    downs.partner()
    grads.turn()
    gain_sum[...] = jnp.zeros_like(gain_sum)
    loads[4].wait()

    def norm_back(part, normed_grad):
        x = tok[part, :].astype(jnp.float32)
        factor = lax.rsqrt(jnp.mean(x * x, axis=-1, keepdims=True) + epsilon)
        unit = x * factor
        gain_sum[...] += jnp.sum(normed_grad * unit, axis=0, keepdims=True)
        scaled = normed_grad * gain[...]
        inner = jnp.mean(scaled * unit, axis=-1, keepdims=True)
        grad[part, :] = grad[part, :] + factor * (scaled - unit * inner)

    grads.total(norm_back)
    gain_grad = gain_sum[...]
    count = mine_gain.shape[0] // 2
    for at in range(count):
        mine_gain[pl.ds(at, 1), :] = gain_grad[:, at * shard : (at + 1) * shard]
        mine_gain[pl.ds(count + at, 1), :] = ffn_gain[:, at * shard : (at + 1) * shard]
    ctx_sum = Share(place, mine_gain, ctx_gain, gain_sem)
    ctx_sum.start()
    qkv_z.step1()
    gu_z.total()
    gus.start()
    out_z.step1()
    ctx_sum.finish()
    plane_sum[...] = jnp.sum(ctx_gain[...], axis=0)
    planes = PlaneShare(place, plane_sum, plane_gain, plane_sem)
    planes.start()
    gus.relay()
    qkv_z.step2()
    gus.rest()
    out_z.step2()
    planes.finish()
    gains[...] = jnp.sum(plane_gain[...], axis=0)
    qkv_z.total()
    qkvs = Gather(place, qkv_z.own(), qkv_all, qkv_cs)
    qkvs.start()
    gus.partner()
    out_z.total()
    outs = Gather(place, out_z.own(), out_all, out_cs)
    qkvs.relay()
    outs.start()
    qkvs.rest()
    outs.relay()
    outs.rest()
    qkvs.partner()
    outs.partner()
    for move in (down_z, gu_z, out_z, qkv_z, downs, gus, outs, qkvs, grads):
        move.finish()
    lows.finish(kept=True)


def back_moves(early, hidden, agrad, mcols, low, q, k, v, att, lse, turns, qkv_w, down_w, tok, gain, ffn_gain, middle,
               second_all, gul, up_all, normed, middle_grad):
    n, planes = lax.axis_size("ctx"), lax.axis_size("fsdp")
    rows, width = tok.shape
    length = n * rows
    wide = hidden.shape[2]
    shard = width // planes
    bf, f32 = jnp.bfloat16, jnp.float32
    shape = jax.ShapeDtypeStruct
    dma = pltpu.SemaphoreType.DMA
    halves = pltpu.VMEM((6, rows // 2, width), bf)
    quads = pltpu.VMEM((4, rows, width), bf)
    small = (2 * planes, shard)
    parts = ((wide // planes, width), (shard, 2 * wide), (shard, rows), (shard, 4 * LANES))
    ring = dma((2, Gather.sems))
    return pl.pallas_call(
        back_moves_kernel,
        out_shape=(
            shape((rows, width), f32), shape((rows, width), bf), shape(small, f32), shape((n,) + low.shape, bf),
        ) + tuple(shape((n,) + part, bf) for part in parts),
        in_specs=[pl.BlockSpec(memory_space=pltpu.SMEM)] + vm(16) + anywhere(5),
        out_specs=vm(3) + anywhere(5),
        scratch_shapes=[pltpu.VMEM((n, rows, width), bf)] * 2 + [pltpu.VMEM(low.shape, bf)]
        + [pltpu.VMEM((planes,) + part, bf) for part in parts]
        + [pltpu.VMEM((planes + 1,) + part, bf) for part in parts]
        + [
            pltpu.VMEM((4, rows, width), f32), quads, quads, halves, halves,
            pltpu.VMEM((length, LANES), f32), pltpu.VMEM((length, LANES), f32),
            pltpu.VMEM((16, 96, 4 * LANES), bf), pltpu.VMEM((n, rows, 4 * LANES), bf),
            pltpu.VMEM((1, width), f32), pltpu.VMEM(small, f32), pltpu.VMEM((n,) + small, f32),
            pltpu.VMEM(small, f32), pltpu.VMEM((planes,) + small, f32),
            pltpu.SemaphoreType.REGULAR, dma((13,)), dma((2, Reduce.sems)), dma((2, Reduce.sems)), ring,
            dma((2, 5)), dma((2, 5)), dma((2, 5)), dma((2, 5)), ring, ring, ring, ring, dma((2, n)), dma((2, planes)),
        ],
        compiler_params=pltpu.CompilerParams(collective_id=6, has_side_effects=True, vmem_limit_bytes=67043328),
        name="back_moves",
    )(early, hidden, agrad, mcols, low, q, k, v, att, lse, turns, qkv_w, down_w, tok, gain, ffn_gain, middle,
      second_all, gul, up_all, normed, middle_grad)


def pack_kernel(down, gu, out, qkv, grad, result, down_o, gu_o, out_o, qkv_o, grad_o, result_o):
    devices, rows = gu.shape[0], gu.shape[1]
    f32 = jnp.float32
    lane = lax.broadcasted_iota(jnp.int32, (rows, LANES), 1)
    half = HEAD_DIM // 2
    down_o[...] = down[0].astype(f32)
    grad_o[...] = grad[...]
    result_o[...] = result[...]
    tiles = gu_o.shape[0] // rows
    spans = gu.shape[2] // (2 * LANES)
    for c in range(devices):
        for s in range(2):
            for z in range(spans):
                piece = gu[c, :, (s * spans + z) * LANES : (s * spans + z + 1) * LANES].astype(f32)
                gu_o[pl.ds((z * devices + c) * 2 + s, rows, stride=tiles), :] = piece

    def head(c, at, halves):
        x = qkv[c, :, at * LANES : (at + 1) * LANES].astype(f32)
        return jnp.where(lane < half, x, pltpu.roll(x, LANES - 64 + half, 1)) if halves else x

    def store(at, heads):
        second, third, fourth = pltpu.roll(heads[1], 96, 1), pltpu.roll(heads[2], 64, 1), pltpu.roll(heads[3], 32, 1)
        qkv_o[:, at : at + LANES] = jnp.where(lane < 96, heads[0], second)
        qkv_o[:, at + LANES : at + 2 * LANES] = jnp.where(lane < 64, second, third)
        qkv_o[:, at + 2 * LANES : at + 3 * LANES] = jnp.where(lane < 32, third, fourth)

    for c in range(0, devices, 2):
        store(c * 192, [head(c + i // 2, i % 2, True) for i in range(4)])
    for c in range(0, devices, 4):
        store(HEADS * HEAD_DIM + c * 96, [head(c + i, 2, True) for i in range(4)])
        store((HEADS + KV_HEADS) * HEAD_DIM + c * 96, [head(c + i, 3, False) for i in range(4)])
    for c in range(0, devices, 2):
        at = c * 192
        first = out[c].astype(f32)
        second = out[c + 1].astype(f32)
        tail = jnp.concatenate([first[:, LANES:], jnp.zeros((rows, 64), f32)], axis=1)
        next_tail = jnp.concatenate([second[:, LANES:], jnp.zeros((rows, 64), f32)], axis=1)
        turned = pltpu.roll(second[:, :LANES], 64, 1)
        out_o[:, at : at + LANES] = first[:, :LANES]
        out_o[:, at + LANES : at + 2 * LANES] = jnp.where(lane < 64, tail, turned)
        out_o[:, at + 2 * LANES : at + 3 * LANES] = jnp.where(lane < 64, turned, pltpu.roll(next_tail, 64, 1))


def pack(down, gu, out, qkv, grad, result):
    n, shard = gu.shape[0], gu.shape[1]
    rows = shard // n
    width = down.shape[2]
    f32 = jnp.float32
    spec = pl.BlockSpec
    shape = jax.ShapeDtypeStruct
    tiles = n * gu.shape[2] // LANES
    quarter = grad.shape[0] // 4
    return pl.pallas_call(
        pack_kernel,
        grid=(n,),
        out_shape=(
            shape((n * down.shape[1], width), f32), shape((shard * tiles, LANES), f32), shape((shard, n * out.shape[2]), f32),
            shape((shard, (HEADS + 2 * KV_HEADS) * HEAD_DIM), f32), shape(grad.shape, f32), shape(result.shape, result.dtype),
        ),
        in_specs=[
            spec((1,) + down.shape[1:], lambda i: (i, 0, 0)), spec((n, rows, gu.shape[2]), lambda i: (0, i, 0)),
            spec((n, rows, out.shape[2]), lambda i: (0, i, 0)), spec((n, rows, qkv.shape[2]), lambda i: (0, i, 0)),
            spec((quarter, width), lambda i: (i // 2, 0)), spec((quarter, width), lambda i: (i // 2, 0)),
        ],
        out_specs=[
            spec((down.shape[1], width), lambda i: (i, 0)), spec((rows * tiles, LANES), lambda i: (i, 0)),
            spec((rows, n * out.shape[2]), lambda i: (i, 0)), spec((rows, (HEADS + 2 * KV_HEADS) * HEAD_DIM), lambda i: (i, 0)),
            spec((quarter, width), lambda i: (i // 2, 0)), spec((quarter, width), lambda i: (i // 2, 0)),
        ],
        name="pack",
    )(down, gu, out, qkv, grad, result)


def fast_body(
    tokens, positions, qkv_weight, out_weight, gate_up_weight, down_weight, attn_gain, ffn_gain, cotangent
):
    me = lax.axis_index("ctx")
    n = lax.axis_size("ctx")
    planes = lax.axis_size("fsdp")
    rows = tokens.shape[1]
    length = n * rows
    width = tokens.shape[2]
    wide = down_weight.shape[1] * planes
    own = wide // n
    piece = own // planes
    shard = qkv_weight.shape[1]
    query_width = HEADS * HEAD_DIM
    key_width = KV_HEADS * HEAD_DIM
    cut = lax.dynamic_slice_in_dim

    qkv = qkv_weight[0]
    q_part = cut(qkv, me * 2 * HEAD_DIM, 2 * HEAD_DIM, 1)
    k_part = cut(qkv, query_width + me * HEAD_DIM, HEAD_DIM, 1)
    v_part = cut(qkv, query_width + key_width + me * HEAD_DIM, HEAD_DIM, 1)
    half = HEAD_DIM // 2
    gap = jnp.zeros((shard, 64 - half), qkv.dtype)
    columns = []
    for part in (q_part[:, :HEAD_DIM], q_part[:, HEAD_DIM:], k_part):
        columns += [part[:, :half], gap, part[:, half:], gap]
    qkv_own = jnp.concatenate(columns + [v_part, gap, gap], axis=1)
    out_own = cut(out_weight[0], me * (shard // n), shard // n, 0)
    pieces = [cut(gate_up_weight[0], at * (wide // planes) + me * piece, piece, 2) for at in range(planes)]
    gate_up_own = jnp.concatenate([x[:, s] for s in range(2) for x in pieces], axis=1)
    down_own = cut(down_weight[0], me * piece, piece, 0)
    gains = jnp.concatenate([attn_gain, ffn_gain, jnp.zeros((6, shard), attn_gain.dtype)], axis=0).astype(jnp.float32)
    spot = jnp.full((8, LANES), positions[0, 0] // (rows // 2), jnp.int32)
    turns = table(length)
    (
        normed, upstream_all, second_all, hidden, gate_up_low, qkv_block, down_block, q, k, v, att, lse, low,
        middle_grad, middle, ffn_partial, spots, gains, attended_grad, middle_cols,
    ) = front_moves(
        tokens[0], cotangent[0].astype(jnp.bfloat16), spot, gains, qkv_own, out_own, gate_up_own, down_own,
        turns.reshape(2 * n, rows // 2, LANES), cotangent[0],
    )
    stream_grad, result, gain_grads, _, down_grad, gate_up_grad, out_grad, qkv_grad = back_moves(
        spots[:, 0, 0], hidden, attended_grad.reshape(2 * n, rows // 2, -1), middle_cols, low, q, k, v, att, lse,
        turns.reshape(2 * n, rows // 2, LANES), qkv_block, down_block, tokens[0], gains[0:1], ffn_partial, middle,
        second_all, gate_up_low, upstream_all, normed, middle_grad,
    )
    gain_grads = gain_grads.reshape(2, planes, shard)
    gain_grads = lax.dynamic_index_in_dim(gain_grads, lax.axis_index("fsdp"), 1, keepdims=False)
    down_grad, gate_up_grad, out_grad, qkv_grad, stream_grad, result = pack(
        down_grad, gate_up_grad, out_grad, qkv_grad, stream_grad, result
    )
    gate_up_grad = gate_up_grad.reshape(shard, wide // LANES, 2, LANES).transpose(0, 2, 1, 3).reshape(shard, 2, wide)
    return (
        result[None],
        stream_grad[None],
        qkv_grad[None],
        out_grad[None],
        gate_up_grad[None],
        down_grad[None],
        gain_grads[0][None],
        gain_grads[1][None],
    )


def solution(mesh):
    split = mesh.shape["ctx"] == KV_HEADS and mesh.shape["fsdp"] == 4
    placed = (
        P("fsdp", "ctx", None),
        P("fsdp", "ctx"),
        P(None, "fsdp", None),
        P(None, "fsdp", None),
        P(None, "fsdp", None, None),
        P(None, "fsdp", None),
        P(None, "fsdp"),
        P(None, "fsdp"),
        P("fsdp", "ctx", None),
    )
    return jax.shard_map(
        fast_body if split else body,
        mesh=mesh,
        in_specs=placed,
        out_specs=(
            P("fsdp", "ctx", None),
            P("fsdp", "ctx", None),
            P(None, "fsdp", None),
            P(None, "fsdp", None),
            P(None, "fsdp", None, None),
            P(None, "fsdp", None),
            P(None, "fsdp"),
            P(None, "fsdp"),
        ),
        check_vma=False,
    )
```

```python
import functools
import jax
import jax.numpy as jnp
from jax import lax
from jax.experimental import pallas as pl
from jax.experimental.pallas import tpu as pltpu
from jax.sharding import PartitionSpec as P

HEADS = 16
KV_HEADS = 8
HEAD_DIM = 96
LAYERS = 1


epsilon = 1e-05
rope_base = 100000.0


def angles(place):
    halfway = HEAD_DIM // 2
    frequency = rope_base ** (-(jnp.arange(halfway, dtype=jnp.float32) * 2.0 / HEAD_DIM))
    phases = place.astype(jnp.float32)[:, None] * frequency[None, :]
    phases = jnp.concatenate([phases, phases], axis=-1)
    return (jnp.cos(phases)[:, None, :], jnp.sin(phases)[:, None, :])


def rotate(vectors, cosine, sine):
    halfway = vectors.shape[-1] // 2
    turned = jnp.concatenate([-vectors[..., halfway:], vectors[..., :halfway]], axis=-1)
    return vectors * cosine + turned * sine


def rotate_back(grads, cosine, sine):
    halfway = grads.shape[-1] // 2
    scaled = grads * sine
    return grads * cosine + jnp.concatenate(
        [scaled[..., halfway:], -scaled[..., :halfway]], axis=-1
    )


def normalize(rows, gain):
    factor = lax.rsqrt(jnp.mean(rows * rows, axis=-1, keepdims=True) + epsilon)
    return (rows * factor * gain, factor)


def normalize_back(upstream, rows, factor, gain):
    unit_rows = rows * factor
    gain_grad = jnp.sum(upstream * unit_rows, axis=0)
    scaled = upstream * gain
    row_inner = jnp.mean(scaled * unit_rows, axis=-1, keepdims=True)
    return (factor * (scaled - unit_rows * row_inner), gain_grad)


def split_blocks(queries, keys_all, values_all, key_place):
    rows = queries.shape[0]
    half = rows // 2
    shards = key_place.shape[0] // rows
    key_blocks = keys_all.reshape(shards, 2, half, KV_HEADS, HEAD_DIM)
    value_blocks = values_all.reshape(shards, 2, half, KV_HEADS, HEAD_DIM)
    place_blocks = key_place.reshape(shards, 2, half)
    return (key_blocks, value_blocks, place_blocks)


def scores_of(queries, key_block, place_block, query_place):
    scaling = HEAD_DIM ** (-0.5)
    scores = (
        jnp.einsum("rkgd,skd->kgrs", queries, key_block, preferred_element_type=jnp.float32)
        * scaling
    )
    allowed = place_block[None, None, None, :] <= query_place[None, None, :, None]
    return (scores, allowed)


def reachable(place_block, query_place):
    return jnp.min(place_block) <= jnp.max(query_place)


def attention_forward(queries, keys_all, values_all, query_place, key_place):
    key_blocks, value_blocks, place_blocks = split_blocks(queries, keys_all, values_all, key_place)
    rows = queries.shape[0]
    half = rows // 2
    groups = HEADS // KV_HEADS
    query_spans = queries.reshape(2, half, KV_HEADS, groups, HEAD_DIM)
    place_spans = query_place.reshape(2, half)

    def sweep_max(carry, inputs):
        key_block, place_block = inputs
        updated_all = []
        for span in range(2):
            state = carry[span]
            for part in range(2):

                def live(current, span=span, part=part):
                    maximum, total = current
                    scores, allowed = scores_of(
                        query_spans[span], key_block[part], place_block[part], place_spans[span]
                    )
                    masked = jnp.where(allowed, scores, -1e30)
                    updated = jnp.maximum(maximum, jnp.max(masked, axis=-1))
                    weights_now = jnp.where(allowed, jnp.exp(masked - updated[..., None]), 0.0)
                    return (
                        updated,
                        total * jnp.exp(maximum - updated) + jnp.sum(weights_now, axis=-1),
                    )

                state = lax.cond(
                    reachable(place_block[part], place_spans[span]),
                    live,
                    lambda current: current,
                    state,
                )
            updated_all.append(state)
        return (tuple(updated_all), None)

    start_max = jnp.full((KV_HEADS, groups, half), -1e30, jnp.float32)
    start_total = jnp.zeros((KV_HEADS, groups, half), jnp.float32)
    start = ((start_max, start_total), (start_max, start_total))
    finals, unused = lax.scan(sweep_max, start, (key_blocks, place_blocks))
    logsum_spans = [finals[span][0] + jnp.log(finals[span][1]) for span in range(2)]

    def sweep_out(results, inputs):
        key_block, value_block, place_block = inputs
        updated_all = []
        for span in range(2):
            result = results[span]
            for part in range(2):

                def live(current, span=span, part=part):
                    scores, allowed = scores_of(
                        query_spans[span], key_block[part], place_block[part], place_spans[span]
                    )
                    softmax_rows = jnp.where(
                        allowed, jnp.exp(scores - logsum_spans[span][..., None]), 0.0
                    ).astype(jnp.bfloat16)
                    return current + jnp.einsum(
                        "kgrs,skd->rkgd",
                        softmax_rows,
                        value_block[part],
                        preferred_element_type=jnp.float32,
                    )

                result = lax.cond(
                    reachable(place_block[part], place_spans[span]),
                    live,
                    lambda current: current,
                    result,
                )
            updated_all.append(result)
        return (tuple(updated_all), None)

    start_out = jnp.zeros((half, KV_HEADS, groups, HEAD_DIM), jnp.float32)
    outs, unused_out = lax.scan(
        sweep_out, (start_out, start_out), (key_blocks, value_blocks, place_blocks)
    )
    logsum = jnp.concatenate(logsum_spans, axis=-1)
    attended = jnp.concatenate([outs[0], outs[1]], axis=0)
    return (logsum, attended)


def attention_backward(
    queries, keys_all, values_all, query_place, key_place, logsum, attended_grad, row_inner
):
    key_blocks, value_blocks, place_blocks = split_blocks(queries, keys_all, values_all, key_place)
    rows = queries.shape[0]
    half = rows // 2
    groups = HEADS // KV_HEADS
    scaling = HEAD_DIM ** (-0.5)
    query_spans = queries.reshape(2, half, KV_HEADS, groups, HEAD_DIM)
    place_spans = query_place.reshape(2, half)
    grad_spans = attended_grad.reshape(2, half, KV_HEADS, groups, HEAD_DIM)
    logsum_spans = logsum.reshape(KV_HEADS, groups, 2, half)
    inner_spans = row_inner.reshape(KV_HEADS, groups, 2, half)

    def sweep_back(query_grads, inputs):
        key_block, value_block, place_block = inputs
        query_grads = list(query_grads)
        key_parts = []
        value_parts = []
        for part in range(2):
            key_acc = jnp.zeros((half, KV_HEADS, HEAD_DIM), jnp.float32)
            value_acc = jnp.zeros((half, KV_HEADS, HEAD_DIM), jnp.float32)
            for span in range(2):

                def live(current, span=span, part=part):
                    query_grad, key_grad, value_grad = current
                    scores, allowed = scores_of(
                        query_spans[span], key_block[part], place_block[part], place_spans[span]
                    )
                    softmax_rows = jnp.where(
                        allowed, jnp.exp(scores - logsum_spans[:, :, span][..., None]), 0.0
                    )
                    rounded = softmax_rows.astype(jnp.bfloat16)
                    weight_grad = jnp.einsum(
                        "rkgd,skd->kgrs",
                        grad_spans[span],
                        value_block[part],
                        preferred_element_type=jnp.float32,
                    )
                    score_grad = (
                        softmax_rows * (weight_grad - inner_spans[:, :, span][..., None])
                    ).astype(jnp.bfloat16)
                    query_grad = (
                        query_grad
                        + jnp.einsum(
                            "kgrs,skd->rkgd",
                            score_grad,
                            key_block[part],
                            preferred_element_type=jnp.float32,
                        )
                        * scaling
                    )
                    key_grad = (
                        key_grad
                        + jnp.einsum(
                            "kgrs,rkgd->skd",
                            score_grad,
                            query_spans[span],
                            preferred_element_type=jnp.float32,
                        )
                        * scaling
                    )
                    value_grad = value_grad + jnp.einsum(
                        "kgrs,rkgd->skd",
                        rounded,
                        grad_spans[span],
                        preferred_element_type=jnp.float32,
                    )
                    return (query_grad, key_grad, value_grad)

                state = (query_grads[span], key_acc, value_acc)
                state = lax.cond(
                    reachable(place_block[part], place_spans[span]),
                    live,
                    lambda current: current,
                    state,
                )
                query_grads[span], key_acc, value_acc = state
            key_parts.append(key_acc)
            value_parts.append(value_acc)
        key_out = jnp.concatenate(key_parts, axis=0)
        value_out = jnp.concatenate(value_parts, axis=0)
        return (tuple(query_grads), (key_out, value_out))

    start_grad = jnp.zeros((half, KV_HEADS, groups, HEAD_DIM), jnp.float32)
    query_pair, (key_grads, value_grads) = lax.scan(
        sweep_back, (start_grad, start_grad), (key_blocks, value_blocks, place_blocks)
    )
    query_grad = jnp.concatenate([query_pair[0], query_pair[1]], axis=0)
    return (
        query_grad,
        key_grads.reshape(-1, KV_HEADS, HEAD_DIM),
        value_grads.reshape(-1, KV_HEADS, HEAD_DIM),
    )


def fetch_layer(qkv_weight, out_weight, gate_up_weight, down_weight, attn_gain, ffn_gain, layer_id):
    return (
        lax.all_gather(qkv_weight[layer_id], "fsdp", axis=0, tiled=True),
        lax.all_gather(out_weight[layer_id], "fsdp", axis=0, tiled=True),
        lax.all_gather(gate_up_weight[layer_id], "fsdp", axis=0, tiled=True),
        lax.all_gather(down_weight[layer_id], "fsdp", axis=0, tiled=True),
        lax.all_gather(attn_gain[layer_id], "fsdp", axis=0, tiled=True),
        lax.all_gather(ffn_gain[layer_id], "fsdp", axis=0, tiled=True),
    )


def fetch_again(qkv_weight, out_weight, gate_up_weight, down_weight, attn_gain, ffn_gain, layer_id):
    return (
        lax.all_gather(qkv_weight[layer_id], "fsdp", axis=0, tiled=True),
        lax.all_gather(out_weight[layer_id], "fsdp", axis=0, tiled=True),
        lax.all_gather(gate_up_weight[layer_id], "fsdp", axis=0, tiled=True),
        lax.all_gather(down_weight[layer_id], "fsdp", axis=0, tiled=True),
        lax.all_gather(attn_gain[layer_id], "fsdp", axis=0, tiled=True),
        lax.all_gather(ffn_gain[layer_id], "fsdp", axis=0, tiled=True),
    )


def forward_layer(stream, query_place, key_place, gathered):
    qkv_full, out_full, gate_up_full, down_full, attn_full, ffn_full = gathered
    rows = stream.shape[0]
    groups = HEADS // KV_HEADS
    query_width = HEADS * HEAD_DIM
    key_width = KV_HEADS * HEAD_DIM
    cosine, sine = angles(query_place)
    normed, first_factor = normalize(stream, attn_full.astype(jnp.float32))
    normed = normed.astype(jnp.bfloat16)
    projected = jnp.dot(normed, qkv_full, preferred_element_type=jnp.float32)
    queries = rotate(projected[:, :query_width].reshape(rows, HEADS, HEAD_DIM), cosine, sine)
    queries = queries.reshape(rows, KV_HEADS, groups, HEAD_DIM).astype(jnp.bfloat16)
    keys_local = rotate(
        projected[:, query_width : query_width + key_width].reshape(rows, KV_HEADS, HEAD_DIM),
        cosine,
        sine,
    ).astype(jnp.bfloat16)
    values_local = (
        projected[:, query_width + key_width :]
        .reshape(rows, KV_HEADS, HEAD_DIM)
        .astype(jnp.bfloat16)
    )
    keys_all, values_all = (
        lax.all_gather(keys_local, "ctx", axis=0, tiled=True),
        lax.all_gather(values_local, "ctx", axis=0, tiled=True),
    )
    logsum, attended = attention_forward(queries, keys_all, values_all, query_place, key_place)
    attended_low = attended.reshape(rows, query_width).astype(jnp.bfloat16)
    middle = stream + jnp.dot(attended_low, out_full, preferred_element_type=jnp.float32)
    second, second_factor = normalize(middle, ffn_full.astype(jnp.float32))
    second = second.astype(jnp.bfloat16)
    gate_up = jnp.einsum("rd,dcf->rcf", second, gate_up_full, preferred_element_type=jnp.float32)
    hidden = (jax.nn.silu(gate_up[:, 0]) * gate_up[:, 1]).astype(jnp.bfloat16)
    result = middle + jnp.dot(hidden, down_full, preferred_element_type=jnp.float32)
    stored = (
        stream,
        first_factor,
        normed,
        queries,
        keys_local,
        values_local,
        keys_all,
        values_all,
        logsum,
        attended,
        attended_low,
        middle,
        second_factor,
        second,
        gate_up,
        hidden,
    )
    return (result, stored)


def backward_layer(upstream, stored, gathered, query_place, key_place, keys_all, values_all):
    (
        stream,
        first_factor,
        normed,
        queries,
        keys_local,
        values_local,
        kept_keys,
        kept_values,
        logsum,
        attended,
        attended_low,
        middle,
        second_factor,
        second,
        gate_up,
        hidden,
    ) = stored
    qkv_full, out_full, gate_up_full, down_full, attn_full, ffn_full = gathered
    rows = stream.shape[0]
    groups = HEADS // KV_HEADS
    cosine, sine = angles(query_place)
    upstream_low = upstream.astype(jnp.bfloat16)
    hidden_grad = jnp.einsum(
        "rd,fd->rf", upstream_low, down_full, preferred_element_type=jnp.float32
    )
    gate_part = gate_up[:, 0]
    up_part = gate_up[:, 1]
    sigmoid = jax.nn.sigmoid(gate_part)
    gate_grad = hidden_grad * up_part * sigmoid * (1.0 + gate_part * (1.0 - sigmoid))
    up_grad = hidden_grad * gate_part * sigmoid
    gate_up_low = jnp.stack([gate_grad, up_grad], axis=1).astype(jnp.bfloat16)
    second_grad = jnp.einsum(
        "rcf,dcf->rd", gate_up_low, gate_up_full, preferred_element_type=jnp.float32
    )
    middle_grad, ffn_gain_grad = normalize_back(
        second_grad, middle, second_factor, ffn_full.astype(jnp.float32)
    )
    middle_grad = middle_grad + upstream
    middle_low = middle_grad.astype(jnp.bfloat16)
    attended_grad = jnp.einsum(
        "rd,od->ro", middle_low, out_full, preferred_element_type=jnp.float32
    )
    attended_grad = attended_grad.astype(jnp.bfloat16).reshape(rows, KV_HEADS, groups, HEAD_DIM)
    row_inner = jnp.einsum("rkgd,rkgd->kgr", attended_grad.astype(jnp.float32), attended)
    query_grad, key_grads, value_grads = attention_backward(
        queries, keys_all, values_all, query_place, key_place, logsum, attended_grad, row_inner
    )
    key_grad, value_grad = (
        lax.psum_scatter(key_grads, "ctx", scatter_dimension=0, tiled=True),
        lax.psum_scatter(value_grads, "ctx", scatter_dimension=0, tiled=True),
    )
    query_grad = rotate_back(query_grad.reshape(rows, HEADS, HEAD_DIM), cosine, sine)
    key_grad = rotate_back(key_grad, cosine, sine)
    projected_grad = jnp.concatenate(
        [query_grad.reshape(rows, -1), key_grad.reshape(rows, -1), value_grad.reshape(rows, -1)],
        axis=1,
    ).astype(jnp.bfloat16)
    normed_grad = jnp.einsum(
        "re,de->rd", projected_grad, qkv_full, preferred_element_type=jnp.float32
    )
    stream_grad, attn_gain_grad = normalize_back(
        normed_grad, stream, first_factor, attn_full.astype(jnp.float32)
    )
    stream_grad = stream_grad + middle_grad
    qkv_grad = jnp.einsum("rd,re->de", normed, projected_grad, preferred_element_type=jnp.float32)
    out_grad = jnp.einsum("ro,rd->od", attended_low, middle_low, preferred_element_type=jnp.float32)
    gate_up_grad = jnp.einsum(
        "rd,rcf->dcf", second, gate_up_low, preferred_element_type=jnp.float32
    )
    down_grad = jnp.einsum("rf,rd->fd", hidden, upstream_low, preferred_element_type=jnp.float32)
    sharded = (
        lax.psum_scatter(qkv_grad, "fsdp", scatter_dimension=0, tiled=True),
        lax.psum_scatter(out_grad, "fsdp", scatter_dimension=0, tiled=True),
        lax.psum_scatter(gate_up_grad, "fsdp", scatter_dimension=0, tiled=True),
        lax.psum_scatter(down_grad, "fsdp", scatter_dimension=0, tiled=True),
        lax.psum_scatter(attn_gain_grad, "fsdp", scatter_dimension=0, tiled=True),
        lax.psum_scatter(ffn_gain_grad, "fsdp", scatter_dimension=0, tiled=True),
    )
    totals = lax.psum(
        (sharded[0], sharded[1], sharded[2], sharded[3], sharded[4], sharded[5]), "ctx"
    )
    return (stream_grad, totals)


def body(
    tokens,
    positions,
    qkv_weight,
    out_weight,
    gate_up_weight,
    down_weight,
    attn_gain,
    ffn_gain,
    cotangent,
):
    query_place = positions[0]
    key_place = lax.all_gather(query_place, "ctx", axis=0, tiled=True)
    stream = tokens[0].astype(jnp.float32)
    gathered_list = []
    layer_id = 0
    gathered = fetch_layer(
        qkv_weight, out_weight, gate_up_weight, down_weight, attn_gain, ffn_gain, layer_id
    )
    stream, stored = forward_layer(stream, query_place, key_place, gathered)
    saved = [stored]
    gathered_list.append(gathered)
    activations = stream.astype(jnp.bfloat16)[None]
    upstream = cotangent[0]
    layer_grads = [None] * LAYERS
    for layer_id in reversed(range(LAYERS)):
        stored = saved[layer_id]
        gathered = fetch_again(
            qkv_weight, out_weight, gate_up_weight, down_weight, attn_gain, ffn_gain, layer_id
        )
        keys_all, values_all = (stored[6], stored[7])
        upstream, totals = backward_layer(
            upstream, stored, gathered, query_place, key_place, keys_all, values_all
        )
        layer_grads[layer_id] = totals
    outputs = [jnp.stack([entry[slot] for entry in layer_grads], axis=0) for slot in range(6)]
    return (
        activations,
        upstream[None],
        outputs[0],
        outputs[1],
        outputs[2],
        outputs[3],
        outputs[4],
        outputs[5],
    )


LANES = 128


def spread(heads):
    half = HEAD_DIM // 2
    pad = ((0, 0), (0, 0), (0, 64 - half))
    return jnp.concatenate([jnp.pad(heads[..., :half], pad), jnp.pad(heads[..., half:], pad)], axis=-1)


def gathered_spread(padded):
    half = HEAD_DIM // 2
    return jnp.concatenate([padded[..., :half], padded[..., 64 : 64 + half]], axis=-1)


def table(length):
    half = HEAD_DIM // 2
    frequency = rope_base ** (-(jnp.arange(half, dtype=jnp.float32) * 2.0 / HEAD_DIM))
    phases = jnp.arange(length, dtype=jnp.float32)[:, None] * frequency[None, :]
    pad = ((0, 0), (0, 64 - half))
    return jnp.concatenate([jnp.pad(jnp.cos(phases), pad), jnp.pad(jnp.sin(phases), pad)], axis=1)


def wave(rows):
    first = lax.broadcasted_iota(jnp.int32, rows.shape, 1) < 64
    other = pltpu.roll(rows, 64, 1)
    return jnp.where(first, rows, other), jnp.where(first, -other, rows)


def nt(left, right):
    return lax.dot_general(left, right, (((1,), (1,)), ((), ())), preferred_element_type=jnp.float32)


def nn(left, right):
    return lax.dot_general(left, right, (((1,), (0,)), ((), ())), preferred_element_type=jnp.float32)


def tn(left, right):
    return lax.dot_general(left, right, (((0,), (0,)), ((), ())), preferred_element_type=jnp.float32)


def causal(width):
    key_at = lax.broadcasted_iota(jnp.int32, (width, 2 * width), 0)
    query_at = lax.broadcasted_iota(jnp.int32, (width, 2 * width), 1)
    query_at = jnp.where(query_at >= width, query_at - width, query_at)
    return key_at <= query_at


def vm(count):
    return [pl.BlockSpec(memory_space=pltpu.VMEM)] * count


MESH = pl.DeviceIdType.MESH


class Place:
    def __init__(self):
        self.me = lax.axis_index("ctx")
        core, x, y = self.me % 2, (self.me // 2) % 2, self.me // 4
        self.dp, self.dx, self.dy = 1 - 2 * core, 2 - 4 * x, 4 - 8 * y
        self.p, self.x, self.y = self.me + self.dp, self.me + self.dx, self.me + self.dy
        self.d = self.x + self.dy
        self.z = lax.axis_index("fsdp")
        self.planes = lax.axis_size("fsdp")
        self.n = lax.axis_size("ctx")


def greet(place, ctx=True, planes=False):
    barrier = pltpu.get_barrier_semaphore()
    count = 0
    if ctx:
        for step in range(1, place.n):
            pl.semaphore_signal(
                barrier, inc=1, device_id={"ctx": lax.rem(place.me + step, place.n)}, device_id_type=MESH
            )
            count += 1
    if planes:
        for step in range(1, place.planes):
            pl.semaphore_signal(
                barrier, inc=1, device_id={"fsdp": lax.rem(place.z + step, place.planes)}, device_id_type=MESH
            )
            count += 1
    pl.semaphore_wait(barrier, count)


def send(source, target, send_sem, recv_sem, **where):
    return pltpu.make_async_remote_copy(
        src_ref=source, dst_ref=target, send_sem=send_sem, recv_sem=recv_sem,
        device_id=where, device_id_type=MESH,
    )


class Gather:
    sems = 14

    def __init__(self, place, own, out, sem):
        self.place, self.own, self.out, self.sem = place, own, out, sem
        self.half = out.shape[1] // 2
        self.started = []
        self.met = False

    def go(self, source, target, index, rank):
        send(source, target, self.sem.at[0, index], self.sem.at[1, index], ctx=rank).start()
        self.started.append(index)

    def whole_block(self, index):
        return index == 6

    def sent(self):
        p = self.place
        for index in self.started:
            part = self.whole(p.me) if self.whole_block(index) else self.part(p.me, 0)
            send(part, part, self.sem.at[0, index], self.sem.at[1, index], ctx=p.p).wait_send()

    def part(self, rank, half):
        return self.out.at[rank, pl.ds(half * self.half, self.half)]

    def whole(self, rank):
        return self.out.at[rank]

    def start(self):
        p = self.place
        keep = pltpu.make_async_copy(self.own, self.whole(p.me), self.sem.at[0, 13])
        keep.start()
        self.keep = keep
        halves = [self.own.at[pl.ds(h * self.half, self.half)] for h in range(2)]
        self.go(halves[0], self.part(p.me, 0), 0, p.x)
        self.go(halves[1], self.part(p.me, 1), 3, p.y)
        self.go(self.own, self.whole(p.me), 6, p.p)
        self.go(halves[1], self.part(p.me, 1), 1, p.x)
        self.go(halves[0], self.part(p.me, 0), 2, p.y)

    def arrived(self, rank, half, index):
        part = self.part(rank, half)
        pltpu.make_async_copy(part, part, self.sem.at[1, index]).wait()
        return part

    def relay(self):
        p = self.place
        part = self.arrived(p.x, 0, 0)
        self.go(part, part, 4, p.y)
        self.go(part, part, 7, p.p)
        part = self.arrived(p.y, 1, 3)
        self.go(part, part, 5, p.x)
        self.go(part, part, 10, p.p)

    def rest(self):
        p = self.place
        for rank, half, index, onward in ((p.x, 1, 1, 8), (p.y, 0, 2, 9), (p.d, 0, 4, 11), (p.d, 1, 5, 12)):
            part = self.arrived(rank, half, index)
            self.go(part, part, onward, p.p)

    def first_partner(self):
        part = self.whole(self.place.p)
        pltpu.make_async_copy(part, part, self.sem.at[1, 6]).wait()
        self.met = True

    def partner(self):
        p = self.place
        if not self.met:
            self.first_partner()
        for rank, half, index in (
            (p.x, 0, 7), (p.y, 1, 10), (p.x, 1, 8), (p.y, 0, 9), (p.d, 0, 11), (p.d, 1, 12),
        ):
            self.arrived(rank + p.dp, half, index)

    def finish(self, kept=False):
        if not kept:
            self.keep.wait()
        self.sent()


class PlaneGather:
    def __init__(self, place, own, out, sem):
        self.place, self.own, self.out, self.sem = place, own, out, sem

    def hop(self, step, up):
        p = self.place
        sign = 1 if up else -1
        source = p.z - sign * step
        target = p.z + sign
        ok = jnp.logical_and(
            jnp.logical_and(source >= 0, source < p.planes),
            jnp.logical_and(target >= 0, target < p.planes),
        )
        source = jnp.clip(source, 0, p.planes - 1)
        target = jnp.clip(target, 0, p.planes - 1)
        block = self.own if step == 0 else self.out.at[source]
        return ok, send(
            block, self.out.at[source], self.sem.at[0 if up else 1, source], self.sem.at[2, source], fsdp=target
        )

    def start(self):
        p = self.place
        self.keep = pltpu.make_async_copy(self.own, self.out.at[p.z], self.sem.at[2, p.z])
        self.keep.start()
        for up in (True, False):
            ok, copy = self.hop(0, up)
            pl.when(ok)(copy.start)

    def got(self, step, up):
        p = self.place
        source = p.z - step if up else p.z + step
        ok = jnp.logical_and(source >= 0, source < p.planes)
        source = jnp.clip(source, 0, p.planes - 1)
        part = self.out.at[source]
        return ok, pltpu.make_async_copy(part, part, self.sem.at[2, source])

    def step(self, number):
        for up in (True, False):
            ok, copy = self.got(number, up)
            pl.when(ok)(copy.wait)
            if number < self.place.planes - 1:
                ok, copy = self.hop(number, up)
                pl.when(ok)(copy.start)

    def finish(self, kept=False):
        if not kept:
            self.keep.wait()
        for number in range(self.place.planes - 1):
            for up in (True, False):
                ok, copy = self.hop(number, up)
                pl.when(ok)(copy.wait_send)


class Exchange:
    def __init__(self, place, blocks, out, sem):
        self.place, self.blocks, self.out, self.sem = place, blocks, out, sem

    def pick(self, rank):
        return self.blocks.at[rank]

    def copy(self, step):
        p = self.place
        rank = lax.rem(p.me + step, p.n)
        return send(self.pick(rank), self.out.at[p.me], self.sem.at[0, step], self.sem.at[1, step], ctx=rank)

    def start(self):
        p = self.place
        for step in range(1, p.n):
            self.copy(step).start()
        self.keep = pltpu.make_async_copy(self.pick(p.me), self.out.at[p.me], self.sem.at[0, 0])
        self.keep.start()

    def finish(self):
        p = self.place
        self.keep.wait()
        for step in range(1, p.n):
            self.copy(step).wait_send()
        for step in range(1, p.n):
            part = self.out.at[lax.rem(p.me + p.n - step, p.n)]
            pltpu.make_async_copy(part, part, self.sem.at[1, step]).wait()


class Share(Exchange):
    def pick(self, rank):
        return self.blocks


class PlaneShare:
    def __init__(self, place, block, out, sem):
        self.place, self.block, self.out, self.sem = place, block, out, sem

    def copy(self, step):
        p = self.place
        plane = lax.rem(p.z + step, p.planes)
        return send(self.block, self.out.at[p.z], self.sem.at[0, step], self.sem.at[1, step], fsdp=plane)

    def start(self):
        p = self.place
        for step in range(1, p.planes):
            self.copy(step).start()
        self.keep = pltpu.make_async_copy(self.block, self.out.at[p.z], self.sem.at[0, 0])
        self.keep.start()

    def finish(self):
        p = self.place
        self.keep.wait()
        for step in range(1, p.planes):
            self.copy(step).wait_send()
        for step in range(1, p.planes):
            part = self.out.at[lax.rem(p.z + p.planes - step, p.planes)]
            pltpu.make_async_copy(part, part, self.sem.at[1, step]).wait()


def anywhere(count):
    return [pl.BlockSpec(memory_space=pl.ANY)] * count


class Reduce:
    sems = 10

    def __init__(self, place, mine, theirs, first, out, second, sem):
        self.place, self.mine, self.theirs, self.first, self.out, self.second, self.sem = (
            place, mine, theirs, first, out, second, sem
        )
        self.half = out.shape[1]
        self.started = []

    def push(self, slot):
        copy = send(
            self.theirs.at[slot], self.first.at[slot], self.sem.at[0, slot], self.sem.at[1, slot], ctx=self.place.p
        )
        copy.start()
        return copy

    def pushed(self):
        for slot in range(4):
            send(
                self.theirs.at[slot], self.first.at[slot], self.sem.at[0, slot], self.sem.at[1, slot],
                ctx=self.place.p,
            ).wait_send()

    def add(self, slot):
        part = self.first.at[slot]
        pltpu.make_async_copy(part, part, self.sem.at[1, slot]).wait()
        self.mine[slot] = self.mine[slot] + self.first[slot].astype(jnp.float32)

    def go(self, index, value, rank):
        self.out[index] = value.astype(jnp.bfloat16)
        self.turned(index, rank).start()
        self.started.append((index, rank))

    def turned(self, index, rank):
        return send(
            self.out.at[index], self.second.at[index], self.sem.at[0, 4 + index], self.sem.at[1, 4 + index], ctx=rank
        )

    def top(self, slot):
        return self.mine[slot, pl.ds(0, self.half), :]

    def low(self, slot):
        return self.mine[slot, pl.ds(self.half, self.half), :]

    def got(self, index):
        part = self.second.at[index]
        pltpu.make_async_copy(part, part, self.sem.at[1, 4 + index]).wait()
        return self.second[index].astype(jnp.float32)

    def across(self):
        self.add(3)
        self.go(1, self.top(3), self.place.x)
        self.go(3, self.low(3), self.place.y)

    def beside(self):
        self.add(1)
        self.go(0, self.top(1), self.place.x)
        self.add(2)
        self.go(2, self.low(2), self.place.y)

    def turn(self):
        self.go(4, self.top(2) + self.got(1), self.place.y)
        self.go(5, self.low(1) + self.got(3), self.place.x)

    def total(self, use):
        self.add(0)
        use(pl.ds(0, self.half), self.top(0) + self.got(0) + self.got(4))
        use(pl.ds(self.half, self.half), self.low(0) + self.got(2) + self.got(5))

    def finish(self):
        self.pushed()
        for index, rank in self.started:
            self.turned(index, rank).wait_send()


def flip(place, i):
    return place.me + (i % 2) * place.dp + ((i // 2) % 2) * place.dx + (i // 4) * place.dy


class HalfGather(Gather):
    sems = 16

    def __init__(self, place, own, out, sem):
        self.place, self.own, self.out, self.sem = place, own, out, sem
        self.half = out.shape[1]
        self.started = []
        self.met = False

    def part(self, rank, half):
        return self.out.at[2 * rank + half]

    def whole_block(self, index):
        return False

    def start(self):
        p = self.place
        halves = [self.own.at[pl.ds(h * self.half, self.half)] for h in range(2)]
        self.kept = [
            pltpu.make_async_copy(halves[h], self.part(p.me, h), self.sem.at[0, (13, 15)[h]]) for h in range(2)
        ]
        self.go(halves[0], self.part(p.me, 0), 0, p.x)
        self.go(halves[1], self.part(p.me, 1), 3, p.y)
        self.go(halves[0], self.part(p.me, 0), 6, p.p)
        self.go(halves[1], self.part(p.me, 1), 14, p.p)
        self.go(halves[1], self.part(p.me, 1), 1, p.x)
        self.go(halves[0], self.part(p.me, 0), 2, p.y)
        for copy in self.kept:
            copy.start()

    def first_partner(self):
        for h in range(2):
            self.arrived(self.place.p, h, (6, 14)[h])
        self.met = True

    def own_in(self):
        for copy in self.kept:
            copy.wait()

    def finish(self):
        self.sent()


def packed(block):
    rows = block.shape[0] // 2
    tail = jnp.concatenate([block[:, LANES:], jnp.zeros((2 * rows, 64), block.dtype)], axis=1)
    first = lax.broadcasted_iota(jnp.int32, (rows, LANES), 1) < 64
    return jnp.concatenate([block[:, :LANES], jnp.where(first, tail[:rows], pltpu.roll(tail[rows:], 64, 1))], axis=0)


def unpacked(block):
    rows = block.shape[0] // 3
    tail = block[2 * rows :].astype(jnp.float32)
    tails = jnp.concatenate([tail, pltpu.roll(tail, 64, 1)], axis=0)[:, :64].astype(block.dtype)
    return jnp.concatenate([block[: 2 * rows], tails], axis=1)


class PlaneReduce:
    def __init__(self, place, block, recv, sem):
        self.place, self.block, self.recv, self.sem = place, block, recv, sem

    def hop(self, ok, part, slot, target, first, wait):
        copy = send(
            self.block.at[part], self.recv.at[slot], self.sem.at[0, part], self.sem.at[1, slot], fsdp=target
        )

        @pl.when(ok)
        def _():
            if wait:
                copy.wait_send()
                return
            if not first:
                self.merge(part, part)
            copy.start()

    def merge(self, part, slot):
        piece = self.recv.at[slot]
        pltpu.make_async_copy(piece, piece, self.sem.at[1, slot]).wait()
        total = self.block[part].astype(jnp.float32) + self.recv[slot].astype(jnp.float32)
        self.block[part] = total.astype(jnp.bfloat16)

    def ends(self, i, wait=False):
        z = self.place.z
        low = z == 0
        part = jnp.where(low, 3 - i, i)
        slot = part if i < 2 else jnp.where(low, part, 4)
        self.hop(jnp.logical_or(low, z == 3), part, slot, jnp.where(low, 1, 2), True, wait)

    def inner(self, up, down, slot_up, slot_down, to_up, to_down, wait=False):
        z = self.place.z
        low = z == 1
        part = jnp.where(low, up, down)
        slot = jnp.where(low, slot_up, slot_down)
        self.hop(jnp.logical_or(low, z == 2), part, slot, jnp.where(low, to_up, to_down), False, wait)

    def start(self, wait=False):
        for i in range(3):
            self.ends(i, wait)

    def step1(self, wait=False):
        self.inner(3, 0, 3, 0, 2, 1, wait)

    def step2(self, wait=False):
        self.inner(2, 1, 2, 4, 2, 1, wait)
        self.inner(0, 3, 4, 3, 0, 3, wait)

    def total(self):
        z = self.place.z

        @pl.when(z > 0)
        def _():
            self.merge(z, z)

        @pl.when(z < 3)
        def _():
            self.merge(z, 4)

    def own(self):
        return self.block.at[self.place.z]

    def finish(self):
        self.start(True)
        self.step1(True)
        self.step2(True)


class Steps:
    def __init__(self, *steps):
        self.steps = list(steps)

    def next(self, count=1):
        for step in self.steps[:count]:
            step()
        self.steps = self.steps[count:]

    def rest(self):
        self.next(len(self.steps))


class OutGather(Gather):
    def __init__(self, place, own, out, sem):
        self.place, self.own, self.out, self.sem = place, own, out, sem
        self.half = out.shape[0] // 2
        self.started = []
        self.met = False

    def part(self, rank, half):
        return self.out.at[pl.ds(half * self.half, self.half), rank]

    def whole(self, rank):
        return self.out.at[:, rank]


def front_kernel(
    tok, up_low, spot, gain_own, qkv_own, out_own, gu_own, down_own, turn_ref, up,
    middle_grad, gain_grad, spots, gains, down_sum,
    hidden_o, qkv_o, down_o, q_o, k_o, v_o, att_o, lse_o, middle_o, normed, agrad, low_all, gu_out, mcols,
    hidden, qkv_w, down_w, q_ref, k_ref, v_ref, att_ref, lse_ref, middle, mcols_send,
    wide_in, up_all, gul, gu_w, out_block, out_w, low_sorted, gain_all, spots_s, order_s, low,
    attended, own, mine, theirs, first, out, second, down_g, down_r,
    tok_sem, up_sem, spot_sem, gain_sem, qkv_sem, out_sem, outc_sem, gu_sem, down_sem, local_sem,
    low_sem, gather_sem, reduce_sem, agrad_sem, lows_sem, down_zs, mcols_sem,
):
    place = Place()
    n = place.n
    rows = tok.shape[0]
    half = rows // 2
    pairs = 8
    heads = rows
    length = n * rows
    width = tok.shape[1]
    greet(place, planes=True)
    spans = Share(place, spot, spots, spot_sem)
    scales = PlaneShare(place, gain_own, gain_all, gain_sem)
    tokens = HalfGather(place, tok, wide_in, tok_sem)
    cots = Gather(place, up_low, up_all, up_sem)
    qkvs = PlaneGather(place, qkv_own, qkv_w, qkv_sem)
    outs = PlaneGather(place, out_own, out_block, out_sem)
    outc = OutGather(place, out_block, out_w, outc_sem)
    gus = PlaneGather(place, gu_own, gu_w, gu_sem)
    downs = PlaneGather(place, down_own, down_w, down_sem)
    fetch = pltpu.make_async_copy(up, middle_grad, local_sem.at[0])
    given = []

    def give(source, target):
        copy = pltpu.make_async_copy(source, target, local_sem.at[5 + len(given)])
        copy.start()
        given.append(copy)

    tokens.start()
    qkvs.start()
    spans.start()
    scales.start()
    fetch.start()
    tokens.relay()
    qkvs.step(1)
    outs.start()
    qkvs.step(2)
    tokens.rest()
    cots.start()
    outs.step(1)
    downs.start()
    qkvs.step(3)
    tokens.partner()
    tokens.own_in()
    spans.finish()
    scales.finish()
    qkvs.keep.wait()
    table = pltpu.make_async_copy(spots, spots_s, local_sem.at[1])
    table.start()
    for g in range(2):
        gains[pl.ds(g, 1), :] = jnp.concatenate([gain_all[z, pl.ds(g, 1), :] for z in range(4)], axis=1)
    table.wait()
    early = [spots_s[j, 0, 0] for j in range(pairs)]
    for t in range(pairs):
        at = 0
        for j in range(pairs):
            at = jnp.where(early[j] == t, j, at)
        order_s[t] = 2 * at
        order_s[2 * pairs - 1 - t] = 2 * at + 1
    cots.relay()

    def project(j, store):
        x = jnp.concatenate([wide_in[order_s[4 * j + i]] for i in range(4)], axis=0).astype(jnp.float32)
        factor = lax.rsqrt(jnp.mean(x * x, axis=-1, keepdims=True) + epsilon)
        scaled = (x * factor * gains[pl.ds(0, 1), :]).astype(jnp.bfloat16)
        store[pl.ds(2 * (j % 2), 2)] = scaled.reshape(2, rows, -1)
        proj = nn(scaled, qkv_w[...].reshape(-1, 4 * LANES))
        for piece in range(4):
            at = 4 * j + piece
            cosine, sine = wave(turn_ref[at])
            mine_rows = proj[piece * half : (piece + 1) * half]

            def turned(part):
                z = mine_rows[:, part * LANES : (part + 1) * LANES]
                return (z * cosine + pltpu.roll(z, 64, 1) * sine).astype(jnp.bfloat16)

            base = (2 * j + piece // 2) * 4 * half + (piece % 2) * half
            q_ref[pl.ds(pl.multiple_of(base, half), half), :] = turned(0)
            q_ref[pl.ds(pl.multiple_of(base + 2 * half, half), half), :] = turned(1)
            k_ref[pl.ds(pl.multiple_of(at * half, half), half), :] = turned(2)
            v_ref[pl.ds(pl.multiple_of(at * half, half), half), :] = mine_rows[:, 3 * LANES :].astype(jnp.bfloat16)

    def project_first(j, carry):
        project(j, theirs)
        return carry

    def project_second(j, carry):
        project(j, first)
        return carry

    lax.fori_loop(0, 2, project_first, 0)
    keep_first = pltpu.make_async_copy(theirs, normed.at[pl.ds(0, 4)], local_sem.at[2])
    keep_first.start()
    lax.fori_loop(2, 4, project_second, 0)
    keep_second = pltpu.make_async_copy(first, normed.at[pl.ds(4, 4)], local_sem.at[3])
    keep_second.start()
    give(q_ref, q_o)
    give(k_ref, k_o)
    give(v_ref, v_o)
    give(qkv_w, qkv_o)
    tokens.finish()
    outs.step(2)
    cots.rest()
    outs.step(3)
    outs.keep.wait()
    outc.start()

    def next_weights():
        downs.step(1)
        gus.start()

    steps = Steps(
        next_weights, lambda: None, lambda: None, lambda: None, outc.relay, lambda: None, lambda: downs.step(2),
        lambda: None,
    )
    scaling = HEAD_DIM ** (-0.5)
    mask = causal(2 * half)
    lane = lax.broadcasted_iota(jnp.int32, (half, LANES), 1)
    values_t = v_ref[...].astype(jnp.float32).T.astype(jnp.bfloat16)
    for pair in range(pairs):
        width_of = (pair + 1) * 2 * half
        q = q_ref[pl.ds(pair * 4 * half, 4 * half), :]
        before = width_of - 2 * half
        parts = [jnp.where(mask, nt(k_ref[pl.ds(before, 2 * half), :], q) * scaling, -1e30)]
        if pair:
            parts.append(nt(k_ref[pl.ds(0, before), :], q) * scaling)
        tops = [jnp.max(part, axis=0, keepdims=True) for part in parts]
        top = jnp.maximum(tops[0], tops[-1])
        parts = [jnp.exp(part - top) for part in parts]
        total = sum(jnp.sum(part, axis=0, keepdims=True) for part in parts)
        parts = [(part * (1.0 / total)).astype(jnp.bfloat16) for part in parts]
        lse_ref[pl.ds(pair, 1), :] = top + jnp.log(total)
        out_t = nn(values_t[:, before:width_of], parts[0])
        if pair:
            out_t = out_t + nn(values_t[:, :before], parts[1])
        att_ref[pl.ds(pair * LANES, LANES), :] = out_t
        result = out_t.T.astype(jnp.bfloat16).astype(jnp.float32)
        for part in range(2):
            left = result[part * half : (part + 1) * half]
            right = pltpu.roll(result[(2 + part) * half : (3 + part) * half], half, 1)
            low_sorted[2 * pair + part, :, 0:LANES] = jnp.where(lane < half, left, right).astype(jnp.bfloat16)
            low_sorted[2 * pair + part, :, LANES:] = right.astype(jnp.bfloat16)
        steps.next()
    give(att_ref, att_o)
    give(lse_ref, lse_o)
    for j in range(pairs):
        upper = low_sorted[early[j]]
        lower = low_sorted[2 * pairs - 1 - early[j]]
        low[j, pl.ds(0, half), :] = upper[:, :LANES]
        low[j, pl.ds(half, half), :] = lower[:, :LANES]
        tails = jnp.where(
            lane < 64, upper[:, LANES:].astype(jnp.float32), pltpu.roll(lower[:, LANES:].astype(jnp.float32), 64, 1)
        )
        low[j, pl.ds(2 * half, half), :] = tails.astype(jnp.bfloat16)
    keep_first.wait()
    keep_second.wait()
    moved = Exchange(place, low, attended, low_sem)
    moved.start()
    outc.rest()
    outc.partner()
    cots.partner()
    outc.keep.wait()
    moved.finish()
    middle[...] = tok[...].astype(jnp.float32)

    def out_project(q, carry):
        middle[...] += nn(unpacked(attended[q]), out_w[q // 2, pl.ds(4 * (q % 2), 4)].reshape(heads, -1))
        return carry

    lax.fori_loop(0, n, out_project, 0)
    give(middle, middle_o)
    gus.step(1)
    total = middle[...]
    factor = lax.rsqrt(jnp.mean(total * total, axis=-1, keepdims=True) + epsilon)
    own[...] = (total * factor * gains[pl.ds(1, 1), :]).astype(jnp.bfloat16)
    seconds = HalfGather(place, own, wide_in, gather_sem)
    seconds.start()
    seconds.relay()
    gus.step(2)
    seconds.rest()
    lows = Gather(place, low, low_all, lows_sem)
    lows.start()
    seconds.partner()
    downs.step(3)
    downs.keep.wait()
    give(down_w, down_o)
    cots.keep.wait()
    seconds.own_in()

    def early_grad(i, carry):
        rank = flip(place, i)
        at = pl.multiple_of((i % 2) * hidden.shape[2], LANES)
        mine[i // 2, :, pl.ds(at, hidden.shape[2])] = nt(up_all[rank], down_w[...].reshape(hidden.shape[2], -1))
        return carry

    lax.fori_loop(0, n, early_grad, 0)
    gus.step(3)
    gus.keep.wait()
    grads = Reduce(place, mine, theirs, first, out, second, reduce_sem)
    wide = hidden.shape[2]

    def block(i):
        rank = flip(place, i)
        gate_up = nn(wide_in[pl.ds(2 * rank, 2)].reshape(rows, -1), gu_w[...].reshape(-1, 2 * wide))
        gate, raised = gate_up[:, :wide], gate_up[:, wide:]
        sigmoid = 1.0 / (1.0 + jnp.exp(-gate))
        silu = gate * sigmoid
        hidden[rank] = (silu * raised).astype(jnp.bfloat16)
        hidden_grad = mine[i // 2, :, pl.ds(pl.multiple_of((i % 2) * wide, LANES), wide)]
        gul[rank, :, pl.ds(0, wide)] = (hidden_grad * raised * sigmoid * (1.0 + gate * (1.0 - sigmoid))).astype(jnp.bfloat16)
        gul[rank, :, pl.ds(wide, wide)] = (hidden_grad * silu).astype(jnp.bfloat16)
        return nt(gul[rank], gu_w[...].reshape(-1, 2 * wide))

    def block_at(t, carry):
        k = lax.rem(t // 2 + 1, 4)
        value = block(2 * k + 1 - t % 2)

        @pl.when(t % 2 == 0)
        def _():
            theirs[k] = value.astype(jnp.bfloat16)
            grads.push(k)

        @pl.when(t % 2 == 1)
        def _():
            mine[k] = value

        @pl.when(t == 2)
        def _():
            lows.relay()

        @pl.when(t == 4)
        def _():
            grads.beside()

        @pl.when(t == 5)
        def _():
            lows.rest()

        @pl.when(t == 6)
        def _():
            grads.across()

        return carry

    lax.fori_loop(0, 8, block_at, 0)
    give(hidden, hidden_o)
    grads.turn()
    down_z = PlaneReduce(place, down_g, down_r, down_zs)
    piece = down_g.shape[1]

    def down_block(t, carry):
        left = hidden[:, :, pl.ds(pl.multiple_of(t * piece, piece), piece)].reshape(length, piece)
        down_g[t] = tn(left, up_all[...].reshape(length, width)).astype(jnp.bfloat16)
        return carry

    lax.fori_loop(0, 4, down_block, 0)
    down_z.start()
    fetch.wait()
    seconds.finish()
    gain_grad[...] = jnp.zeros_like(gain_grad)

    def norm_back(part, second_grad):
        x = middle[part, :]
        factor = lax.rsqrt(jnp.mean(x * x, axis=-1, keepdims=True) + epsilon)
        unit = x * factor
        gain_grad[...] += jnp.sum(second_grad * unit, axis=0, keepdims=True)
        scaled = second_grad * gains[pl.ds(1, 1), :]
        inner = jnp.mean(scaled * unit, axis=-1, keepdims=True)
        grad = middle_grad[part, :] + factor * (scaled - unit * inner)
        middle_grad[part, :] = grad
        own[part, :] = grad.astype(jnp.bfloat16)

    gus.finish(kept=True)
    shard = gu_w.shape[1]

    def gu_block(t, carry):
        left = wide_in[:, :, pl.ds(pl.multiple_of(t * shard, shard), shard)].reshape(length, shard)
        gu_w[t] = tn(left, gul[...].reshape(length, 2 * wide)).astype(jnp.bfloat16)
        return carry

    lax.fori_loop(0, 4, gu_block, 0)
    give(gu_w, gu_out)
    down_z.step1()
    grads.total(norm_back)

    def head_grads(q, carry):
        weight = out_w[q // 2, pl.ds(4 * (q % 2), 4)].reshape(heads, -1)
        attended[q] = packed(nt(own[...], weight)).astype(jnp.bfloat16)
        return carry

    lax.fori_loop(0, n, head_grads, 0)
    heads_back = Exchange(place, attended, agrad, agrad_sem)
    heads_back.start()
    for q in range(8):
        mcols_send[q] = packed(own[:, q * heads : (q + 1) * heads].astype(jnp.float32)).astype(jnp.bfloat16)
    columns = Exchange(place, mcols_send, mcols, mcols_sem)
    columns.start()
    down_z.step2()
    lows.partner()
    heads_back.finish()
    down_z.total()
    down_sum[...] = down_g[place.z]
    for move in (qkvs, outs, downs, cots, outc):
        move.finish(kept=True)
    lows.finish()
    columns.finish()
    for copy in given:
        copy.wait()
    grads.finish()
    down_z.finish()


def front_moves(tok, up_low, spot, gain_own, qkv_own, out_own, gu_own, down_own, turns, up):
    n, planes = lax.axis_size("ctx"), lax.axis_size("fsdp")
    rows, width = tok.shape
    length = n * rows
    wide = planes * down_own.shape[0]
    bf, f32 = jnp.bfloat16, jnp.float32
    shape = jax.ShapeDtypeStruct
    dma = pltpu.SemaphoreType.DMA
    pairs = length // 192
    halves = pltpu.VMEM((6, rows // 2, width), bf)
    quads = pltpu.VMEM((4, rows, width), bf)
    small = (n, 3 * rows // 2, LANES)
    all_of = lambda x: shape((planes,) + x.shape, x.dtype)
    gathered = lambda x: pltpu.VMEM((planes,) + x.shape, x.dtype)
    ring = dma((2, Gather.sems))
    half_ring = dma((2, HalfGather.sems))
    line = dma((3, planes))
    swap = dma((2, n))
    kept = (
        shape((n, rows, wide), bf), all_of(qkv_own), all_of(down_own),
        shape((2 * length, LANES), bf), shape((length, LANES), bf), shape((length, LANES), bf),
        shape((pairs * LANES, 384), f32), shape((pairs, 384), f32), shape((rows, width), f32),
    )
    return pl.pallas_call(
        front_kernel,
        out_shape=(
            shape((rows, width), f32), shape((1, width), f32), shape((n,) + spot.shape, spot.dtype), shape((2, width), f32),
            shape(down_own.shape, bf),
        ) + kept + (shape((n, rows, width), bf), shape(small, bf), shape((n,) + small, bf), all_of(gu_own), shape(small, bf)),
        in_specs=vm(9) + anywhere(1),
        out_specs=vm(5) + anywhere(14),
        scratch_shapes=[pltpu.VMEM(x.shape, x.dtype) for x in kept] + [
            pltpu.VMEM(small, bf),
            pltpu.VMEM((2 * n, rows // 2, width), bf), pltpu.VMEM((n, rows, width), bf), pltpu.VMEM((n, rows, 2 * wide), bf),
            gathered(gu_own), gathered(out_own), pltpu.VMEM((planes, n) + out_own.shape, bf),
            pltpu.VMEM((16, 96, 2 * LANES), bf), gathered(gain_own), pltpu.SMEM((n,) + spot.shape, jnp.int32),
            pltpu.SMEM((2 * n,), jnp.int32), pltpu.VMEM(small, bf),
            pltpu.VMEM(small, bf), pltpu.VMEM((rows, width), bf),
            pltpu.VMEM((4, rows, width), f32), quads, quads, halves, halves,
            gathered(down_own), pltpu.VMEM((planes + 1,) + down_own.shape, bf),
            half_ring, ring, swap, dma((2, planes)), line, line, ring, line, line, dma((15,)),
            swap, half_ring, dma((2, Reduce.sems)), swap, ring, dma((2, planes + 1)), swap,
        ],
        compiler_params=pltpu.CompilerParams(collective_id=1, has_side_effects=True, vmem_limit_bytes=67043328),
        name="front_moves",
    )(tok, up_low, spot, gain_own, qkv_own, out_own, gu_own, down_own, turns, up)


def back_moves_kernel(
    early_ref, tok, gain, ffn_gain, down_sum,
    gu_i, middle_grad_i, hidden_i, down_i, k_i, q_i, v_i, agrad_i, att_i, lse_i, turn_i, normed_i, middle_i, qkv_i, mcols_i, low_i,
    grad, result, gains, down_all, gu_all, out_all, qkv_all,
    gu_g, hidden, down_w, k_ref, q_ref, v_ref, agrad, att_ref, lse_ref, turn_ref, normed_in, middle, qkv_w, mcols_in, low_in, out_g, qkv_g, gu_r, out_r, qkv_r,
    mine, theirs, first, out, second, dk_ref, dv_ref, pg_sorted, mcols,
    gain_sum, mine_gain, ctx_gain, plane_sum, plane_gain,
    free, local_sem, sum_sem, reduce_sem, gu_zs, out_zs, qkv_zs, down_cs, gu_cs, out_cs, qkv_cs,
    gain_sem, plane_sem,
):
    place = Place()
    n = place.n
    rows = tok.shape[0]
    half = rows // 2
    pairs = 8
    width = tok.shape[1]
    length = n * rows
    loads = [
        pltpu.make_async_copy(source, target, local_sem.at[at])
        for at, (source, target) in enumerate((
            (gu_i, gu_g), (hidden_i, hidden), (down_i, down_w), (k_i, k_ref), (q_i, q_ref), (v_i, v_ref),
            (agrad_i, agrad), (att_i, att_ref), (lse_i, lse_ref), (turn_i, turn_ref), (middle_i, middle),
            (normed_i, normed_in), (qkv_i, qkv_w), (mcols_i, mcols_in), (low_i, low_in), (middle_grad_i, grad),
        ))
    ]
    for load in loads:
        load.start()
    greet(place, planes=True)
    early = [early_ref[j] for j in range(pairs)]
    holder = []
    for t in range(pairs):
        at = 0
        for j in range(pairs):
            at = jnp.where(early[j] == t, j, at)
        holder.append(at)
    gu_z = PlaneReduce(place, gu_g, gu_r, gu_zs)
    out_z = PlaneReduce(place, out_g, out_r, out_zs)
    qkv_z = PlaneReduce(place, qkv_g, qkv_r, qkv_zs)
    sums = Reduce(place, mine, theirs, first, out, second, sum_sem)
    downs = Gather(place, down_sum, down_all, down_cs)
    gus = Gather(place, gu_z.own(), gu_all, gu_cs)
    loads[0].wait()
    gu_z.start()
    downs.start()
    loads[1].wait()
    loads[2].wait()

    def other(k, carry):
        theirs[k] = nn(hidden[flip(place, 2 * k + 1)], down_w[...].reshape(-1, width)).astype(jnp.bfloat16)
        sums.push(k)
        return carry

    def ours(k, carry):
        mine[k] = nn(hidden[flip(place, 2 * k)], down_w[...].reshape(-1, width))
        return carry

    lax.fori_loop(0, 4, other, 0)
    lax.fori_loop(0, 4, ours, 0)
    downs.relay()
    sums.across()
    sums.beside()
    for load in loads[3:11]:
        load.wait()

    def finish_rows(part, down_out):
        result[part, :] = (middle[part, :] + down_out).astype(jnp.bfloat16)

    def sums_done():
        sums.total(finish_rows)
        sums.finish()
        for rank in (place.p, place.x, place.y):
            pl.semaphore_signal(free, inc=1, device_id={"ctx": rank}, device_id_type=MESH)

    def columns_done():
        loads[13].wait()

        def unpack(q, carry):
            mcols[q] = unpacked(mcols_in[q])
            return carry

        lax.fori_loop(0, n, unpack, 0)

    steps = Steps(
        lambda: None, downs.rest, lambda: None, gu_z.step1, downs.partner, sums.turn, columns_done, lambda: None,
    )
    scaling = HEAD_DIM ** (-0.5)
    mask = causal(2 * half)
    lane = lax.broadcasted_iota(jnp.int32, (half, LANES), 1)
    keys_t = k_ref[...].astype(jnp.float32).T.astype(jnp.bfloat16)
    for pair in reversed(range(pairs)):
        q = q_ref[pl.ds(pair * 4 * half, 4 * half), :]
        firsts, seconds = [], []
        for part in range(2):
            s = 2 * pair + part
            side = 0 if s < pairs else 1
            piece_of = agrad[holder[s] if s < pairs else holder[2 * pairs - 1 - s]].astype(jnp.float32)
            left = piece_of[side * half : (side + 1) * half]
            tail = piece_of[2 * half :]
            right = tail if side == 0 else pltpu.roll(tail, 64, 1)
            firsts.append(jnp.where(lane < half, left, 0.0))
            seconds.append(
                jnp.where(lane < half, pltpu.roll(jnp.where(lane < half, right, left), LANES - half, 1), 0.0)
            )
        grads = jnp.concatenate(firsts + seconds, axis=0)
        delta = jnp.sum(grads.T * att_ref[pl.ds(pair * LANES, LANES), :], axis=0, keepdims=True)
        grads = grads.astype(jnp.bfloat16)
        before = pair * 2 * half
        cuts = [(before, 2 * half)] + [(at, min(768, before - at)) for at in range(0, before, 768)]
        dq_t = None
        for at, count in cuts:
            keys = pl.ds(at, count)
            weights = jnp.exp(nt(k_ref[keys, :], q) * scaling - lse_ref[pl.ds(pair, 1), :])
            if at == before:
                weights = jnp.where(mask, weights, 0.0)
            dp = nt(v_ref[keys, :], grads)
            ds = (weights * (dp - delta)).astype(jnp.bfloat16)
            dk = nn(ds, q) * scaling
            dv = nn(weights.astype(jnp.bfloat16), grads)
            if pair == pairs - 1:
                dk_ref[keys, :] = dk
                dv_ref[keys, :] = dv
            else:
                dk_ref[keys, :] += dk
                dv_ref[keys, :] += dv
            term = nn(keys_t[:, at : at + count], ds)
            dq_t = term if dq_t is None else dq_t + term
        dq = dq_t.T * scaling
        for part in range(2):
            cosine, sine = wave(turn_ref[2 * pair + part])
            for head in range(2):
                z = dq[(2 * head + part) * half : (2 * head + part + 1) * half]
                pg_sorted[2 * pair + part, :, head * LANES : (head + 1) * LANES] = (
                    z * cosine - pltpu.roll(z, 64, 1) * sine
                ).astype(jnp.bfloat16)
        steps.next()
    for s in range(2 * pairs):
        spot = pl.ds(s * half, half)
        cosine, sine = wave(turn_ref[s])
        z = dk_ref[spot, :]
        pg_sorted[s, :, 2 * LANES : 3 * LANES] = (z * cosine - pltpu.roll(z, 64, 1) * sine).astype(jnp.bfloat16)
        pg_sorted[s, :, 3 * LANES :] = dv_ref[spot, :].astype(jnp.bfloat16)

    loads[11].wait()
    loads[12].wait()
    shard = gu_g.shape[1]

    def qkv_block(t, carry):
        left = normed_in[:, :, pl.ds(pl.multiple_of(t * shard, shard), shard)].reshape(length, shard)
        qkv_g[t] = tn(left, pg_sorted[...].reshape(length, 4 * LANES)).astype(jnp.bfloat16)
        return carry

    sums_done()
    lax.fori_loop(0, 4, qkv_block, 0)
    qkv_z.start()
    gu_z.step2()
    pl.semaphore_wait(free, 3)
    grads = Reduce(place, mine, theirs, first, out, second, reduce_sem)

    def chunk(i):
        at = early_ref[flip(place, i)]
        rows_of = jnp.concatenate([pg_sorted[at], pg_sorted[2 * pairs - 1 - at]], axis=0)
        return nt(rows_of, qkv_w[...].reshape(width, -1))

    def push(k, carry):
        theirs[k] = chunk(2 * k + 1).astype(jnp.bfloat16)
        grads.push(k)
        return carry

    def keep(k, carry):
        mine[k] = chunk(2 * k)
        return carry

    lax.fori_loop(0, 4, push, 0)
    lax.fori_loop(0, 4, keep, 0)
    grads.across()
    grads.beside()
    loads[14].wait()
    loads[15].wait()

    def out_block(src, carry):
        heads = low_in[src, :, pl.ds(0, rows), :].reshape(length, LANES)
        tails = low_in[src, :, pl.ds(rows, half), :].reshape(length // 2, LANES)
        upper = tn(heads, mcols[...].reshape(length, rows))
        from_a = tn(tails, mcols[:, pl.ds(0, half), :].reshape(length // 2, rows))
        from_b = tn(tails, mcols[:, pl.ds(half, half), :].reshape(length // 2, rows))
        at = pl.multiple_of((src % 2) * rows, rows)
        out_g[src // 2, pl.ds(at, LANES), :] = upper.astype(jnp.bfloat16)
        out_g[src // 2, pl.ds(pl.multiple_of(at + LANES, 64), 64), :] = (from_a[:64] + from_b[64:]).astype(jnp.bfloat16)
        return carry

    lax.fori_loop(0, 8, out_block, 0)
    out_z.start()
    grads.turn()
    gu_z.total()
    gus.start()
    gain_sum[...] = jnp.zeros_like(gain_sum)

    def norm_back(part, normed_grad):
        x = tok[part, :].astype(jnp.float32)
        factor = lax.rsqrt(jnp.mean(x * x, axis=-1, keepdims=True) + epsilon)
        unit = x * factor
        gain_sum[...] += jnp.sum(normed_grad * unit, axis=0, keepdims=True)
        scaled = normed_grad * gain[...]
        inner = jnp.mean(scaled * unit, axis=-1, keepdims=True)
        grad[part, :] = grad[part, :] + factor * (scaled - unit * inner)

    qkv_z.step1()
    grads.total(norm_back)
    gain_grad = gain_sum[...]
    count = mine_gain.shape[0] // 2
    for at in range(count):
        mine_gain[pl.ds(at, 1), :] = gain_grad[:, at * shard : (at + 1) * shard]
        mine_gain[pl.ds(count + at, 1), :] = ffn_gain[:, at * shard : (at + 1) * shard]
    ctx_sum = Share(place, mine_gain, ctx_gain, gain_sem)
    ctx_sum.start()
    gus.relay()
    qkv_z.step2()
    out_z.step1()
    ctx_sum.finish()
    plane_sum[...] = jnp.sum(ctx_gain[...], axis=0)
    planes = PlaneShare(place, plane_sum, plane_gain, plane_sem)
    planes.start()
    out_z.step2()
    qkv_z.total()
    gus.rest()
    qkvs = Gather(place, qkv_z.own(), qkv_all, qkv_cs)
    qkvs.start()
    out_z.total()
    outs = Gather(place, out_z.own(), out_all, out_cs)
    qkvs.relay()
    outs.start()
    qkvs.rest()
    outs.relay()
    outs.rest()
    planes.finish()
    gains[...] = jnp.sum(plane_gain[...], axis=0)
    gus.partner()
    qkvs.partner()
    outs.partner()
    for move in (gu_z, out_z, qkv_z, downs, gus, outs, qkvs, grads):
        move.finish()


def back_moves(early, tok, gain, ffn_gain, down_sum, *moved):
    n, planes = lax.axis_size("ctx"), lax.axis_size("fsdp")
    rows, width = tok.shape
    length = n * rows
    shard = width // planes
    bf, f32 = jnp.bfloat16, jnp.float32
    shape = jax.ShapeDtypeStruct
    dma = pltpu.SemaphoreType.DMA
    halves = pltpu.VMEM((6, rows // 2, width), bf)
    quads = pltpu.VMEM((4, rows, width), bf)
    small = (2 * planes, shard)
    parts = (moved[0].shape[1:], (shard, rows), (shard, 4 * LANES))
    ring = dma((2, Gather.sems))
    return pl.pallas_call(
        back_moves_kernel,
        out_shape=(shape((rows, width), f32), shape((rows, width), bf), shape(small, f32))
        + tuple(shape((n,) + part, bf) for part in (down_sum.shape,) + parts),
        in_specs=[pl.BlockSpec(memory_space=pltpu.SMEM)] + vm(4) + anywhere(len(moved)),
        out_specs=vm(3) + anywhere(4),
        scratch_shapes=[pltpu.VMEM(x.shape, x.dtype) for at, x in enumerate(moved) if at != 1]
        + [pltpu.VMEM((planes,) + part, bf) for part in parts[1:]]
        + [pltpu.VMEM((planes + 1,) + part, bf) for part in parts]
        + [
            pltpu.VMEM((4, rows, width), f32), quads, quads, halves, halves,
            pltpu.VMEM((length, LANES), f32), pltpu.VMEM((length, LANES), f32), pltpu.VMEM((16, 96, 4 * LANES), bf),
            pltpu.VMEM((n, rows, rows), bf),
            pltpu.VMEM((1, width), f32), pltpu.VMEM(small, f32), pltpu.VMEM((n,) + small, f32),
            pltpu.VMEM(small, f32), pltpu.VMEM((planes,) + small, f32),
            pltpu.SemaphoreType.REGULAR, dma((16,)), dma((2, Reduce.sems)), dma((2, Reduce.sems)),
            dma((2, 5)), dma((2, 5)), dma((2, 5)), ring, ring, ring, ring, dma((2, n)), dma((2, planes)),
        ],
        compiler_params=pltpu.CompilerParams(collective_id=6, has_side_effects=True, vmem_limit_bytes=67043328),
        name="back_moves",
    )(early, tok, gain, ffn_gain, down_sum, *moved)


def pack_kernel(down, gu, out, qkv, grad, result, down_o, gu_o, out_o, qkv_o, grad_o, result_o):
    devices, rows = gu.shape[0], gu.shape[1]
    f32 = jnp.float32
    lane = lax.broadcasted_iota(jnp.int32, (rows, LANES), 1)
    half = HEAD_DIM // 2
    down_o[...] = down[0].astype(f32)
    grad_o[...] = grad[...]
    result_o[...] = result[...]
    tiles = gu_o.shape[0] // rows
    spans = gu.shape[2] // (2 * LANES)
    for c in range(devices):
        for s in range(2):
            for z in range(spans):
                piece = gu[c, :, (s * spans + z) * LANES : (s * spans + z + 1) * LANES].astype(f32)
                gu_o[pl.ds((z * devices + c) * 2 + s, rows, stride=tiles), :] = piece

    def head(c, at, halves):
        x = qkv[c, :, at * LANES : (at + 1) * LANES].astype(f32)
        return jnp.where(lane < half, x, pltpu.roll(x, LANES - 64 + half, 1)) if halves else x

    def store(at, heads):
        second, third, fourth = pltpu.roll(heads[1], 96, 1), pltpu.roll(heads[2], 64, 1), pltpu.roll(heads[3], 32, 1)
        qkv_o[:, at : at + LANES] = jnp.where(lane < 96, heads[0], second)
        qkv_o[:, at + LANES : at + 2 * LANES] = jnp.where(lane < 64, second, third)
        qkv_o[:, at + 2 * LANES : at + 3 * LANES] = jnp.where(lane < 32, third, fourth)

    for c in range(0, devices, 2):
        store(c * 192, [head(c + i // 2, i % 2, True) for i in range(4)])
    for c in range(0, devices, 4):
        store(HEADS * HEAD_DIM + c * 96, [head(c + i, 2, True) for i in range(4)])
        store((HEADS + KV_HEADS) * HEAD_DIM + c * 96, [head(c + i, 3, False) for i in range(4)])
    for c in range(0, devices, 2):
        at = c * 192
        first = out[c].astype(f32)
        second = out[c + 1].astype(f32)
        tail = jnp.concatenate([first[:, LANES:], jnp.zeros((rows, 64), f32)], axis=1)
        next_tail = jnp.concatenate([second[:, LANES:], jnp.zeros((rows, 64), f32)], axis=1)
        turned = pltpu.roll(second[:, :LANES], 64, 1)
        out_o[:, at : at + LANES] = first[:, :LANES]
        out_o[:, at + LANES : at + 2 * LANES] = jnp.where(lane < 64, tail, turned)
        out_o[:, at + 2 * LANES : at + 3 * LANES] = jnp.where(lane < 64, turned, pltpu.roll(next_tail, 64, 1))


def pack(down, gu, out, qkv, grad, result):
    n, shard = gu.shape[0], gu.shape[1]
    rows = shard // n
    width = down.shape[2]
    f32 = jnp.float32
    spec = pl.BlockSpec
    shape = jax.ShapeDtypeStruct
    tiles = n * gu.shape[2] // LANES
    quarter = grad.shape[0] // 4
    return pl.pallas_call(
        pack_kernel,
        grid=(n,),
        out_shape=(
            shape((n * down.shape[1], width), f32), shape((shard * tiles, LANES), f32), shape((shard, n * out.shape[2]), f32),
            shape((shard, (HEADS + 2 * KV_HEADS) * HEAD_DIM), f32), shape(grad.shape, f32), shape(result.shape, result.dtype),
        ),
        in_specs=[
            spec((1,) + down.shape[1:], lambda i: (i, 0, 0)), spec((n, rows, gu.shape[2]), lambda i: (0, i, 0)),
            spec((n, rows, out.shape[2]), lambda i: (0, i, 0)), spec((n, rows, qkv.shape[2]), lambda i: (0, i, 0)),
            spec((quarter, width), lambda i: (i // 2, 0)), spec((quarter, width), lambda i: (i // 2, 0)),
        ],
        out_specs=[
            spec((down.shape[1], width), lambda i: (i, 0)), spec((rows * tiles, LANES), lambda i: (i, 0)),
            spec((rows, n * out.shape[2]), lambda i: (i, 0)), spec((rows, (HEADS + 2 * KV_HEADS) * HEAD_DIM), lambda i: (i, 0)),
            spec((quarter, width), lambda i: (i // 2, 0)), spec((quarter, width), lambda i: (i // 2, 0)),
        ],
        name="pack",
    )(down, gu, out, qkv, grad, result)


def fast_body(
    tokens, positions, qkv_weight, out_weight, gate_up_weight, down_weight, attn_gain, ffn_gain, cotangent
):
    me = lax.axis_index("ctx")
    n = lax.axis_size("ctx")
    planes = lax.axis_size("fsdp")
    rows = tokens.shape[1]
    length = n * rows
    width = tokens.shape[2]
    wide = down_weight.shape[1] * planes
    own = wide // n
    piece = own // planes
    shard = qkv_weight.shape[1]
    query_width = HEADS * HEAD_DIM
    key_width = KV_HEADS * HEAD_DIM
    cut = lax.dynamic_slice_in_dim

    qkv = qkv_weight[0]
    q_part = cut(qkv, me * 2 * HEAD_DIM, 2 * HEAD_DIM, 1)
    k_part = cut(qkv, query_width + me * HEAD_DIM, HEAD_DIM, 1)
    v_part = cut(qkv, query_width + key_width + me * HEAD_DIM, HEAD_DIM, 1)
    half = HEAD_DIM // 2
    gap = jnp.zeros((shard, 64 - half), qkv.dtype)
    columns = []
    for part in (q_part[:, :HEAD_DIM], q_part[:, HEAD_DIM:], k_part):
        columns += [part[:, :half], gap, part[:, half:], gap]
    qkv_own = jnp.concatenate(columns + [v_part, gap, gap], axis=1)
    out_own = cut(out_weight[0], me * (shard // n), shard // n, 0)
    pieces = [cut(gate_up_weight[0], at * (wide // planes) + me * piece, piece, 2) for at in range(planes)]
    gate_up_own = jnp.concatenate([x[:, s] for s in range(2) for x in pieces], axis=1)
    down_own = cut(down_weight[0], me * piece, piece, 0)
    gains = jnp.concatenate([attn_gain, ffn_gain, jnp.zeros((6, shard), attn_gain.dtype)], axis=0).astype(jnp.float32)
    spot = jnp.full((8, LANES), positions[0, 0] // (rows // 2), jnp.int32)
    turns = table(length)
    turns = turns.reshape(2 * n, rows // 2, LANES)
    (
        middle_grad, ffn_partial, spots, gains, down_sum, hidden, qkv_block, down_block, q, k, v, att, lse, middle,
        normed, attended_grad, low_all, gate_up_grad, middle_cols,
    ) = front_moves(
        tokens[0], cotangent[0].astype(jnp.bfloat16), spot, gains, qkv_own, out_own, gate_up_own, down_own, turns,
        cotangent[0],
    )
    stream_grad, result, gain_grads, down_grad, gate_up_grad, out_grad, qkv_grad = back_moves(
        spots[:, 0, 0], tokens[0], gains[0:1], ffn_partial, down_sum,
        gate_up_grad, middle_grad, hidden, down_block, k, q, v, attended_grad, att, lse, turns, normed, middle,
        qkv_block, middle_cols, low_all,
    )
    gain_grads = gain_grads.reshape(2, planes, shard)
    gain_grads = lax.dynamic_index_in_dim(gain_grads, lax.axis_index("fsdp"), 1, keepdims=False)
    down_grad, gate_up_grad, out_grad, qkv_grad, stream_grad, result = pack(
        down_grad, gate_up_grad, out_grad, qkv_grad, stream_grad, result
    )
    gate_up_grad = gate_up_grad.reshape(shard, wide // LANES, 2, LANES).transpose(0, 2, 1, 3).reshape(shard, 2, wide)
    return (
        result[None],
        stream_grad[None],
        qkv_grad[None],
        out_grad[None],
        gate_up_grad[None],
        down_grad[None],
        gain_grads[0][None],
        gain_grads[1][None],
    )


def solution(mesh):
    split = mesh.shape["ctx"] == KV_HEADS and mesh.shape["fsdp"] == 4
    placed = (
        P("fsdp", "ctx", None),
        P("fsdp", "ctx"),
        P(None, "fsdp", None),
        P(None, "fsdp", None),
        P(None, "fsdp", None, None),
        P(None, "fsdp", None),
        P(None, "fsdp"),
        P(None, "fsdp"),
        P("fsdp", "ctx", None),
    )
    return jax.shard_map(
        fast_body if split else body,
        mesh=mesh,
        in_specs=placed,
        out_specs=(
            P("fsdp", "ctx", None),
            P("fsdp", "ctx", None),
            P(None, "fsdp", None),
            P(None, "fsdp", None),
            P(None, "fsdp", None, None),
            P(None, "fsdp", None),
            P(None, "fsdp"),
            P(None, "fsdp"),
        ),
        check_vma=False,
    )
```

```python
import jax
import jax.numpy as jnp
import numpy as np
from jax import lax
from jax.experimental import pallas as pl
from jax.experimental.pallas import tpu as pltpu
from jax.sharding import PartitionSpec as P

HEADS = 16
KV_HEADS = 8
HEAD_DIM = 96
LAYERS = 1


epsilon = 1e-05
rope_base = 100000.0


def angles(place):
    halfway = HEAD_DIM // 2
    frequency = rope_base ** (-(jnp.arange(halfway, dtype=jnp.float32) * 2.0 / HEAD_DIM))
    phases = place.astype(jnp.float32)[:, None] * frequency[None, :]
    phases = jnp.concatenate([phases, phases], axis=-1)
    return (jnp.cos(phases)[:, None, :], jnp.sin(phases)[:, None, :])


def rotate(vectors, cosine, sine):
    halfway = vectors.shape[-1] // 2
    turned = jnp.concatenate([-vectors[..., halfway:], vectors[..., :halfway]], axis=-1)
    return vectors * cosine + turned * sine


def rotate_back(grads, cosine, sine):
    halfway = grads.shape[-1] // 2
    scaled = grads * sine
    return grads * cosine + jnp.concatenate(
        [scaled[..., halfway:], -scaled[..., :halfway]], axis=-1
    )


def normalize(rows, gain):
    factor = lax.rsqrt(jnp.mean(rows * rows, axis=-1, keepdims=True) + epsilon)
    return (rows * factor * gain, factor)


def normalize_back(upstream, rows, factor, gain):
    unit_rows = rows * factor
    gain_grad = jnp.sum(upstream * unit_rows, axis=0)
    scaled = upstream * gain
    row_inner = jnp.mean(scaled * unit_rows, axis=-1, keepdims=True)
    return (factor * (scaled - unit_rows * row_inner), gain_grad)


def split_blocks(queries, keys_all, values_all, key_place):
    rows = queries.shape[0]
    half = rows // 2
    shards = key_place.shape[0] // rows
    key_blocks = keys_all.reshape(shards, 2, half, KV_HEADS, HEAD_DIM)
    value_blocks = values_all.reshape(shards, 2, half, KV_HEADS, HEAD_DIM)
    place_blocks = key_place.reshape(shards, 2, half)
    return (key_blocks, value_blocks, place_blocks)


def scores_of(queries, key_block, place_block, query_place):
    scaling = HEAD_DIM ** (-0.5)
    scores = (
        jnp.einsum("rkgd,skd->kgrs", queries, key_block, preferred_element_type=jnp.float32)
        * scaling
    )
    allowed = place_block[None, None, None, :] <= query_place[None, None, :, None]
    return (scores, allowed)


def reachable(place_block, query_place):
    return jnp.min(place_block) <= jnp.max(query_place)


def attention_forward(queries, keys_all, values_all, query_place, key_place):
    key_blocks, value_blocks, place_blocks = split_blocks(queries, keys_all, values_all, key_place)
    rows = queries.shape[0]
    half = rows // 2
    groups = HEADS // KV_HEADS
    query_spans = queries.reshape(2, half, KV_HEADS, groups, HEAD_DIM)
    place_spans = query_place.reshape(2, half)

    def sweep_max(carry, inputs):
        key_block, place_block = inputs
        updated_all = []
        for span in range(2):
            state = carry[span]
            for part in range(2):

                def live(current, span=span, part=part):
                    maximum, total = current
                    scores, allowed = scores_of(
                        query_spans[span], key_block[part], place_block[part], place_spans[span]
                    )
                    masked = jnp.where(allowed, scores, -1e30)
                    updated = jnp.maximum(maximum, jnp.max(masked, axis=-1))
                    weights_now = jnp.where(allowed, jnp.exp(masked - updated[..., None]), 0.0)
                    return (
                        updated,
                        total * jnp.exp(maximum - updated) + jnp.sum(weights_now, axis=-1),
                    )

                state = lax.cond(
                    reachable(place_block[part], place_spans[span]),
                    live,
                    lambda current: current,
                    state,
                )
            updated_all.append(state)
        return (tuple(updated_all), None)

    start_max = jnp.full((KV_HEADS, groups, half), -1e30, jnp.float32)
    start_total = jnp.zeros((KV_HEADS, groups, half), jnp.float32)
    start = ((start_max, start_total), (start_max, start_total))
    finals, unused = lax.scan(sweep_max, start, (key_blocks, place_blocks))
    logsum_spans = [finals[span][0] + jnp.log(finals[span][1]) for span in range(2)]

    def sweep_out(results, inputs):
        key_block, value_block, place_block = inputs
        updated_all = []
        for span in range(2):
            result = results[span]
            for part in range(2):

                def live(current, span=span, part=part):
                    scores, allowed = scores_of(
                        query_spans[span], key_block[part], place_block[part], place_spans[span]
                    )
                    softmax_rows = jnp.where(
                        allowed, jnp.exp(scores - logsum_spans[span][..., None]), 0.0
                    ).astype(jnp.bfloat16)
                    return current + jnp.einsum(
                        "kgrs,skd->rkgd",
                        softmax_rows,
                        value_block[part],
                        preferred_element_type=jnp.float32,
                    )

                result = lax.cond(
                    reachable(place_block[part], place_spans[span]),
                    live,
                    lambda current: current,
                    result,
                )
            updated_all.append(result)
        return (tuple(updated_all), None)

    start_out = jnp.zeros((half, KV_HEADS, groups, HEAD_DIM), jnp.float32)
    outs, unused_out = lax.scan(
        sweep_out, (start_out, start_out), (key_blocks, value_blocks, place_blocks)
    )
    logsum = jnp.concatenate(logsum_spans, axis=-1)
    attended = jnp.concatenate([outs[0], outs[1]], axis=0)
    return (logsum, attended)


def attention_backward(
    queries, keys_all, values_all, query_place, key_place, logsum, attended_grad, row_inner
):
    key_blocks, value_blocks, place_blocks = split_blocks(queries, keys_all, values_all, key_place)
    rows = queries.shape[0]
    half = rows // 2
    groups = HEADS // KV_HEADS
    scaling = HEAD_DIM ** (-0.5)
    query_spans = queries.reshape(2, half, KV_HEADS, groups, HEAD_DIM)
    place_spans = query_place.reshape(2, half)
    grad_spans = attended_grad.reshape(2, half, KV_HEADS, groups, HEAD_DIM)
    logsum_spans = logsum.reshape(KV_HEADS, groups, 2, half)
    inner_spans = row_inner.reshape(KV_HEADS, groups, 2, half)

    def sweep_back(query_grads, inputs):
        key_block, value_block, place_block = inputs
        query_grads = list(query_grads)
        key_parts = []
        value_parts = []
        for part in range(2):
            key_acc = jnp.zeros((half, KV_HEADS, HEAD_DIM), jnp.float32)
            value_acc = jnp.zeros((half, KV_HEADS, HEAD_DIM), jnp.float32)
            for span in range(2):

                def live(current, span=span, part=part):
                    query_grad, key_grad, value_grad = current
                    scores, allowed = scores_of(
                        query_spans[span], key_block[part], place_block[part], place_spans[span]
                    )
                    softmax_rows = jnp.where(
                        allowed, jnp.exp(scores - logsum_spans[:, :, span][..., None]), 0.0
                    )
                    rounded = softmax_rows.astype(jnp.bfloat16)
                    weight_grad = jnp.einsum(
                        "rkgd,skd->kgrs",
                        grad_spans[span],
                        value_block[part],
                        preferred_element_type=jnp.float32,
                    )
                    score_grad = (
                        softmax_rows * (weight_grad - inner_spans[:, :, span][..., None])
                    ).astype(jnp.bfloat16)
                    query_grad = (
                        query_grad
                        + jnp.einsum(
                            "kgrs,skd->rkgd",
                            score_grad,
                            key_block[part],
                            preferred_element_type=jnp.float32,
                        )
                        * scaling
                    )
                    key_grad = (
                        key_grad
                        + jnp.einsum(
                            "kgrs,rkgd->skd",
                            score_grad,
                            query_spans[span],
                            preferred_element_type=jnp.float32,
                        )
                        * scaling
                    )
                    value_grad = value_grad + jnp.einsum(
                        "kgrs,rkgd->skd",
                        rounded,
                        grad_spans[span],
                        preferred_element_type=jnp.float32,
                    )
                    return (query_grad, key_grad, value_grad)

                state = (query_grads[span], key_acc, value_acc)
                state = lax.cond(
                    reachable(place_block[part], place_spans[span]),
                    live,
                    lambda current: current,
                    state,
                )
                query_grads[span], key_acc, value_acc = state
            key_parts.append(key_acc)
            value_parts.append(value_acc)
        key_out = jnp.concatenate(key_parts, axis=0)
        value_out = jnp.concatenate(value_parts, axis=0)
        return (tuple(query_grads), (key_out, value_out))

    start_grad = jnp.zeros((half, KV_HEADS, groups, HEAD_DIM), jnp.float32)
    query_pair, (key_grads, value_grads) = lax.scan(
        sweep_back, (start_grad, start_grad), (key_blocks, value_blocks, place_blocks)
    )
    query_grad = jnp.concatenate([query_pair[0], query_pair[1]], axis=0)
    return (
        query_grad,
        key_grads.reshape(-1, KV_HEADS, HEAD_DIM),
        value_grads.reshape(-1, KV_HEADS, HEAD_DIM),
    )


def fetch_layer(qkv_weight, out_weight, gate_up_weight, down_weight, attn_gain, ffn_gain, layer_id):
    return (
        lax.all_gather(qkv_weight[layer_id], "fsdp", axis=0, tiled=True),
        lax.all_gather(out_weight[layer_id], "fsdp", axis=0, tiled=True),
        lax.all_gather(gate_up_weight[layer_id], "fsdp", axis=0, tiled=True),
        lax.all_gather(down_weight[layer_id], "fsdp", axis=0, tiled=True),
        lax.all_gather(attn_gain[layer_id], "fsdp", axis=0, tiled=True),
        lax.all_gather(ffn_gain[layer_id], "fsdp", axis=0, tiled=True),
    )


def fetch_again(qkv_weight, out_weight, gate_up_weight, down_weight, attn_gain, ffn_gain, layer_id):
    return (
        lax.all_gather(qkv_weight[layer_id], "fsdp", axis=0, tiled=True),
        lax.all_gather(out_weight[layer_id], "fsdp", axis=0, tiled=True),
        lax.all_gather(gate_up_weight[layer_id], "fsdp", axis=0, tiled=True),
        lax.all_gather(down_weight[layer_id], "fsdp", axis=0, tiled=True),
        lax.all_gather(attn_gain[layer_id], "fsdp", axis=0, tiled=True),
        lax.all_gather(ffn_gain[layer_id], "fsdp", axis=0, tiled=True),
    )


def forward_layer(stream, query_place, key_place, gathered):
    qkv_full, out_full, gate_up_full, down_full, attn_full, ffn_full = gathered
    rows = stream.shape[0]
    groups = HEADS // KV_HEADS
    query_width = HEADS * HEAD_DIM
    key_width = KV_HEADS * HEAD_DIM
    cosine, sine = angles(query_place)
    normed, first_factor = normalize(stream, attn_full.astype(jnp.float32))
    normed = normed.astype(jnp.bfloat16)
    projected = jnp.dot(normed, qkv_full, preferred_element_type=jnp.float32)
    queries = rotate(projected[:, :query_width].reshape(rows, HEADS, HEAD_DIM), cosine, sine)
    queries = queries.reshape(rows, KV_HEADS, groups, HEAD_DIM).astype(jnp.bfloat16)
    keys_local = rotate(
        projected[:, query_width : query_width + key_width].reshape(rows, KV_HEADS, HEAD_DIM),
        cosine,
        sine,
    ).astype(jnp.bfloat16)
    values_local = (
        projected[:, query_width + key_width :]
        .reshape(rows, KV_HEADS, HEAD_DIM)
        .astype(jnp.bfloat16)
    )
    keys_all, values_all = (
        lax.all_gather(keys_local, "ctx", axis=0, tiled=True),
        lax.all_gather(values_local, "ctx", axis=0, tiled=True),
    )
    logsum, attended = attention_forward(queries, keys_all, values_all, query_place, key_place)
    attended_low = attended.reshape(rows, query_width).astype(jnp.bfloat16)
    middle = stream + jnp.dot(attended_low, out_full, preferred_element_type=jnp.float32)
    second, second_factor = normalize(middle, ffn_full.astype(jnp.float32))
    second = second.astype(jnp.bfloat16)
    gate_up = jnp.einsum("rd,dcf->rcf", second, gate_up_full, preferred_element_type=jnp.float32)
    hidden = (jax.nn.silu(gate_up[:, 0]) * gate_up[:, 1]).astype(jnp.bfloat16)
    result = middle + jnp.dot(hidden, down_full, preferred_element_type=jnp.float32)
    stored = (
        stream,
        first_factor,
        normed,
        queries,
        keys_local,
        values_local,
        keys_all,
        values_all,
        logsum,
        attended,
        attended_low,
        middle,
        second_factor,
        second,
        gate_up,
        hidden,
    )
    return (result, stored)


def backward_layer(upstream, stored, gathered, query_place, key_place, keys_all, values_all):
    (
        stream,
        first_factor,
        normed,
        queries,
        keys_local,
        values_local,
        kept_keys,
        kept_values,
        logsum,
        attended,
        attended_low,
        middle,
        second_factor,
        second,
        gate_up,
        hidden,
    ) = stored
    qkv_full, out_full, gate_up_full, down_full, attn_full, ffn_full = gathered
    rows = stream.shape[0]
    groups = HEADS // KV_HEADS
    cosine, sine = angles(query_place)
    upstream_low = upstream.astype(jnp.bfloat16)
    hidden_grad = jnp.einsum(
        "rd,fd->rf", upstream_low, down_full, preferred_element_type=jnp.float32
    )
    gate_part = gate_up[:, 0]
    up_part = gate_up[:, 1]
    sigmoid = jax.nn.sigmoid(gate_part)
    gate_grad = hidden_grad * up_part * sigmoid * (1.0 + gate_part * (1.0 - sigmoid))
    up_grad = hidden_grad * gate_part * sigmoid
    gate_up_low = jnp.stack([gate_grad, up_grad], axis=1).astype(jnp.bfloat16)
    second_grad = jnp.einsum(
        "rcf,dcf->rd", gate_up_low, gate_up_full, preferred_element_type=jnp.float32
    )
    middle_grad, ffn_gain_grad = normalize_back(
        second_grad, middle, second_factor, ffn_full.astype(jnp.float32)
    )
    middle_grad = middle_grad + upstream
    middle_low = middle_grad.astype(jnp.bfloat16)
    attended_grad = jnp.einsum(
        "rd,od->ro", middle_low, out_full, preferred_element_type=jnp.float32
    )
    attended_grad = attended_grad.astype(jnp.bfloat16).reshape(rows, KV_HEADS, groups, HEAD_DIM)
    row_inner = jnp.einsum("rkgd,rkgd->kgr", attended_grad.astype(jnp.float32), attended)
    query_grad, key_grads, value_grads = attention_backward(
        queries, keys_all, values_all, query_place, key_place, logsum, attended_grad, row_inner
    )
    key_grad, value_grad = (
        lax.psum_scatter(key_grads, "ctx", scatter_dimension=0, tiled=True),
        lax.psum_scatter(value_grads, "ctx", scatter_dimension=0, tiled=True),
    )
    query_grad = rotate_back(query_grad.reshape(rows, HEADS, HEAD_DIM), cosine, sine)
    key_grad = rotate_back(key_grad, cosine, sine)
    projected_grad = jnp.concatenate(
        [query_grad.reshape(rows, -1), key_grad.reshape(rows, -1), value_grad.reshape(rows, -1)],
        axis=1,
    ).astype(jnp.bfloat16)
    normed_grad = jnp.einsum(
        "re,de->rd", projected_grad, qkv_full, preferred_element_type=jnp.float32
    )
    stream_grad, attn_gain_grad = normalize_back(
        normed_grad, stream, first_factor, attn_full.astype(jnp.float32)
    )
    stream_grad = stream_grad + middle_grad
    qkv_grad = jnp.einsum("rd,re->de", normed, projected_grad, preferred_element_type=jnp.float32)
    out_grad = jnp.einsum("ro,rd->od", attended_low, middle_low, preferred_element_type=jnp.float32)
    gate_up_grad = jnp.einsum(
        "rd,rcf->dcf", second, gate_up_low, preferred_element_type=jnp.float32
    )
    down_grad = jnp.einsum("rf,rd->fd", hidden, upstream_low, preferred_element_type=jnp.float32)
    sharded = (
        lax.psum_scatter(qkv_grad, "fsdp", scatter_dimension=0, tiled=True),
        lax.psum_scatter(out_grad, "fsdp", scatter_dimension=0, tiled=True),
        lax.psum_scatter(gate_up_grad, "fsdp", scatter_dimension=0, tiled=True),
        lax.psum_scatter(down_grad, "fsdp", scatter_dimension=0, tiled=True),
        lax.psum_scatter(attn_gain_grad, "fsdp", scatter_dimension=0, tiled=True),
        lax.psum_scatter(ffn_gain_grad, "fsdp", scatter_dimension=0, tiled=True),
    )
    totals = lax.psum(
        (sharded[0], sharded[1], sharded[2], sharded[3], sharded[4], sharded[5]), "ctx"
    )
    return (stream_grad, totals)


def body(
    tokens,
    positions,
    qkv_weight,
    out_weight,
    gate_up_weight,
    down_weight,
    attn_gain,
    ffn_gain,
    cotangent,
):
    query_place = positions[0]
    key_place = lax.all_gather(query_place, "ctx", axis=0, tiled=True)
    stream = tokens[0].astype(jnp.float32)
    gathered_list = []
    layer_id = 0
    gathered = fetch_layer(
        qkv_weight, out_weight, gate_up_weight, down_weight, attn_gain, ffn_gain, layer_id
    )
    stream, stored = forward_layer(stream, query_place, key_place, gathered)
    saved = [stored]
    gathered_list.append(gathered)
    activations = stream.astype(jnp.bfloat16)[None]
    upstream = cotangent[0]
    layer_grads = [None] * LAYERS
    for layer_id in reversed(range(LAYERS)):
        stored = saved[layer_id]
        gathered = fetch_again(
            qkv_weight, out_weight, gate_up_weight, down_weight, attn_gain, ffn_gain, layer_id
        )
        keys_all, values_all = (stored[6], stored[7])
        upstream, totals = backward_layer(
            upstream, stored, gathered, query_place, key_place, keys_all, values_all
        )
        layer_grads[layer_id] = totals
    outputs = [jnp.stack([entry[slot] for entry in layer_grads], axis=0) for slot in range(6)]
    return (
        activations,
        upstream[None],
        outputs[0],
        outputs[1],
        outputs[2],
        outputs[3],
        outputs[4],
        outputs[5],
    )


LANES = 128


def spread(heads):
    half = HEAD_DIM // 2
    pad = ((0, 0), (0, 0), (0, 64 - half))
    return jnp.concatenate([jnp.pad(heads[..., :half], pad), jnp.pad(heads[..., half:], pad)], axis=-1)


def gathered_spread(padded):
    half = HEAD_DIM // 2
    return jnp.concatenate([padded[..., :half], padded[..., 64 : 64 + half]], axis=-1)


def turn_parts(spans, rows):
    half = HEAD_DIM // 2
    frequency = rope_base ** (-(np.arange(half, dtype=np.float64) * 2.0 / HEAD_DIM))

    def waves(place):
        phases = place[:, None] * frequency[None, :]
        pad = ((0, 0), (0, 64 - half))
        return np.pad(np.cos(phases), pad), np.pad(np.sin(phases), pad)

    cosine, sine = waves(np.arange(spans) * float(rows))
    parts = (
        np.concatenate([cosine, cosine], axis=1), np.concatenate([-sine, sine], axis=1),
        np.concatenate(waves(np.arange(rows, dtype=np.float64)), axis=1),
    )
    return tuple(jnp.asarray(part, jnp.float32) for part in parts)


def spread_heads(proj):
    lane = lax.broadcasted_iota(jnp.int32, (proj.shape[0], LANES), 1)
    tiles = [proj[:, at * LANES : (at + 1) * LANES] for at in range(3)]

    def put(*pieces):
        out = jnp.zeros_like(tiles[0])
        for tile, source, target, count in pieces:
            shift = (target - source) % LANES
            moved = pltpu.roll(tiles[tile], shift, 1) if shift else tiles[tile]
            out = jnp.where(jnp.logical_and(lane >= target, lane < target + count), moved, out)
        return out

    return (
        put((0, 0, 0, 48), (0, 48, 64, 48)),
        put((0, 96, 0, 32), (1, 0, 32, 16), (1, 16, 64, 48)),
        put((1, 64, 0, 48), (1, 112, 64, 16), (2, 0, 80, 32)),
        put((2, 32, 0, 96)),
    )


def close_halves(head):
    lane = lax.broadcasted_iota(jnp.int32, head.shape, 1)
    return jnp.where(lane < HEAD_DIM // 2, head, pltpu.roll(head, LANES - 64 + HEAD_DIM // 2, 1))


def wave(rows):
    first = lax.broadcasted_iota(jnp.int32, rows.shape, 1) < 64
    other = pltpu.roll(rows, 64, 1)
    return jnp.where(first, rows, other), jnp.where(first, -other, rows)


def nt(left, right):
    return lax.dot_general(left, right, (((1,), (1,)), ((), ())), preferred_element_type=jnp.float32)


def nn(left, right):
    return lax.dot_general(left, right, (((1,), (0,)), ((), ())), preferred_element_type=jnp.float32)


def tn(left, right):
    return lax.dot_general(left, right, (((0,), (0,)), ((), ())), preferred_element_type=jnp.float32)


def causal(width):
    key_at = lax.broadcasted_iota(jnp.int32, (width, 2 * width), 0)
    query_at = lax.broadcasted_iota(jnp.int32, (width, 2 * width), 1)
    query_at = jnp.where(query_at >= width, query_at - width, query_at)
    return key_at <= query_at


def vm(count):
    return [pl.BlockSpec(memory_space=pltpu.VMEM)] * count


MESH = pl.DeviceIdType.MESH


class Place:
    def __init__(self):
        self.me = lax.axis_index("ctx")
        core, x, y = self.me % 2, (self.me // 2) % 2, self.me // 4
        self.dp, self.dx, self.dy = 1 - 2 * core, 2 - 4 * x, 4 - 8 * y
        self.p, self.x, self.y = self.me + self.dp, self.me + self.dx, self.me + self.dy
        self.d = self.x + self.dy
        self.z = lax.axis_index("fsdp")
        self.planes = lax.axis_size("fsdp")
        self.n = lax.axis_size("ctx")


def greet(place, ctx=True, planes=False):
    barrier = pltpu.get_barrier_semaphore()
    count = 0
    if ctx:
        for step in range(1, place.n):
            pl.semaphore_signal(
                barrier, inc=1, device_id={"ctx": lax.rem(place.me + step, place.n)}, device_id_type=MESH
            )
            count += 1
    if planes:
        for step in range(1, place.planes):
            pl.semaphore_signal(
                barrier, inc=1, device_id={"fsdp": lax.rem(place.z + step, place.planes)}, device_id_type=MESH
            )
            count += 1
    pl.semaphore_wait(barrier, count)


def send(source, target, send_sem, recv_sem, **where):
    return pltpu.make_async_remote_copy(
        src_ref=source, dst_ref=target, send_sem=send_sem, recv_sem=recv_sem,
        device_id=where, device_id_type=MESH,
    )


class Gather:
    sems = 14

    def __init__(self, place, own, out, sem):
        self.place, self.own, self.out, self.sem = place, own, out, sem
        self.half = out.shape[1] // 2
        self.started = []
        self.met = False

    def go(self, source, target, index, rank):
        send(source, target, self.sem.at[0, index], self.sem.at[1, index], ctx=rank).start()
        self.started.append(index)

    def whole_block(self, index):
        return index == 6

    def sent(self):
        p = self.place
        for index in self.started:
            part = self.whole(p.me) if self.whole_block(index) else self.part(p.me, 0)
            send(part, part, self.sem.at[0, index], self.sem.at[1, index], ctx=p.p).wait_send()

    def part(self, rank, half):
        return self.out.at[rank, pl.ds(half * self.half, self.half)]

    def whole(self, rank):
        return self.out.at[rank]

    def start(self):
        p = self.place
        keep = pltpu.make_async_copy(self.own, self.whole(p.me), self.sem.at[0, 13])
        keep.start()
        self.keep = keep
        halves = [self.own.at[pl.ds(h * self.half, self.half)] for h in range(2)]
        self.go(halves[0], self.part(p.me, 0), 0, p.x)
        self.go(halves[1], self.part(p.me, 1), 3, p.y)
        self.go(self.own, self.whole(p.me), 6, p.p)
        self.go(halves[1], self.part(p.me, 1), 1, p.x)
        self.go(halves[0], self.part(p.me, 0), 2, p.y)

    def arrived(self, rank, half, index):
        part = self.part(rank, half)
        pltpu.make_async_copy(part, part, self.sem.at[1, index]).wait()
        return part

    def relay(self):
        p = self.place
        part = self.arrived(p.x, 0, 0)
        self.go(part, part, 4, p.y)
        self.go(part, part, 7, p.p)
        part = self.arrived(p.y, 1, 3)
        self.go(part, part, 5, p.x)
        self.go(part, part, 10, p.p)

    def rest(self):
        p = self.place
        for rank, half, index, onward in ((p.x, 1, 1, 8), (p.y, 0, 2, 9), (p.d, 0, 4, 11), (p.d, 1, 5, 12)):
            part = self.arrived(rank, half, index)
            self.go(part, part, onward, p.p)

    def first_partner(self):
        part = self.whole(self.place.p)
        pltpu.make_async_copy(part, part, self.sem.at[1, 6]).wait()
        self.met = True

    def partner(self):
        p = self.place
        if not self.met:
            self.first_partner()
        for rank, half, index in (
            (p.x, 0, 7), (p.y, 1, 10), (p.x, 1, 8), (p.y, 0, 9), (p.d, 0, 11), (p.d, 1, 12),
        ):
            self.arrived(rank + p.dp, half, index)

    def finish(self, kept=False):
        if not kept:
            self.keep.wait()
        self.sent()


class PlaneGather:
    def __init__(self, place, own, out, sem):
        self.place, self.own, self.out, self.sem = place, own, out, sem

    def hop(self, step, up):
        p = self.place
        sign = 1 if up else -1
        source = p.z - sign * step
        target = p.z + sign
        ok = jnp.logical_and(
            jnp.logical_and(source >= 0, source < p.planes),
            jnp.logical_and(target >= 0, target < p.planes),
        )
        source = jnp.clip(source, 0, p.planes - 1)
        target = jnp.clip(target, 0, p.planes - 1)
        block = self.own if step == 0 else self.out.at[source]
        return ok, send(
            block, self.out.at[source], self.sem.at[0 if up else 1, source], self.sem.at[2, source], fsdp=target
        )

    def start(self):
        p = self.place
        self.keep = pltpu.make_async_copy(self.own, self.out.at[p.z], self.sem.at[2, p.z])
        self.keep.start()
        for up in (True, False):
            ok, copy = self.hop(0, up)
            pl.when(ok)(copy.start)

    def got(self, step, up):
        p = self.place
        source = p.z - step if up else p.z + step
        ok = jnp.logical_and(source >= 0, source < p.planes)
        source = jnp.clip(source, 0, p.planes - 1)
        part = self.out.at[source]
        return ok, pltpu.make_async_copy(part, part, self.sem.at[2, source])

    def step(self, number):
        for up in (True, False):
            ok, copy = self.got(number, up)
            pl.when(ok)(copy.wait)
            if number < self.place.planes - 1:
                ok, copy = self.hop(number, up)
                pl.when(ok)(copy.start)

    def finish(self, kept=False):
        if not kept:
            self.keep.wait()
        for number in range(self.place.planes - 1):
            for up in (True, False):
                ok, copy = self.hop(number, up)
                pl.when(ok)(copy.wait_send)


class Exchange:
    def __init__(self, place, blocks, out, sem):
        self.place, self.blocks, self.out, self.sem = place, blocks, out, sem

    def pick(self, rank):
        return self.blocks.at[rank]

    def copy(self, step):
        p = self.place
        rank = lax.rem(p.me + step, p.n)
        return send(self.pick(rank), self.out.at[p.me], self.sem.at[0, step], self.sem.at[1, step], ctx=rank)

    def start(self):
        p = self.place
        for step in range(1, p.n):
            self.copy(step).start()
        self.keep = pltpu.make_async_copy(self.pick(p.me), self.out.at[p.me], self.sem.at[0, 0])
        self.keep.start()

    def finish(self):
        p = self.place
        self.keep.wait()
        for step in range(1, p.n):
            self.copy(step).wait_send()
        for step in range(1, p.n):
            part = self.out.at[lax.rem(p.me + p.n - step, p.n)]
            pltpu.make_async_copy(part, part, self.sem.at[1, step]).wait()


class Share(Exchange):
    def pick(self, rank):
        return self.blocks


class PlaneShare:
    def __init__(self, place, block, out, sem):
        self.place, self.block, self.out, self.sem = place, block, out, sem

    def copy(self, step):
        p = self.place
        plane = lax.rem(p.z + step, p.planes)
        return send(self.block, self.out.at[p.z], self.sem.at[0, step], self.sem.at[1, step], fsdp=plane)

    def start(self):
        p = self.place
        for step in range(1, p.planes):
            self.copy(step).start()
        self.keep = pltpu.make_async_copy(self.block, self.out.at[p.z], self.sem.at[0, 0])
        self.keep.start()

    def finish(self):
        p = self.place
        self.keep.wait()
        for step in range(1, p.planes):
            self.copy(step).wait_send()
        for step in range(1, p.planes):
            part = self.out.at[lax.rem(p.z + p.planes - step, p.planes)]
            pltpu.make_async_copy(part, part, self.sem.at[1, step]).wait()


def anywhere(count):
    return [pl.BlockSpec(memory_space=pl.ANY)] * count


class Reduce:
    sems = 10

    def __init__(self, place, mine, theirs, first, out, second, sem):
        self.place, self.mine, self.theirs, self.first, self.out, self.second, self.sem = (
            place, mine, theirs, first, out, second, sem
        )
        self.half = out.shape[1]
        self.started = []

    def push(self, slot):
        copy = send(
            self.theirs.at[slot], self.first.at[slot], self.sem.at[0, slot], self.sem.at[1, slot], ctx=self.place.p
        )
        copy.start()
        return copy

    def pushed(self):
        for slot in range(4):
            send(
                self.theirs.at[slot], self.first.at[slot], self.sem.at[0, slot], self.sem.at[1, slot],
                ctx=self.place.p,
            ).wait_send()

    def add(self, slot):
        part = self.first.at[slot]
        pltpu.make_async_copy(part, part, self.sem.at[1, slot]).wait()
        self.mine[slot] = self.mine[slot] + self.first[slot].astype(jnp.float32)

    def go(self, index, value, rank):
        self.out[index] = value.astype(jnp.bfloat16)
        self.turned(index, rank).start()
        self.started.append((index, rank))

    def turned(self, index, rank):
        return send(
            self.out.at[index], self.second.at[index], self.sem.at[0, 4 + index], self.sem.at[1, 4 + index], ctx=rank
        )

    def top(self, slot):
        return self.mine[slot, pl.ds(0, self.half), :]

    def low(self, slot):
        return self.mine[slot, pl.ds(self.half, self.half), :]

    def got(self, index):
        part = self.second.at[index]
        pltpu.make_async_copy(part, part, self.sem.at[1, 4 + index]).wait()
        return self.second[index].astype(jnp.float32)

    def across(self):
        self.add(3)
        self.go(1, self.top(3), self.place.x)
        self.go(3, self.low(3), self.place.y)

    def beside(self):
        self.add(1)
        self.go(0, self.top(1), self.place.x)
        self.add(2)
        self.go(2, self.low(2), self.place.y)

    def turn(self):
        self.go(4, self.top(2) + self.got(1), self.place.y)
        self.go(5, self.low(1) + self.got(3), self.place.x)

    def total(self, use):
        self.add(0)
        use(pl.ds(0, self.half), self.top(0) + self.got(0) + self.got(4))
        use(pl.ds(self.half, self.half), self.low(0) + self.got(2) + self.got(5))

    def finish(self):
        self.pushed()
        for index, rank in self.started:
            self.turned(index, rank).wait_send()


def flip(place, i):
    return place.me + (i % 2) * place.dp + ((i // 2) % 2) * place.dx + (i // 4) * place.dy


class HalfGather(Gather):
    sems = 16

    def __init__(self, place, own, out, sem):
        self.place, self.own, self.out, self.sem = place, own, out, sem
        self.half = out.shape[1]
        self.started = []
        self.met = False

    def part(self, rank, half):
        return self.out.at[2 * rank + half]

    def whole_block(self, index):
        return False

    def start(self):
        p = self.place
        halves = [self.own.at[pl.ds(h * self.half, self.half)] for h in range(2)]
        self.kept = [
            pltpu.make_async_copy(halves[h], self.part(p.me, h), self.sem.at[0, (13, 15)[h]]) for h in range(2)
        ]
        self.go(halves[0], self.part(p.me, 0), 0, p.x)
        self.go(halves[1], self.part(p.me, 1), 3, p.y)
        self.go(halves[0], self.part(p.me, 0), 6, p.p)
        self.go(halves[1], self.part(p.me, 1), 14, p.p)
        self.go(halves[1], self.part(p.me, 1), 1, p.x)
        self.go(halves[0], self.part(p.me, 0), 2, p.y)
        for copy in self.kept:
            copy.start()

    def first_partner(self):
        for h in range(2):
            self.arrived(self.place.p, h, (6, 14)[h])
        self.met = True

    def own_in(self):
        for copy in self.kept:
            copy.wait()

    def finish(self):
        self.sent()


def packed(block):
    rows = block.shape[0] // 2
    tail = jnp.concatenate([block[:, LANES:], jnp.zeros((2 * rows, 64), block.dtype)], axis=1)
    first = lax.broadcasted_iota(jnp.int32, (rows, LANES), 1) < 64
    return jnp.concatenate([block[:, :LANES], jnp.where(first, tail[:rows], pltpu.roll(tail[rows:], 64, 1))], axis=0)


def unpacked(block):
    rows = block.shape[0] // 3
    tail = block[2 * rows :].astype(jnp.float32)
    tails = jnp.concatenate([tail, pltpu.roll(tail, 64, 1)], axis=0)[:, :64].astype(block.dtype)
    return jnp.concatenate([block[: 2 * rows], tails], axis=1)


class PlaneReduce:
    def __init__(self, place, block, recv, sem):
        self.place, self.block, self.recv, self.sem = place, block, recv, sem

    def hop(self, ok, part, slot, target, first, wait):
        copy = send(
            self.block.at[part], self.recv.at[slot], self.sem.at[0, part], self.sem.at[1, slot], fsdp=target
        )

        @pl.when(ok)
        def _():
            if wait:
                copy.wait_send()
                return
            if not first:
                self.merge(part, part)
            copy.start()

    def merge(self, part, slot):
        piece = self.recv.at[slot]
        pltpu.make_async_copy(piece, piece, self.sem.at[1, slot]).wait()
        total = self.block[part].astype(jnp.float32) + self.recv[slot].astype(jnp.float32)
        self.block[part] = total.astype(jnp.bfloat16)

    def ends(self, i, wait=False):
        z = self.place.z
        low = z == 0
        part = jnp.where(low, 3 - i, i)
        slot = part if i < 2 else jnp.where(low, part, 4)
        self.hop(jnp.logical_or(low, z == 3), part, slot, jnp.where(low, 1, 2), True, wait)

    def inner(self, up, down, slot_up, slot_down, to_up, to_down, wait=False):
        z = self.place.z
        low = z == 1
        part = jnp.where(low, up, down)
        slot = jnp.where(low, slot_up, slot_down)
        self.hop(jnp.logical_or(low, z == 2), part, slot, jnp.where(low, to_up, to_down), False, wait)

    def start(self, wait=False):
        for i in range(3):
            self.ends(i, wait)

    def step1(self, wait=False):
        self.inner(3, 0, 3, 0, 2, 1, wait)

    def step2(self, wait=False):
        self.inner(2, 1, 2, 4, 2, 1, wait)
        self.inner(0, 3, 4, 3, 0, 3, wait)

    def total(self):
        z = self.place.z

        @pl.when(z > 0)
        def _():
            self.merge(z, z)

        @pl.when(z < 3)
        def _():
            self.merge(z, 4)

    def own(self):
        return self.block.at[self.place.z]

    def finish(self):
        self.start(True)
        self.step1(True)
        self.step2(True)


class Steps:
    def __init__(self, *steps):
        self.steps = list(steps)

    def next(self, count=1):
        for step in self.steps[:count]:
            step()
        self.steps = self.steps[count:]

    def rest(self):
        self.next(len(self.steps))


class OutGather(Gather):
    def __init__(self, place, own, out, sem):
        self.place, self.own, self.out, self.sem = place, own, out, sem
        self.half = out.shape[0] // 2
        self.started = []
        self.met = False

    def part(self, rank, half):
        return self.out.at[pl.ds(half * self.half, self.half), rank]

    def whole(self, rank):
        return self.out.at[:, rank]


def front_kernel(
    tok, pos, attn_own, ffn_own, qkv_own, gu_own, far_cos, far_sin, near, out_weight, down_weight, up,
    middle_grad, gain_grad, spots, gains, down_sum,
    hidden_o, qkv_o, down_o, q_o, k_o, v_o, att_o, lse_o, middle_o, turn_o, normed, agrad, low_all, gu_out, mcols,
    hidden, qkv_w, down_w, q_ref, k_ref, v_ref, att_ref, lse_ref, middle, turn_ref, mcols_send, up_low, spot, gain_own,
    wide_in, up_all, gul, gu_w, out_block, out_w, low_sorted, gain_all, spots_s, order_s, low,
    attended, own, mine, theirs, first, out, second, down_g, down_r,
    tok_sem, up_sem, spot_sem, gain_sem, qkv_sem, out_sem, outc_sem, gu_sem, down_sem, local_sem,
    low_sem, gather_sem, reduce_sem, agrad_sem, lows_sem, down_zs, mcols_sem,
):
    place = Place()
    n = place.n
    rows = tok.shape[0]
    half = rows // 2
    pairs = 8
    heads = rows
    length = n * rows
    width = tok.shape[1]
    out_own = out_weight.at[0, pl.ds(place.me * (out_weight.shape[1] // 8), out_weight.shape[1] // 8)]
    down_own = down_weight.at[0, pl.ds(place.me * (down_weight.shape[1] // 8), down_weight.shape[1] // 8)]
    spot[...] = jnp.broadcast_to(pos[0:1, 0:1], spot.shape)
    gain_own[pl.ds(0, 1), :] = attn_own[...].astype(jnp.float32)
    gain_own[pl.ds(1, 1), :] = ffn_own[...].astype(jnp.float32)
    fetch = pltpu.make_async_copy(up, middle_grad, local_sem.at[0])
    fetch.start()
    greet(place, planes=True)
    spans = Share(place, spot, spots, spot_sem)
    scales = PlaneShare(place, gain_own, gain_all, gain_sem)
    tokens = HalfGather(place, tok, wide_in, tok_sem)
    cots = Gather(place, up_low, up_all, up_sem)
    qkvs = PlaneGather(place, qkv_own, qkv_w, qkv_sem)
    outs = PlaneGather(place, out_own, out_block, out_sem)
    outc = OutGather(place, out_block, out_w, outc_sem)
    gus = PlaneGather(place, gu_own, gu_w, gu_sem)
    downs = PlaneGather(place, down_own, down_w, down_sem)
    given = []

    def give(source, target):
        copy = pltpu.make_async_copy(source, target, local_sem.at[5 + len(given)])
        copy.start()
        given.append(copy)

    tokens.start()
    qkvs.start()
    spans.start()
    scales.start()

    def turn_rows(at, carry):
        base = near[...]
        turn_ref[at] = base * far_cos[pl.ds(at, 1), :] + pltpu.roll(base, 64, 1) * far_sin[pl.ds(at, 1), :]
        return carry

    lax.fori_loop(0, 2 * pairs, turn_rows, 0)
    give(turn_ref, turn_o)
    fetch.wait()
    up_low[...] = middle_grad[...].astype(jnp.bfloat16)
    tokens.relay()
    qkvs.step(1)
    outs.start()
    qkvs.step(2)
    tokens.rest()
    cots.start()
    outs.step(1)
    downs.start()
    qkvs.step(3)
    tokens.partner()
    tokens.own_in()
    spans.finish()
    scales.finish()
    qkvs.keep.wait()
    table = pltpu.make_async_copy(spots, spots_s, local_sem.at[1])
    table.start()
    for g in range(2):
        gains[pl.ds(g, 1), :] = jnp.concatenate([gain_all[z, pl.ds(g, 1), :] for z in range(4)], axis=1)
    table.wait()
    early = [lax.div(spots_s[j, 0, 0], half) for j in range(pairs)]
    for t in range(pairs):
        at = 0
        for j in range(pairs):
            at = jnp.where(early[j] == t, j, at)
        order_s[t] = 2 * at
        order_s[2 * pairs - 1 - t] = 2 * at + 1
    cots.relay()

    def project(j, store):
        x = jnp.concatenate([wide_in[order_s[4 * j + i]] for i in range(4)], axis=0).astype(jnp.float32)
        factor = lax.rsqrt(jnp.mean(x * x, axis=-1, keepdims=True) + epsilon)
        scaled = (x * factor * gains[pl.ds(0, 1), :]).astype(jnp.bfloat16)
        store[pl.ds(2 * (j % 2), 2)] = scaled.reshape(2, rows, -1)
        proj = nn(scaled, qkv_w[...].reshape(-1, 3 * LANES))
        spread = spread_heads(proj)
        for piece in range(4):
            at = 4 * j + piece
            cosine, sine = wave(turn_ref[at])

            def turned(part):
                z = spread[part][piece * half : (piece + 1) * half]
                return (z * cosine + pltpu.roll(z, 64, 1) * sine).astype(jnp.bfloat16)

            base = (2 * j + piece // 2) * 4 * half + (piece % 2) * half
            q_ref[pl.ds(pl.multiple_of(base, half), half), :] = turned(0)
            q_ref[pl.ds(pl.multiple_of(base + 2 * half, half), half), :] = turned(1)
            k_ref[pl.ds(pl.multiple_of(at * half, half), half), :] = turned(2)
            v_ref[pl.ds(pl.multiple_of(at * half, half), half), :] = spread[3][piece * half : (piece + 1) * half].astype(jnp.bfloat16)

    def project_first(j, carry):
        project(j, theirs)
        return carry

    def project_second(j, carry):
        project(j, first)
        return carry

    lax.fori_loop(0, 2, project_first, 0)
    keep_first = pltpu.make_async_copy(theirs, normed.at[pl.ds(0, 4)], local_sem.at[2])
    keep_first.start()
    lax.fori_loop(2, 4, project_second, 0)
    keep_second = pltpu.make_async_copy(first, normed.at[pl.ds(4, 4)], local_sem.at[3])
    keep_second.start()
    give(q_ref, q_o)
    give(k_ref, k_o)
    give(v_ref, v_o)
    give(qkv_w, qkv_o)
    tokens.finish()
    outs.step(2)
    cots.rest()
    outs.step(3)
    outs.keep.wait()
    outc.start()

    def next_weights():
        downs.step(1)
        gus.start()

    steps = Steps(
        next_weights, lambda: None, lambda: None, lambda: None, outc.relay, lambda: None, lambda: downs.step(2),
        lambda: None,
    )
    scaling = HEAD_DIM ** (-0.5)
    mask = causal(2 * half)
    lane = lax.broadcasted_iota(jnp.int32, (half, LANES), 1)
    values_t = v_ref[...].astype(jnp.float32).T.astype(jnp.bfloat16)
    for pair in range(pairs):
        width_of = (pair + 1) * 2 * half
        q = q_ref[pl.ds(pair * 4 * half, 4 * half), :]
        before = width_of - 2 * half
        parts = [jnp.where(mask, nt(k_ref[pl.ds(before, 2 * half), :], q) * scaling, -1e30)]
        if pair:
            parts.append(nt(k_ref[pl.ds(0, before), :], q) * scaling)
        tops = [jnp.max(part, axis=0, keepdims=True) for part in parts]
        top = jnp.maximum(tops[0], tops[-1])
        parts = [jnp.exp(part - top) for part in parts]
        total = sum(jnp.sum(part, axis=0, keepdims=True) for part in parts)
        parts = [(part * (1.0 / total)).astype(jnp.bfloat16) for part in parts]
        lse_ref[pl.ds(pair, 1), :] = top + jnp.log(total)
        out_t = nn(values_t[:, before:width_of], parts[0])
        if pair:
            out_t = out_t + nn(values_t[:, :before], parts[1])
        att_ref[pl.ds(pair * LANES, LANES), :] = out_t
        result = out_t.T.astype(jnp.bfloat16).astype(jnp.float32)
        for part in range(2):
            left = result[part * half : (part + 1) * half]
            right = pltpu.roll(result[(2 + part) * half : (3 + part) * half], half, 1)
            low_sorted[2 * pair + part, :, 0:LANES] = jnp.where(lane < half, left, right).astype(jnp.bfloat16)
            low_sorted[2 * pair + part, :, LANES:] = right.astype(jnp.bfloat16)
        steps.next()
    give(att_ref, att_o)
    give(lse_ref, lse_o)
    for j in range(pairs):
        upper = low_sorted[early[j]]
        lower = low_sorted[2 * pairs - 1 - early[j]]
        low[j, pl.ds(0, half), :] = upper[:, :LANES]
        low[j, pl.ds(half, half), :] = lower[:, :LANES]
        tails = jnp.where(
            lane < 64, upper[:, LANES:].astype(jnp.float32), pltpu.roll(lower[:, LANES:].astype(jnp.float32), 64, 1)
        )
        low[j, pl.ds(2 * half, half), :] = tails.astype(jnp.bfloat16)
    keep_first.wait()
    keep_second.wait()
    moved = Exchange(place, low, attended, low_sem)
    moved.start()
    outc.rest()
    outc.partner()
    cots.partner()
    outc.keep.wait()
    moved.finish()
    middle[...] = tok[...].astype(jnp.float32)

    def out_project(q, carry):
        middle[...] += nn(unpacked(attended[q]), out_w[q // 2, pl.ds(4 * (q % 2), 4)].reshape(heads, -1))
        return carry

    lax.fori_loop(0, n, out_project, 0)
    give(middle, middle_o)
    gus.step(1)
    total = middle[...]
    factor = lax.rsqrt(jnp.mean(total * total, axis=-1, keepdims=True) + epsilon)
    own[...] = (total * factor * gains[pl.ds(1, 1), :]).astype(jnp.bfloat16)
    seconds = HalfGather(place, own, wide_in, gather_sem)
    seconds.start()
    seconds.relay()
    gus.step(2)
    seconds.rest()
    lows = Gather(place, low, low_all, lows_sem)
    lows.start()
    seconds.partner()
    downs.step(3)
    downs.keep.wait()
    give(down_w, down_o)
    cots.keep.wait()
    seconds.own_in()

    def early_grad(i, carry):
        rank = flip(place, i)
        at = pl.multiple_of((i % 2) * hidden.shape[2], LANES)
        mine[i // 2, :, pl.ds(at, hidden.shape[2])] = nt(up_all[rank], down_w[...].reshape(hidden.shape[2], -1))
        return carry

    lax.fori_loop(0, n, early_grad, 0)
    gus.step(3)
    gus.keep.wait()
    grads = Reduce(place, mine, theirs, first, out, second, reduce_sem)
    wide = hidden.shape[2]

    def block(i):
        rank = flip(place, i)
        gate_up = nn(wide_in[pl.ds(2 * rank, 2)].reshape(rows, -1), gu_w[...].reshape(-1, 2 * wide))
        gate, raised = gate_up[:, :wide], gate_up[:, wide:]
        sigmoid = 1.0 / (1.0 + jnp.exp(-gate))
        silu = gate * sigmoid
        hidden[rank] = (silu * raised).astype(jnp.bfloat16)
        hidden_grad = mine[i // 2, :, pl.ds(pl.multiple_of((i % 2) * wide, LANES), wide)]
        gul[rank, :, pl.ds(0, wide)] = (hidden_grad * raised * sigmoid * (1.0 + gate * (1.0 - sigmoid))).astype(jnp.bfloat16)
        gul[rank, :, pl.ds(wide, wide)] = (hidden_grad * silu).astype(jnp.bfloat16)
        return nt(gul[rank], gu_w[...].reshape(-1, 2 * wide))

    def block_at(t, carry):
        k = lax.rem(t // 2 + 1, 4)
        value = block(2 * k + 1 - t % 2)

        @pl.when(t % 2 == 0)
        def _():
            theirs[k] = value.astype(jnp.bfloat16)
            grads.push(k)

        @pl.when(t % 2 == 1)
        def _():
            mine[k] = value

        @pl.when(t == 2)
        def _():
            lows.relay()

        @pl.when(t == 4)
        def _():
            grads.beside()

        @pl.when(t == 5)
        def _():
            lows.rest()

        @pl.when(t == 6)
        def _():
            grads.across()

        return carry

    lax.fori_loop(0, 8, block_at, 0)
    give(hidden, hidden_o)
    grads.turn()
    down_z = PlaneReduce(place, down_g, down_r, down_zs)
    piece = down_g.shape[1]

    def down_block(t, carry):
        left = hidden[:, :, pl.ds(pl.multiple_of(t * piece, piece), piece)].reshape(length, piece)
        down_g[t] = tn(left, up_all[...].reshape(length, width)).astype(jnp.bfloat16)
        return carry

    lax.fori_loop(0, 4, down_block, 0)
    down_z.start()
    seconds.finish()
    gain_grad[...] = jnp.zeros_like(gain_grad)

    def norm_back(part, second_grad):
        x = middle[part, :]
        factor = lax.rsqrt(jnp.mean(x * x, axis=-1, keepdims=True) + epsilon)
        unit = x * factor
        gain_grad[...] += jnp.sum(second_grad * unit, axis=0, keepdims=True)
        scaled = second_grad * gains[pl.ds(1, 1), :]
        inner = jnp.mean(scaled * unit, axis=-1, keepdims=True)
        grad = middle_grad[part, :] + factor * (scaled - unit * inner)
        middle_grad[part, :] = grad
        own[part, :] = grad.astype(jnp.bfloat16)

    gus.finish(kept=True)
    shard = gu_w.shape[1]

    def gu_block(t, carry):
        left = wide_in[:, :, pl.ds(pl.multiple_of(t * shard, shard), shard)].reshape(length, shard)
        gu_w[t] = tn(left, gul[...].reshape(length, 2 * wide)).astype(jnp.bfloat16)
        return carry

    lax.fori_loop(0, 4, gu_block, 0)
    give(gu_w, gu_out)
    down_z.step1()
    grads.total(norm_back)

    def head_grads(q, carry):
        weight = out_w[q // 2, pl.ds(4 * (q % 2), 4)].reshape(heads, -1)
        attended[q] = packed(nt(own[...], weight)).astype(jnp.bfloat16)
        return carry

    lax.fori_loop(0, n, head_grads, 0)
    heads_back = Exchange(place, attended, agrad, agrad_sem)
    heads_back.start()
    for q in range(8):
        mcols_send[q] = packed(own[:, q * heads : (q + 1) * heads].astype(jnp.float32)).astype(jnp.bfloat16)
    columns = Exchange(place, mcols_send, mcols, mcols_sem)
    columns.start()
    down_z.step2()
    lows.partner()
    heads_back.finish()
    down_z.total()
    down_sum[...] = down_g[place.z]
    for move in (qkvs, outs, downs, cots, outc):
        move.finish(kept=True)
    lows.finish()
    columns.finish()
    for copy in given:
        copy.wait()
    grads.finish()
    down_z.finish()


def front_moves(tok, pos, attn_own, ffn_own, qkv_own, gu_own, far_cos, far_sin, near, out_weight, down_weight, up):
    n, planes = lax.axis_size("ctx"), lax.axis_size("fsdp")
    rows, width = tok.shape
    length = n * rows
    bf, f32 = jnp.bfloat16, jnp.float32
    shape = jax.ShapeDtypeStruct
    out_own = shape((out_weight.shape[1] // n, width), bf)
    down_own = shape((down_weight.shape[1] // n, width), bf)
    spot = shape((8, LANES), jnp.int32)
    gain_own = shape((8, attn_own.shape[1]), f32)
    wide = planes * down_own.shape[0]
    dma = pltpu.SemaphoreType.DMA
    pairs = length // 192
    halves = pltpu.VMEM((6, rows // 2, width), bf)
    quads = pltpu.VMEM((4, rows, width), bf)
    small = (n, 3 * rows // 2, LANES)
    all_of = lambda x: shape((planes,) + x.shape, x.dtype)
    gathered = lambda x: pltpu.VMEM((planes,) + x.shape, x.dtype)
    ring = dma((2, Gather.sems))
    half_ring = dma((2, HalfGather.sems))
    line = dma((3, planes))
    swap = dma((2, n))
    kept = (
        shape((n, rows, wide), bf), all_of(qkv_own), all_of(down_own),
        shape((2 * length, LANES), bf), shape((length, LANES), bf), shape((length, LANES), bf),
        shape((pairs * LANES, 384), f32), shape((pairs, 384), f32), shape((rows, width), f32),
        shape((2 * n, rows // 2, LANES), f32),
    )
    return pl.pallas_call(
        front_kernel,
        out_shape=(
            shape((rows, width), f32), shape((1, width), f32), shape((n,) + spot.shape, spot.dtype), shape((2, width), f32),
            shape(down_own.shape, bf),
        ) + kept + (shape((n, rows, width), bf), shape(small, bf), shape((n,) + small, bf), all_of(gu_own), shape(small, bf)),
        in_specs=vm(9) + anywhere(3),
        out_specs=vm(5) + anywhere(15),
        scratch_shapes=[pltpu.VMEM(x.shape, x.dtype) for x in kept] + [
            pltpu.VMEM(small, bf), pltpu.VMEM((rows, width), bf), pltpu.VMEM(spot.shape, jnp.int32), pltpu.VMEM(gain_own.shape, f32),
            pltpu.VMEM((2 * n, rows // 2, width), bf), pltpu.VMEM((n, rows, width), bf), pltpu.VMEM((n, rows, 2 * wide), bf),
            gathered(gu_own), gathered(out_own), pltpu.VMEM((planes, n) + out_own.shape, bf),
            pltpu.VMEM((16, 96, 2 * LANES), bf), gathered(gain_own), pltpu.SMEM((n,) + spot.shape, jnp.int32),
            pltpu.SMEM((2 * n,), jnp.int32), pltpu.VMEM(small, bf),
            pltpu.VMEM(small, bf), pltpu.VMEM((rows, width), bf),
            pltpu.VMEM((4, rows, width), f32), quads, quads, halves, halves,
            gathered(down_own), pltpu.VMEM((planes + 1,) + down_own.shape, bf),
            half_ring, ring, swap, dma((2, planes)), line, line, ring, line, line, dma((16,)),
            swap, half_ring, dma((2, Reduce.sems)), swap, ring, dma((2, planes + 1)), swap,
        ],
        compiler_params=pltpu.CompilerParams(collective_id=1, has_side_effects=True, vmem_limit_bytes=67043328),
        name="front_moves",
    )(tok, pos, attn_own, ffn_own, qkv_own, gu_own, far_cos, far_sin, near, out_weight, down_weight, up)


def back_moves_kernel(
    tok, gain, ffn_gain, down_sum, spots_i,
    gu_i, middle_grad_i, hidden_i, down_i, k_i, q_i, v_i, agrad_i, att_i, lse_i, turn_i, normed_i, middle_i, qkv_i, mcols_i, low_i,
    grad, result, attn_sum, ffn_sum, down_all, gu_all, out_all, qkv_all,
    spots_s, gu_g, hidden, down_w, k_ref, q_ref, v_ref, agrad, att_ref, lse_ref, turn_ref, normed_in, middle, qkv_w, mcols_in, low_in, out_g, qkv_g, gu_r, out_r, qkv_r,
    mine, theirs, first, out, second, dk_ref, dv_ref, pg_sorted, mcols,
    gain_sum, mine_gain, ctx_gain, plane_sum, plane_gain,
    free, local_sem, sum_sem, reduce_sem, gu_zs, out_zs, qkv_zs, down_cs, gu_cs, out_cs, qkv_cs,
    gain_sem, plane_sem,
):
    place = Place()
    n = place.n
    rows = tok.shape[0]
    half = rows // 2
    pairs = 8
    width = tok.shape[1]
    length = n * rows
    loads = [
        pltpu.make_async_copy(source, target, local_sem.at[at])
        for at, (source, target) in enumerate((
            (gu_i, gu_g), (hidden_i, hidden), (down_i, down_w), (k_i, k_ref), (q_i, q_ref), (v_i, v_ref),
            (agrad_i, agrad), (att_i, att_ref), (lse_i, lse_ref), (turn_i, turn_ref), (middle_i, middle),
            (normed_i, normed_in), (qkv_i, qkv_w), (mcols_i, mcols_in), (low_i, low_in), (middle_grad_i, grad),
        ))
    ]
    table = pltpu.make_async_copy(spots_i, spots_s, local_sem.at[16])
    table.start()
    for load in loads:
        load.start()
    greet(place, planes=True)
    table.wait()
    early = [lax.div(spots_s[j, 0, 0], half) for j in range(pairs)]
    holder = []
    for t in range(pairs):
        at = 0
        for j in range(pairs):
            at = jnp.where(early[j] == t, j, at)
        holder.append(at)
    gu_z = PlaneReduce(place, gu_g, gu_r, gu_zs)
    out_z = PlaneReduce(place, out_g, out_r, out_zs)
    qkv_z = PlaneReduce(place, qkv_g, qkv_r, qkv_zs)
    sums = Reduce(place, mine, theirs, first, out, second, sum_sem)
    downs = Gather(place, down_sum, down_all, down_cs)
    gus = Gather(place, gu_z.own(), gu_all, gu_cs)
    loads[0].wait()
    gu_z.start()
    downs.start()
    loads[1].wait()
    loads[2].wait()

    def other(k, carry):
        theirs[k] = nn(hidden[flip(place, 2 * k + 1)], down_w[...].reshape(-1, width)).astype(jnp.bfloat16)
        sums.push(k)
        return carry

    def ours(k, carry):
        mine[k] = nn(hidden[flip(place, 2 * k)], down_w[...].reshape(-1, width))
        return carry

    lax.fori_loop(0, 4, other, 0)
    lax.fori_loop(0, 4, ours, 0)
    downs.relay()
    sums.across()
    sums.beside()
    for load in loads[3:11]:
        load.wait()

    def finish_rows(part, down_out):
        result[part, :] = (middle[part, :] + down_out).astype(jnp.bfloat16)

    def sums_done():
        sums.total(finish_rows)
        sums.finish()
        for rank in (place.p, place.x, place.y):
            pl.semaphore_signal(free, inc=1, device_id={"ctx": rank}, device_id_type=MESH)

    def columns_done():
        loads[13].wait()

        def unpack(q, carry):
            mcols[q] = unpacked(mcols_in[q])
            return carry

        lax.fori_loop(0, n, unpack, 0)

    steps = Steps(
        lambda: None, downs.rest, lambda: None, gu_z.step1, downs.partner, sums.turn, columns_done, lambda: None,
    )
    scaling = HEAD_DIM ** (-0.5)
    mask = causal(2 * half)
    lane = lax.broadcasted_iota(jnp.int32, (half, LANES), 1)
    keys_t = k_ref[...].astype(jnp.float32).T.astype(jnp.bfloat16)
    for pair in reversed(range(pairs)):
        q = q_ref[pl.ds(pair * 4 * half, 4 * half), :]
        firsts, seconds = [], []
        for part in range(2):
            s = 2 * pair + part
            side = 0 if s < pairs else 1
            piece_of = agrad[holder[s] if s < pairs else holder[2 * pairs - 1 - s]].astype(jnp.float32)
            left = piece_of[side * half : (side + 1) * half]
            tail = piece_of[2 * half :]
            right = tail if side == 0 else pltpu.roll(tail, 64, 1)
            firsts.append(jnp.where(lane < half, left, 0.0))
            seconds.append(
                jnp.where(lane < half, pltpu.roll(jnp.where(lane < half, right, left), LANES - half, 1), 0.0)
            )
        grads = jnp.concatenate(firsts + seconds, axis=0)
        delta = jnp.sum(grads.T * att_ref[pl.ds(pair * LANES, LANES), :], axis=0, keepdims=True)
        grads = grads.astype(jnp.bfloat16)
        before = pair * 2 * half
        cuts = [(before, 2 * half)] + [(at, min(768, before - at)) for at in range(0, before, 768)]
        dq_t = None
        for at, count in cuts:
            keys = pl.ds(at, count)
            weights = jnp.exp(nt(k_ref[keys, :], q) * scaling - lse_ref[pl.ds(pair, 1), :])
            if at == before:
                weights = jnp.where(mask, weights, 0.0)
            dp = nt(v_ref[keys, :], grads)
            ds = (weights * (dp - delta)).astype(jnp.bfloat16)
            dk = nn(ds, q) * scaling
            dv = nn(weights.astype(jnp.bfloat16), grads)
            if pair == pairs - 1:
                dk_ref[keys, :] = dk
                dv_ref[keys, :] = dv
            else:
                dk_ref[keys, :] += dk
                dv_ref[keys, :] += dv
            term = nn(keys_t[:, at : at + count], ds)
            dq_t = term if dq_t is None else dq_t + term
        dq = dq_t.T * scaling
        for part in range(2):
            cosine, sine = wave(turn_ref[2 * pair + part])
            turned = []
            for head in range(2):
                z = dq[(2 * head + part) * half : (2 * head + part + 1) * half]
                turned.append(close_halves(z * cosine - pltpu.roll(z, 64, 1) * sine))
            second_head = pltpu.roll(turned[1], 96, 1)
            pg_sorted[2 * pair + part, :, 0:LANES] = jnp.where(lane < 96, turned[0], second_head).astype(jnp.bfloat16)
            pg_sorted[2 * pair + part, :, LANES : 2 * LANES] = second_head.astype(jnp.bfloat16)
        steps.next()
    for s in range(2 * pairs):
        spot = pl.ds(s * half, half)
        cosine, sine = wave(turn_ref[s])
        z = dk_ref[spot, :]
        key_head = pltpu.roll(close_halves(z * cosine - pltpu.roll(z, 64, 1) * sine), 64, 1)
        queries_too = pg_sorted[s, :, LANES : 2 * LANES].astype(jnp.float32)
        pg_sorted[s, :, LANES : 2 * LANES] = jnp.where(lane < 64, queries_too, key_head).astype(jnp.bfloat16)
        pg_sorted[s, :, 2 * LANES :] = jnp.where(lane < 32, key_head, pltpu.roll(dv_ref[spot, :], 32, 1)).astype(jnp.bfloat16)

    loads[11].wait()
    loads[12].wait()
    shard = gu_g.shape[1]

    def qkv_block(t, carry):
        left = normed_in[:, :, pl.ds(pl.multiple_of(t * shard, shard), shard)].reshape(length, shard)
        qkv_g[t] = tn(left, pg_sorted[...].reshape(length, 3 * LANES)).astype(jnp.bfloat16)
        return carry

    sums_done()
    lax.fori_loop(0, 4, qkv_block, 0)
    qkv_z.start()
    gu_z.step2()
    pl.semaphore_wait(free, 3)
    grads = Reduce(place, mine, theirs, first, out, second, reduce_sem)

    def chunk(i):
        at = lax.div(spots_s[flip(place, i), 0, 0], half)
        rows_of = jnp.concatenate([pg_sorted[at], pg_sorted[2 * pairs - 1 - at]], axis=0)
        return nt(rows_of, qkv_w[...].reshape(width, -1))

    def push(k, carry):
        theirs[k] = chunk(2 * k + 1).astype(jnp.bfloat16)
        grads.push(k)
        return carry

    def keep(k, carry):
        mine[k] = chunk(2 * k)
        return carry

    lax.fori_loop(0, 4, push, 0)
    lax.fori_loop(0, 4, keep, 0)
    grads.across()
    grads.beside()
    loads[14].wait()
    loads[15].wait()

    def out_block(src, carry):
        heads = low_in[src, :, pl.ds(0, rows), :].reshape(length, LANES)
        tails = low_in[src, :, pl.ds(rows, half), :].reshape(length // 2, LANES)
        upper = tn(heads, mcols[...].reshape(length, rows))
        from_a = tn(tails, mcols[:, pl.ds(0, half), :].reshape(length // 2, rows))
        from_b = tn(tails, mcols[:, pl.ds(half, half), :].reshape(length // 2, rows))
        at = pl.multiple_of((src % 2) * rows, rows)
        out_g[src // 2, pl.ds(at, LANES), :] = upper.astype(jnp.bfloat16)
        out_g[src // 2, pl.ds(pl.multiple_of(at + LANES, 64), 64), :] = (from_a[:64] + from_b[64:]).astype(jnp.bfloat16)
        return carry

    lax.fori_loop(0, 8, out_block, 0)
    out_z.start()
    grads.turn()
    gu_z.total()
    gus.start()
    gain_sum[...] = jnp.zeros_like(gain_sum)

    def norm_back(part, normed_grad):
        x = tok[part, :].astype(jnp.float32)
        factor = lax.rsqrt(jnp.mean(x * x, axis=-1, keepdims=True) + epsilon)
        unit = x * factor
        gain_sum[...] += jnp.sum(normed_grad * unit, axis=0, keepdims=True)
        scaled = normed_grad * gain[pl.ds(0, 1), :]
        inner = jnp.mean(scaled * unit, axis=-1, keepdims=True)
        grad[part, :] = grad[part, :] + factor * (scaled - unit * inner)

    qkv_z.step1()
    grads.total(norm_back)
    gain_grad = gain_sum[...]
    count = mine_gain.shape[0] // 2
    for at in range(count):
        mine_gain[pl.ds(at, 1), :] = gain_grad[:, at * shard : (at + 1) * shard]
        mine_gain[pl.ds(count + at, 1), :] = ffn_gain[:, at * shard : (at + 1) * shard]
    ctx_sum = Share(place, mine_gain, ctx_gain, gain_sem)
    ctx_sum.start()
    gus.relay()
    qkv_z.step2()
    out_z.step1()
    ctx_sum.finish()
    plane_sum[...] = jnp.sum(ctx_gain[...], axis=0)
    planes = PlaneShare(place, plane_sum, plane_gain, plane_sem)
    planes.start()
    out_z.step2()
    qkv_z.total()
    gus.rest()
    qkvs = Gather(place, qkv_z.own(), qkv_all, qkv_cs)
    qkvs.start()
    out_z.total()
    outs = Gather(place, out_z.own(), out_all, out_cs)
    qkvs.relay()
    outs.start()
    qkvs.rest()
    outs.relay()
    outs.rest()
    planes.finish()
    plane_sum[...] = jnp.sum(plane_gain[...], axis=0)
    attn_sum[...] = plane_sum[pl.ds(place.z, 1), :]
    ffn_sum[...] = plane_sum[pl.ds(count + place.z, 1), :]
    gus.partner()
    qkvs.partner()
    outs.partner()
    for move in (gu_z, out_z, qkv_z, downs, gus, outs, qkvs, grads):
        move.finish()


def back_moves(tok, gain, ffn_gain, down_sum, spots, *moved):
    n, planes = lax.axis_size("ctx"), lax.axis_size("fsdp")
    rows, width = tok.shape
    length = n * rows
    shard = width // planes
    bf, f32 = jnp.bfloat16, jnp.float32
    shape = jax.ShapeDtypeStruct
    dma = pltpu.SemaphoreType.DMA
    halves = pltpu.VMEM((6, rows // 2, width), bf)
    quads = pltpu.VMEM((4, rows, width), bf)
    small = (2 * planes, shard)
    parts = (moved[0].shape[1:], (shard, rows), (shard, 3 * LANES))
    ring = dma((2, Gather.sems))
    return pl.pallas_call(
        back_moves_kernel,
        out_shape=(shape((rows, width), f32), shape((rows, width), bf), shape((1, shard), f32), shape((1, shard), f32))
        + tuple(shape((n,) + part, bf) for part in (down_sum.shape,) + parts),
        in_specs=vm(4) + anywhere(1 + len(moved)),
        out_specs=vm(4) + anywhere(4),
        scratch_shapes=[pltpu.SMEM(spots.shape, jnp.int32)] + [pltpu.VMEM(x.shape, x.dtype) for at, x in enumerate(moved) if at != 1]
        + [pltpu.VMEM((planes,) + part, bf) for part in parts[1:]]
        + [pltpu.VMEM((planes + 1,) + part, bf) for part in parts]
        + [
            pltpu.VMEM((4, rows, width), f32), quads, quads, halves, halves,
            pltpu.VMEM((length, LANES), f32), pltpu.VMEM((length, LANES), f32), pltpu.VMEM((16, 96, 3 * LANES), bf),
            pltpu.VMEM((n, rows, rows), bf),
            pltpu.VMEM((1, width), f32), pltpu.VMEM(small, f32), pltpu.VMEM((n,) + small, f32),
            pltpu.VMEM(small, f32), pltpu.VMEM((planes,) + small, f32),
            pltpu.SemaphoreType.REGULAR, dma((17,)), dma((2, Reduce.sems)), dma((2, Reduce.sems)),
            dma((2, 5)), dma((2, 5)), dma((2, 5)), ring, ring, ring, ring, dma((2, n)), dma((2, planes)),
        ],
        compiler_params=pltpu.CompilerParams(collective_id=6, has_side_effects=True, vmem_limit_bytes=67043328),
        name="back_moves",
    )(tok, gain, ffn_gain, down_sum, spots, *moved)


def pack_kernel(
    down, gu, out, qkv, grad, result, attn, ffn, down_o, gu_o, out_o, qkv_o, grad_o, result_o, attn_o, ffn_o
):
    devices, rows = gu.shape[0], gu.shape[1]
    f32 = jnp.float32
    lane = lax.broadcasted_iota(jnp.int32, (rows, LANES), 1)
    down_o[...] = down[0].astype(f32)
    grad_o[...] = grad[...]
    result_o[...] = result[...]
    attn_o[...] = attn[...]
    ffn_o[...] = ffn[...]
    tiles = gu_o.shape[0] // rows
    spans = gu.shape[2] // (2 * LANES)
    for c in range(devices):
        for s in range(2):
            for z in range(spans):
                piece = gu[c, :, (s * spans + z) * LANES : (s * spans + z + 1) * LANES].astype(f32)
                gu_o[pl.ds((z * devices + c) * 2 + s, rows, stride=tiles), :] = piece

    def tile(c, at):
        return qkv[c, :, at * LANES : (at + 1) * LANES].astype(f32)

    def key_head(c):
        return jnp.where(lane < 64, pltpu.roll(tile(c, 1), 64, 1), pltpu.roll(tile(c, 2), 64, 1))

    def value_head(c):
        return pltpu.roll(tile(c, 2), 96, 1)

    def store(at, heads):
        second, third, fourth = pltpu.roll(heads[1], 96, 1), pltpu.roll(heads[2], 64, 1), pltpu.roll(heads[3], 32, 1)
        qkv_o[:, at : at + LANES] = jnp.where(lane < 96, heads[0], second)
        qkv_o[:, at + LANES : at + 2 * LANES] = jnp.where(lane < 64, second, third)
        qkv_o[:, at + 2 * LANES : at + 3 * LANES] = jnp.where(lane < 32, third, fourth)

    for c in range(0, devices, 2):
        at = c * 192
        turned = pltpu.roll(tile(c + 1, 0), 64, 1)
        qkv_o[:, at : at + LANES] = tile(c, 0)
        qkv_o[:, at + LANES : at + 2 * LANES] = jnp.where(lane < 64, tile(c, 1), turned)
        qkv_o[:, at + 2 * LANES : at + 3 * LANES] = jnp.where(lane < 64, turned, pltpu.roll(tile(c + 1, 1), 64, 1))
    for c in range(0, devices, 4):
        store(HEADS * HEAD_DIM + c * 96, [key_head(c + i) for i in range(4)])
        store((HEADS + KV_HEADS) * HEAD_DIM + c * 96, [value_head(c + i) for i in range(4)])
    for c in range(0, devices, 2):
        at = c * 192
        first = out[c].astype(f32)
        second = out[c + 1].astype(f32)
        tail = jnp.concatenate([first[:, LANES:], jnp.zeros((rows, 64), f32)], axis=1)
        next_tail = jnp.concatenate([second[:, LANES:], jnp.zeros((rows, 64), f32)], axis=1)
        turned = pltpu.roll(second[:, :LANES], 64, 1)
        out_o[:, at : at + LANES] = first[:, :LANES]
        out_o[:, at + LANES : at + 2 * LANES] = jnp.where(lane < 64, tail, turned)
        out_o[:, at + 2 * LANES : at + 3 * LANES] = jnp.where(lane < 64, turned, pltpu.roll(next_tail, 64, 1))


def pack(down, gu, out, qkv, grad, result, attn, ffn):
    n, shard = gu.shape[0], gu.shape[1]
    rows = shard // n
    width = down.shape[2]
    f32 = jnp.float32
    spec = pl.BlockSpec
    shape = jax.ShapeDtypeStruct
    tiles = n * gu.shape[2] // LANES
    quarter = grad.shape[0] // 4
    return pl.pallas_call(
        pack_kernel,
        grid=(n,),
        out_shape=(
            shape((n * down.shape[1], width), f32), shape((shard * tiles, LANES), f32), shape((shard, n * out.shape[2]), f32),
            shape((shard, (HEADS + 2 * KV_HEADS) * HEAD_DIM), f32), shape(grad.shape, f32), shape(result.shape, result.dtype), shape(attn.shape, f32), shape(ffn.shape, f32),
        ),
        in_specs=[
            spec((1,) + down.shape[1:], lambda i: (i, 0, 0)), spec((n, rows, gu.shape[2]), lambda i: (0, i, 0)),
            spec((n, rows, out.shape[2]), lambda i: (0, i, 0)), spec((n, rows, qkv.shape[2]), lambda i: (0, i, 0)),
            spec((quarter, width), lambda i: (i // 2, 0)), spec((quarter, width), lambda i: (i // 2, 0)),
            spec(attn.shape, lambda i: (0, 0)), spec(ffn.shape, lambda i: (0, 0)),
        ],
        out_specs=[
            spec((down.shape[1], width), lambda i: (i, 0)), spec((rows * tiles, LANES), lambda i: (i, 0)),
            spec((rows, n * out.shape[2]), lambda i: (i, 0)), spec((rows, (HEADS + 2 * KV_HEADS) * HEAD_DIM), lambda i: (i, 0)),
            spec((quarter, width), lambda i: (i // 2, 0)), spec((quarter, width), lambda i: (i // 2, 0)),
            spec(attn.shape, lambda i: (0, 0)), spec(ffn.shape, lambda i: (0, 0)),
        ],
        name="pack",
    )(down, gu, out, qkv, grad, result, attn, ffn)


def fast_body(
    tokens, positions, qkv_weight, out_weight, gate_up_weight, down_weight, attn_gain, ffn_gain, cotangent
):
    me = lax.axis_index("ctx")
    n = lax.axis_size("ctx")
    planes = lax.axis_size("fsdp")
    rows = tokens.shape[1]
    length = n * rows
    width = tokens.shape[2]
    wide = down_weight.shape[1] * planes
    own = wide // n
    piece = own // planes
    shard = qkv_weight.shape[1]
    query_width = HEADS * HEAD_DIM
    key_width = KV_HEADS * HEAD_DIM
    cut = lax.dynamic_slice_in_dim

    qkv = qkv_weight[0]
    q_part = cut(qkv, me * 2 * HEAD_DIM, 2 * HEAD_DIM, 1)
    k_part = cut(qkv, query_width + me * HEAD_DIM, HEAD_DIM, 1)
    v_part = cut(qkv, query_width + key_width + me * HEAD_DIM, HEAD_DIM, 1)
    qkv_own = jnp.concatenate([q_part, k_part, v_part], axis=1)
    pieces = [cut(gate_up_weight[0], at * (wide // planes) + me * piece, piece, 2) for at in range(planes)]
    gate_up_own = jnp.concatenate([x[:, s] for s in range(2) for x in pieces], axis=1)
    (
        middle_grad, ffn_partial, spots, gains, down_sum, hidden, qkv_block, down_block, q, k, v, att, lse, middle,
        turns, normed, attended_grad, low_all, gate_up_grad, middle_cols,
    ) = front_moves(
        tokens[0], positions, attn_gain, ffn_gain, qkv_own, gate_up_own, *turn_parts(2 * n, rows // 2),
        out_weight, down_weight, cotangent[0],
    )
    stream_grad, result, attn_sum, ffn_sum, down_grad, gate_up_grad, out_grad, qkv_grad = back_moves(
        tokens[0], gains, ffn_partial, down_sum, spots,
        gate_up_grad, middle_grad, hidden, down_block, k, q, v, attended_grad, att, lse, turns, normed, middle,
        qkv_block, middle_cols, low_all,
    )
    down_grad, gate_up_grad, out_grad, qkv_grad, stream_grad, result, attn_sum, ffn_sum = pack(
        down_grad, gate_up_grad, out_grad, qkv_grad, stream_grad, result, attn_sum, ffn_sum
    )
    gate_up_grad = gate_up_grad.reshape(shard, wide // LANES, 2, LANES).transpose(0, 2, 1, 3).reshape(shard, 2, wide)
    return (
        result[None],
        stream_grad[None],
        qkv_grad[None],
        out_grad[None],
        gate_up_grad[None],
        down_grad[None],
        attn_sum,
        ffn_sum,
    )


def solution(mesh):
    split = mesh.shape["ctx"] == KV_HEADS and mesh.shape["fsdp"] == 4
    placed = (
        P("fsdp", "ctx", None),
        P("fsdp", "ctx"),
        P(None, "fsdp", None),
        P(None, "fsdp", None),
        P(None, "fsdp", None, None),
        P(None, "fsdp", None),
        P(None, "fsdp"),
        P(None, "fsdp"),
        P("fsdp", "ctx", None),
    )
    return jax.shard_map(
        fast_body if split else body,
        mesh=mesh,
        in_specs=placed,
        out_specs=(
            P("fsdp", "ctx", None),
            P("fsdp", "ctx", None),
            P(None, "fsdp", None),
            P(None, "fsdp", None),
            P(None, "fsdp", None, None),
            P(None, "fsdp", None),
            P(None, "fsdp"),
            P(None, "fsdp"),
        ),
        check_vma=False,
    )
```

```python
import jax
import jax.numpy as jnp
import numpy as np
from jax import lax
from jax.experimental import pallas as pl
from jax.experimental.pallas import tpu as pltpu
from jax.sharding import PartitionSpec as P

HEADS = 16
KV_HEADS = 8
HEAD_DIM = 96
LAYERS = 1


epsilon = 1e-05
rope_base = 100000.0


def angles(place):
    halfway = HEAD_DIM // 2
    frequency = rope_base ** (-(jnp.arange(halfway, dtype=jnp.float32) * 2.0 / HEAD_DIM))
    phases = place.astype(jnp.float32)[:, None] * frequency[None, :]
    phases = jnp.concatenate([phases, phases], axis=-1)
    return (jnp.cos(phases)[:, None, :], jnp.sin(phases)[:, None, :])


def rotate(vectors, cosine, sine):
    halfway = vectors.shape[-1] // 2
    turned = jnp.concatenate([-vectors[..., halfway:], vectors[..., :halfway]], axis=-1)
    return vectors * cosine + turned * sine


def rotate_back(grads, cosine, sine):
    halfway = grads.shape[-1] // 2
    scaled = grads * sine
    return grads * cosine + jnp.concatenate(
        [scaled[..., halfway:], -scaled[..., :halfway]], axis=-1
    )


def normalize(rows, gain):
    factor = lax.rsqrt(jnp.mean(rows * rows, axis=-1, keepdims=True) + epsilon)
    return (rows * factor * gain, factor)


def normalize_back(upstream, rows, factor, gain):
    unit_rows = rows * factor
    gain_grad = jnp.sum(upstream * unit_rows, axis=0)
    scaled = upstream * gain
    row_inner = jnp.mean(scaled * unit_rows, axis=-1, keepdims=True)
    return (factor * (scaled - unit_rows * row_inner), gain_grad)


def split_blocks(queries, keys_all, values_all, key_place):
    rows = queries.shape[0]
    half = rows // 2
    shards = key_place.shape[0] // rows
    key_blocks = keys_all.reshape(shards, 2, half, KV_HEADS, HEAD_DIM)
    value_blocks = values_all.reshape(shards, 2, half, KV_HEADS, HEAD_DIM)
    place_blocks = key_place.reshape(shards, 2, half)
    return (key_blocks, value_blocks, place_blocks)


def scores_of(queries, key_block, place_block, query_place):
    scaling = HEAD_DIM ** (-0.5)
    scores = (
        jnp.einsum("rkgd,skd->kgrs", queries, key_block, preferred_element_type=jnp.float32)
        * scaling
    )
    allowed = place_block[None, None, None, :] <= query_place[None, None, :, None]
    return (scores, allowed)


def reachable(place_block, query_place):
    return jnp.min(place_block) <= jnp.max(query_place)


def attention_forward(queries, keys_all, values_all, query_place, key_place):
    key_blocks, value_blocks, place_blocks = split_blocks(queries, keys_all, values_all, key_place)
    rows = queries.shape[0]
    half = rows // 2
    groups = HEADS // KV_HEADS
    query_spans = queries.reshape(2, half, KV_HEADS, groups, HEAD_DIM)
    place_spans = query_place.reshape(2, half)

    def sweep_max(carry, inputs):
        key_block, place_block = inputs
        updated_all = []
        for span in range(2):
            state = carry[span]
            for part in range(2):

                def live(current, span=span, part=part):
                    maximum, total = current
                    scores, allowed = scores_of(
                        query_spans[span], key_block[part], place_block[part], place_spans[span]
                    )
                    masked = jnp.where(allowed, scores, -1e30)
                    updated = jnp.maximum(maximum, jnp.max(masked, axis=-1))
                    weights_now = jnp.where(allowed, jnp.exp(masked - updated[..., None]), 0.0)
                    return (
                        updated,
                        total * jnp.exp(maximum - updated) + jnp.sum(weights_now, axis=-1),
                    )

                state = lax.cond(
                    reachable(place_block[part], place_spans[span]),
                    live,
                    lambda current: current,
                    state,
                )
            updated_all.append(state)
        return (tuple(updated_all), None)

    start_max = jnp.full((KV_HEADS, groups, half), -1e30, jnp.float32)
    start_total = jnp.zeros((KV_HEADS, groups, half), jnp.float32)
    start = ((start_max, start_total), (start_max, start_total))
    finals, unused = lax.scan(sweep_max, start, (key_blocks, place_blocks))
    logsum_spans = [finals[span][0] + jnp.log(finals[span][1]) for span in range(2)]

    def sweep_out(results, inputs):
        key_block, value_block, place_block = inputs
        updated_all = []
        for span in range(2):
            result = results[span]
            for part in range(2):

                def live(current, span=span, part=part):
                    scores, allowed = scores_of(
                        query_spans[span], key_block[part], place_block[part], place_spans[span]
                    )
                    softmax_rows = jnp.where(
                        allowed, jnp.exp(scores - logsum_spans[span][..., None]), 0.0
                    ).astype(jnp.bfloat16)
                    return current + jnp.einsum(
                        "kgrs,skd->rkgd",
                        softmax_rows,
                        value_block[part],
                        preferred_element_type=jnp.float32,
                    )

                result = lax.cond(
                    reachable(place_block[part], place_spans[span]),
                    live,
                    lambda current: current,
                    result,
                )
            updated_all.append(result)
        return (tuple(updated_all), None)

    start_out = jnp.zeros((half, KV_HEADS, groups, HEAD_DIM), jnp.float32)
    outs, unused_out = lax.scan(
        sweep_out, (start_out, start_out), (key_blocks, value_blocks, place_blocks)
    )
    logsum = jnp.concatenate(logsum_spans, axis=-1)
    attended = jnp.concatenate([outs[0], outs[1]], axis=0)
    return (logsum, attended)


def attention_backward(
    queries, keys_all, values_all, query_place, key_place, logsum, attended_grad, row_inner
):
    key_blocks, value_blocks, place_blocks = split_blocks(queries, keys_all, values_all, key_place)
    rows = queries.shape[0]
    half = rows // 2
    groups = HEADS // KV_HEADS
    scaling = HEAD_DIM ** (-0.5)
    query_spans = queries.reshape(2, half, KV_HEADS, groups, HEAD_DIM)
    place_spans = query_place.reshape(2, half)
    grad_spans = attended_grad.reshape(2, half, KV_HEADS, groups, HEAD_DIM)
    logsum_spans = logsum.reshape(KV_HEADS, groups, 2, half)
    inner_spans = row_inner.reshape(KV_HEADS, groups, 2, half)

    def sweep_back(query_grads, inputs):
        key_block, value_block, place_block = inputs
        query_grads = list(query_grads)
        key_parts = []
        value_parts = []
        for part in range(2):
            key_acc = jnp.zeros((half, KV_HEADS, HEAD_DIM), jnp.float32)
            value_acc = jnp.zeros((half, KV_HEADS, HEAD_DIM), jnp.float32)
            for span in range(2):

                def live(current, span=span, part=part):
                    query_grad, key_grad, value_grad = current
                    scores, allowed = scores_of(
                        query_spans[span], key_block[part], place_block[part], place_spans[span]
                    )
                    softmax_rows = jnp.where(
                        allowed, jnp.exp(scores - logsum_spans[:, :, span][..., None]), 0.0
                    )
                    rounded = softmax_rows.astype(jnp.bfloat16)
                    weight_grad = jnp.einsum(
                        "rkgd,skd->kgrs",
                        grad_spans[span],
                        value_block[part],
                        preferred_element_type=jnp.float32,
                    )
                    score_grad = (
                        softmax_rows * (weight_grad - inner_spans[:, :, span][..., None])
                    ).astype(jnp.bfloat16)
                    query_grad = (
                        query_grad
                        + jnp.einsum(
                            "kgrs,skd->rkgd",
                            score_grad,
                            key_block[part],
                            preferred_element_type=jnp.float32,
                        )
                        * scaling
                    )
                    key_grad = (
                        key_grad
                        + jnp.einsum(
                            "kgrs,rkgd->skd",
                            score_grad,
                            query_spans[span],
                            preferred_element_type=jnp.float32,
                        )
                        * scaling
                    )
                    value_grad = value_grad + jnp.einsum(
                        "kgrs,rkgd->skd",
                        rounded,
                        grad_spans[span],
                        preferred_element_type=jnp.float32,
                    )
                    return (query_grad, key_grad, value_grad)

                state = (query_grads[span], key_acc, value_acc)
                state = lax.cond(
                    reachable(place_block[part], place_spans[span]),
                    live,
                    lambda current: current,
                    state,
                )
                query_grads[span], key_acc, value_acc = state
            key_parts.append(key_acc)
            value_parts.append(value_acc)
        key_out = jnp.concatenate(key_parts, axis=0)
        value_out = jnp.concatenate(value_parts, axis=0)
        return (tuple(query_grads), (key_out, value_out))

    start_grad = jnp.zeros((half, KV_HEADS, groups, HEAD_DIM), jnp.float32)
    query_pair, (key_grads, value_grads) = lax.scan(
        sweep_back, (start_grad, start_grad), (key_blocks, value_blocks, place_blocks)
    )
    query_grad = jnp.concatenate([query_pair[0], query_pair[1]], axis=0)
    return (
        query_grad,
        key_grads.reshape(-1, KV_HEADS, HEAD_DIM),
        value_grads.reshape(-1, KV_HEADS, HEAD_DIM),
    )


def fetch_layer(qkv_weight, out_weight, gate_up_weight, down_weight, attn_gain, ffn_gain, layer_id):
    return (
        lax.all_gather(qkv_weight[layer_id], "fsdp", axis=0, tiled=True),
        lax.all_gather(out_weight[layer_id], "fsdp", axis=0, tiled=True),
        lax.all_gather(gate_up_weight[layer_id], "fsdp", axis=0, tiled=True),
        lax.all_gather(down_weight[layer_id], "fsdp", axis=0, tiled=True),
        lax.all_gather(attn_gain[layer_id], "fsdp", axis=0, tiled=True),
        lax.all_gather(ffn_gain[layer_id], "fsdp", axis=0, tiled=True),
    )


def fetch_again(qkv_weight, out_weight, gate_up_weight, down_weight, attn_gain, ffn_gain, layer_id):
    return (
        lax.all_gather(qkv_weight[layer_id], "fsdp", axis=0, tiled=True),
        lax.all_gather(out_weight[layer_id], "fsdp", axis=0, tiled=True),
        lax.all_gather(gate_up_weight[layer_id], "fsdp", axis=0, tiled=True),
        lax.all_gather(down_weight[layer_id], "fsdp", axis=0, tiled=True),
        lax.all_gather(attn_gain[layer_id], "fsdp", axis=0, tiled=True),
        lax.all_gather(ffn_gain[layer_id], "fsdp", axis=0, tiled=True),
    )


def forward_layer(stream, query_place, key_place, gathered):
    qkv_full, out_full, gate_up_full, down_full, attn_full, ffn_full = gathered
    rows = stream.shape[0]
    groups = HEADS // KV_HEADS
    query_width = HEADS * HEAD_DIM
    key_width = KV_HEADS * HEAD_DIM
    cosine, sine = angles(query_place)
    normed, first_factor = normalize(stream, attn_full.astype(jnp.float32))
    normed = normed.astype(jnp.bfloat16)
    projected = jnp.dot(normed, qkv_full, preferred_element_type=jnp.float32)
    queries = rotate(projected[:, :query_width].reshape(rows, HEADS, HEAD_DIM), cosine, sine)
    queries = queries.reshape(rows, KV_HEADS, groups, HEAD_DIM).astype(jnp.bfloat16)
    keys_local = rotate(
        projected[:, query_width : query_width + key_width].reshape(rows, KV_HEADS, HEAD_DIM),
        cosine,
        sine,
    ).astype(jnp.bfloat16)
    values_local = (
        projected[:, query_width + key_width :]
        .reshape(rows, KV_HEADS, HEAD_DIM)
        .astype(jnp.bfloat16)
    )
    keys_all, values_all = (
        lax.all_gather(keys_local, "ctx", axis=0, tiled=True),
        lax.all_gather(values_local, "ctx", axis=0, tiled=True),
    )
    logsum, attended = attention_forward(queries, keys_all, values_all, query_place, key_place)
    attended_low = attended.reshape(rows, query_width).astype(jnp.bfloat16)
    middle = stream + jnp.dot(attended_low, out_full, preferred_element_type=jnp.float32)
    second, second_factor = normalize(middle, ffn_full.astype(jnp.float32))
    second = second.astype(jnp.bfloat16)
    gate_up = jnp.einsum("rd,dcf->rcf", second, gate_up_full, preferred_element_type=jnp.float32)
    hidden = (jax.nn.silu(gate_up[:, 0]) * gate_up[:, 1]).astype(jnp.bfloat16)
    result = middle + jnp.dot(hidden, down_full, preferred_element_type=jnp.float32)
    stored = (
        stream,
        first_factor,
        normed,
        queries,
        keys_local,
        values_local,
        keys_all,
        values_all,
        logsum,
        attended,
        attended_low,
        middle,
        second_factor,
        second,
        gate_up,
        hidden,
    )
    return (result, stored)


def backward_layer(upstream, stored, gathered, query_place, key_place, keys_all, values_all):
    (
        stream,
        first_factor,
        normed,
        queries,
        keys_local,
        values_local,
        kept_keys,
        kept_values,
        logsum,
        attended,
        attended_low,
        middle,
        second_factor,
        second,
        gate_up,
        hidden,
    ) = stored
    qkv_full, out_full, gate_up_full, down_full, attn_full, ffn_full = gathered
    rows = stream.shape[0]
    groups = HEADS // KV_HEADS
    cosine, sine = angles(query_place)
    upstream_low = upstream.astype(jnp.bfloat16)
    hidden_grad = jnp.einsum(
        "rd,fd->rf", upstream_low, down_full, preferred_element_type=jnp.float32
    )
    gate_part = gate_up[:, 0]
    up_part = gate_up[:, 1]
    sigmoid = jax.nn.sigmoid(gate_part)
    gate_grad = hidden_grad * up_part * sigmoid * (1.0 + gate_part * (1.0 - sigmoid))
    up_grad = hidden_grad * gate_part * sigmoid
    gate_up_low = jnp.stack([gate_grad, up_grad], axis=1).astype(jnp.bfloat16)
    second_grad = jnp.einsum(
        "rcf,dcf->rd", gate_up_low, gate_up_full, preferred_element_type=jnp.float32
    )
    middle_grad, ffn_gain_grad = normalize_back(
        second_grad, middle, second_factor, ffn_full.astype(jnp.float32)
    )
    middle_grad = middle_grad + upstream
    middle_low = middle_grad.astype(jnp.bfloat16)
    attended_grad = jnp.einsum(
        "rd,od->ro", middle_low, out_full, preferred_element_type=jnp.float32
    )
    attended_grad = attended_grad.astype(jnp.bfloat16).reshape(rows, KV_HEADS, groups, HEAD_DIM)
    row_inner = jnp.einsum("rkgd,rkgd->kgr", attended_grad.astype(jnp.float32), attended)
    query_grad, key_grads, value_grads = attention_backward(
        queries, keys_all, values_all, query_place, key_place, logsum, attended_grad, row_inner
    )
    key_grad, value_grad = (
        lax.psum_scatter(key_grads, "ctx", scatter_dimension=0, tiled=True),
        lax.psum_scatter(value_grads, "ctx", scatter_dimension=0, tiled=True),
    )
    query_grad = rotate_back(query_grad.reshape(rows, HEADS, HEAD_DIM), cosine, sine)
    key_grad = rotate_back(key_grad, cosine, sine)
    projected_grad = jnp.concatenate(
        [query_grad.reshape(rows, -1), key_grad.reshape(rows, -1), value_grad.reshape(rows, -1)],
        axis=1,
    ).astype(jnp.bfloat16)
    normed_grad = jnp.einsum(
        "re,de->rd", projected_grad, qkv_full, preferred_element_type=jnp.float32
    )
    stream_grad, attn_gain_grad = normalize_back(
        normed_grad, stream, first_factor, attn_full.astype(jnp.float32)
    )
    stream_grad = stream_grad + middle_grad
    qkv_grad = jnp.einsum("rd,re->de", normed, projected_grad, preferred_element_type=jnp.float32)
    out_grad = jnp.einsum("ro,rd->od", attended_low, middle_low, preferred_element_type=jnp.float32)
    gate_up_grad = jnp.einsum(
        "rd,rcf->dcf", second, gate_up_low, preferred_element_type=jnp.float32
    )
    down_grad = jnp.einsum("rf,rd->fd", hidden, upstream_low, preferred_element_type=jnp.float32)
    sharded = (
        lax.psum_scatter(qkv_grad, "fsdp", scatter_dimension=0, tiled=True),
        lax.psum_scatter(out_grad, "fsdp", scatter_dimension=0, tiled=True),
        lax.psum_scatter(gate_up_grad, "fsdp", scatter_dimension=0, tiled=True),
        lax.psum_scatter(down_grad, "fsdp", scatter_dimension=0, tiled=True),
        lax.psum_scatter(attn_gain_grad, "fsdp", scatter_dimension=0, tiled=True),
        lax.psum_scatter(ffn_gain_grad, "fsdp", scatter_dimension=0, tiled=True),
    )
    totals = lax.psum(
        (sharded[0], sharded[1], sharded[2], sharded[3], sharded[4], sharded[5]), "ctx"
    )
    return (stream_grad, totals)


def body(
    tokens,
    positions,
    qkv_weight,
    out_weight,
    gate_up_weight,
    down_weight,
    attn_gain,
    ffn_gain,
    cotangent,
):
    query_place = positions[0]
    key_place = lax.all_gather(query_place, "ctx", axis=0, tiled=True)
    stream = tokens[0].astype(jnp.float32)
    gathered_list = []
    layer_id = 0
    gathered = fetch_layer(
        qkv_weight, out_weight, gate_up_weight, down_weight, attn_gain, ffn_gain, layer_id
    )
    stream, stored = forward_layer(stream, query_place, key_place, gathered)
    saved = [stored]
    gathered_list.append(gathered)
    activations = stream.astype(jnp.bfloat16)[None]
    upstream = cotangent[0]
    layer_grads = [None] * LAYERS
    for layer_id in reversed(range(LAYERS)):
        stored = saved[layer_id]
        gathered = fetch_again(
            qkv_weight, out_weight, gate_up_weight, down_weight, attn_gain, ffn_gain, layer_id
        )
        keys_all, values_all = (stored[6], stored[7])
        upstream, totals = backward_layer(
            upstream, stored, gathered, query_place, key_place, keys_all, values_all
        )
        layer_grads[layer_id] = totals
    outputs = [jnp.stack([entry[slot] for entry in layer_grads], axis=0) for slot in range(6)]
    return (
        activations,
        upstream[None],
        outputs[0],
        outputs[1],
        outputs[2],
        outputs[3],
        outputs[4],
        outputs[5],
    )


LANES = 128


def spread(heads):
    half = HEAD_DIM // 2
    pad = ((0, 0), (0, 0), (0, 64 - half))
    return jnp.concatenate([jnp.pad(heads[..., :half], pad), jnp.pad(heads[..., half:], pad)], axis=-1)


def gathered_spread(padded):
    half = HEAD_DIM // 2
    return jnp.concatenate([padded[..., :half], padded[..., 64 : 64 + half]], axis=-1)


def turn_parts(spans, rows):
    half = HEAD_DIM // 2
    frequency = rope_base ** (-(np.arange(half, dtype=np.float64) * 2.0 / HEAD_DIM))

    def waves(place):
        phases = place[:, None] * frequency[None, :]
        pad = ((0, 0), (0, 64 - half))
        return np.pad(np.cos(phases), pad), np.pad(np.sin(phases), pad)

    cosine, sine = waves(np.arange(spans) * float(rows))
    parts = (
        np.concatenate([cosine, cosine], axis=1), np.concatenate([-sine, sine], axis=1),
        np.concatenate(waves(np.arange(rows, dtype=np.float64)), axis=1),
    )
    return tuple(jnp.asarray(part, jnp.float32) for part in parts)


def spread_heads(proj):
    lane = lax.broadcasted_iota(jnp.int32, (proj.shape[0], LANES), 1)
    tiles = [proj[:, at * LANES : (at + 1) * LANES] for at in range(3)]

    def put(*pieces):
        out = jnp.zeros_like(tiles[0])
        for tile, source, target, count in pieces:
            shift = (target - source) % LANES
            moved = pltpu.roll(tiles[tile], shift, 1) if shift else tiles[tile]
            out = jnp.where(jnp.logical_and(lane >= target, lane < target + count), moved, out)
        return out

    return (
        put((0, 0, 0, 48), (0, 48, 64, 48)),
        put((0, 96, 0, 32), (1, 0, 32, 16), (1, 16, 64, 48)),
        put((1, 64, 0, 48), (1, 112, 64, 16), (2, 0, 80, 32)),
        put((2, 32, 0, 96)),
    )


def close_halves(head):
    lane = lax.broadcasted_iota(jnp.int32, head.shape, 1)
    return jnp.where(lane < HEAD_DIM // 2, head, pltpu.roll(head, LANES - 64 + HEAD_DIM // 2, 1))


def wave(rows):
    first = lax.broadcasted_iota(jnp.int32, rows.shape, 1) < 64
    other = pltpu.roll(rows, 64, 1)
    return jnp.where(first, rows, other), jnp.where(first, -other, rows)


def nt(left, right):
    return lax.dot_general(left, right, (((1,), (1,)), ((), ())), preferred_element_type=jnp.float32)


def nn(left, right):
    return lax.dot_general(left, right, (((1,), (0,)), ((), ())), preferred_element_type=jnp.float32)


def tn(left, right):
    return lax.dot_general(left, right, (((0,), (0,)), ((), ())), preferred_element_type=jnp.float32)


def causal(width, place):
    key_at = lax.broadcasted_iota(jnp.int32, (2 * width, 2 * width), 0)
    query_at = lax.broadcasted_iota(jnp.int32, (2 * width, 2 * width), 1)
    query_at = jnp.where(query_at >= width, query_at - width, query_at)
    return key_at <= query_at + place * width


def vm(count):
    return [pl.BlockSpec(memory_space=pltpu.VMEM)] * count


MESH = pl.DeviceIdType.MESH


class Place:
    def __init__(self):
        self.me = lax.axis_index("ctx")
        core, x, y = self.me % 2, (self.me // 2) % 2, self.me // 4
        self.dp, self.dx, self.dy = 1 - 2 * core, 2 - 4 * x, 4 - 8 * y
        self.p, self.x, self.y = self.me + self.dp, self.me + self.dx, self.me + self.dy
        self.d = self.x + self.dy
        self.z = lax.axis_index("fsdp")
        self.planes = lax.axis_size("fsdp")
        self.n = lax.axis_size("ctx")


def greet(place, ctx=True, planes=False):
    barrier = pltpu.get_barrier_semaphore()
    count = 0
    if ctx:
        for step in range(1, place.n):
            pl.semaphore_signal(
                barrier, inc=1, device_id={"ctx": lax.rem(place.me + step, place.n)}, device_id_type=MESH
            )
            count += 1
    if planes:
        for step in range(1, place.planes):
            pl.semaphore_signal(
                barrier, inc=1, device_id={"fsdp": lax.rem(place.z + step, place.planes)}, device_id_type=MESH
            )
            count += 1
    pl.semaphore_wait(barrier, count)


def send(source, target, send_sem, recv_sem, **where):
    return pltpu.make_async_remote_copy(
        src_ref=source, dst_ref=target, send_sem=send_sem, recv_sem=recv_sem,
        device_id=where, device_id_type=MESH,
    )


class Gather:
    sems = 14

    def __init__(self, place, own, out, sem):
        self.place, self.own, self.out, self.sem = place, own, out, sem
        self.half = out.shape[1] // 2
        self.started = []
        self.met = False

    def go(self, source, target, index, rank):
        send(source, target, self.sem.at[0, index], self.sem.at[1, index], ctx=rank).start()
        self.started.append(index)

    def whole_block(self, index):
        return index == 6

    def sent(self):
        p = self.place
        for index in self.started:
            part = self.whole(p.me) if self.whole_block(index) else self.part(p.me, 0)
            send(part, part, self.sem.at[0, index], self.sem.at[1, index], ctx=p.p).wait_send()

    def part(self, rank, half):
        return self.out.at[rank, pl.ds(half * self.half, self.half)]

    def whole(self, rank):
        return self.out.at[rank]

    def start(self):
        p = self.place
        keep = pltpu.make_async_copy(self.own, self.whole(p.me), self.sem.at[0, 13])
        keep.start()
        self.keep = keep
        halves = [self.own.at[pl.ds(h * self.half, self.half)] for h in range(2)]
        self.go(halves[0], self.part(p.me, 0), 0, p.x)
        self.go(halves[1], self.part(p.me, 1), 3, p.y)
        self.go(self.own, self.whole(p.me), 6, p.p)
        self.go(halves[1], self.part(p.me, 1), 1, p.x)
        self.go(halves[0], self.part(p.me, 0), 2, p.y)

    def arrived(self, rank, half, index):
        part = self.part(rank, half)
        pltpu.make_async_copy(part, part, self.sem.at[1, index]).wait()
        return part

    def relay(self):
        p = self.place
        part = self.arrived(p.x, 0, 0)
        self.go(part, part, 4, p.y)
        self.go(part, part, 7, p.p)
        part = self.arrived(p.y, 1, 3)
        self.go(part, part, 5, p.x)
        self.go(part, part, 10, p.p)

    def rest(self):
        p = self.place
        for rank, half, index, onward in ((p.x, 1, 1, 8), (p.y, 0, 2, 9), (p.d, 0, 4, 11), (p.d, 1, 5, 12)):
            part = self.arrived(rank, half, index)
            self.go(part, part, onward, p.p)

    def first_partner(self):
        part = self.whole(self.place.p)
        pltpu.make_async_copy(part, part, self.sem.at[1, 6]).wait()
        self.met = True

    def partner(self):
        p = self.place
        if not self.met:
            self.first_partner()
        for rank, half, index in (
            (p.x, 0, 7), (p.y, 1, 10), (p.x, 1, 8), (p.y, 0, 9), (p.d, 0, 11), (p.d, 1, 12),
        ):
            self.arrived(rank + p.dp, half, index)

    def finish(self, kept=False):
        if not kept:
            self.keep.wait()
        self.sent()


class PlaneGather:
    def __init__(self, place, own, out, sem):
        self.place, self.own, self.out, self.sem = place, own, out, sem

    def hop(self, step, up):
        p = self.place
        sign = 1 if up else -1
        source = p.z - sign * step
        target = p.z + sign
        ok = jnp.logical_and(
            jnp.logical_and(source >= 0, source < p.planes),
            jnp.logical_and(target >= 0, target < p.planes),
        )
        source = jnp.clip(source, 0, p.planes - 1)
        target = jnp.clip(target, 0, p.planes - 1)
        block = self.own if step == 0 else self.out.at[source]
        return ok, send(
            block, self.out.at[source], self.sem.at[0 if up else 1, source], self.sem.at[2, source], fsdp=target
        )

    def start(self):
        p = self.place
        self.keep = pltpu.make_async_copy(self.own, self.out.at[p.z], self.sem.at[2, p.z])
        self.keep.start()
        for up in (True, False):
            ok, copy = self.hop(0, up)
            pl.when(ok)(copy.start)

    def got(self, step, up):
        p = self.place
        source = p.z - step if up else p.z + step
        ok = jnp.logical_and(source >= 0, source < p.planes)
        source = jnp.clip(source, 0, p.planes - 1)
        part = self.out.at[source]
        return ok, pltpu.make_async_copy(part, part, self.sem.at[2, source])

    def step(self, number):
        for up in (True, False):
            ok, copy = self.got(number, up)
            pl.when(ok)(copy.wait)
            if number < self.place.planes - 1:
                ok, copy = self.hop(number, up)
                pl.when(ok)(copy.start)

    def finish(self, kept=False):
        if not kept:
            self.keep.wait()
        for number in range(self.place.planes - 1):
            for up in (True, False):
                ok, copy = self.hop(number, up)
                pl.when(ok)(copy.wait_send)


class Exchange:
    def __init__(self, place, blocks, out, sem):
        self.place, self.blocks, self.out, self.sem = place, blocks, out, sem

    def pick(self, rank):
        return self.blocks.at[rank]

    def copy(self, step):
        p = self.place
        rank = lax.rem(p.me + step, p.n)
        return send(self.pick(rank), self.out.at[p.me], self.sem.at[0, step], self.sem.at[1, step], ctx=rank)

    def start(self):
        p = self.place
        for step in range(1, p.n):
            self.copy(step).start()
        self.keep = pltpu.make_async_copy(self.pick(p.me), self.out.at[p.me], self.sem.at[0, 0])
        self.keep.start()

    def finish(self):
        p = self.place
        self.keep.wait()
        for step in range(1, p.n):
            self.copy(step).wait_send()
        for step in range(1, p.n):
            part = self.out.at[lax.rem(p.me + p.n - step, p.n)]
            pltpu.make_async_copy(part, part, self.sem.at[1, step]).wait()


class Share(Exchange):
    def pick(self, rank):
        return self.blocks


class PlaneShare:
    def __init__(self, place, block, out, sem):
        self.place, self.block, self.out, self.sem = place, block, out, sem

    def copy(self, step):
        p = self.place
        plane = lax.rem(p.z + step, p.planes)
        return send(self.block, self.out.at[p.z], self.sem.at[0, step], self.sem.at[1, step], fsdp=plane)

    def start(self):
        p = self.place
        for step in range(1, p.planes):
            self.copy(step).start()
        self.keep = pltpu.make_async_copy(self.block, self.out.at[p.z], self.sem.at[0, 0])
        self.keep.start()

    def finish(self):
        p = self.place
        self.keep.wait()
        for step in range(1, p.planes):
            self.copy(step).wait_send()
        for step in range(1, p.planes):
            part = self.out.at[lax.rem(p.z + p.planes - step, p.planes)]
            pltpu.make_async_copy(part, part, self.sem.at[1, step]).wait()


def anywhere(count):
    return [pl.BlockSpec(memory_space=pl.ANY)] * count


class Reduce:
    sems = 10

    def __init__(self, place, mine, theirs, first, out, second, sem):
        self.place, self.mine, self.theirs, self.first, self.out, self.second, self.sem = (
            place, mine, theirs, first, out, second, sem
        )
        self.half = out.shape[1]
        self.started = []

    def push(self, slot):
        copy = send(
            self.theirs.at[slot], self.first.at[slot], self.sem.at[0, slot], self.sem.at[1, slot], ctx=self.place.p
        )
        copy.start()
        return copy

    def pushed(self):
        for slot in range(4):
            send(
                self.theirs.at[slot], self.first.at[slot], self.sem.at[0, slot], self.sem.at[1, slot],
                ctx=self.place.p,
            ).wait_send()

    def add(self, slot):
        part = self.first.at[slot]
        pltpu.make_async_copy(part, part, self.sem.at[1, slot]).wait()
        self.mine[slot] = self.mine[slot] + self.first[slot].astype(jnp.float32)

    def go(self, index, value, rank):
        self.out[index] = value.astype(jnp.bfloat16)
        self.turned(index, rank).start()
        self.started.append((index, rank))

    def turned(self, index, rank):
        return send(
            self.out.at[index], self.second.at[index], self.sem.at[0, 4 + index], self.sem.at[1, 4 + index], ctx=rank
        )

    def top(self, slot):
        return self.mine[slot, pl.ds(0, self.half), :]

    def low(self, slot):
        return self.mine[slot, pl.ds(self.half, self.half), :]

    def got(self, index):
        part = self.second.at[index]
        pltpu.make_async_copy(part, part, self.sem.at[1, 4 + index]).wait()
        return self.second[index].astype(jnp.float32)

    def across(self):
        self.add(3)
        self.go(1, self.top(3), self.place.x)
        self.go(3, self.low(3), self.place.y)

    def beside(self):
        self.add(1)
        self.go(0, self.top(1), self.place.x)
        self.add(2)
        self.go(2, self.low(2), self.place.y)

    def turn(self):
        self.go(4, self.top(2) + self.got(1), self.place.y)
        self.go(5, self.low(1) + self.got(3), self.place.x)

    def total(self, use):
        self.add(0)
        use(pl.ds(0, self.half), self.top(0) + self.got(0) + self.got(4))
        use(pl.ds(self.half, self.half), self.low(0) + self.got(2) + self.got(5))

    def finish(self):
        self.pushed()
        for index, rank in self.started:
            self.turned(index, rank).wait_send()


def flip(place, i):
    return place.me + (i % 2) * place.dp + ((i // 2) % 2) * place.dx + (i // 4) * place.dy


class HalfGather(Gather):
    sems = 16

    def __init__(self, place, own, out, sem):
        self.place, self.own, self.out, self.sem = place, own, out, sem
        self.half = out.shape[1]
        self.started = []
        self.met = False

    def part(self, rank, half):
        return self.out.at[2 * rank + half]

    def whole_block(self, index):
        return False

    def start(self):
        p = self.place
        halves = [self.own.at[pl.ds(h * self.half, self.half)] for h in range(2)]
        self.kept = [
            pltpu.make_async_copy(halves[h], self.part(p.me, h), self.sem.at[0, (13, 15)[h]]) for h in range(2)
        ]
        self.go(halves[0], self.part(p.me, 0), 0, p.x)
        self.go(halves[1], self.part(p.me, 1), 3, p.y)
        self.go(halves[0], self.part(p.me, 0), 6, p.p)
        self.go(halves[1], self.part(p.me, 1), 14, p.p)
        self.go(halves[1], self.part(p.me, 1), 1, p.x)
        self.go(halves[0], self.part(p.me, 0), 2, p.y)
        for copy in self.kept:
            copy.start()

    def first_partner(self):
        for h in range(2):
            self.arrived(self.place.p, h, (6, 14)[h])
        self.met = True

    def own_in(self):
        for copy in self.kept:
            copy.wait()

    def finish(self):
        self.sent()


def packed(block):
    rows = block.shape[0] // 2
    tail = jnp.concatenate([block[:, LANES:], jnp.zeros((2 * rows, 64), block.dtype)], axis=1)
    first = lax.broadcasted_iota(jnp.int32, (rows, LANES), 1) < 64
    return jnp.concatenate([block[:, :LANES], jnp.where(first, tail[:rows], pltpu.roll(tail[rows:], 64, 1))], axis=0)


def unpacked(block):
    rows = block.shape[0] // 3
    tail = block[2 * rows :].astype(jnp.float32)
    tails = jnp.concatenate([tail, pltpu.roll(tail, 64, 1)], axis=0)[:, :64].astype(block.dtype)
    return jnp.concatenate([block[: 2 * rows], tails], axis=1)


class PlaneReduce:
    def __init__(self, place, block, recv, sem):
        self.place, self.block, self.recv, self.sem = place, block, recv, sem

    def hop(self, ok, part, slot, target, first, wait):
        copy = send(
            self.block.at[part], self.recv.at[slot], self.sem.at[0, part], self.sem.at[1, slot], fsdp=target
        )

        @pl.when(ok)
        def _():
            if wait:
                copy.wait_send()
                return
            if not first:
                self.merge(part, part)
            copy.start()

    def merge(self, part, slot):
        piece = self.recv.at[slot]
        pltpu.make_async_copy(piece, piece, self.sem.at[1, slot]).wait()
        total = self.block[part].astype(jnp.float32) + self.recv[slot].astype(jnp.float32)
        self.block[part] = total.astype(jnp.bfloat16)

    def ends(self, i, wait=False):
        z = self.place.z
        low = z == 0
        part = jnp.where(low, 3 - i, i)
        slot = part if i < 2 else jnp.where(low, part, 4)
        self.hop(jnp.logical_or(low, z == 3), part, slot, jnp.where(low, 1, 2), True, wait)

    def inner(self, up, down, slot_up, slot_down, to_up, to_down, wait=False):
        z = self.place.z
        low = z == 1
        part = jnp.where(low, up, down)
        slot = jnp.where(low, slot_up, slot_down)
        self.hop(jnp.logical_or(low, z == 2), part, slot, jnp.where(low, to_up, to_down), False, wait)

    def start(self, wait=False):
        for i in range(3):
            self.ends(i, wait)

    def step1(self, wait=False):
        self.inner(3, 0, 3, 0, 2, 1, wait)

    def step2(self, wait=False):
        self.inner(2, 1, 2, 4, 2, 1, wait)
        self.inner(0, 3, 4, 3, 0, 3, wait)

    def total(self):
        z = self.place.z

        @pl.when(z > 0)
        def _():
            self.merge(z, z)

        @pl.when(z < 3)
        def _():
            self.merge(z, 4)

    def own(self):
        return self.block.at[self.place.z]

    def finish(self):
        self.start(True)
        self.step1(True)
        self.step2(True)


class Steps:
    def __init__(self, *steps):
        self.steps = list(steps)

    def next(self, count=1):
        for step in self.steps[:count]:
            step()
        self.steps = self.steps[count:]

    def rest(self):
        self.next(len(self.steps))


class OutGather(Gather):
    def __init__(self, place, own, out, sem):
        self.place, self.own, self.out, self.sem = place, own, out, sem
        self.half = out.shape[0] // 2
        self.started = []
        self.met = False

    def part(self, rank, half):
        return self.out.at[pl.ds(half * self.half, self.half), rank]

    def whole(self, rank):
        return self.out.at[:, rank]


def front_kernel(
    tok, pos, attn_own, ffn_own, qkv_own, gu_own, far_cos, far_sin, near, out_weight, down_weight, up,
    middle_grad, gain_grad, spots, gains, down_sum,
    hidden_o, qkv_o, down_o, q_o, k_o, v_o, att_o, lse_o, middle_o, turn_o, normed, agrad, low_all, gu_out, mcols,
    hidden, qkv_w, down_w, q_ref, k_ref, v_ref, att_ref, lse_ref, middle, turn_ref, mcols_send, up_low, spot, gain_own,
    wide_in, up_all, gul, gu_w, out_block, out_w, low_sorted, gain_all, spots_s, order_s, low,
    attended, own, mine, theirs, first, out, second, down_g, down_r,
    tok_sem, up_sem, spot_sem, gain_sem, qkv_sem, out_sem, outc_sem, gu_sem, down_sem, local_sem,
    low_sem, gather_sem, reduce_sem, agrad_sem, lows_sem, down_zs, mcols_sem,
):
    place = Place()
    n = place.n
    rows = tok.shape[0]
    half = rows // 2
    pairs = 8
    heads = rows
    length = n * rows
    width = tok.shape[1]
    out_own = out_weight.at[0, pl.ds(place.me * (out_weight.shape[1] // 8), out_weight.shape[1] // 8)]
    down_own = down_weight.at[0, pl.ds(place.me * (down_weight.shape[1] // 8), down_weight.shape[1] // 8)]
    spot[...] = jnp.broadcast_to(pos[0:1, 0:1], spot.shape)
    gain_own[pl.ds(0, 1), :] = attn_own[...].astype(jnp.float32)
    gain_own[pl.ds(1, 1), :] = ffn_own[...].astype(jnp.float32)
    fetch = pltpu.make_async_copy(up, middle_grad, local_sem.at[0])
    fetch.start()
    greet(place, planes=True)
    spans = Share(place, spot, spots, spot_sem)
    scales = PlaneShare(place, gain_own, gain_all, gain_sem)
    tokens = HalfGather(place, tok, wide_in, tok_sem)
    cots = Gather(place, up_low, up_all, up_sem)
    qkvs = PlaneGather(place, qkv_own, qkv_w, qkv_sem)
    outs = PlaneGather(place, out_own, out_block, out_sem)
    outc = OutGather(place, out_block, out_w, outc_sem)
    gus = PlaneGather(place, gu_own, gu_w, gu_sem)
    downs = PlaneGather(place, down_own, down_w, down_sem)
    given = []

    def give(source, target):
        copy = pltpu.make_async_copy(source, target, local_sem.at[5 + len(given)])
        copy.start()
        given.append(copy)

    tokens.start()
    qkvs.start()
    spans.start()
    scales.start()

    def turn_rows(at, carry):
        base = near[...]
        turn_ref[at] = base * far_cos[pl.ds(at, 1), :] + pltpu.roll(base, 64, 1) * far_sin[pl.ds(at, 1), :]
        return carry

    lax.fori_loop(0, 2 * pairs, turn_rows, 0)
    give(turn_ref, turn_o)
    fetch.wait()
    up_low[...] = middle_grad[...].astype(jnp.bfloat16)
    tokens.relay()
    qkvs.step(1)
    outs.start()
    qkvs.step(2)
    tokens.rest()
    cots.start()
    outs.step(1)
    downs.start()
    qkvs.step(3)
    tokens.partner()
    tokens.own_in()
    spans.finish()
    scales.finish()
    qkvs.keep.wait()
    table = pltpu.make_async_copy(spots, spots_s, local_sem.at[1])
    table.start()
    for g in range(2):
        gains[pl.ds(g, 1), :] = jnp.concatenate([gain_all[z, pl.ds(g, 1), :] for z in range(4)], axis=1)
    table.wait()
    early = [lax.div(spots_s[j, 0, 0], half) for j in range(pairs)]
    for t in range(pairs):
        at = 0
        for j in range(pairs):
            at = jnp.where(early[j] == t, j, at)
        order_s[t] = 2 * at
        order_s[2 * pairs - 1 - t] = 2 * at + 1
    cots.relay()

    def project(j, store):
        x = jnp.concatenate([wide_in[order_s[4 * j + i]] for i in range(4)], axis=0).astype(jnp.float32)
        factor = lax.rsqrt(jnp.mean(x * x, axis=-1, keepdims=True) + epsilon)
        scaled = (x * factor * gains[pl.ds(0, 1), :]).astype(jnp.bfloat16)
        store[pl.ds(2 * (j % 2), 2)] = scaled.reshape(2, rows, -1)
        proj = nn(scaled, qkv_w[...].reshape(-1, 3 * LANES))
        spread = spread_heads(proj)
        for piece in range(4):
            at = 4 * j + piece
            cosine, sine = wave(turn_ref[at])

            def turned(part):
                z = spread[part][piece * half : (piece + 1) * half]
                return (z * cosine + pltpu.roll(z, 64, 1) * sine).astype(jnp.bfloat16)

            base = (2 * j + piece // 2) * 4 * half + (piece % 2) * half
            q_ref[pl.ds(pl.multiple_of(base, half), half), :] = turned(0)
            q_ref[pl.ds(pl.multiple_of(base + 2 * half, half), half), :] = turned(1)
            k_ref[pl.ds(pl.multiple_of(at * half, half), half), :] = turned(2)
            v_ref[pl.ds(pl.multiple_of(at * half, half), half), :] = spread[3][piece * half : (piece + 1) * half].astype(jnp.bfloat16)

    def project_first(j, carry):
        project(j, theirs)
        return carry

    def project_second(j, carry):
        project(j, first)
        return carry

    lax.fori_loop(0, 2, project_first, 0)
    keep_first = pltpu.make_async_copy(theirs, normed.at[pl.ds(0, 4)], local_sem.at[2])
    keep_first.start()
    lax.fori_loop(2, 4, project_second, 0)
    keep_second = pltpu.make_async_copy(first, normed.at[pl.ds(4, 4)], local_sem.at[3])
    keep_second.start()
    give(q_ref, q_o)
    give(k_ref, k_o)
    give(v_ref, v_o)
    give(qkv_w, qkv_o)
    tokens.finish()
    outs.step(2)
    cots.rest()
    outs.step(3)
    outs.keep.wait()
    outc.start()

    def next_weights():
        downs.step(1)
        gus.start()

    steps = Steps(next_weights, lambda: None, outc.relay, lambda: downs.step(2))
    scaling = HEAD_DIM ** (-0.5)
    lane = lax.broadcasted_iota(jnp.int32, (half, LANES), 1)
    values_t = v_ref[...].astype(jnp.float32).T.astype(jnp.bfloat16)
    def attend_group(group):
        before = group * 4 * half

        def attend(place_of, carry):
            pair = 2 * group + place_of
            q = q_ref[pl.ds(pl.multiple_of(pair * 4 * half, 4 * half), 4 * half), :]
            scores = nt(k_ref[pl.ds(before, 4 * half), :], q) * scaling
            parts = [jnp.where(causal(2 * half, place_of), scores, -1e30)]
            if group:
                parts.append(nt(k_ref[pl.ds(0, before), :], q) * scaling)
            tops = [jnp.max(part, axis=0, keepdims=True) for part in parts]
            top = jnp.maximum(tops[0], tops[-1])
            parts = [jnp.exp(part - top) for part in parts]
            total = sum(jnp.sum(part, axis=0, keepdims=True) for part in parts)
            parts = [(part * (1.0 / total)).astype(jnp.bfloat16) for part in parts]
            lse_ref[pl.ds(pair, 1), :] = top + jnp.log(total)
            out_t = nn(values_t[:, before : before + 4 * half], parts[0])
            if group:
                out_t = out_t + nn(values_t[:, :before], parts[1])
            att_ref[pl.ds(pl.multiple_of(pair * LANES, LANES), LANES), :] = out_t
            result = out_t.T.astype(jnp.bfloat16).astype(jnp.float32)
            for part in range(2):
                left = result[part * half : (part + 1) * half]
                right = pltpu.roll(result[(2 + part) * half : (3 + part) * half], half, 1)
                low_sorted[2 * pair + part, :, 0:LANES] = jnp.where(lane < half, left, right).astype(jnp.bfloat16)
                low_sorted[2 * pair + part, :, LANES:] = right.astype(jnp.bfloat16)
            return carry

        lax.fori_loop(0, 2, attend, 0)

    for group in range(pairs // 2):
        attend_group(group)
        steps.next()
    give(att_ref, att_o)
    give(lse_ref, lse_o)
    for j in range(pairs):
        upper = low_sorted[early[j]]
        lower = low_sorted[2 * pairs - 1 - early[j]]
        low[j, pl.ds(0, half), :] = upper[:, :LANES]
        low[j, pl.ds(half, half), :] = lower[:, :LANES]
        tails = jnp.where(
            lane < 64, upper[:, LANES:].astype(jnp.float32), pltpu.roll(lower[:, LANES:].astype(jnp.float32), 64, 1)
        )
        low[j, pl.ds(2 * half, half), :] = tails.astype(jnp.bfloat16)
    keep_first.wait()
    keep_second.wait()
    moved = Exchange(place, low, attended, low_sem)
    moved.start()
    outc.rest()
    outc.partner()
    cots.partner()
    outc.keep.wait()
    moved.finish()
    middle[...] = tok[...].astype(jnp.float32)

    def out_project(q, carry):
        middle[...] += nn(unpacked(attended[q]), out_w[q // 2, pl.ds(4 * (q % 2), 4)].reshape(heads, -1))
        return carry

    lax.fori_loop(0, n, out_project, 0)
    give(middle, middle_o)
    gus.step(1)
    total = middle[...]
    factor = lax.rsqrt(jnp.mean(total * total, axis=-1, keepdims=True) + epsilon)
    own[...] = (total * factor * gains[pl.ds(1, 1), :]).astype(jnp.bfloat16)
    seconds = HalfGather(place, own, wide_in, gather_sem)
    seconds.start()
    seconds.relay()
    gus.step(2)
    seconds.rest()
    lows = Gather(place, low, low_all, lows_sem)
    lows.start()
    seconds.partner()
    downs.step(3)
    downs.keep.wait()
    give(down_w, down_o)
    cots.keep.wait()
    seconds.own_in()

    def early_grad(i, carry):
        rank = flip(place, i)
        at = pl.multiple_of((i % 2) * hidden.shape[2], LANES)
        mine[i // 2, :, pl.ds(at, hidden.shape[2])] = nt(up_all[rank], down_w[...].reshape(hidden.shape[2], -1))
        return carry

    lax.fori_loop(0, n, early_grad, 0)
    gus.step(3)
    gus.keep.wait()
    grads = Reduce(place, mine, theirs, first, out, second, reduce_sem)
    wide = hidden.shape[2]

    def block(i):
        rank = flip(place, i)
        gate_up = nn(wide_in[pl.ds(2 * rank, 2)].reshape(rows, -1), gu_w[...].reshape(-1, 2 * wide))
        gate, raised = gate_up[:, :wide], gate_up[:, wide:]
        sigmoid = 1.0 / (1.0 + jnp.exp(-gate))
        silu = gate * sigmoid
        hidden[rank] = (silu * raised).astype(jnp.bfloat16)
        hidden_grad = mine[i // 2, :, pl.ds(pl.multiple_of((i % 2) * wide, LANES), wide)]
        gul[rank, :, pl.ds(0, wide)] = (hidden_grad * raised * sigmoid * (1.0 + gate * (1.0 - sigmoid))).astype(jnp.bfloat16)
        gul[rank, :, pl.ds(wide, wide)] = (hidden_grad * silu).astype(jnp.bfloat16)
        return nt(gul[rank], gu_w[...].reshape(-1, 2 * wide))

    def block_at(t, carry):
        k = lax.rem(t // 2 + 1, 4)
        value = block(2 * k + 1 - t % 2)

        @pl.when(t % 2 == 0)
        def _():
            theirs[k] = value.astype(jnp.bfloat16)
            grads.push(k)

        @pl.when(t % 2 == 1)
        def _():
            mine[k] = value

        @pl.when(t == 2)
        def _():
            lows.relay()

        @pl.when(t == 4)
        def _():
            grads.beside()

        @pl.when(t == 5)
        def _():
            lows.rest()

        @pl.when(t == 6)
        def _():
            grads.across()

        return carry

    lax.fori_loop(0, 8, block_at, 0)
    give(hidden, hidden_o)
    grads.turn()
    down_z = PlaneReduce(place, down_g, down_r, down_zs)
    piece = down_g.shape[1]

    def down_block(t, carry):
        left = hidden[:, :, pl.ds(pl.multiple_of(t * piece, piece), piece)].reshape(length, piece)
        down_g[t] = tn(left, up_all[...].reshape(length, width)).astype(jnp.bfloat16)
        return carry

    lax.fori_loop(0, 4, down_block, 0)
    down_z.start()
    seconds.finish()
    gain_grad[...] = jnp.zeros_like(gain_grad)

    def norm_back(part, second_grad):
        x = middle[part, :]
        factor = lax.rsqrt(jnp.mean(x * x, axis=-1, keepdims=True) + epsilon)
        unit = x * factor
        gain_grad[...] += jnp.sum(second_grad * unit, axis=0, keepdims=True)
        scaled = second_grad * gains[pl.ds(1, 1), :]
        inner = jnp.mean(scaled * unit, axis=-1, keepdims=True)
        grad = middle_grad[part, :] + factor * (scaled - unit * inner)
        middle_grad[part, :] = grad
        own[part, :] = grad.astype(jnp.bfloat16)

    gus.finish(kept=True)
    shard = gu_w.shape[1]

    def gu_block(t, carry):
        left = wide_in[:, :, pl.ds(pl.multiple_of(t * shard, shard), shard)].reshape(length, shard)
        gu_w[t] = tn(left, gul[...].reshape(length, 2 * wide)).astype(jnp.bfloat16)
        return carry

    lax.fori_loop(0, 4, gu_block, 0)
    give(gu_w, gu_out)
    down_z.step1()
    grads.total(norm_back)

    def head_grads(q, carry):
        weight = out_w[q // 2, pl.ds(4 * (q % 2), 4)].reshape(heads, -1)
        attended[q] = packed(nt(own[...], weight)).astype(jnp.bfloat16)
        return carry

    lax.fori_loop(0, n, head_grads, 0)
    heads_back = Exchange(place, attended, agrad, agrad_sem)
    heads_back.start()
    for q in range(8):
        mcols_send[q] = packed(own[:, q * heads : (q + 1) * heads].astype(jnp.float32)).astype(jnp.bfloat16)
    columns = Exchange(place, mcols_send, mcols, mcols_sem)
    columns.start()
    down_z.step2()
    lows.partner()
    heads_back.finish()
    down_z.total()
    down_sum[...] = down_g[place.z]
    for move in (qkvs, outs, downs, cots, outc):
        move.finish(kept=True)
    lows.finish()
    columns.finish()
    for copy in given:
        copy.wait()
    grads.finish()
    down_z.finish()


def front_moves(tok, pos, attn_own, ffn_own, qkv_own, gu_own, far_cos, far_sin, near, out_weight, down_weight, up):
    n, planes = lax.axis_size("ctx"), lax.axis_size("fsdp")
    rows, width = tok.shape
    length = n * rows
    bf, f32 = jnp.bfloat16, jnp.float32
    shape = jax.ShapeDtypeStruct
    out_own = shape((out_weight.shape[1] // n, width), bf)
    down_own = shape((down_weight.shape[1] // n, width), bf)
    spot = shape((8, LANES), jnp.int32)
    gain_own = shape((8, attn_own.shape[1]), f32)
    wide = planes * down_own.shape[0]
    dma = pltpu.SemaphoreType.DMA
    pairs = length // 192
    halves = pltpu.VMEM((6, rows // 2, width), bf)
    quads = pltpu.VMEM((4, rows, width), bf)
    small = (n, 3 * rows // 2, LANES)
    all_of = lambda x: shape((planes,) + x.shape, x.dtype)
    gathered = lambda x: pltpu.VMEM((planes,) + x.shape, x.dtype)
    ring = dma((2, Gather.sems))
    half_ring = dma((2, HalfGather.sems))
    line = dma((3, planes))
    swap = dma((2, n))
    kept = (
        shape((n, rows, wide), bf), all_of(qkv_own), all_of(down_own),
        shape((2 * length, LANES), bf), shape((length, LANES), bf), shape((length, LANES), bf),
        shape((pairs * LANES, 384), f32), shape((pairs, 384), f32), shape((rows, width), f32),
        shape((2 * n, rows // 2, LANES), f32),
    )
    return pl.pallas_call(
        front_kernel,
        out_shape=(
            shape((rows, width), f32), shape((1, width), f32), shape((n,) + spot.shape, spot.dtype), shape((2, width), f32),
            shape(down_own.shape, bf),
        ) + kept + (shape((n, rows, width), bf), shape(small, bf), shape((n,) + small, bf), all_of(gu_own), shape(small, bf)),
        in_specs=vm(9) + anywhere(3),
        out_specs=vm(5) + anywhere(15),
        scratch_shapes=[pltpu.VMEM(x.shape, x.dtype) for x in kept] + [
            pltpu.VMEM(small, bf), pltpu.VMEM((rows, width), bf), pltpu.VMEM(spot.shape, jnp.int32), pltpu.VMEM(gain_own.shape, f32),
            pltpu.VMEM((2 * n, rows // 2, width), bf), pltpu.VMEM((n, rows, width), bf), pltpu.VMEM((n, rows, 2 * wide), bf),
            gathered(gu_own), gathered(out_own), pltpu.VMEM((planes, n) + out_own.shape, bf),
            pltpu.VMEM((16, 96, 2 * LANES), bf), gathered(gain_own), pltpu.SMEM((n,) + spot.shape, jnp.int32),
            pltpu.SMEM((2 * n,), jnp.int32), pltpu.VMEM(small, bf),
            pltpu.VMEM(small, bf), pltpu.VMEM((rows, width), bf),
            pltpu.VMEM((4, rows, width), f32), quads, quads, halves, halves,
            gathered(down_own), pltpu.VMEM((planes + 1,) + down_own.shape, bf),
            half_ring, ring, swap, dma((2, planes)), line, line, ring, line, line, dma((16,)),
            swap, half_ring, dma((2, Reduce.sems)), swap, ring, dma((2, planes + 1)), swap,
        ],
        compiler_params=pltpu.CompilerParams(collective_id=1, has_side_effects=True, vmem_limit_bytes=67043328),
        name="front_moves",
    )(tok, pos, attn_own, ffn_own, qkv_own, gu_own, far_cos, far_sin, near, out_weight, down_weight, up)


def back_moves_kernel(
    tok, gain, ffn_gain, down_sum, spots_i,
    gu_i, middle_grad_i, hidden_i, down_i, k_i, q_i, v_i, agrad_i, att_i, lse_i, turn_i, normed_i, middle_i, qkv_i, mcols_i, low_i,
    grad, result, attn_sum, ffn_sum, down_all, gu_all, out_all, qkv_all,
    spots_s, agrad_at, gu_g, hidden, down_w, k_ref, q_ref, v_ref, agrad, att_ref, lse_ref, turn_ref, normed_in, middle, qkv_w, mcols_in, low_in, out_g, qkv_g, gu_r, out_r, qkv_r,
    mine, theirs, first, out, second, dk_ref, dv_ref, pg_sorted, mcols,
    gain_sum, mine_gain, ctx_gain, plane_sum, plane_gain,
    free, local_sem, sum_sem, reduce_sem, gu_zs, out_zs, qkv_zs, down_cs, gu_cs, out_cs, qkv_cs,
    gain_sem, plane_sem,
):
    place = Place()
    n = place.n
    rows = tok.shape[0]
    half = rows // 2
    pairs = 8
    width = tok.shape[1]
    length = n * rows
    loads = [
        pltpu.make_async_copy(source, target, local_sem.at[at])
        for at, (source, target) in enumerate((
            (gu_i, gu_g), (hidden_i, hidden), (down_i, down_w), (k_i, k_ref), (q_i, q_ref), (v_i, v_ref),
            (agrad_i, agrad), (att_i, att_ref), (lse_i, lse_ref), (turn_i, turn_ref), (middle_i, middle),
            (normed_i, normed_in), (qkv_i, qkv_w), (mcols_i, mcols_in), (low_i, low_in), (middle_grad_i, grad),
        ))
    ]
    table = pltpu.make_async_copy(spots_i, spots_s, local_sem.at[16])
    table.start()
    for load in loads:
        load.start()
    greet(place, planes=True)
    table.wait()
    early = [lax.div(spots_s[j, 0, 0], half) for j in range(pairs)]
    holder = []
    for t in range(pairs):
        at = 0
        for j in range(pairs):
            at = jnp.where(early[j] == t, j, at)
        holder.append(at)
    gu_z = PlaneReduce(place, gu_g, gu_r, gu_zs)
    out_z = PlaneReduce(place, out_g, out_r, out_zs)
    qkv_z = PlaneReduce(place, qkv_g, qkv_r, qkv_zs)
    sums = Reduce(place, mine, theirs, first, out, second, sum_sem)
    downs = Gather(place, down_sum, down_all, down_cs)
    gus = Gather(place, gu_z.own(), gu_all, gu_cs)
    loads[0].wait()
    gu_z.start()
    downs.start()
    loads[1].wait()
    loads[2].wait()

    def other(k, carry):
        theirs[k] = nn(hidden[flip(place, 2 * k + 1)], down_w[...].reshape(-1, width)).astype(jnp.bfloat16)
        sums.push(k)
        return carry

    def ours(k, carry):
        mine[k] = nn(hidden[flip(place, 2 * k)], down_w[...].reshape(-1, width))
        return carry

    lax.fori_loop(0, 4, other, 0)
    lax.fori_loop(0, 4, ours, 0)
    downs.relay()
    sums.across()
    sums.beside()
    for load in loads[3:11]:
        load.wait()

    def finish_rows(part, down_out):
        result[part, :] = (middle[part, :] + down_out).astype(jnp.bfloat16)

    def sums_done():
        sums.total(finish_rows)
        sums.finish()
        for rank in (place.p, place.x, place.y):
            pl.semaphore_signal(free, inc=1, device_id={"ctx": rank}, device_id_type=MESH)

    def columns_done():
        loads[13].wait()

        def unpack(q, carry):
            mcols[q] = unpacked(mcols_in[q])
            return carry

        lax.fori_loop(0, n, unpack, 0)

    steps = Steps(downs.rest, gu_z.step1, lambda: (downs.partner(), sums.turn()), columns_done)
    scaling = HEAD_DIM ** (-0.5)
    lane = lax.broadcasted_iota(jnp.int32, (half, LANES), 1)
    keys_t = k_ref[...].astype(jnp.float32).T.astype(jnp.bfloat16)
    ranks_s = agrad_at
    for t in range(pairs):
        ranks_s[t] = holder[t]
        ranks_s[2 * pairs - 1 - t] = holder[t]
    dk_ref[...] = jnp.zeros_like(dk_ref)
    dv_ref[...] = jnp.zeros_like(dv_ref)

    def back_group(group):
        before = group * 4 * half
        side = 0 if group < pairs // 4 else 1
        cuts = [(before, 4 * half)] + [(at, min(768, before - at)) for at in range(0, before, 768)]

        def back(place_of, carry):
            pair = 2 * group + place_of
            q = q_ref[pl.ds(pl.multiple_of(pair * 4 * half, 4 * half), 4 * half), :]
            firsts, seconds = [], []
            for part in range(2):
                piece_of = agrad[ranks_s[2 * pair + part]].astype(jnp.float32)
                left = piece_of[side * half : (side + 1) * half]
                tail = piece_of[2 * half :]
                right = tail if side == 0 else pltpu.roll(tail, 64, 1)
                firsts.append(jnp.where(lane < half, left, 0.0))
                seconds.append(
                    jnp.where(lane < half, pltpu.roll(jnp.where(lane < half, right, left), LANES - half, 1), 0.0)
                )
            grads = jnp.concatenate(firsts + seconds, axis=0)
            att_t = att_ref[pl.ds(pl.multiple_of(pair * LANES, LANES), LANES), :]
            delta = jnp.sum(grads.T * att_t, axis=0, keepdims=True)
            grads = grads.astype(jnp.bfloat16)
            dq_t = None
            for at, count in cuts:
                keys = pl.ds(at, count)
                weights = jnp.exp(
                    jnp.where(
                        causal(2 * half, place_of), nt(k_ref[keys, :], q) * scaling - lse_ref[pl.ds(pair, 1), :], -1e30
                    )
                    if at == before
                    else nt(k_ref[keys, :], q) * scaling - lse_ref[pl.ds(pair, 1), :]
                )
                dp = nt(v_ref[keys, :], grads)
                ds = (weights * (dp - delta)).astype(jnp.bfloat16)
                dk_ref[keys, :] += nn(ds, q) * scaling
                dv_ref[keys, :] += nn(weights.astype(jnp.bfloat16), grads)
                term = nn(keys_t[:, at : at + count], ds)
                dq_t = term if dq_t is None else dq_t + term
            dq = dq_t.T * scaling
            for part in range(2):
                cosine, sine = wave(turn_ref[2 * pair + part])
                turned = []
                for head in range(2):
                    z = dq[(2 * head + part) * half : (2 * head + part + 1) * half]
                    turned.append(close_halves(z * cosine - pltpu.roll(z, 64, 1) * sine))
                second_head = pltpu.roll(turned[1], 96, 1)
                pg_sorted[2 * pair + part, :, 0:LANES] = jnp.where(lane < 96, turned[0], second_head).astype(jnp.bfloat16)
                pg_sorted[2 * pair + part, :, LANES : 2 * LANES] = second_head.astype(jnp.bfloat16)
            return carry

        lax.fori_loop(0, 2, back, 0)

    for group in reversed(range(pairs // 2)):
        back_group(group)
        steps.next()
    for s in range(2 * pairs):
        spot = pl.ds(s * half, half)
        cosine, sine = wave(turn_ref[s])
        z = dk_ref[spot, :]
        key_head = pltpu.roll(close_halves(z * cosine - pltpu.roll(z, 64, 1) * sine), 64, 1)
        queries_too = pg_sorted[s, :, LANES : 2 * LANES].astype(jnp.float32)
        pg_sorted[s, :, LANES : 2 * LANES] = jnp.where(lane < 64, queries_too, key_head).astype(jnp.bfloat16)
        pg_sorted[s, :, 2 * LANES :] = jnp.where(lane < 32, key_head, pltpu.roll(dv_ref[spot, :], 32, 1)).astype(jnp.bfloat16)

    loads[11].wait()
    loads[12].wait()
    shard = gu_g.shape[1]

    def qkv_block(t, carry):
        left = normed_in[:, :, pl.ds(pl.multiple_of(t * shard, shard), shard)].reshape(length, shard)
        qkv_g[t] = tn(left, pg_sorted[...].reshape(length, 3 * LANES)).astype(jnp.bfloat16)
        return carry

    sums_done()
    lax.fori_loop(0, 4, qkv_block, 0)
    qkv_z.start()
    gu_z.step2()
    pl.semaphore_wait(free, 3)
    grads = Reduce(place, mine, theirs, first, out, second, reduce_sem)

    def chunk(i):
        at = lax.div(spots_s[flip(place, i), 0, 0], half)
        rows_of = jnp.concatenate([pg_sorted[at], pg_sorted[2 * pairs - 1 - at]], axis=0)
        return nt(rows_of, qkv_w[...].reshape(width, -1))

    def push(k, carry):
        theirs[k] = chunk(2 * k + 1).astype(jnp.bfloat16)
        grads.push(k)
        return carry

    def keep(k, carry):
        mine[k] = chunk(2 * k)
        return carry

    lax.fori_loop(0, 4, push, 0)
    lax.fori_loop(0, 4, keep, 0)
    grads.across()
    grads.beside()
    loads[14].wait()
    loads[15].wait()

    def out_block(src, carry):
        heads = low_in[src, :, pl.ds(0, rows), :].reshape(length, LANES)
        tails = low_in[src, :, pl.ds(rows, half), :].reshape(length // 2, LANES)
        upper = tn(heads, mcols[...].reshape(length, rows))
        from_a = tn(tails, mcols[:, pl.ds(0, half), :].reshape(length // 2, rows))
        from_b = tn(tails, mcols[:, pl.ds(half, half), :].reshape(length // 2, rows))
        at = pl.multiple_of((src % 2) * rows, rows)
        out_g[src // 2, pl.ds(at, LANES), :] = upper.astype(jnp.bfloat16)
        out_g[src // 2, pl.ds(pl.multiple_of(at + LANES, 64), 64), :] = (from_a[:64] + from_b[64:]).astype(jnp.bfloat16)
        return carry

    lax.fori_loop(0, 8, out_block, 0)
    out_z.start()
    grads.turn()
    gu_z.total()
    gus.start()
    gain_sum[...] = jnp.zeros_like(gain_sum)

    def norm_back(part, normed_grad):
        x = tok[part, :].astype(jnp.float32)
        factor = lax.rsqrt(jnp.mean(x * x, axis=-1, keepdims=True) + epsilon)
        unit = x * factor
        gain_sum[...] += jnp.sum(normed_grad * unit, axis=0, keepdims=True)
        scaled = normed_grad * gain[pl.ds(0, 1), :]
        inner = jnp.mean(scaled * unit, axis=-1, keepdims=True)
        grad[part, :] = grad[part, :] + factor * (scaled - unit * inner)

    qkv_z.step1()
    grads.total(norm_back)
    gain_grad = gain_sum[...]
    count = mine_gain.shape[0] // 2
    for at in range(count):
        mine_gain[pl.ds(at, 1), :] = gain_grad[:, at * shard : (at + 1) * shard]
        mine_gain[pl.ds(count + at, 1), :] = ffn_gain[:, at * shard : (at + 1) * shard]
    ctx_sum = Share(place, mine_gain, ctx_gain, gain_sem)
    ctx_sum.start()
    gus.relay()
    qkv_z.step2()
    out_z.step1()
    ctx_sum.finish()
    plane_sum[...] = jnp.sum(ctx_gain[...], axis=0)
    planes = PlaneShare(place, plane_sum, plane_gain, plane_sem)
    planes.start()
    out_z.step2()
    qkv_z.total()
    gus.rest()
    qkvs = Gather(place, qkv_z.own(), qkv_all, qkv_cs)
    qkvs.start()
    out_z.total()
    outs = Gather(place, out_z.own(), out_all, out_cs)
    qkvs.relay()
    outs.start()
    qkvs.rest()
    outs.relay()
    outs.rest()
    planes.finish()
    plane_sum[...] = jnp.sum(plane_gain[...], axis=0)
    attn_sum[...] = plane_sum[pl.ds(place.z, 1), :]
    ffn_sum[...] = plane_sum[pl.ds(count + place.z, 1), :]
    gus.partner()
    qkvs.partner()
    outs.partner()
    for move in (gu_z, out_z, qkv_z, downs, gus, outs, qkvs, grads):
        move.finish()


def back_moves(tok, gain, ffn_gain, down_sum, spots, *moved):
    n, planes = lax.axis_size("ctx"), lax.axis_size("fsdp")
    rows, width = tok.shape
    length = n * rows
    shard = width // planes
    bf, f32 = jnp.bfloat16, jnp.float32
    shape = jax.ShapeDtypeStruct
    dma = pltpu.SemaphoreType.DMA
    halves = pltpu.VMEM((6, rows // 2, width), bf)
    quads = pltpu.VMEM((4, rows, width), bf)
    small = (2 * planes, shard)
    parts = (moved[0].shape[1:], (shard, rows), (shard, 3 * LANES))
    ring = dma((2, Gather.sems))
    return pl.pallas_call(
        back_moves_kernel,
        out_shape=(shape((rows, width), f32), shape((rows, width), bf), shape((1, shard), f32), shape((1, shard), f32))
        + tuple(shape((n,) + part, bf) for part in (down_sum.shape,) + parts),
        in_specs=vm(4) + anywhere(1 + len(moved)),
        out_specs=vm(4) + anywhere(4),
        scratch_shapes=[pltpu.SMEM(spots.shape, jnp.int32), pltpu.SMEM((2 * n,), jnp.int32)] + [pltpu.VMEM(x.shape, x.dtype) for at, x in enumerate(moved) if at != 1]
        + [pltpu.VMEM((planes,) + part, bf) for part in parts[1:]]
        + [pltpu.VMEM((planes + 1,) + part, bf) for part in parts]
        + [
            pltpu.VMEM((4, rows, width), f32), quads, quads, halves, halves,
            pltpu.VMEM((length, LANES), f32), pltpu.VMEM((length, LANES), f32), pltpu.VMEM((16, 96, 3 * LANES), bf),
            pltpu.VMEM((n, rows, rows), bf),
            pltpu.VMEM((1, width), f32), pltpu.VMEM(small, f32), pltpu.VMEM((n,) + small, f32),
            pltpu.VMEM(small, f32), pltpu.VMEM((planes,) + small, f32),
            pltpu.SemaphoreType.REGULAR, dma((17,)), dma((2, Reduce.sems)), dma((2, Reduce.sems)),
            dma((2, 5)), dma((2, 5)), dma((2, 5)), ring, ring, ring, ring, dma((2, n)), dma((2, planes)),
        ],
        compiler_params=pltpu.CompilerParams(collective_id=6, has_side_effects=True, vmem_limit_bytes=67043328),
        name="back_moves",
    )(tok, gain, ffn_gain, down_sum, spots, *moved)


def pack_kernel(
    down, gu, out, qkv, grad, result, attn, ffn, down_o, gu_o, out_o, qkv_o, grad_o, result_o, attn_o, ffn_o
):
    devices, rows = gu.shape[0], gu.shape[1]
    f32 = jnp.float32
    lane = lax.broadcasted_iota(jnp.int32, (rows, LANES), 1)
    down_o[...] = down[0].astype(f32)
    grad_o[...] = grad[...]
    result_o[...] = result[...]
    attn_o[...] = attn[...]
    ffn_o[...] = ffn[...]
    tiles = gu_o.shape[0] // rows
    spans = gu.shape[2] // (2 * LANES)
    for r in range(0, rows, 16):
        pieces = [
            gu[c, pl.ds(r, 16), (s * spans + z) * LANES : (s * spans + z + 1) * LANES].astype(f32)
            for z in range(spans) for c in range(devices) for s in range(2)
        ]
        gu_o[pl.ds(r * tiles, 16 * tiles), :] = jnp.swapaxes(jnp.stack(pieces, axis=0), 0, 1).reshape(16 * tiles, LANES)

    def tile(c, at):
        return qkv[c, :, at * LANES : (at + 1) * LANES].astype(f32)

    def key_head(c):
        return jnp.where(lane < 64, pltpu.roll(tile(c, 1), 64, 1), pltpu.roll(tile(c, 2), 64, 1))

    def value_head(c):
        return pltpu.roll(tile(c, 2), 96, 1)

    def store(at, heads):
        second, third, fourth = pltpu.roll(heads[1], 96, 1), pltpu.roll(heads[2], 64, 1), pltpu.roll(heads[3], 32, 1)
        qkv_o[:, at : at + LANES] = jnp.where(lane < 96, heads[0], second)
        qkv_o[:, at + LANES : at + 2 * LANES] = jnp.where(lane < 64, second, third)
        qkv_o[:, at + 2 * LANES : at + 3 * LANES] = jnp.where(lane < 32, third, fourth)

    for c in range(0, devices, 2):
        at = c * 192
        turned = pltpu.roll(tile(c + 1, 0), 64, 1)
        qkv_o[:, at : at + LANES] = tile(c, 0)
        qkv_o[:, at + LANES : at + 2 * LANES] = jnp.where(lane < 64, tile(c, 1), turned)
        qkv_o[:, at + 2 * LANES : at + 3 * LANES] = jnp.where(lane < 64, turned, pltpu.roll(tile(c + 1, 1), 64, 1))
    for c in range(0, devices, 4):
        store(HEADS * HEAD_DIM + c * 96, [key_head(c + i) for i in range(4)])
        store((HEADS + KV_HEADS) * HEAD_DIM + c * 96, [value_head(c + i) for i in range(4)])
    for c in range(0, devices, 2):
        at = c * 192
        first = out[c].astype(f32)
        second = out[c + 1].astype(f32)
        tail = jnp.concatenate([first[:, LANES:], jnp.zeros((rows, 64), f32)], axis=1)
        next_tail = jnp.concatenate([second[:, LANES:], jnp.zeros((rows, 64), f32)], axis=1)
        turned = pltpu.roll(second[:, :LANES], 64, 1)
        out_o[:, at : at + LANES] = first[:, :LANES]
        out_o[:, at + LANES : at + 2 * LANES] = jnp.where(lane < 64, tail, turned)
        out_o[:, at + 2 * LANES : at + 3 * LANES] = jnp.where(lane < 64, turned, pltpu.roll(next_tail, 64, 1))


def pack(down, gu, out, qkv, grad, result, attn, ffn):
    n, shard = gu.shape[0], gu.shape[1]
    rows = shard // n
    width = down.shape[2]
    f32 = jnp.float32
    spec = pl.BlockSpec
    shape = jax.ShapeDtypeStruct
    tiles = n * gu.shape[2] // LANES
    quarter = grad.shape[0] // 4
    return pl.pallas_call(
        pack_kernel,
        grid=(n,),
        out_shape=(
            shape((n * down.shape[1], width), f32), shape((shard * tiles, LANES), f32), shape((shard, n * out.shape[2]), f32),
            shape((shard, (HEADS + 2 * KV_HEADS) * HEAD_DIM), f32), shape(grad.shape, f32), shape(result.shape, result.dtype), shape(attn.shape, f32), shape(ffn.shape, f32),
        ),
        in_specs=[
            spec((1,) + down.shape[1:], lambda i: (i, 0, 0)), spec((n, rows, gu.shape[2]), lambda i: (0, i, 0)),
            spec((n, rows, out.shape[2]), lambda i: (0, i, 0)), spec((n, rows, qkv.shape[2]), lambda i: (0, i, 0)),
            spec((quarter, width), lambda i: (i // 2, 0)), spec((quarter, width), lambda i: (i // 2, 0)),
            spec(attn.shape, lambda i: (0, 0)), spec(ffn.shape, lambda i: (0, 0)),
        ],
        out_specs=[
            spec((down.shape[1], width), lambda i: (i, 0)), spec((rows * tiles, LANES), lambda i: (i, 0)),
            spec((rows, n * out.shape[2]), lambda i: (i, 0)), spec((rows, (HEADS + 2 * KV_HEADS) * HEAD_DIM), lambda i: (i, 0)),
            spec((quarter, width), lambda i: (i // 2, 0)), spec((quarter, width), lambda i: (i // 2, 0)),
            spec(attn.shape, lambda i: (0, 0)), spec(ffn.shape, lambda i: (0, 0)),
        ],
        name="pack",
    )(down, gu, out, qkv, grad, result, attn, ffn)


def fast_body(
    tokens, positions, qkv_weight, out_weight, gate_up_weight, down_weight, attn_gain, ffn_gain, cotangent
):
    me = lax.axis_index("ctx")
    n = lax.axis_size("ctx")
    planes = lax.axis_size("fsdp")
    rows = tokens.shape[1]
    length = n * rows
    width = tokens.shape[2]
    wide = down_weight.shape[1] * planes
    own = wide // n
    piece = own // planes
    shard = qkv_weight.shape[1]
    query_width = HEADS * HEAD_DIM
    key_width = KV_HEADS * HEAD_DIM
    cut = lax.dynamic_slice_in_dim

    qkv = qkv_weight[0]
    q_part = cut(qkv, me * 2 * HEAD_DIM, 2 * HEAD_DIM, 1)
    k_part = cut(qkv, query_width + me * HEAD_DIM, HEAD_DIM, 1)
    v_part = cut(qkv, query_width + key_width + me * HEAD_DIM, HEAD_DIM, 1)
    qkv_own = jnp.concatenate([q_part, k_part, v_part], axis=1)
    pieces = [cut(gate_up_weight[0], at * (wide // planes) + me * piece, piece, 2) for at in range(planes)]
    gate_up_own = jnp.concatenate([x[:, s] for s in range(2) for x in pieces], axis=1)
    (
        middle_grad, ffn_partial, spots, gains, down_sum, hidden, qkv_block, down_block, q, k, v, att, lse, middle,
        turns, normed, attended_grad, low_all, gate_up_grad, middle_cols,
    ) = front_moves(
        tokens[0], positions, attn_gain, ffn_gain, qkv_own, gate_up_own, *turn_parts(2 * n, rows // 2),
        out_weight, down_weight, cotangent[0],
    )
    stream_grad, result, attn_sum, ffn_sum, down_grad, gate_up_grad, out_grad, qkv_grad = back_moves(
        tokens[0], gains, ffn_partial, down_sum, spots,
        gate_up_grad, middle_grad, hidden, down_block, k, q, v, attended_grad, att, lse, turns, normed, middle,
        qkv_block, middle_cols, low_all,
    )
    down_grad, gate_up_grad, out_grad, qkv_grad, stream_grad, result, attn_sum, ffn_sum = pack(
        down_grad, gate_up_grad, out_grad, qkv_grad, stream_grad, result, attn_sum, ffn_sum
    )
    gate_up_grad = gate_up_grad.reshape(shard, wide // LANES, 2, LANES).transpose(0, 2, 1, 3).reshape(shard, 2, wide)
    return (
        result[None],
        stream_grad[None],
        qkv_grad[None],
        out_grad[None],
        gate_up_grad[None],
        down_grad[None],
        attn_sum,
        ffn_sum,
    )


def solution(mesh):
    split = mesh.shape["ctx"] == KV_HEADS and mesh.shape["fsdp"] == 4
    placed = (
        P("fsdp", "ctx", None),
        P("fsdp", "ctx"),
        P(None, "fsdp", None),
        P(None, "fsdp", None),
        P(None, "fsdp", None, None),
        P(None, "fsdp", None),
        P(None, "fsdp"),
        P(None, "fsdp"),
        P("fsdp", "ctx", None),
    )
    return jax.shard_map(
        fast_body if split else body,
        mesh=mesh,
        in_specs=placed,
        out_specs=(
            P("fsdp", "ctx", None),
            P("fsdp", "ctx", None),
            P(None, "fsdp", None),
            P(None, "fsdp", None),
            P(None, "fsdp", None, None),
            P(None, "fsdp", None),
            P(None, "fsdp"),
            P(None, "fsdp"),
        ),
        check_vma=False,
    )
```

```python
import jax
import jax.numpy as jnp
import numpy as np
from jax import lax
from jax.experimental import pallas as pl
from jax.experimental.pallas import tpu as pltpu
from jax.sharding import PartitionSpec as P

HEADS = 16
KV_HEADS = 8
HEAD_DIM = 96
LAYERS = 1


epsilon = 1e-05
rope_base = 100000.0


def angles(place):
    halfway = HEAD_DIM // 2
    frequency = rope_base ** (-(jnp.arange(halfway, dtype=jnp.float32) * 2.0 / HEAD_DIM))
    phases = place.astype(jnp.float32)[:, None] * frequency[None, :]
    phases = jnp.concatenate([phases, phases], axis=-1)
    return (jnp.cos(phases)[:, None, :], jnp.sin(phases)[:, None, :])


def rotate(vectors, cosine, sine):
    halfway = vectors.shape[-1] // 2
    turned = jnp.concatenate([-vectors[..., halfway:], vectors[..., :halfway]], axis=-1)
    return vectors * cosine + turned * sine


def rotate_back(grads, cosine, sine):
    halfway = grads.shape[-1] // 2
    scaled = grads * sine
    return grads * cosine + jnp.concatenate(
        [scaled[..., halfway:], -scaled[..., :halfway]], axis=-1
    )


def normalize(rows, gain):
    factor = lax.rsqrt(jnp.mean(rows * rows, axis=-1, keepdims=True) + epsilon)
    return (rows * factor * gain, factor)


def normalize_back(upstream, rows, factor, gain):
    unit_rows = rows * factor
    gain_grad = jnp.sum(upstream * unit_rows, axis=0)
    scaled = upstream * gain
    row_inner = jnp.mean(scaled * unit_rows, axis=-1, keepdims=True)
    return (factor * (scaled - unit_rows * row_inner), gain_grad)


def split_blocks(queries, keys_all, values_all, key_place):
    rows = queries.shape[0]
    half = rows // 2
    shards = key_place.shape[0] // rows
    key_blocks = keys_all.reshape(shards, 2, half, KV_HEADS, HEAD_DIM)
    value_blocks = values_all.reshape(shards, 2, half, KV_HEADS, HEAD_DIM)
    place_blocks = key_place.reshape(shards, 2, half)
    return (key_blocks, value_blocks, place_blocks)


def scores_of(queries, key_block, place_block, query_place):
    scaling = HEAD_DIM ** (-0.5)
    scores = (
        jnp.einsum("rkgd,skd->kgrs", queries, key_block, preferred_element_type=jnp.float32)
        * scaling
    )
    allowed = place_block[None, None, None, :] <= query_place[None, None, :, None]
    return (scores, allowed)


def reachable(place_block, query_place):
    return jnp.min(place_block) <= jnp.max(query_place)


def attention_forward(queries, keys_all, values_all, query_place, key_place):
    key_blocks, value_blocks, place_blocks = split_blocks(queries, keys_all, values_all, key_place)
    rows = queries.shape[0]
    half = rows // 2
    groups = HEADS // KV_HEADS
    query_spans = queries.reshape(2, half, KV_HEADS, groups, HEAD_DIM)
    place_spans = query_place.reshape(2, half)

    def sweep_max(carry, inputs):
        key_block, place_block = inputs
        updated_all = []
        for span in range(2):
            state = carry[span]
            for part in range(2):

                def live(current, span=span, part=part):
                    maximum, total = current
                    scores, allowed = scores_of(
                        query_spans[span], key_block[part], place_block[part], place_spans[span]
                    )
                    masked = jnp.where(allowed, scores, -1e30)
                    updated = jnp.maximum(maximum, jnp.max(masked, axis=-1))
                    weights_now = jnp.where(allowed, jnp.exp(masked - updated[..., None]), 0.0)
                    return (
                        updated,
                        total * jnp.exp(maximum - updated) + jnp.sum(weights_now, axis=-1),
                    )

                state = lax.cond(
                    reachable(place_block[part], place_spans[span]),
                    live,
                    lambda current: current,
                    state,
                )
            updated_all.append(state)
        return (tuple(updated_all), None)

    start_max = jnp.full((KV_HEADS, groups, half), -1e30, jnp.float32)
    start_total = jnp.zeros((KV_HEADS, groups, half), jnp.float32)
    start = ((start_max, start_total), (start_max, start_total))
    finals, unused = lax.scan(sweep_max, start, (key_blocks, place_blocks))
    logsum_spans = [finals[span][0] + jnp.log(finals[span][1]) for span in range(2)]

    def sweep_out(results, inputs):
        key_block, value_block, place_block = inputs
        updated_all = []
        for span in range(2):
            result = results[span]
            for part in range(2):

                def live(current, span=span, part=part):
                    scores, allowed = scores_of(
                        query_spans[span], key_block[part], place_block[part], place_spans[span]
                    )
                    softmax_rows = jnp.where(
                        allowed, jnp.exp(scores - logsum_spans[span][..., None]), 0.0
                    ).astype(jnp.bfloat16)
                    return current + jnp.einsum(
                        "kgrs,skd->rkgd",
                        softmax_rows,
                        value_block[part],
                        preferred_element_type=jnp.float32,
                    )

                result = lax.cond(
                    reachable(place_block[part], place_spans[span]),
                    live,
                    lambda current: current,
                    result,
                )
            updated_all.append(result)
        return (tuple(updated_all), None)

    start_out = jnp.zeros((half, KV_HEADS, groups, HEAD_DIM), jnp.float32)
    outs, unused_out = lax.scan(
        sweep_out, (start_out, start_out), (key_blocks, value_blocks, place_blocks)
    )
    logsum = jnp.concatenate(logsum_spans, axis=-1)
    attended = jnp.concatenate([outs[0], outs[1]], axis=0)
    return (logsum, attended)


def attention_backward(
    queries, keys_all, values_all, query_place, key_place, logsum, attended_grad, row_inner
):
    key_blocks, value_blocks, place_blocks = split_blocks(queries, keys_all, values_all, key_place)
    rows = queries.shape[0]
    half = rows // 2
    groups = HEADS // KV_HEADS
    scaling = HEAD_DIM ** (-0.5)
    query_spans = queries.reshape(2, half, KV_HEADS, groups, HEAD_DIM)
    place_spans = query_place.reshape(2, half)
    grad_spans = attended_grad.reshape(2, half, KV_HEADS, groups, HEAD_DIM)
    logsum_spans = logsum.reshape(KV_HEADS, groups, 2, half)
    inner_spans = row_inner.reshape(KV_HEADS, groups, 2, half)

    def sweep_back(query_grads, inputs):
        key_block, value_block, place_block = inputs
        query_grads = list(query_grads)
        key_parts = []
        value_parts = []
        for part in range(2):
            key_acc = jnp.zeros((half, KV_HEADS, HEAD_DIM), jnp.float32)
            value_acc = jnp.zeros((half, KV_HEADS, HEAD_DIM), jnp.float32)
            for span in range(2):

                def live(current, span=span, part=part):
                    query_grad, key_grad, value_grad = current
                    scores, allowed = scores_of(
                        query_spans[span], key_block[part], place_block[part], place_spans[span]
                    )
                    softmax_rows = jnp.where(
                        allowed, jnp.exp(scores - logsum_spans[:, :, span][..., None]), 0.0
                    )
                    rounded = softmax_rows.astype(jnp.bfloat16)
                    weight_grad = jnp.einsum(
                        "rkgd,skd->kgrs",
                        grad_spans[span],
                        value_block[part],
                        preferred_element_type=jnp.float32,
                    )
                    score_grad = (
                        softmax_rows * (weight_grad - inner_spans[:, :, span][..., None])
                    ).astype(jnp.bfloat16)
                    query_grad = (
                        query_grad
                        + jnp.einsum(
                            "kgrs,skd->rkgd",
                            score_grad,
                            key_block[part],
                            preferred_element_type=jnp.float32,
                        )
                        * scaling
                    )
                    key_grad = (
                        key_grad
                        + jnp.einsum(
                            "kgrs,rkgd->skd",
                            score_grad,
                            query_spans[span],
                            preferred_element_type=jnp.float32,
                        )
                        * scaling
                    )
                    value_grad = value_grad + jnp.einsum(
                        "kgrs,rkgd->skd",
                        rounded,
                        grad_spans[span],
                        preferred_element_type=jnp.float32,
                    )
                    return (query_grad, key_grad, value_grad)

                state = (query_grads[span], key_acc, value_acc)
                state = lax.cond(
                    reachable(place_block[part], place_spans[span]),
                    live,
                    lambda current: current,
                    state,
                )
                query_grads[span], key_acc, value_acc = state
            key_parts.append(key_acc)
            value_parts.append(value_acc)
        key_out = jnp.concatenate(key_parts, axis=0)
        value_out = jnp.concatenate(value_parts, axis=0)
        return (tuple(query_grads), (key_out, value_out))

    start_grad = jnp.zeros((half, KV_HEADS, groups, HEAD_DIM), jnp.float32)
    query_pair, (key_grads, value_grads) = lax.scan(
        sweep_back, (start_grad, start_grad), (key_blocks, value_blocks, place_blocks)
    )
    query_grad = jnp.concatenate([query_pair[0], query_pair[1]], axis=0)
    return (
        query_grad,
        key_grads.reshape(-1, KV_HEADS, HEAD_DIM),
        value_grads.reshape(-1, KV_HEADS, HEAD_DIM),
    )


def fetch_layer(qkv_weight, out_weight, gate_up_weight, down_weight, attn_gain, ffn_gain, layer_id):
    return (
        lax.all_gather(qkv_weight[layer_id], "fsdp", axis=0, tiled=True),
        lax.all_gather(out_weight[layer_id], "fsdp", axis=0, tiled=True),
        lax.all_gather(gate_up_weight[layer_id], "fsdp", axis=0, tiled=True),
        lax.all_gather(down_weight[layer_id], "fsdp", axis=0, tiled=True),
        lax.all_gather(attn_gain[layer_id], "fsdp", axis=0, tiled=True),
        lax.all_gather(ffn_gain[layer_id], "fsdp", axis=0, tiled=True),
    )


def fetch_again(qkv_weight, out_weight, gate_up_weight, down_weight, attn_gain, ffn_gain, layer_id):
    return (
        lax.all_gather(qkv_weight[layer_id], "fsdp", axis=0, tiled=True),
        lax.all_gather(out_weight[layer_id], "fsdp", axis=0, tiled=True),
        lax.all_gather(gate_up_weight[layer_id], "fsdp", axis=0, tiled=True),
        lax.all_gather(down_weight[layer_id], "fsdp", axis=0, tiled=True),
        lax.all_gather(attn_gain[layer_id], "fsdp", axis=0, tiled=True),
        lax.all_gather(ffn_gain[layer_id], "fsdp", axis=0, tiled=True),
    )


def forward_layer(stream, query_place, key_place, gathered):
    qkv_full, out_full, gate_up_full, down_full, attn_full, ffn_full = gathered
    rows = stream.shape[0]
    groups = HEADS // KV_HEADS
    query_width = HEADS * HEAD_DIM
    key_width = KV_HEADS * HEAD_DIM
    cosine, sine = angles(query_place)
    normed, first_factor = normalize(stream, attn_full.astype(jnp.float32))
    normed = normed.astype(jnp.bfloat16)
    projected = jnp.dot(normed, qkv_full, preferred_element_type=jnp.float32)
    queries = rotate(projected[:, :query_width].reshape(rows, HEADS, HEAD_DIM), cosine, sine)
    queries = queries.reshape(rows, KV_HEADS, groups, HEAD_DIM).astype(jnp.bfloat16)
    keys_local = rotate(
        projected[:, query_width : query_width + key_width].reshape(rows, KV_HEADS, HEAD_DIM),
        cosine,
        sine,
    ).astype(jnp.bfloat16)
    values_local = (
        projected[:, query_width + key_width :]
        .reshape(rows, KV_HEADS, HEAD_DIM)
        .astype(jnp.bfloat16)
    )
    keys_all, values_all = (
        lax.all_gather(keys_local, "ctx", axis=0, tiled=True),
        lax.all_gather(values_local, "ctx", axis=0, tiled=True),
    )
    logsum, attended = attention_forward(queries, keys_all, values_all, query_place, key_place)
    attended_low = attended.reshape(rows, query_width).astype(jnp.bfloat16)
    middle = stream + jnp.dot(attended_low, out_full, preferred_element_type=jnp.float32)
    second, second_factor = normalize(middle, ffn_full.astype(jnp.float32))
    second = second.astype(jnp.bfloat16)
    gate_up = jnp.einsum("rd,dcf->rcf", second, gate_up_full, preferred_element_type=jnp.float32)
    hidden = (jax.nn.silu(gate_up[:, 0]) * gate_up[:, 1]).astype(jnp.bfloat16)
    result = middle + jnp.dot(hidden, down_full, preferred_element_type=jnp.float32)
    stored = (
        stream,
        first_factor,
        normed,
        queries,
        keys_local,
        values_local,
        keys_all,
        values_all,
        logsum,
        attended,
        attended_low,
        middle,
        second_factor,
        second,
        gate_up,
        hidden,
    )
    return (result, stored)


def backward_layer(upstream, stored, gathered, query_place, key_place, keys_all, values_all):
    (
        stream,
        first_factor,
        normed,
        queries,
        keys_local,
        values_local,
        kept_keys,
        kept_values,
        logsum,
        attended,
        attended_low,
        middle,
        second_factor,
        second,
        gate_up,
        hidden,
    ) = stored
    qkv_full, out_full, gate_up_full, down_full, attn_full, ffn_full = gathered
    rows = stream.shape[0]
    groups = HEADS // KV_HEADS
    cosine, sine = angles(query_place)
    upstream_low = upstream.astype(jnp.bfloat16)
    hidden_grad = jnp.einsum(
        "rd,fd->rf", upstream_low, down_full, preferred_element_type=jnp.float32
    )
    gate_part = gate_up[:, 0]
    up_part = gate_up[:, 1]
    sigmoid = jax.nn.sigmoid(gate_part)
    gate_grad = hidden_grad * up_part * sigmoid * (1.0 + gate_part * (1.0 - sigmoid))
    up_grad = hidden_grad * gate_part * sigmoid
    gate_up_low = jnp.stack([gate_grad, up_grad], axis=1).astype(jnp.bfloat16)
    second_grad = jnp.einsum(
        "rcf,dcf->rd", gate_up_low, gate_up_full, preferred_element_type=jnp.float32
    )
    middle_grad, ffn_gain_grad = normalize_back(
        second_grad, middle, second_factor, ffn_full.astype(jnp.float32)
    )
    middle_grad = middle_grad + upstream
    middle_low = middle_grad.astype(jnp.bfloat16)
    attended_grad = jnp.einsum(
        "rd,od->ro", middle_low, out_full, preferred_element_type=jnp.float32
    )
    attended_grad = attended_grad.astype(jnp.bfloat16).reshape(rows, KV_HEADS, groups, HEAD_DIM)
    row_inner = jnp.einsum("rkgd,rkgd->kgr", attended_grad.astype(jnp.float32), attended)
    query_grad, key_grads, value_grads = attention_backward(
        queries, keys_all, values_all, query_place, key_place, logsum, attended_grad, row_inner
    )
    key_grad, value_grad = (
        lax.psum_scatter(key_grads, "ctx", scatter_dimension=0, tiled=True),
        lax.psum_scatter(value_grads, "ctx", scatter_dimension=0, tiled=True),
    )
    query_grad = rotate_back(query_grad.reshape(rows, HEADS, HEAD_DIM), cosine, sine)
    key_grad = rotate_back(key_grad, cosine, sine)
    projected_grad = jnp.concatenate(
        [query_grad.reshape(rows, -1), key_grad.reshape(rows, -1), value_grad.reshape(rows, -1)],
        axis=1,
    ).astype(jnp.bfloat16)
    normed_grad = jnp.einsum(
        "re,de->rd", projected_grad, qkv_full, preferred_element_type=jnp.float32
    )
    stream_grad, attn_gain_grad = normalize_back(
        normed_grad, stream, first_factor, attn_full.astype(jnp.float32)
    )
    stream_grad = stream_grad + middle_grad
    qkv_grad = jnp.einsum("rd,re->de", normed, projected_grad, preferred_element_type=jnp.float32)
    out_grad = jnp.einsum("ro,rd->od", attended_low, middle_low, preferred_element_type=jnp.float32)
    gate_up_grad = jnp.einsum(
        "rd,rcf->dcf", second, gate_up_low, preferred_element_type=jnp.float32
    )
    down_grad = jnp.einsum("rf,rd->fd", hidden, upstream_low, preferred_element_type=jnp.float32)
    sharded = (
        lax.psum_scatter(qkv_grad, "fsdp", scatter_dimension=0, tiled=True),
        lax.psum_scatter(out_grad, "fsdp", scatter_dimension=0, tiled=True),
        lax.psum_scatter(gate_up_grad, "fsdp", scatter_dimension=0, tiled=True),
        lax.psum_scatter(down_grad, "fsdp", scatter_dimension=0, tiled=True),
        lax.psum_scatter(attn_gain_grad, "fsdp", scatter_dimension=0, tiled=True),
        lax.psum_scatter(ffn_gain_grad, "fsdp", scatter_dimension=0, tiled=True),
    )
    totals = lax.psum(
        (sharded[0], sharded[1], sharded[2], sharded[3], sharded[4], sharded[5]), "ctx"
    )
    return (stream_grad, totals)


def body(
    tokens,
    positions,
    qkv_weight,
    out_weight,
    gate_up_weight,
    down_weight,
    attn_gain,
    ffn_gain,
    cotangent,
):
    query_place = positions[0]
    key_place = lax.all_gather(query_place, "ctx", axis=0, tiled=True)
    stream = tokens[0].astype(jnp.float32)
    gathered_list = []
    layer_id = 0
    gathered = fetch_layer(
        qkv_weight, out_weight, gate_up_weight, down_weight, attn_gain, ffn_gain, layer_id
    )
    stream, stored = forward_layer(stream, query_place, key_place, gathered)
    saved = [stored]
    gathered_list.append(gathered)
    activations = stream.astype(jnp.bfloat16)[None]
    upstream = cotangent[0]
    layer_grads = [None] * LAYERS
    for layer_id in reversed(range(LAYERS)):
        stored = saved[layer_id]
        gathered = fetch_again(
            qkv_weight, out_weight, gate_up_weight, down_weight, attn_gain, ffn_gain, layer_id
        )
        keys_all, values_all = (stored[6], stored[7])
        upstream, totals = backward_layer(
            upstream, stored, gathered, query_place, key_place, keys_all, values_all
        )
        layer_grads[layer_id] = totals
    outputs = [jnp.stack([entry[slot] for entry in layer_grads], axis=0) for slot in range(6)]
    return (
        activations,
        upstream[None],
        outputs[0],
        outputs[1],
        outputs[2],
        outputs[3],
        outputs[4],
        outputs[5],
    )


LANES = 128


def spread(heads):
    half = HEAD_DIM // 2
    pad = ((0, 0), (0, 0), (0, 64 - half))
    return jnp.concatenate([jnp.pad(heads[..., :half], pad), jnp.pad(heads[..., half:], pad)], axis=-1)


def gathered_spread(padded):
    half = HEAD_DIM // 2
    return jnp.concatenate([padded[..., :half], padded[..., 64 : 64 + half]], axis=-1)


def turn_parts(spans, rows):
    half = HEAD_DIM // 2
    frequency = rope_base ** (-(np.arange(half, dtype=np.float64) * 2.0 / HEAD_DIM))

    def waves(place):
        phases = place[:, None] * frequency[None, :]
        pad = ((0, 0), (0, 64 - half))
        return np.pad(np.cos(phases), pad), np.pad(np.sin(phases), pad)

    cosine, sine = waves(np.arange(spans) * float(rows))
    parts = (
        np.concatenate([cosine, cosine], axis=1), np.concatenate([-sine, sine], axis=1),
        np.concatenate(waves(np.arange(rows, dtype=np.float64)), axis=1),
    )
    return tuple(jnp.asarray(part, jnp.float32) for part in parts)


def spread_heads(proj):
    lane = lax.broadcasted_iota(jnp.int32, (proj.shape[0], LANES), 1)
    tiles = [proj[:, at * LANES : (at + 1) * LANES] for at in range(3)]

    def put(*pieces):
        out = jnp.zeros_like(tiles[0])
        for tile, source, target, count in pieces:
            shift = (target - source) % LANES
            moved = pltpu.roll(tiles[tile], shift, 1) if shift else tiles[tile]
            out = jnp.where(jnp.logical_and(lane >= target, lane < target + count), moved, out)
        return out

    return (
        put((0, 0, 0, 48), (0, 48, 64, 48)),
        put((0, 96, 0, 32), (1, 0, 32, 16), (1, 16, 64, 48)),
        put((1, 64, 0, 48), (1, 112, 64, 16), (2, 0, 80, 32)),
        put((2, 32, 0, 96)),
    )


def close_halves(head):
    lane = lax.broadcasted_iota(jnp.int32, head.shape, 1)
    return jnp.where(lane < HEAD_DIM // 2, head, pltpu.roll(head, LANES - 64 + HEAD_DIM // 2, 1))


def wave(rows):
    first = lax.broadcasted_iota(jnp.int32, rows.shape, 1) < 64
    other = pltpu.roll(rows, 64, 1)
    return jnp.where(first, rows, other), jnp.where(first, -other, rows)


def nt(left, right):
    return lax.dot_general(left, right, (((1,), (1,)), ((), ())), preferred_element_type=jnp.float32)


def nn(left, right):
    return lax.dot_general(left, right, (((1,), (0,)), ((), ())), preferred_element_type=jnp.float32)


def tn(left, right):
    return lax.dot_general(left, right, (((0,), (0,)), ((), ())), preferred_element_type=jnp.float32)


def causal(width, place):
    key_at = lax.broadcasted_iota(jnp.int32, (2 * width, 2 * width), 0)
    query_at = lax.broadcasted_iota(jnp.int32, (2 * width, 2 * width), 1)
    query_at = jnp.where(query_at >= width, query_at - width, query_at)
    return key_at <= query_at + place * width


def vm(count):
    return [pl.BlockSpec(memory_space=pltpu.VMEM)] * count


MESH = pl.DeviceIdType.MESH


class Place:
    def __init__(self):
        self.me = lax.axis_index("ctx")
        core, x, y = self.me % 2, (self.me // 2) % 2, self.me // 4
        self.dp, self.dx, self.dy = 1 - 2 * core, 2 - 4 * x, 4 - 8 * y
        self.p, self.x, self.y = self.me + self.dp, self.me + self.dx, self.me + self.dy
        self.d = self.x + self.dy
        self.z = lax.axis_index("fsdp")
        self.planes = lax.axis_size("fsdp")
        self.n = lax.axis_size("ctx")


def greet(place, ctx=True, planes=False):
    barrier = pltpu.get_barrier_semaphore()
    count = 0
    if ctx:
        for step in range(1, place.n):
            pl.semaphore_signal(
                barrier, inc=1, device_id={"ctx": lax.rem(place.me + step, place.n)}, device_id_type=MESH
            )
            count += 1
    if planes:
        for step in range(1, place.planes):
            pl.semaphore_signal(
                barrier, inc=1, device_id={"fsdp": lax.rem(place.z + step, place.planes)}, device_id_type=MESH
            )
            count += 1
    pl.semaphore_wait(barrier, count)


def send(source, target, send_sem, recv_sem, **where):
    return pltpu.make_async_remote_copy(
        src_ref=source, dst_ref=target, send_sem=send_sem, recv_sem=recv_sem,
        device_id=where, device_id_type=MESH,
    )


class Gather:
    sems = 14

    def __init__(self, place, own, out, sem):
        self.place, self.own, self.out, self.sem = place, own, out, sem
        self.half = out.shape[1] // 2
        self.started = []
        self.met = False

    def go(self, source, target, index, rank):
        send(source, target, self.sem.at[0, index], self.sem.at[1, index], ctx=rank).start()
        self.started.append(index)

    def whole_block(self, index):
        return index == 6

    def sent(self):
        p = self.place
        for index in self.started:
            part = self.whole(p.me) if self.whole_block(index) else self.part(p.me, 0)
            send(part, part, self.sem.at[0, index], self.sem.at[1, index], ctx=p.p).wait_send()

    def part(self, rank, half):
        return self.out.at[rank, pl.ds(half * self.half, self.half)]

    def whole(self, rank):
        return self.out.at[rank]

    def start(self):
        p = self.place
        keep = pltpu.make_async_copy(self.own, self.whole(p.me), self.sem.at[0, 13])
        keep.start()
        self.keep = keep
        halves = [self.own.at[pl.ds(h * self.half, self.half)] for h in range(2)]
        self.go(halves[0], self.part(p.me, 0), 0, p.x)
        self.go(halves[1], self.part(p.me, 1), 3, p.y)
        self.go(self.own, self.whole(p.me), 6, p.p)
        self.go(halves[1], self.part(p.me, 1), 1, p.x)
        self.go(halves[0], self.part(p.me, 0), 2, p.y)

    def arrived(self, rank, half, index):
        part = self.part(rank, half)
        pltpu.make_async_copy(part, part, self.sem.at[1, index]).wait()
        return part

    def relay(self):
        p = self.place
        part = self.arrived(p.x, 0, 0)
        self.go(part, part, 4, p.y)
        self.go(part, part, 7, p.p)
        part = self.arrived(p.y, 1, 3)
        self.go(part, part, 5, p.x)
        self.go(part, part, 10, p.p)

    def rest(self):
        p = self.place
        for rank, half, index, onward in ((p.x, 1, 1, 8), (p.y, 0, 2, 9), (p.d, 0, 4, 11), (p.d, 1, 5, 12)):
            part = self.arrived(rank, half, index)
            self.go(part, part, onward, p.p)

    def first_partner(self):
        part = self.whole(self.place.p)
        pltpu.make_async_copy(part, part, self.sem.at[1, 6]).wait()
        self.met = True

    def partner(self):
        p = self.place
        if not self.met:
            self.first_partner()
        for rank, half, index in (
            (p.x, 0, 7), (p.y, 1, 10), (p.x, 1, 8), (p.y, 0, 9), (p.d, 0, 11), (p.d, 1, 12),
        ):
            self.arrived(rank + p.dp, half, index)

    def finish(self, kept=False):
        if not kept:
            self.keep.wait()
        self.sent()


class PlaneGather:
    def __init__(self, place, own, out, sem):
        self.place, self.own, self.out, self.sem = place, own, out, sem

    def hop(self, step, up):
        p = self.place
        sign = 1 if up else -1
        source = p.z - sign * step
        target = p.z + sign
        ok = jnp.logical_and(
            jnp.logical_and(source >= 0, source < p.planes),
            jnp.logical_and(target >= 0, target < p.planes),
        )
        source = jnp.clip(source, 0, p.planes - 1)
        target = jnp.clip(target, 0, p.planes - 1)
        block = self.own if step == 0 else self.out.at[source]
        return ok, send(
            block, self.out.at[source], self.sem.at[0 if up else 1, source], self.sem.at[2, source], fsdp=target
        )

    def start(self):
        p = self.place
        self.keep = pltpu.make_async_copy(self.own, self.out.at[p.z], self.sem.at[2, p.z])
        self.keep.start()
        for up in (True, False):
            ok, copy = self.hop(0, up)
            pl.when(ok)(copy.start)

    def got(self, step, up):
        p = self.place
        source = p.z - step if up else p.z + step
        ok = jnp.logical_and(source >= 0, source < p.planes)
        source = jnp.clip(source, 0, p.planes - 1)
        part = self.out.at[source]
        return ok, pltpu.make_async_copy(part, part, self.sem.at[2, source])

    def step(self, number):
        for up in (True, False):
            ok, copy = self.got(number, up)
            pl.when(ok)(copy.wait)
            if number < self.place.planes - 1:
                ok, copy = self.hop(number, up)
                pl.when(ok)(copy.start)

    def finish(self, kept=False):
        if not kept:
            self.keep.wait()
        for number in range(self.place.planes - 1):
            for up in (True, False):
                ok, copy = self.hop(number, up)
                pl.when(ok)(copy.wait_send)


class Exchange:
    def __init__(self, place, blocks, out, sem):
        self.place, self.blocks, self.out, self.sem = place, blocks, out, sem

    def pick(self, rank):
        return self.blocks.at[rank]

    def copy(self, step):
        p = self.place
        rank = lax.rem(p.me + step, p.n)
        return send(self.pick(rank), self.out.at[p.me], self.sem.at[0, step], self.sem.at[1, step], ctx=rank)

    def start(self):
        p = self.place
        for step in range(1, p.n):
            self.copy(step).start()
        self.keep = pltpu.make_async_copy(self.pick(p.me), self.out.at[p.me], self.sem.at[0, 0])
        self.keep.start()

    def finish(self):
        p = self.place
        self.keep.wait()
        for step in range(1, p.n):
            self.copy(step).wait_send()
        for step in range(1, p.n):
            part = self.out.at[lax.rem(p.me + p.n - step, p.n)]
            pltpu.make_async_copy(part, part, self.sem.at[1, step]).wait()


class Share(Exchange):
    def pick(self, rank):
        return self.blocks


class PlaneShare:
    def __init__(self, place, block, out, sem):
        self.place, self.block, self.out, self.sem = place, block, out, sem

    def copy(self, step):
        p = self.place
        plane = lax.rem(p.z + step, p.planes)
        return send(self.block, self.out.at[p.z], self.sem.at[0, step], self.sem.at[1, step], fsdp=plane)

    def start(self):
        p = self.place
        for step in range(1, p.planes):
            self.copy(step).start()
        self.keep = pltpu.make_async_copy(self.block, self.out.at[p.z], self.sem.at[0, 0])
        self.keep.start()

    def finish(self):
        p = self.place
        self.keep.wait()
        for step in range(1, p.planes):
            self.copy(step).wait_send()
        for step in range(1, p.planes):
            part = self.out.at[lax.rem(p.z + p.planes - step, p.planes)]
            pltpu.make_async_copy(part, part, self.sem.at[1, step]).wait()


def anywhere(count):
    return [pl.BlockSpec(memory_space=pl.ANY)] * count


class Reduce:
    sems = 10

    def __init__(self, place, mine, theirs, first, out, second, sem):
        self.place, self.mine, self.theirs, self.first, self.out, self.second, self.sem = (
            place, mine, theirs, first, out, second, sem
        )
        self.half = out.shape[1]
        self.started = []

    def push(self, slot):
        copy = send(
            self.theirs.at[slot], self.first.at[slot], self.sem.at[0, slot], self.sem.at[1, slot], ctx=self.place.p
        )
        copy.start()
        return copy

    def pushed(self):
        for slot in range(4):
            send(
                self.theirs.at[slot], self.first.at[slot], self.sem.at[0, slot], self.sem.at[1, slot],
                ctx=self.place.p,
            ).wait_send()

    def add(self, slot):
        part = self.first.at[slot]
        pltpu.make_async_copy(part, part, self.sem.at[1, slot]).wait()
        self.mine[slot] = self.mine[slot] + self.first[slot].astype(jnp.float32)

    def go(self, index, value, rank):
        self.out[index] = value.astype(jnp.bfloat16)
        self.turned(index, rank).start()
        self.started.append((index, rank))

    def turned(self, index, rank):
        return send(
            self.out.at[index], self.second.at[index], self.sem.at[0, 4 + index], self.sem.at[1, 4 + index], ctx=rank
        )

    def top(self, slot):
        return self.mine[slot, pl.ds(0, self.half), :]

    def low(self, slot):
        return self.mine[slot, pl.ds(self.half, self.half), :]

    def got(self, index):
        part = self.second.at[index]
        pltpu.make_async_copy(part, part, self.sem.at[1, 4 + index]).wait()
        return self.second[index].astype(jnp.float32)

    def across(self):
        self.add(3)
        self.go(1, self.top(3), self.place.x)
        self.go(3, self.low(3), self.place.y)

    def beside(self):
        self.add(1)
        self.go(0, self.top(1), self.place.x)
        self.add(2)
        self.go(2, self.low(2), self.place.y)

    def turn(self):
        self.go(4, self.top(2) + self.got(1), self.place.y)
        self.go(5, self.low(1) + self.got(3), self.place.x)

    def total(self, use):
        self.add(0)
        use(pl.ds(0, self.half), self.top(0) + self.got(0) + self.got(4))
        use(pl.ds(self.half, self.half), self.low(0) + self.got(2) + self.got(5))

    def finish(self):
        self.pushed()
        for index, rank in self.started:
            self.turned(index, rank).wait_send()


def flip(place, i):
    return place.me + (i % 2) * place.dp + ((i // 2) % 2) * place.dx + (i // 4) * place.dy


class HalfGather(Gather):
    sems = 16

    def __init__(self, place, own, out, sem):
        self.place, self.own, self.out, self.sem = place, own, out, sem
        self.half = out.shape[1]
        self.started = []
        self.met = False

    def part(self, rank, half):
        return self.out.at[2 * rank + half]

    def whole_block(self, index):
        return False

    def start(self):
        p = self.place
        halves = [self.own.at[pl.ds(h * self.half, self.half)] for h in range(2)]
        self.kept = [
            pltpu.make_async_copy(halves[h], self.part(p.me, h), self.sem.at[0, (13, 15)[h]]) for h in range(2)
        ]
        self.go(halves[0], self.part(p.me, 0), 0, p.x)
        self.go(halves[1], self.part(p.me, 1), 3, p.y)
        self.go(halves[0], self.part(p.me, 0), 6, p.p)
        self.go(halves[1], self.part(p.me, 1), 14, p.p)
        self.go(halves[1], self.part(p.me, 1), 1, p.x)
        self.go(halves[0], self.part(p.me, 0), 2, p.y)
        for copy in self.kept:
            copy.start()

    def first_partner(self):
        for h in range(2):
            self.arrived(self.place.p, h, (6, 14)[h])
        self.met = True

    def own_in(self):
        for copy in self.kept:
            copy.wait()

    def finish(self):
        self.sent()


def packed(block):
    rows = block.shape[0] // 2
    tail = jnp.concatenate([block[:, LANES:], jnp.zeros((2 * rows, 64), block.dtype)], axis=1)
    first = lax.broadcasted_iota(jnp.int32, (rows, LANES), 1) < 64
    return jnp.concatenate([block[:, :LANES], jnp.where(first, tail[:rows], pltpu.roll(tail[rows:], 64, 1))], axis=0)


def unpacked(block):
    rows = block.shape[0] // 3
    tail = block[2 * rows :].astype(jnp.float32)
    tails = jnp.concatenate([tail, pltpu.roll(tail, 64, 1)], axis=0)[:, :64].astype(block.dtype)
    return jnp.concatenate([block[: 2 * rows], tails], axis=1)


class PlaneReduce:
    def __init__(self, place, block, recv, sem):
        self.place, self.block, self.recv, self.sem = place, block, recv, sem

    def hop(self, ok, part, slot, target, first, wait):
        copy = send(
            self.block.at[part], self.recv.at[slot], self.sem.at[0, part], self.sem.at[1, slot], fsdp=target
        )

        @pl.when(ok)
        def _():
            if wait:
                copy.wait_send()
                return
            if not first:
                self.merge(part, part)
            copy.start()

    def merge(self, part, slot):
        piece = self.recv.at[slot]
        pltpu.make_async_copy(piece, piece, self.sem.at[1, slot]).wait()
        total = self.block[part].astype(jnp.float32) + self.recv[slot].astype(jnp.float32)
        self.block[part] = total.astype(jnp.bfloat16)

    def ends(self, i, wait=False):
        z = self.place.z
        low = z == 0
        part = jnp.where(low, 3 - i, i)
        slot = part if i < 2 else jnp.where(low, part, 4)
        self.hop(jnp.logical_or(low, z == 3), part, slot, jnp.where(low, 1, 2), True, wait)

    def inner(self, up, down, slot_up, slot_down, to_up, to_down, wait=False):
        z = self.place.z
        low = z == 1
        part = jnp.where(low, up, down)
        slot = jnp.where(low, slot_up, slot_down)
        self.hop(jnp.logical_or(low, z == 2), part, slot, jnp.where(low, to_up, to_down), False, wait)

    def start(self, wait=False):
        for i in range(3):
            self.ends(i, wait)

    def step1(self, wait=False):
        self.inner(3, 0, 3, 0, 2, 1, wait)

    def step2(self, wait=False):
        self.inner(2, 1, 2, 4, 2, 1, wait)
        self.inner(0, 3, 4, 3, 0, 3, wait)

    def total(self):
        z = self.place.z

        @pl.when(z > 0)
        def _():
            self.merge(z, z)

        @pl.when(z < 3)
        def _():
            self.merge(z, 4)

    def own(self):
        return self.block.at[self.place.z]

    def finish(self):
        self.start(True)
        self.step1(True)
        self.step2(True)


class Steps:
    def __init__(self, *steps):
        self.steps = list(steps)

    def next(self, count=1):
        for step in self.steps[:count]:
            step()
        self.steps = self.steps[count:]

    def rest(self):
        self.next(len(self.steps))


class OutGather(Gather):
    def __init__(self, place, own, out, sem):
        self.place, self.own, self.out, self.sem = place, own, out, sem
        self.half = out.shape[0] // 2
        self.started = []
        self.met = False

    def part(self, rank, half):
        return self.out.at[pl.ds(half * self.half, self.half), rank]

    def whole(self, rank):
        return self.out.at[:, rank]


def front_kernel(
    tok, pos, attn_own, ffn_own, qkv_own, gu_own, far_cos, far_sin, near, out_weight, down_weight, up,
    middle_grad, gain_grad, spots, gains, down_sum,
    hidden_o, qkv_o, down_o, q_o, k_o, v_o, att_o, lse_o, middle_o, turn_o, normed, agrad, low_all, gu_out, mcols,
    hidden, qkv_w, down_w, q_ref, k_ref, v_ref, att_ref, lse_ref, middle, turn_ref, mcols_send, up_low, spot, gain_own,
    wide_in, up_all, gul, gu_w, out_block, out_w, low_sorted, gain_all, spots_s, order_s, low,
    attended, own, mine, theirs, first, out, second, down_g, down_r,
    tok_sem, up_sem, spot_sem, gain_sem, qkv_sem, out_sem, outc_sem, gu_sem, down_sem, local_sem,
    low_sem, gather_sem, reduce_sem, agrad_sem, lows_sem, down_zs, mcols_sem,
):
    place = Place()
    n = place.n
    rows = tok.shape[0]
    half = rows // 2
    pairs = 8
    heads = rows
    length = n * rows
    width = tok.shape[1]
    out_own = out_weight.at[0, pl.ds(place.me * (out_weight.shape[1] // 8), out_weight.shape[1] // 8)]
    down_own = down_weight.at[0, pl.ds(place.me * (down_weight.shape[1] // 8), down_weight.shape[1] // 8)]
    spot[...] = jnp.broadcast_to(pos[0:1, 0:1], spot.shape)
    gain_own[pl.ds(0, 1), :] = attn_own[...].astype(jnp.float32)
    gain_own[pl.ds(1, 1), :] = ffn_own[...].astype(jnp.float32)
    fetch = pltpu.make_async_copy(up, middle_grad, local_sem.at[0])
    fetch.start()
    greet(place, planes=True)
    spans = Share(place, spot, spots, spot_sem)
    scales = PlaneShare(place, gain_own, gain_all, gain_sem)
    tokens = HalfGather(place, tok, wide_in, tok_sem)
    cots = Gather(place, up_low, up_all, up_sem)
    qkvs = PlaneGather(place, qkv_own, qkv_w, qkv_sem)
    outs = PlaneGather(place, out_own, out_block, out_sem)
    outc = OutGather(place, out_block, out_w, outc_sem)
    gus = PlaneGather(place, gu_own, gu_w, gu_sem)
    downs = PlaneGather(place, down_own, down_w, down_sem)
    given = []

    def give(source, target):
        copy = pltpu.make_async_copy(source, target, local_sem.at[5 + len(given)])
        copy.start()
        given.append(copy)

    tokens.start()
    qkvs.start()
    spans.start()
    scales.start()

    def turn_rows(at, carry):
        base = near[...]
        turn_ref[at] = base * far_cos[pl.ds(at, 1), :] + pltpu.roll(base, 64, 1) * far_sin[pl.ds(at, 1), :]
        return carry

    lax.fori_loop(0, 2 * pairs, turn_rows, 0)
    give(turn_ref, turn_o)
    fetch.wait()
    up_low[...] = middle_grad[...].astype(jnp.bfloat16)
    tokens.relay()
    qkvs.step(1)
    outs.start()
    qkvs.step(2)
    tokens.rest()
    cots.start()
    outs.step(1)
    downs.start()
    qkvs.step(3)
    tokens.partner()
    tokens.own_in()
    spans.finish()
    scales.finish()
    qkvs.keep.wait()
    table = pltpu.make_async_copy(spots, spots_s, local_sem.at[1])
    table.start()
    for g in range(2):
        gains[pl.ds(g, 1), :] = jnp.concatenate([gain_all[z, pl.ds(g, 1), :] for z in range(4)], axis=1)
    table.wait()
    early = [lax.div(spots_s[j, 0, 0], half) for j in range(pairs)]
    for t in range(pairs):
        at = 0
        for j in range(pairs):
            at = jnp.where(early[j] == t, j, at)
        order_s[t] = 2 * at
        order_s[2 * pairs - 1 - t] = 2 * at + 1
    cots.relay()

    def project(j, store):
        x = jnp.concatenate([wide_in[order_s[4 * j + i]] for i in range(4)], axis=0).astype(jnp.float32)
        factor = lax.rsqrt(jnp.mean(x * x, axis=-1, keepdims=True) + epsilon)
        scaled = (x * factor * gains[pl.ds(0, 1), :]).astype(jnp.bfloat16)
        store[pl.ds(2 * (j % 2), 2)] = scaled.reshape(2, rows, -1)
        proj = nn(scaled, qkv_w[...].reshape(-1, 3 * LANES))
        spread = spread_heads(proj)
        for piece in range(4):
            at = 4 * j + piece
            cosine, sine = wave(turn_ref[at])

            def turned(part):
                z = spread[part][piece * half : (piece + 1) * half]
                return (z * cosine + pltpu.roll(z, 64, 1) * sine).astype(jnp.bfloat16)

            base = (2 * j + piece // 2) * 4 * half + (piece % 2) * half
            q_ref[pl.ds(pl.multiple_of(base, half), half), :] = turned(0)
            q_ref[pl.ds(pl.multiple_of(base + 2 * half, half), half), :] = turned(1)
            k_ref[pl.ds(pl.multiple_of(at * half, half), half), :] = turned(2)
            v_ref[pl.ds(pl.multiple_of(at * half, half), half), :] = spread[3][piece * half : (piece + 1) * half].astype(jnp.bfloat16)

    def project_first(j, carry):
        project(j, theirs)
        return carry

    def project_second(j, carry):
        project(j, first)
        return carry

    lax.fori_loop(0, 2, project_first, 0)
    keep_first = pltpu.make_async_copy(theirs.at[pl.ds(0, 4)], normed.at[pl.ds(0, 4)], local_sem.at[2])
    keep_first.start()
    lax.fori_loop(2, 4, project_second, 0)
    keep_second = pltpu.make_async_copy(first, normed.at[pl.ds(4, 4)], local_sem.at[3])
    keep_second.start()
    give(q_ref, q_o)
    give(k_ref, k_o)
    give(v_ref, v_o)
    give(qkv_w, qkv_o)
    tokens.finish()
    outs.step(2)
    cots.rest()
    outs.step(3)
    outs.keep.wait()
    outc.start()

    def next_weights():
        downs.step(1)
        gus.start()

    steps = Steps(next_weights, lambda: None, outc.relay, lambda: downs.step(2))
    scaling = HEAD_DIM ** (-0.5)
    lane = lax.broadcasted_iota(jnp.int32, (half, LANES), 1)
    values_t = v_ref[...].astype(jnp.float32).T.astype(jnp.bfloat16)
    def attend_group(group):
        before = group * 4 * half

        def attend(place_of, carry):
            pair = 2 * group + place_of
            q = q_ref[pl.ds(pl.multiple_of(pair * 4 * half, 4 * half), 4 * half), :]
            scores = nt(k_ref[pl.ds(before, 4 * half), :], q) * scaling
            parts = [jnp.where(causal(2 * half, place_of), scores, -1e30)]
            if group:
                parts.append(nt(k_ref[pl.ds(0, before), :], q) * scaling)
            tops = [jnp.max(part, axis=0, keepdims=True) for part in parts]
            top = jnp.maximum(tops[0], tops[-1])
            parts = [jnp.exp(part - top) for part in parts]
            total = sum(jnp.sum(part, axis=0, keepdims=True) for part in parts)
            parts = [(part * (1.0 / total)).astype(jnp.bfloat16) for part in parts]
            lse_ref[pl.ds(pair, 1), :] = top + jnp.log(total)
            out_t = nn(values_t[:, before : before + 4 * half], parts[0])
            if group:
                out_t = out_t + nn(values_t[:, :before], parts[1])
            att_ref[pl.ds(pl.multiple_of(pair * LANES, LANES), LANES), :] = out_t
            result = out_t.T.astype(jnp.bfloat16).astype(jnp.float32)
            for part in range(2):
                left = result[part * half : (part + 1) * half]
                right = pltpu.roll(result[(2 + part) * half : (3 + part) * half], half, 1)
                low_sorted[2 * pair + part, :, 0:LANES] = jnp.where(lane < half, left, right).astype(jnp.bfloat16)
                low_sorted[2 * pair + part, :, LANES:] = right.astype(jnp.bfloat16)
            return carry

        lax.fori_loop(0, 2, attend, 0)

    for group in range(pairs // 2):
        attend_group(group)
        steps.next()
    give(att_ref, att_o)
    give(lse_ref, lse_o)
    for j in range(pairs):
        upper = low_sorted[early[j]]
        lower = low_sorted[2 * pairs - 1 - early[j]]
        low[j, pl.ds(0, half), :] = upper[:, :LANES]
        low[j, pl.ds(half, half), :] = lower[:, :LANES]
        tails = jnp.where(
            lane < 64, upper[:, LANES:].astype(jnp.float32), pltpu.roll(lower[:, LANES:].astype(jnp.float32), 64, 1)
        )
        low[j, pl.ds(2 * half, half), :] = tails.astype(jnp.bfloat16)
    keep_first.wait()
    keep_second.wait()
    moved = Exchange(place, low, attended, low_sem)
    moved.start()
    outc.rest()
    outc.partner()
    cots.partner()
    outc.keep.wait()
    moved.finish()
    middle[...] = tok[...].astype(jnp.float32)

    def out_project(q, carry):
        middle[...] += nn(unpacked(attended[q]), out_w[q // 2, pl.ds(4 * (q % 2), 4)].reshape(heads, -1))
        return carry

    lax.fori_loop(0, n, out_project, 0)
    give(middle, middle_o)
    gus.step(1)
    total = middle[...]
    factor = lax.rsqrt(jnp.mean(total * total, axis=-1, keepdims=True) + epsilon)
    own[...] = (total * factor * gains[pl.ds(1, 1), :]).astype(jnp.bfloat16)
    seconds = HalfGather(place, own, wide_in, gather_sem)
    seconds.start()
    seconds.relay()
    gus.step(2)
    seconds.rest()
    lows = Gather(place, low, low_all, lows_sem)
    lows.start()
    seconds.partner()
    downs.step(3)
    downs.keep.wait()
    give(down_w, down_o)
    cots.keep.wait()
    seconds.own_in()

    def early_grad(i, carry):
        rank = flip(place, i)
        at = pl.multiple_of((i % 2) * hidden.shape[2], LANES)
        mine[i // 2, :, pl.ds(at, hidden.shape[2])] = nt(up_all[rank], down_w[...].reshape(hidden.shape[2], -1))
        return carry

    lax.fori_loop(0, n, early_grad, 0)
    gus.step(3)
    gus.keep.wait()
    grads = Reduce(place, mine, theirs, first, out, second, reduce_sem)
    wide = hidden.shape[2]

    def block(i):
        rank = flip(place, i)
        gate_up = nn(wide_in[pl.ds(2 * rank, 2)].reshape(rows, -1), gu_w[...].reshape(-1, 2 * wide))
        gate, raised = gate_up[:, :wide], gate_up[:, wide:]
        sigmoid = 1.0 / (1.0 + jnp.exp(-gate))
        silu = gate * sigmoid
        hidden[rank] = (silu * raised).astype(jnp.bfloat16)
        hidden_grad = mine[i // 2, :, pl.ds(pl.multiple_of((i % 2) * wide, LANES), wide)]
        gul[rank, :, pl.ds(0, wide)] = (hidden_grad * raised * sigmoid * (1.0 + gate * (1.0 - sigmoid))).astype(jnp.bfloat16)
        gul[rank, :, pl.ds(wide, wide)] = (hidden_grad * silu).astype(jnp.bfloat16)
        return nt(gul[rank], gu_w[...].reshape(-1, 2 * wide))

    def block_at(t, carry):
        k = lax.rem(t // 2 + 1, 4)
        value = block(2 * k + 1 - t % 2)

        odd = t % 2
        theirs[k * (1 - odd) + 4 * odd] = value.astype(jnp.bfloat16)
        mine[k * odd + 4 * (1 - odd)] = value

        @pl.when(t % 2 == 0)
        def _():
            grads.push(k)

        @pl.when(t == 2)
        def _():
            lows.relay()

        @pl.when(t == 4)
        def _():
            grads.beside()

        @pl.when(t == 5)
        def _():
            lows.rest()

        @pl.when(t == 6)
        def _():
            grads.across()

        return carry

    lax.fori_loop(0, 8, block_at, 0)
    give(hidden, hidden_o)
    down_z = PlaneReduce(place, down_g, down_r, down_zs)
    piece = down_g.shape[1]

    def down_block(t, carry):
        left = hidden[:, :, pl.ds(pl.multiple_of(t * piece, piece), piece)].reshape(length, piece)
        down_g[t] = tn(left, up_all[...].reshape(length, width)).astype(jnp.bfloat16)
        return carry

    lax.fori_loop(0, 4, down_block, 0)
    down_z.start()
    grads.turn()
    seconds.finish()
    gain_grad[...] = jnp.zeros_like(gain_grad)

    def norm_back(part, second_grad):
        x = middle[part, :]
        factor = lax.rsqrt(jnp.mean(x * x, axis=-1, keepdims=True) + epsilon)
        unit = x * factor
        gain_grad[...] += jnp.sum(second_grad * unit, axis=0, keepdims=True)
        scaled = second_grad * gains[pl.ds(1, 1), :]
        inner = jnp.mean(scaled * unit, axis=-1, keepdims=True)
        grad = middle_grad[part, :] + factor * (scaled - unit * inner)
        middle_grad[part, :] = grad
        own[part, :] = grad.astype(jnp.bfloat16)

    gus.finish(kept=True)
    shard = gu_w.shape[1]

    def gu_block(t, carry):
        left = wide_in[:, :, pl.ds(pl.multiple_of(t * shard, shard), shard)].reshape(length, shard)
        gu_w[t] = tn(left, gul[...].reshape(length, 2 * wide)).astype(jnp.bfloat16)
        return carry

    lax.fori_loop(0, 4, gu_block, 0)
    give(gu_w, gu_out)
    down_z.step1()
    grads.total(norm_back)

    def head_grads(q, carry):
        weight = out_w[q // 2, pl.ds(4 * (q % 2), 4)].reshape(heads, -1)
        attended[q] = packed(nt(own[...], weight)).astype(jnp.bfloat16)
        return carry

    lax.fori_loop(0, n, head_grads, 0)
    heads_back = Exchange(place, attended, agrad, agrad_sem)
    heads_back.start()
    for q in range(8):
        mcols_send[q] = packed(own[:, q * heads : (q + 1) * heads].astype(jnp.float32)).astype(jnp.bfloat16)
    columns = Exchange(place, mcols_send, mcols, mcols_sem)
    columns.start()
    down_z.step2()
    lows.partner()
    heads_back.finish()
    down_z.total()
    down_sum[...] = down_g[place.z]
    for move in (qkvs, outs, downs, cots, outc):
        move.finish(kept=True)
    lows.finish()
    columns.finish()
    for copy in given:
        copy.wait()
    grads.finish()
    down_z.finish()


def front_moves(tok, pos, attn_own, ffn_own, qkv_own, gu_own, far_cos, far_sin, near, out_weight, down_weight, up):
    n, planes = lax.axis_size("ctx"), lax.axis_size("fsdp")
    rows, width = tok.shape
    length = n * rows
    bf, f32 = jnp.bfloat16, jnp.float32
    shape = jax.ShapeDtypeStruct
    out_own = shape((out_weight.shape[1] // n, width), bf)
    down_own = shape((down_weight.shape[1] // n, width), bf)
    spot = shape((8, LANES), jnp.int32)
    gain_own = shape((8, attn_own.shape[1]), f32)
    wide = planes * down_own.shape[0]
    dma = pltpu.SemaphoreType.DMA
    pairs = length // 192
    halves = pltpu.VMEM((6, rows // 2, width), bf)
    quads = pltpu.VMEM((4, rows, width), bf)
    small = (n, 3 * rows // 2, LANES)
    all_of = lambda x: shape((planes,) + x.shape, x.dtype)
    gathered = lambda x: pltpu.VMEM((planes,) + x.shape, x.dtype)
    ring = dma((2, Gather.sems))
    half_ring = dma((2, HalfGather.sems))
    line = dma((3, planes))
    swap = dma((2, n))
    kept = (
        shape((n, rows, wide), bf), all_of(qkv_own), all_of(down_own),
        shape((2 * length, LANES), bf), shape((length, LANES), bf), shape((length, LANES), bf),
        shape((pairs * LANES, 384), f32), shape((pairs, 384), f32), shape((rows, width), f32),
        shape((2 * n, rows // 2, LANES), f32),
    )
    return pl.pallas_call(
        front_kernel,
        out_shape=(
            shape((rows, width), f32), shape((1, width), f32), shape((n,) + spot.shape, spot.dtype), shape((2, width), f32),
            shape(down_own.shape, bf),
        ) + kept + (shape((n, rows, width), bf), shape(small, bf), shape((n,) + small, bf), all_of(gu_own), shape(small, bf)),
        in_specs=vm(9) + anywhere(3),
        out_specs=vm(5) + anywhere(15),
        scratch_shapes=[pltpu.VMEM(x.shape, x.dtype) for x in kept] + [
            pltpu.VMEM(small, bf), pltpu.VMEM((rows, width), bf), pltpu.VMEM(spot.shape, jnp.int32), pltpu.VMEM(gain_own.shape, f32),
            pltpu.VMEM((2 * n, rows // 2, width), bf), pltpu.VMEM((n, rows, width), bf), pltpu.VMEM((n, rows, 2 * wide), bf),
            gathered(gu_own), gathered(out_own), pltpu.VMEM((planes, n) + out_own.shape, bf),
            pltpu.VMEM((16, 96, 2 * LANES), bf), gathered(gain_own), pltpu.SMEM((n,) + spot.shape, jnp.int32),
            pltpu.SMEM((2 * n,), jnp.int32), pltpu.VMEM(small, bf),
            pltpu.VMEM(small, bf), pltpu.VMEM((rows, width), bf),
            pltpu.VMEM((5, rows, width), f32), pltpu.VMEM((5, rows, width), bf), quads, halves, halves,
            gathered(down_own), pltpu.VMEM((planes + 1,) + down_own.shape, bf),
            half_ring, ring, swap, dma((2, planes)), line, line, ring, line, line, dma((16,)),
            swap, half_ring, dma((2, Reduce.sems)), swap, ring, dma((2, planes + 1)), swap,
        ],
        compiler_params=pltpu.CompilerParams(collective_id=1, has_side_effects=True, vmem_limit_bytes=67043328),
        name="front_moves",
    )(tok, pos, attn_own, ffn_own, qkv_own, gu_own, far_cos, far_sin, near, out_weight, down_weight, up)


def back_moves_kernel(
    tok, gain, ffn_gain, down_sum, spots_i,
    gu_i, middle_grad_i, hidden_i, down_i, k_i, q_i, v_i, agrad_i, att_i, lse_i, turn_i, normed_i, middle_i, qkv_i, mcols_i, low_i,
    grad, result, attn_sum, ffn_sum, down_all, gu_all, out_all, qkv_all,
    spots_s, agrad_at, gu_g, hidden, down_w, k_ref, q_ref, v_ref, agrad, att_ref, lse_ref, turn_ref, normed_in, middle, qkv_w, mcols_in, low_in, out_g, qkv_g, gu_r, out_r, qkv_r,
    mine, theirs, first, out, second, dk_ref, dv_ref, pg_sorted, mcols,
    gain_sum, mine_gain, ctx_gain, plane_sum, plane_gain,
    free, local_sem, sum_sem, reduce_sem, gu_zs, out_zs, qkv_zs, down_cs, gu_cs, out_cs, qkv_cs,
    gain_sem, plane_sem,
):
    place = Place()
    n = place.n
    rows = tok.shape[0]
    half = rows // 2
    pairs = 8
    width = tok.shape[1]
    length = n * rows
    loads = [
        pltpu.make_async_copy(source, target, local_sem.at[at])
        for at, (source, target) in enumerate((
            (gu_i, gu_g), (hidden_i, hidden), (down_i, down_w), (k_i, k_ref), (q_i, q_ref), (v_i, v_ref),
            (agrad_i, agrad), (att_i, att_ref), (lse_i, lse_ref), (turn_i, turn_ref), (middle_i, middle),
            (normed_i, normed_in), (qkv_i, qkv_w), (mcols_i, mcols_in), (low_i, low_in), (middle_grad_i, grad),
        ))
    ]
    table = pltpu.make_async_copy(spots_i, spots_s, local_sem.at[16])
    table.start()
    for load in loads:
        load.start()
    greet(place, planes=True)
    table.wait()
    early = [lax.div(spots_s[j, 0, 0], half) for j in range(pairs)]
    holder = []
    for t in range(pairs):
        at = 0
        for j in range(pairs):
            at = jnp.where(early[j] == t, j, at)
        holder.append(at)
    gu_z = PlaneReduce(place, gu_g, gu_r, gu_zs)
    out_z = PlaneReduce(place, out_g, out_r, out_zs)
    qkv_z = PlaneReduce(place, qkv_g, qkv_r, qkv_zs)
    sums = Reduce(place, mine, theirs, first, out, second, sum_sem)
    downs = Gather(place, down_sum, down_all, down_cs)
    gus = Gather(place, gu_z.own(), gu_all, gu_cs)
    loads[0].wait()
    gu_z.start()
    downs.start()
    loads[1].wait()
    loads[2].wait()

    def other(k, carry):
        theirs[k] = nn(hidden[flip(place, 2 * k + 1)], down_w[...].reshape(-1, width)).astype(jnp.bfloat16)
        sums.push(k)
        return carry

    def ours(k, carry):
        mine[k] = nn(hidden[flip(place, 2 * k)], down_w[...].reshape(-1, width))
        return carry

    lax.fori_loop(0, 4, other, 0)
    lax.fori_loop(0, 4, ours, 0)
    downs.relay()
    sums.across()
    sums.beside()
    for load in loads[3:11]:
        load.wait()

    def finish_rows(part, down_out):
        result[part, :] = (middle[part, :] + down_out).astype(jnp.bfloat16)

    def sums_done():
        sums.total(finish_rows)
        sums.finish()
        for rank in (place.p, place.x, place.y):
            pl.semaphore_signal(free, inc=1, device_id={"ctx": rank}, device_id_type=MESH)

    def columns_done():
        loads[13].wait()

        def unpack(q, carry):
            mcols[q] = unpacked(mcols_in[q])
            return carry

        lax.fori_loop(0, n, unpack, 0)

    steps = Steps(downs.rest, gu_z.step1, lambda: (downs.partner(), sums.turn()), columns_done)
    scaling = HEAD_DIM ** (-0.5)
    lane = lax.broadcasted_iota(jnp.int32, (half, LANES), 1)
    keys_t = k_ref[...].astype(jnp.float32).T.astype(jnp.bfloat16)
    ranks_s = agrad_at
    for t in range(pairs):
        ranks_s[t] = holder[t]
        ranks_s[2 * pairs - 1 - t] = holder[t]
    dk_ref[...] = jnp.zeros_like(dk_ref)
    dv_ref[...] = jnp.zeros_like(dv_ref)

    def back_group(group):
        before = group * 4 * half
        side = 0 if group < pairs // 4 else 1
        cuts = [(before, 4 * half)] + [(at, min(768, before - at)) for at in range(0, before, 768)]

        def back(place_of, carry):
            pair = 2 * group + place_of
            q = q_ref[pl.ds(pl.multiple_of(pair * 4 * half, 4 * half), 4 * half), :]
            firsts, seconds = [], []
            for part in range(2):
                piece_of = agrad[ranks_s[2 * pair + part]].astype(jnp.float32)
                left = piece_of[side * half : (side + 1) * half]
                tail = piece_of[2 * half :]
                right = tail if side == 0 else pltpu.roll(tail, 64, 1)
                firsts.append(jnp.where(lane < half, left, 0.0))
                seconds.append(
                    jnp.where(lane < half, pltpu.roll(jnp.where(lane < half, right, left), LANES - half, 1), 0.0)
                )
            grads = jnp.concatenate(firsts + seconds, axis=0)
            att_t = att_ref[pl.ds(pl.multiple_of(pair * LANES, LANES), LANES), :]
            delta = jnp.sum(grads.T * att_t, axis=0, keepdims=True)
            grads = grads.astype(jnp.bfloat16)
            dq_t = None
            for at, count in cuts:
                keys = pl.ds(at, count)
                weights = jnp.exp(
                    jnp.where(
                        causal(2 * half, place_of), nt(k_ref[keys, :], q) * scaling - lse_ref[pl.ds(pair, 1), :], -1e30
                    )
                    if at == before
                    else nt(k_ref[keys, :], q) * scaling - lse_ref[pl.ds(pair, 1), :]
                )
                dp = nt(v_ref[keys, :], grads)
                ds = (weights * (dp - delta)).astype(jnp.bfloat16)
                dk_ref[keys, :] += nn(ds, q) * scaling
                dv_ref[keys, :] += nn(weights.astype(jnp.bfloat16), grads)
                term = nn(keys_t[:, at : at + count], ds)
                dq_t = term if dq_t is None else dq_t + term
            dq = dq_t.T * scaling
            for part in range(2):
                cosine, sine = wave(turn_ref[2 * pair + part])
                turned = []
                for head in range(2):
                    z = dq[(2 * head + part) * half : (2 * head + part + 1) * half]
                    turned.append(close_halves(z * cosine - pltpu.roll(z, 64, 1) * sine))
                second_head = pltpu.roll(turned[1], 96, 1)
                pg_sorted[2 * pair + part, :, 0:LANES] = jnp.where(lane < 96, turned[0], second_head).astype(jnp.bfloat16)
                pg_sorted[2 * pair + part, :, LANES : 2 * LANES] = second_head.astype(jnp.bfloat16)
            return carry

        lax.fori_loop(0, 2, back, 0)

    for group in reversed(range(pairs // 2)):
        back_group(group)
        steps.next()
    for s in range(2 * pairs):
        spot = pl.ds(s * half, half)
        cosine, sine = wave(turn_ref[s])
        z = dk_ref[spot, :]
        key_head = pltpu.roll(close_halves(z * cosine - pltpu.roll(z, 64, 1) * sine), 64, 1)
        queries_too = pg_sorted[s, :, LANES : 2 * LANES].astype(jnp.float32)
        pg_sorted[s, :, LANES : 2 * LANES] = jnp.where(lane < 64, queries_too, key_head).astype(jnp.bfloat16)
        pg_sorted[s, :, 2 * LANES :] = jnp.where(lane < 32, key_head, pltpu.roll(dv_ref[spot, :], 32, 1)).astype(jnp.bfloat16)

    loads[11].wait()
    loads[12].wait()
    shard = gu_g.shape[1]

    def qkv_block(t, carry):
        left = normed_in[:, :, pl.ds(pl.multiple_of(t * shard, shard), shard)].reshape(length, shard)
        qkv_g[t] = tn(left, pg_sorted[...].reshape(length, 3 * LANES)).astype(jnp.bfloat16)
        return carry

    sums_done()
    lax.fori_loop(0, 4, qkv_block, 0)
    qkv_z.start()
    gu_z.step2()
    pl.semaphore_wait(free, 3)
    grads = Reduce(place, mine, theirs, first, out, second, reduce_sem)

    def chunk(i):
        at = lax.div(spots_s[flip(place, i), 0, 0], half)
        rows_of = jnp.concatenate([pg_sorted[at], pg_sorted[2 * pairs - 1 - at]], axis=0)
        return nt(rows_of, qkv_w[...].reshape(width, -1))

    def push(k, carry):
        theirs[k] = chunk(2 * k + 1).astype(jnp.bfloat16)
        grads.push(k)
        return carry

    def keep(k, carry):
        mine[k] = chunk(2 * k)
        return carry

    lax.fori_loop(0, 4, push, 0)
    lax.fori_loop(0, 4, keep, 0)
    grads.across()
    grads.beside()
    loads[14].wait()
    loads[15].wait()

    def out_block(src, carry):
        heads = low_in[src, :, pl.ds(0, rows), :].reshape(length, LANES)
        tails = low_in[src, :, pl.ds(rows, half), :].reshape(length // 2, LANES)
        upper = tn(heads, mcols[...].reshape(length, rows))
        from_a = tn(tails, mcols[:, pl.ds(0, half), :].reshape(length // 2, rows))
        from_b = tn(tails, mcols[:, pl.ds(half, half), :].reshape(length // 2, rows))
        at = pl.multiple_of((src % 2) * rows, rows)
        out_g[src // 2, pl.ds(at, LANES), :] = upper.astype(jnp.bfloat16)
        out_g[src // 2, pl.ds(pl.multiple_of(at + LANES, 64), 64), :] = (from_a[:64] + from_b[64:]).astype(jnp.bfloat16)
        return carry

    lax.fori_loop(0, 8, out_block, 0)
    out_z.start()
    grads.turn()
    gu_z.total()
    gus.start()
    gain_sum[...] = jnp.zeros_like(gain_sum)

    def norm_back(part, normed_grad):
        x = tok[part, :].astype(jnp.float32)
        factor = lax.rsqrt(jnp.mean(x * x, axis=-1, keepdims=True) + epsilon)
        unit = x * factor
        gain_sum[...] += jnp.sum(normed_grad * unit, axis=0, keepdims=True)
        scaled = normed_grad * gain[pl.ds(0, 1), :]
        inner = jnp.mean(scaled * unit, axis=-1, keepdims=True)
        grad[part, :] = grad[part, :] + factor * (scaled - unit * inner)

    qkv_z.step1()
    grads.total(norm_back)
    gain_grad = gain_sum[...]
    count = mine_gain.shape[0] // 2
    for at in range(count):
        mine_gain[pl.ds(at, 1), :] = gain_grad[:, at * shard : (at + 1) * shard]
        mine_gain[pl.ds(count + at, 1), :] = ffn_gain[:, at * shard : (at + 1) * shard]
    ctx_sum = Share(place, mine_gain, ctx_gain, gain_sem)
    ctx_sum.start()
    gus.relay()
    qkv_z.step2()
    out_z.step1()
    ctx_sum.finish()
    plane_sum[...] = jnp.sum(ctx_gain[...], axis=0)
    planes = PlaneShare(place, plane_sum, plane_gain, plane_sem)
    planes.start()
    out_z.step2()
    qkv_z.total()
    gus.rest()
    qkvs = Gather(place, qkv_z.own(), qkv_all, qkv_cs)
    qkvs.start()
    out_z.total()
    outs = Gather(place, out_z.own(), out_all, out_cs)
    qkvs.relay()
    outs.start()
    qkvs.rest()
    outs.relay()
    outs.rest()
    planes.finish()
    plane_sum[...] = jnp.sum(plane_gain[...], axis=0)
    attn_sum[...] = plane_sum[pl.ds(place.z, 1), :]
    ffn_sum[...] = plane_sum[pl.ds(count + place.z, 1), :]
    gus.partner()
    qkvs.partner()
    outs.partner()
    for move in (gu_z, out_z, qkv_z, downs, gus, outs, qkvs, grads):
        move.finish()


def back_moves(tok, gain, ffn_gain, down_sum, spots, *moved):
    n, planes = lax.axis_size("ctx"), lax.axis_size("fsdp")
    rows, width = tok.shape
    length = n * rows
    shard = width // planes
    bf, f32 = jnp.bfloat16, jnp.float32
    shape = jax.ShapeDtypeStruct
    dma = pltpu.SemaphoreType.DMA
    halves = pltpu.VMEM((6, rows // 2, width), bf)
    quads = pltpu.VMEM((4, rows, width), bf)
    small = (2 * planes, shard)
    parts = (moved[0].shape[1:], (shard, rows), (shard, 3 * LANES))
    ring = dma((2, Gather.sems))
    return pl.pallas_call(
        back_moves_kernel,
        out_shape=(shape((rows, width), f32), shape((rows, width), bf), shape((1, shard), f32), shape((1, shard), f32))
        + tuple(shape((n,) + part, bf) for part in (down_sum.shape,) + parts),
        in_specs=vm(4) + anywhere(1 + len(moved)),
        out_specs=vm(4) + anywhere(4),
        scratch_shapes=[pltpu.SMEM(spots.shape, jnp.int32), pltpu.SMEM((2 * n,), jnp.int32)] + [pltpu.VMEM(x.shape, x.dtype) for at, x in enumerate(moved) if at != 1]
        + [pltpu.VMEM((planes,) + part, bf) for part in parts[1:]]
        + [pltpu.VMEM((planes + 1,) + part, bf) for part in parts]
        + [
            pltpu.VMEM((4, rows, width), f32), quads, quads, halves, halves,
            pltpu.VMEM((length, LANES), f32), pltpu.VMEM((length, LANES), f32), pltpu.VMEM((16, 96, 3 * LANES), bf),
            pltpu.VMEM((n, rows, rows), bf),
            pltpu.VMEM((1, width), f32), pltpu.VMEM(small, f32), pltpu.VMEM((n,) + small, f32),
            pltpu.VMEM(small, f32), pltpu.VMEM((planes,) + small, f32),
            pltpu.SemaphoreType.REGULAR, dma((17,)), dma((2, Reduce.sems)), dma((2, Reduce.sems)),
            dma((2, 5)), dma((2, 5)), dma((2, 5)), ring, ring, ring, ring, dma((2, n)), dma((2, planes)),
        ],
        compiler_params=pltpu.CompilerParams(collective_id=6, has_side_effects=True, vmem_limit_bytes=67043328),
        name="back_moves",
    )(tok, gain, ffn_gain, down_sum, spots, *moved)


def pack_kernel(
    down, gu, out, qkv, grad, result, attn, ffn, down_o, gu_o, out_o, qkv_o, grad_o, result_o, attn_o, ffn_o
):
    devices, rows = gu.shape[0], gu.shape[1]
    f32 = jnp.float32
    lane = lax.broadcasted_iota(jnp.int32, (rows, LANES), 1)
    down_o[...] = down[0].astype(f32)
    grad_o[...] = grad[...]
    result_o[...] = result[...]
    attn_o[...] = attn[...]
    ffn_o[...] = ffn[...]
    tiles = gu_o.shape[0] // rows
    spans = gu.shape[2] // (2 * LANES)
    for r in range(0, rows, 16):
        pieces = [
            gu[c, pl.ds(r, 16), (s * spans + z) * LANES : (s * spans + z + 1) * LANES].astype(f32)
            for z in range(spans) for c in range(devices) for s in range(2)
        ]
        gu_o[pl.ds(r * tiles, 16 * tiles), :] = jnp.swapaxes(jnp.stack(pieces, axis=0), 0, 1).reshape(16 * tiles, LANES)

    def tile(c, at):
        return qkv[c, :, at * LANES : (at + 1) * LANES].astype(f32)

    def key_head(c):
        return jnp.where(lane < 64, pltpu.roll(tile(c, 1), 64, 1), pltpu.roll(tile(c, 2), 64, 1))

    def value_head(c):
        return pltpu.roll(tile(c, 2), 96, 1)

    def store(at, heads):
        second, third, fourth = pltpu.roll(heads[1], 96, 1), pltpu.roll(heads[2], 64, 1), pltpu.roll(heads[3], 32, 1)
        qkv_o[:, at : at + LANES] = jnp.where(lane < 96, heads[0], second)
        qkv_o[:, at + LANES : at + 2 * LANES] = jnp.where(lane < 64, second, third)
        qkv_o[:, at + 2 * LANES : at + 3 * LANES] = jnp.where(lane < 32, third, fourth)

    for c in range(0, devices, 2):
        at = c * 192
        turned = pltpu.roll(tile(c + 1, 0), 64, 1)
        qkv_o[:, at : at + LANES] = tile(c, 0)
        qkv_o[:, at + LANES : at + 2 * LANES] = jnp.where(lane < 64, tile(c, 1), turned)
        qkv_o[:, at + 2 * LANES : at + 3 * LANES] = jnp.where(lane < 64, turned, pltpu.roll(tile(c + 1, 1), 64, 1))
    for c in range(0, devices, 4):
        store(HEADS * HEAD_DIM + c * 96, [key_head(c + i) for i in range(4)])
        store((HEADS + KV_HEADS) * HEAD_DIM + c * 96, [value_head(c + i) for i in range(4)])
    for c in range(0, devices, 2):
        at = c * 192
        first = out[c].astype(f32)
        second = out[c + 1].astype(f32)
        tail = jnp.concatenate([first[:, LANES:], jnp.zeros((rows, 64), f32)], axis=1)
        next_tail = jnp.concatenate([second[:, LANES:], jnp.zeros((rows, 64), f32)], axis=1)
        turned = pltpu.roll(second[:, :LANES], 64, 1)
        out_o[:, at : at + LANES] = first[:, :LANES]
        out_o[:, at + LANES : at + 2 * LANES] = jnp.where(lane < 64, tail, turned)
        out_o[:, at + 2 * LANES : at + 3 * LANES] = jnp.where(lane < 64, turned, pltpu.roll(next_tail, 64, 1))


def pack(down, gu, out, qkv, grad, result, attn, ffn):
    n, shard = gu.shape[0], gu.shape[1]
    rows = shard // n
    width = down.shape[2]
    f32 = jnp.float32
    spec = pl.BlockSpec
    shape = jax.ShapeDtypeStruct
    tiles = n * gu.shape[2] // LANES
    quarter = grad.shape[0] // 4
    return pl.pallas_call(
        pack_kernel,
        grid=(n,),
        out_shape=(
            shape((n * down.shape[1], width), f32), shape((shard * tiles, LANES), f32), shape((shard, n * out.shape[2]), f32),
            shape((shard, (HEADS + 2 * KV_HEADS) * HEAD_DIM), f32), shape(grad.shape, f32), shape(result.shape, result.dtype), shape(attn.shape, f32), shape(ffn.shape, f32),
        ),
        in_specs=[
            spec((1,) + down.shape[1:], lambda i: (i, 0, 0)), spec((n, rows, gu.shape[2]), lambda i: (0, i, 0)),
            spec((n, rows, out.shape[2]), lambda i: (0, i, 0)), spec((n, rows, qkv.shape[2]), lambda i: (0, i, 0)),
            spec((quarter, width), lambda i: (i // 2, 0)), spec((quarter, width), lambda i: (i // 2, 0)),
            spec(attn.shape, lambda i: (0, 0)), spec(ffn.shape, lambda i: (0, 0)),
        ],
        out_specs=[
            spec((down.shape[1], width), lambda i: (i, 0)), spec((rows * tiles, LANES), lambda i: (i, 0)),
            spec((rows, n * out.shape[2]), lambda i: (i, 0)), spec((rows, (HEADS + 2 * KV_HEADS) * HEAD_DIM), lambda i: (i, 0)),
            spec((quarter, width), lambda i: (i // 2, 0)), spec((quarter, width), lambda i: (i // 2, 0)),
            spec(attn.shape, lambda i: (0, 0)), spec(ffn.shape, lambda i: (0, 0)),
        ],
        name="pack",
    )(down, gu, out, qkv, grad, result, attn, ffn)


def fast_body(
    tokens, positions, qkv_weight, out_weight, gate_up_weight, down_weight, attn_gain, ffn_gain, cotangent
):
    me = lax.axis_index("ctx")
    n = lax.axis_size("ctx")
    planes = lax.axis_size("fsdp")
    rows = tokens.shape[1]
    length = n * rows
    width = tokens.shape[2]
    wide = down_weight.shape[1] * planes
    own = wide // n
    piece = own // planes
    shard = qkv_weight.shape[1]
    query_width = HEADS * HEAD_DIM
    key_width = KV_HEADS * HEAD_DIM
    cut = lax.dynamic_slice_in_dim

    qkv = qkv_weight[0]
    q_part = cut(qkv, me * 2 * HEAD_DIM, 2 * HEAD_DIM, 1)
    k_part = cut(qkv, query_width + me * HEAD_DIM, HEAD_DIM, 1)
    v_part = cut(qkv, query_width + key_width + me * HEAD_DIM, HEAD_DIM, 1)
    qkv_own = jnp.concatenate([q_part, k_part, v_part], axis=1)
    pieces = [cut(gate_up_weight[0], at * (wide // planes) + me * piece, piece, 2) for at in range(planes)]
    gate_up_own = jnp.concatenate(pieces, axis=2).reshape(shard, 2 * own)
    (
        middle_grad, ffn_partial, spots, gains, down_sum, hidden, qkv_block, down_block, q, k, v, att, lse, middle,
        turns, normed, attended_grad, low_all, gate_up_grad, middle_cols,
    ) = front_moves(
        tokens[0], positions, attn_gain, ffn_gain, qkv_own, gate_up_own, *turn_parts(2 * n, rows // 2),
        out_weight, down_weight, cotangent[0],
    )
    stream_grad, result, attn_sum, ffn_sum, down_grad, gate_up_grad, out_grad, qkv_grad = back_moves(
        tokens[0], gains, ffn_partial, down_sum, spots,
        gate_up_grad, middle_grad, hidden, down_block, k, q, v, attended_grad, att, lse, turns, normed, middle,
        qkv_block, middle_cols, low_all,
    )
    down_grad, gate_up_grad, out_grad, qkv_grad, stream_grad, result, attn_sum, ffn_sum = pack(
        down_grad, gate_up_grad, out_grad, qkv_grad, stream_grad, result, attn_sum, ffn_sum
    )
    gate_up_grad = gate_up_grad.reshape(shard, wide // LANES, 2, LANES).transpose(0, 2, 1, 3).reshape(shard, 2, wide)
    return (
        result[None],
        stream_grad[None],
        qkv_grad[None],
        out_grad[None],
        gate_up_grad[None],
        down_grad[None],
        attn_sum,
        ffn_sum,
    )


def solution(mesh):
    split = mesh.shape["ctx"] == KV_HEADS and mesh.shape["fsdp"] == 4
    placed = (
        P("fsdp", "ctx", None),
        P("fsdp", "ctx"),
        P(None, "fsdp", None),
        P(None, "fsdp", None),
        P(None, "fsdp", None, None),
        P(None, "fsdp", None),
        P(None, "fsdp"),
        P(None, "fsdp"),
        P("fsdp", "ctx", None),
    )
    return jax.shard_map(
        fast_body if split else body,
        mesh=mesh,
        in_specs=placed,
        out_specs=(
            P("fsdp", "ctx", None),
            P("fsdp", "ctx", None),
            P(None, "fsdp", None),
            P(None, "fsdp", None),
            P(None, "fsdp", None, None),
            P(None, "fsdp", None),
            P(None, "fsdp"),
            P(None, "fsdp"),
        ),
        check_vma=False,
    )
```

```python
import jax
import jax.numpy as jnp
import numpy as np
from jax import lax
from jax.experimental import pallas as pl
from jax.experimental.pallas import tpu as pltpu
from jax.sharding import PartitionSpec as P

HEADS = 16
KV_HEADS = 8
HEAD_DIM = 96
LAYERS = 1


epsilon = 1e-05
rope_base = 100000.0


def angles(place):
    halfway = HEAD_DIM // 2
    frequency = rope_base ** (-(jnp.arange(halfway, dtype=jnp.float32) * 2.0 / HEAD_DIM))
    phases = place.astype(jnp.float32)[:, None] * frequency[None, :]
    phases = jnp.concatenate([phases, phases], axis=-1)
    return (jnp.cos(phases)[:, None, :], jnp.sin(phases)[:, None, :])


def rotate(vectors, cosine, sine):
    halfway = vectors.shape[-1] // 2
    turned = jnp.concatenate([-vectors[..., halfway:], vectors[..., :halfway]], axis=-1)
    return vectors * cosine + turned * sine


def rotate_back(grads, cosine, sine):
    halfway = grads.shape[-1] // 2
    scaled = grads * sine
    return grads * cosine + jnp.concatenate(
        [scaled[..., halfway:], -scaled[..., :halfway]], axis=-1
    )


def normalize(rows, gain):
    factor = lax.rsqrt(jnp.mean(rows * rows, axis=-1, keepdims=True) + epsilon)
    return (rows * factor * gain, factor)


def normalize_back(upstream, rows, factor, gain):
    unit_rows = rows * factor
    gain_grad = jnp.sum(upstream * unit_rows, axis=0)
    scaled = upstream * gain
    row_inner = jnp.mean(scaled * unit_rows, axis=-1, keepdims=True)
    return (factor * (scaled - unit_rows * row_inner), gain_grad)


def split_blocks(queries, keys_all, values_all, key_place):
    rows = queries.shape[0]
    half = rows // 2
    shards = key_place.shape[0] // rows
    key_blocks = keys_all.reshape(shards, 2, half, KV_HEADS, HEAD_DIM)
    value_blocks = values_all.reshape(shards, 2, half, KV_HEADS, HEAD_DIM)
    place_blocks = key_place.reshape(shards, 2, half)
    return (key_blocks, value_blocks, place_blocks)


def scores_of(queries, key_block, place_block, query_place):
    scaling = HEAD_DIM ** (-0.5)
    scores = (
        jnp.einsum("rkgd,skd->kgrs", queries, key_block, preferred_element_type=jnp.float32)
        * scaling
    )
    allowed = place_block[None, None, None, :] <= query_place[None, None, :, None]
    return (scores, allowed)


def reachable(place_block, query_place):
    return jnp.min(place_block) <= jnp.max(query_place)


def attention_forward(queries, keys_all, values_all, query_place, key_place):
    key_blocks, value_blocks, place_blocks = split_blocks(queries, keys_all, values_all, key_place)
    rows = queries.shape[0]
    half = rows // 2
    groups = HEADS // KV_HEADS
    query_spans = queries.reshape(2, half, KV_HEADS, groups, HEAD_DIM)
    place_spans = query_place.reshape(2, half)

    def sweep_max(carry, inputs):
        key_block, place_block = inputs
        updated_all = []
        for span in range(2):
            state = carry[span]
            for part in range(2):

                def live(current, span=span, part=part):
                    maximum, total = current
                    scores, allowed = scores_of(
                        query_spans[span], key_block[part], place_block[part], place_spans[span]
                    )
                    masked = jnp.where(allowed, scores, -1e30)
                    updated = jnp.maximum(maximum, jnp.max(masked, axis=-1))
                    weights_now = jnp.where(allowed, jnp.exp(masked - updated[..., None]), 0.0)
                    return (
                        updated,
                        total * jnp.exp(maximum - updated) + jnp.sum(weights_now, axis=-1),
                    )

                state = lax.cond(
                    reachable(place_block[part], place_spans[span]),
                    live,
                    lambda current: current,
                    state,
                )
            updated_all.append(state)
        return (tuple(updated_all), None)

    start_max = jnp.full((KV_HEADS, groups, half), -1e30, jnp.float32)
    start_total = jnp.zeros((KV_HEADS, groups, half), jnp.float32)
    start = ((start_max, start_total), (start_max, start_total))
    finals, unused = lax.scan(sweep_max, start, (key_blocks, place_blocks))
    logsum_spans = [finals[span][0] + jnp.log(finals[span][1]) for span in range(2)]

    def sweep_out(results, inputs):
        key_block, value_block, place_block = inputs
        updated_all = []
        for span in range(2):
            result = results[span]
            for part in range(2):

                def live(current, span=span, part=part):
                    scores, allowed = scores_of(
                        query_spans[span], key_block[part], place_block[part], place_spans[span]
                    )
                    softmax_rows = jnp.where(
                        allowed, jnp.exp(scores - logsum_spans[span][..., None]), 0.0
                    ).astype(jnp.bfloat16)
                    return current + jnp.einsum(
                        "kgrs,skd->rkgd",
                        softmax_rows,
                        value_block[part],
                        preferred_element_type=jnp.float32,
                    )

                result = lax.cond(
                    reachable(place_block[part], place_spans[span]),
                    live,
                    lambda current: current,
                    result,
                )
            updated_all.append(result)
        return (tuple(updated_all), None)

    start_out = jnp.zeros((half, KV_HEADS, groups, HEAD_DIM), jnp.float32)
    outs, unused_out = lax.scan(
        sweep_out, (start_out, start_out), (key_blocks, value_blocks, place_blocks)
    )
    logsum = jnp.concatenate(logsum_spans, axis=-1)
    attended = jnp.concatenate([outs[0], outs[1]], axis=0)
    return (logsum, attended)


def attention_backward(
    queries, keys_all, values_all, query_place, key_place, logsum, attended_grad, row_inner
):
    key_blocks, value_blocks, place_blocks = split_blocks(queries, keys_all, values_all, key_place)
    rows = queries.shape[0]
    half = rows // 2
    groups = HEADS // KV_HEADS
    scaling = HEAD_DIM ** (-0.5)
    query_spans = queries.reshape(2, half, KV_HEADS, groups, HEAD_DIM)
    place_spans = query_place.reshape(2, half)
    grad_spans = attended_grad.reshape(2, half, KV_HEADS, groups, HEAD_DIM)
    logsum_spans = logsum.reshape(KV_HEADS, groups, 2, half)
    inner_spans = row_inner.reshape(KV_HEADS, groups, 2, half)

    def sweep_back(query_grads, inputs):
        key_block, value_block, place_block = inputs
        query_grads = list(query_grads)
        key_parts = []
        value_parts = []
        for part in range(2):
            key_acc = jnp.zeros((half, KV_HEADS, HEAD_DIM), jnp.float32)
            value_acc = jnp.zeros((half, KV_HEADS, HEAD_DIM), jnp.float32)
            for span in range(2):

                def live(current, span=span, part=part):
                    query_grad, key_grad, value_grad = current
                    scores, allowed = scores_of(
                        query_spans[span], key_block[part], place_block[part], place_spans[span]
                    )
                    softmax_rows = jnp.where(
                        allowed, jnp.exp(scores - logsum_spans[:, :, span][..., None]), 0.0
                    )
                    rounded = softmax_rows.astype(jnp.bfloat16)
                    weight_grad = jnp.einsum(
                        "rkgd,skd->kgrs",
                        grad_spans[span],
                        value_block[part],
                        preferred_element_type=jnp.float32,
                    )
                    score_grad = (
                        softmax_rows * (weight_grad - inner_spans[:, :, span][..., None])
                    ).astype(jnp.bfloat16)
                    query_grad = (
                        query_grad
                        + jnp.einsum(
                            "kgrs,skd->rkgd",
                            score_grad,
                            key_block[part],
                            preferred_element_type=jnp.float32,
                        )
                        * scaling
                    )
                    key_grad = (
                        key_grad
                        + jnp.einsum(
                            "kgrs,rkgd->skd",
                            score_grad,
                            query_spans[span],
                            preferred_element_type=jnp.float32,
                        )
                        * scaling
                    )
                    value_grad = value_grad + jnp.einsum(
                        "kgrs,rkgd->skd",
                        rounded,
                        grad_spans[span],
                        preferred_element_type=jnp.float32,
                    )
                    return (query_grad, key_grad, value_grad)

                state = (query_grads[span], key_acc, value_acc)
                state = lax.cond(
                    reachable(place_block[part], place_spans[span]),
                    live,
                    lambda current: current,
                    state,
                )
                query_grads[span], key_acc, value_acc = state
            key_parts.append(key_acc)
            value_parts.append(value_acc)
        key_out = jnp.concatenate(key_parts, axis=0)
        value_out = jnp.concatenate(value_parts, axis=0)
        return (tuple(query_grads), (key_out, value_out))

    start_grad = jnp.zeros((half, KV_HEADS, groups, HEAD_DIM), jnp.float32)
    query_pair, (key_grads, value_grads) = lax.scan(
        sweep_back, (start_grad, start_grad), (key_blocks, value_blocks, place_blocks)
    )
    query_grad = jnp.concatenate([query_pair[0], query_pair[1]], axis=0)
    return (
        query_grad,
        key_grads.reshape(-1, KV_HEADS, HEAD_DIM),
        value_grads.reshape(-1, KV_HEADS, HEAD_DIM),
    )


def fetch_layer(qkv_weight, out_weight, gate_up_weight, down_weight, attn_gain, ffn_gain, layer_id):
    return (
        lax.all_gather(qkv_weight[layer_id], "fsdp", axis=0, tiled=True),
        lax.all_gather(out_weight[layer_id], "fsdp", axis=0, tiled=True),
        lax.all_gather(gate_up_weight[layer_id], "fsdp", axis=0, tiled=True),
        lax.all_gather(down_weight[layer_id], "fsdp", axis=0, tiled=True),
        lax.all_gather(attn_gain[layer_id], "fsdp", axis=0, tiled=True),
        lax.all_gather(ffn_gain[layer_id], "fsdp", axis=0, tiled=True),
    )


def fetch_again(qkv_weight, out_weight, gate_up_weight, down_weight, attn_gain, ffn_gain, layer_id):
    return (
        lax.all_gather(qkv_weight[layer_id], "fsdp", axis=0, tiled=True),
        lax.all_gather(out_weight[layer_id], "fsdp", axis=0, tiled=True),
        lax.all_gather(gate_up_weight[layer_id], "fsdp", axis=0, tiled=True),
        lax.all_gather(down_weight[layer_id], "fsdp", axis=0, tiled=True),
        lax.all_gather(attn_gain[layer_id], "fsdp", axis=0, tiled=True),
        lax.all_gather(ffn_gain[layer_id], "fsdp", axis=0, tiled=True),
    )


def forward_layer(stream, query_place, key_place, gathered):
    qkv_full, out_full, gate_up_full, down_full, attn_full, ffn_full = gathered
    rows = stream.shape[0]
    groups = HEADS // KV_HEADS
    query_width = HEADS * HEAD_DIM
    key_width = KV_HEADS * HEAD_DIM
    cosine, sine = angles(query_place)
    normed, first_factor = normalize(stream, attn_full.astype(jnp.float32))
    normed = normed.astype(jnp.bfloat16)
    projected = jnp.dot(normed, qkv_full, preferred_element_type=jnp.float32)
    queries = rotate(projected[:, :query_width].reshape(rows, HEADS, HEAD_DIM), cosine, sine)
    queries = queries.reshape(rows, KV_HEADS, groups, HEAD_DIM).astype(jnp.bfloat16)
    keys_local = rotate(
        projected[:, query_width : query_width + key_width].reshape(rows, KV_HEADS, HEAD_DIM),
        cosine,
        sine,
    ).astype(jnp.bfloat16)
    values_local = (
        projected[:, query_width + key_width :]
        .reshape(rows, KV_HEADS, HEAD_DIM)
        .astype(jnp.bfloat16)
    )
    keys_all, values_all = (
        lax.all_gather(keys_local, "ctx", axis=0, tiled=True),
        lax.all_gather(values_local, "ctx", axis=0, tiled=True),
    )
    logsum, attended = attention_forward(queries, keys_all, values_all, query_place, key_place)
    attended_low = attended.reshape(rows, query_width).astype(jnp.bfloat16)
    middle = stream + jnp.dot(attended_low, out_full, preferred_element_type=jnp.float32)
    second, second_factor = normalize(middle, ffn_full.astype(jnp.float32))
    second = second.astype(jnp.bfloat16)
    gate_up = jnp.einsum("rd,dcf->rcf", second, gate_up_full, preferred_element_type=jnp.float32)
    hidden = (jax.nn.silu(gate_up[:, 0]) * gate_up[:, 1]).astype(jnp.bfloat16)
    result = middle + jnp.dot(hidden, down_full, preferred_element_type=jnp.float32)
    stored = (
        stream,
        first_factor,
        normed,
        queries,
        keys_local,
        values_local,
        keys_all,
        values_all,
        logsum,
        attended,
        attended_low,
        middle,
        second_factor,
        second,
        gate_up,
        hidden,
    )
    return (result, stored)


def backward_layer(upstream, stored, gathered, query_place, key_place, keys_all, values_all):
    (
        stream,
        first_factor,
        normed,
        queries,
        keys_local,
        values_local,
        kept_keys,
        kept_values,
        logsum,
        attended,
        attended_low,
        middle,
        second_factor,
        second,
        gate_up,
        hidden,
    ) = stored
    qkv_full, out_full, gate_up_full, down_full, attn_full, ffn_full = gathered
    rows = stream.shape[0]
    groups = HEADS // KV_HEADS
    cosine, sine = angles(query_place)
    upstream_low = upstream.astype(jnp.bfloat16)
    hidden_grad = jnp.einsum(
        "rd,fd->rf", upstream_low, down_full, preferred_element_type=jnp.float32
    )
    gate_part = gate_up[:, 0]
    up_part = gate_up[:, 1]
    sigmoid = jax.nn.sigmoid(gate_part)
    gate_grad = hidden_grad * up_part * sigmoid * (1.0 + gate_part * (1.0 - sigmoid))
    up_grad = hidden_grad * gate_part * sigmoid
    gate_up_low = jnp.stack([gate_grad, up_grad], axis=1).astype(jnp.bfloat16)
    second_grad = jnp.einsum(
        "rcf,dcf->rd", gate_up_low, gate_up_full, preferred_element_type=jnp.float32
    )
    middle_grad, ffn_gain_grad = normalize_back(
        second_grad, middle, second_factor, ffn_full.astype(jnp.float32)
    )
    middle_grad = middle_grad + upstream
    middle_low = middle_grad.astype(jnp.bfloat16)
    attended_grad = jnp.einsum(
        "rd,od->ro", middle_low, out_full, preferred_element_type=jnp.float32
    )
    attended_grad = attended_grad.astype(jnp.bfloat16).reshape(rows, KV_HEADS, groups, HEAD_DIM)
    row_inner = jnp.einsum("rkgd,rkgd->kgr", attended_grad.astype(jnp.float32), attended)
    query_grad, key_grads, value_grads = attention_backward(
        queries, keys_all, values_all, query_place, key_place, logsum, attended_grad, row_inner
    )
    key_grad, value_grad = (
        lax.psum_scatter(key_grads, "ctx", scatter_dimension=0, tiled=True),
        lax.psum_scatter(value_grads, "ctx", scatter_dimension=0, tiled=True),
    )
    query_grad = rotate_back(query_grad.reshape(rows, HEADS, HEAD_DIM), cosine, sine)
    key_grad = rotate_back(key_grad, cosine, sine)
    projected_grad = jnp.concatenate(
        [query_grad.reshape(rows, -1), key_grad.reshape(rows, -1), value_grad.reshape(rows, -1)],
        axis=1,
    ).astype(jnp.bfloat16)
    normed_grad = jnp.einsum(
        "re,de->rd", projected_grad, qkv_full, preferred_element_type=jnp.float32
    )
    stream_grad, attn_gain_grad = normalize_back(
        normed_grad, stream, first_factor, attn_full.astype(jnp.float32)
    )
    stream_grad = stream_grad + middle_grad
    qkv_grad = jnp.einsum("rd,re->de", normed, projected_grad, preferred_element_type=jnp.float32)
    out_grad = jnp.einsum("ro,rd->od", attended_low, middle_low, preferred_element_type=jnp.float32)
    gate_up_grad = jnp.einsum(
        "rd,rcf->dcf", second, gate_up_low, preferred_element_type=jnp.float32
    )
    down_grad = jnp.einsum("rf,rd->fd", hidden, upstream_low, preferred_element_type=jnp.float32)
    sharded = (
        lax.psum_scatter(qkv_grad, "fsdp", scatter_dimension=0, tiled=True),
        lax.psum_scatter(out_grad, "fsdp", scatter_dimension=0, tiled=True),
        lax.psum_scatter(gate_up_grad, "fsdp", scatter_dimension=0, tiled=True),
        lax.psum_scatter(down_grad, "fsdp", scatter_dimension=0, tiled=True),
        lax.psum_scatter(attn_gain_grad, "fsdp", scatter_dimension=0, tiled=True),
        lax.psum_scatter(ffn_gain_grad, "fsdp", scatter_dimension=0, tiled=True),
    )
    totals = lax.psum(
        (sharded[0], sharded[1], sharded[2], sharded[3], sharded[4], sharded[5]), "ctx"
    )
    return (stream_grad, totals)


def body(
    tokens,
    positions,
    qkv_weight,
    out_weight,
    gate_up_weight,
    down_weight,
    attn_gain,
    ffn_gain,
    cotangent,
):
    query_place = positions[0]
    key_place = lax.all_gather(query_place, "ctx", axis=0, tiled=True)
    stream = tokens[0].astype(jnp.float32)
    gathered_list = []
    layer_id = 0
    gathered = fetch_layer(
        qkv_weight, out_weight, gate_up_weight, down_weight, attn_gain, ffn_gain, layer_id
    )
    stream, stored = forward_layer(stream, query_place, key_place, gathered)
    saved = [stored]
    gathered_list.append(gathered)
    activations = stream.astype(jnp.bfloat16)[None]
    upstream = cotangent[0]
    layer_grads = [None] * LAYERS
    for layer_id in reversed(range(LAYERS)):
        stored = saved[layer_id]
        gathered = fetch_again(
            qkv_weight, out_weight, gate_up_weight, down_weight, attn_gain, ffn_gain, layer_id
        )
        keys_all, values_all = (stored[6], stored[7])
        upstream, totals = backward_layer(
            upstream, stored, gathered, query_place, key_place, keys_all, values_all
        )
        layer_grads[layer_id] = totals
    outputs = [jnp.stack([entry[slot] for entry in layer_grads], axis=0) for slot in range(6)]
    return (
        activations,
        upstream[None],
        outputs[0],
        outputs[1],
        outputs[2],
        outputs[3],
        outputs[4],
        outputs[5],
    )


LANES = 128


def spread(heads):
    half = HEAD_DIM // 2
    pad = ((0, 0), (0, 0), (0, 64 - half))
    return jnp.concatenate([jnp.pad(heads[..., :half], pad), jnp.pad(heads[..., half:], pad)], axis=-1)


def gathered_spread(padded):
    half = HEAD_DIM // 2
    return jnp.concatenate([padded[..., :half], padded[..., 64 : 64 + half]], axis=-1)


def turn_parts(spans, rows):
    half = HEAD_DIM // 2
    frequency = rope_base ** (-(np.arange(half, dtype=np.float64) * 2.0 / HEAD_DIM))

    def waves(place):
        phases = place[:, None] * frequency[None, :]
        pad = ((0, 0), (0, 64 - half))
        return np.pad(np.cos(phases), pad), np.pad(np.sin(phases), pad)

    cosine, sine = waves(np.arange(spans) * float(rows))
    parts = (
        np.concatenate([cosine, cosine], axis=1), np.concatenate([-sine, sine], axis=1),
        np.concatenate(waves(np.arange(rows, dtype=np.float64)), axis=1),
    )
    return tuple(jnp.asarray(part, jnp.float32) for part in parts)


def spread_heads(proj):
    lane = lax.broadcasted_iota(jnp.int32, (proj.shape[0], LANES), 1)
    tiles = [proj[:, at * LANES : (at + 1) * LANES] for at in range(3)]

    def put(*pieces):
        out = jnp.zeros_like(tiles[0])
        for tile, source, target, count in pieces:
            shift = (target - source) % LANES
            moved = pltpu.roll(tiles[tile], shift, 1) if shift else tiles[tile]
            out = jnp.where(jnp.logical_and(lane >= target, lane < target + count), moved, out)
        return out

    return (
        put((0, 0, 0, 48), (0, 48, 64, 48)),
        put((0, 96, 0, 32), (1, 0, 32, 16), (1, 16, 64, 48)),
        put((1, 64, 0, 48), (1, 112, 64, 16), (2, 0, 80, 32)),
        put((2, 32, 0, 96)),
    )


def close_halves(head):
    lane = lax.broadcasted_iota(jnp.int32, head.shape, 1)
    return jnp.where(lane < HEAD_DIM // 2, head, pltpu.roll(head, LANES - 64 + HEAD_DIM // 2, 1))


def wave(rows):
    first = lax.broadcasted_iota(jnp.int32, rows.shape, 1) < 64
    other = pltpu.roll(rows, 64, 1)
    return jnp.where(first, rows, other), jnp.where(first, -other, rows)


def nt(left, right):
    return lax.dot_general(left, right, (((1,), (1,)), ((), ())), preferred_element_type=jnp.float32)


def nn(left, right):
    return lax.dot_general(left, right, (((1,), (0,)), ((), ())), preferred_element_type=jnp.float32)


def tn(left, right):
    return lax.dot_general(left, right, (((0,), (0,)), ((), ())), preferred_element_type=jnp.float32)


def causal(width, place):
    key_at = lax.broadcasted_iota(jnp.int32, (2 * width, 2 * width), 0)
    query_at = lax.broadcasted_iota(jnp.int32, (2 * width, 2 * width), 1)
    query_at = jnp.where(query_at >= width, query_at - width, query_at)
    return key_at <= query_at + place * width


def vm(count):
    return [pl.BlockSpec(memory_space=pltpu.VMEM)] * count


MESH = pl.DeviceIdType.MESH


class Place:
    def __init__(self):
        self.me = lax.axis_index("ctx")
        core, x, y = self.me % 2, (self.me // 2) % 2, self.me // 4
        self.dp, self.dx, self.dy = 1 - 2 * core, 2 - 4 * x, 4 - 8 * y
        self.p, self.x, self.y = self.me + self.dp, self.me + self.dx, self.me + self.dy
        self.d = self.x + self.dy
        self.z = lax.axis_index("fsdp")
        self.planes = lax.axis_size("fsdp")
        self.n = lax.axis_size("ctx")


def greet(place, ctx=True, planes=False):
    barrier = pltpu.get_barrier_semaphore()
    count = 0
    if ctx:
        for step in range(1, place.n):
            pl.semaphore_signal(
                barrier, inc=1, device_id={"ctx": lax.rem(place.me + step, place.n)}, device_id_type=MESH
            )
            count += 1
    if planes:
        for step in range(1, place.planes):
            pl.semaphore_signal(
                barrier, inc=1, device_id={"fsdp": lax.rem(place.z + step, place.planes)}, device_id_type=MESH
            )
            count += 1
    pl.semaphore_wait(barrier, count)


def send(source, target, send_sem, recv_sem, **where):
    return pltpu.make_async_remote_copy(
        src_ref=source, dst_ref=target, send_sem=send_sem, recv_sem=recv_sem,
        device_id=where, device_id_type=MESH,
    )


class Gather:
    sems = 14

    def __init__(self, place, own, out, sem):
        self.place, self.own, self.out, self.sem = place, own, out, sem
        self.half = out.shape[1] // 2
        self.started = []
        self.met = False

    def go(self, source, target, index, rank):
        send(source, target, self.sem.at[0, index], self.sem.at[1, index], ctx=rank).start()
        self.started.append(index)

    def whole_block(self, index):
        return index == 6

    def sent(self):
        p = self.place
        for index in self.started:
            part = self.whole(p.me) if self.whole_block(index) else self.part(p.me, 0)
            send(part, part, self.sem.at[0, index], self.sem.at[1, index], ctx=p.p).wait_send()

    def part(self, rank, half):
        return self.out.at[rank, pl.ds(half * self.half, self.half)]

    def whole(self, rank):
        return self.out.at[rank]

    def start(self):
        p = self.place
        keep = pltpu.make_async_copy(self.own, self.whole(p.me), self.sem.at[0, 13])
        keep.start()
        self.keep = keep
        halves = [self.own.at[pl.ds(h * self.half, self.half)] for h in range(2)]
        self.go(halves[0], self.part(p.me, 0), 0, p.x)
        self.go(halves[1], self.part(p.me, 1), 3, p.y)
        self.go(self.own, self.whole(p.me), 6, p.p)
        self.go(halves[1], self.part(p.me, 1), 1, p.x)
        self.go(halves[0], self.part(p.me, 0), 2, p.y)

    def arrived(self, rank, half, index):
        part = self.part(rank, half)
        pltpu.make_async_copy(part, part, self.sem.at[1, index]).wait()
        return part

    def relay(self):
        p = self.place
        part = self.arrived(p.x, 0, 0)
        self.go(part, part, 4, p.y)
        self.go(part, part, 7, p.p)
        part = self.arrived(p.y, 1, 3)
        self.go(part, part, 5, p.x)
        self.go(part, part, 10, p.p)

    def rest(self):
        p = self.place
        for rank, half, index, onward in ((p.x, 1, 1, 8), (p.y, 0, 2, 9), (p.d, 0, 4, 11), (p.d, 1, 5, 12)):
            part = self.arrived(rank, half, index)
            self.go(part, part, onward, p.p)

    def first_partner(self):
        part = self.whole(self.place.p)
        pltpu.make_async_copy(part, part, self.sem.at[1, 6]).wait()
        self.met = True

    def partner(self):
        p = self.place
        if not self.met:
            self.first_partner()
        for rank, half, index in (
            (p.x, 0, 7), (p.y, 1, 10), (p.x, 1, 8), (p.y, 0, 9), (p.d, 0, 11), (p.d, 1, 12),
        ):
            self.arrived(rank + p.dp, half, index)

    def finish(self, kept=False):
        if not kept:
            self.keep.wait()
        self.sent()


class PlaneGather:
    def __init__(self, place, own, out, sem):
        self.place, self.own, self.out, self.sem = place, own, out, sem

    def hop(self, step, up):
        p = self.place
        sign = 1 if up else -1
        source = p.z - sign * step
        target = p.z + sign
        ok = jnp.logical_and(
            jnp.logical_and(source >= 0, source < p.planes),
            jnp.logical_and(target >= 0, target < p.planes),
        )
        source = jnp.clip(source, 0, p.planes - 1)
        target = jnp.clip(target, 0, p.planes - 1)
        block = self.own if step == 0 else self.out.at[source]
        return ok, send(
            block, self.out.at[source], self.sem.at[0 if up else 1, source], self.sem.at[2, source], fsdp=target
        )

    def start(self):
        p = self.place
        self.keep = pltpu.make_async_copy(self.own, self.out.at[p.z], self.sem.at[2, p.z])
        self.keep.start()
        for up in (True, False):
            ok, copy = self.hop(0, up)
            pl.when(ok)(copy.start)

    def got(self, step, up):
        p = self.place
        source = p.z - step if up else p.z + step
        ok = jnp.logical_and(source >= 0, source < p.planes)
        source = jnp.clip(source, 0, p.planes - 1)
        part = self.out.at[source]
        return ok, pltpu.make_async_copy(part, part, self.sem.at[2, source])

    def step(self, number):
        for up in (True, False):
            ok, copy = self.got(number, up)
            pl.when(ok)(copy.wait)
            if number < self.place.planes - 1:
                ok, copy = self.hop(number, up)
                pl.when(ok)(copy.start)

    def finish(self, kept=False):
        if not kept:
            self.keep.wait()
        for number in range(self.place.planes - 1):
            for up in (True, False):
                ok, copy = self.hop(number, up)
                pl.when(ok)(copy.wait_send)


class Exchange:
    def __init__(self, place, blocks, out, sem):
        self.place, self.blocks, self.out, self.sem = place, blocks, out, sem

    def pick(self, rank):
        return self.blocks.at[rank]

    def copy(self, step):
        p = self.place
        rank = lax.rem(p.me + step, p.n)
        return send(self.pick(rank), self.out.at[p.me], self.sem.at[0, step], self.sem.at[1, step], ctx=rank)

    def start(self):
        p = self.place
        for step in range(1, p.n):
            self.copy(step).start()
        self.keep = pltpu.make_async_copy(self.pick(p.me), self.out.at[p.me], self.sem.at[0, 0])
        self.keep.start()

    def finish(self):
        p = self.place
        self.keep.wait()
        for step in range(1, p.n):
            self.copy(step).wait_send()
        for step in range(1, p.n):
            part = self.out.at[lax.rem(p.me + p.n - step, p.n)]
            pltpu.make_async_copy(part, part, self.sem.at[1, step]).wait()


class Share(Exchange):
    def pick(self, rank):
        return self.blocks


class PlaneShare:
    def __init__(self, place, block, out, sem):
        self.place, self.block, self.out, self.sem = place, block, out, sem

    def copy(self, step):
        p = self.place
        plane = lax.rem(p.z + step, p.planes)
        return send(self.block, self.out.at[p.z], self.sem.at[0, step], self.sem.at[1, step], fsdp=plane)

    def start(self):
        p = self.place
        for step in range(1, p.planes):
            self.copy(step).start()
        self.keep = pltpu.make_async_copy(self.block, self.out.at[p.z], self.sem.at[0, 0])
        self.keep.start()

    def finish(self):
        p = self.place
        self.keep.wait()
        for step in range(1, p.planes):
            self.copy(step).wait_send()
        for step in range(1, p.planes):
            part = self.out.at[lax.rem(p.z + p.planes - step, p.planes)]
            pltpu.make_async_copy(part, part, self.sem.at[1, step]).wait()


def anywhere(count):
    return [pl.BlockSpec(memory_space=pl.ANY)] * count


class Reduce:
    sems = 10

    def __init__(self, place, mine, theirs, first, out, second, sem):
        self.place, self.mine, self.theirs, self.first, self.out, self.second, self.sem = (
            place, mine, theirs, first, out, second, sem
        )
        self.half = out.shape[1]
        self.started = []

    def push(self, slot):
        copy = send(
            self.theirs.at[slot], self.first.at[slot], self.sem.at[0, slot], self.sem.at[1, slot], ctx=self.place.p
        )
        copy.start()
        return copy

    def pushed(self):
        for slot in range(4):
            send(
                self.theirs.at[slot], self.first.at[slot], self.sem.at[0, slot], self.sem.at[1, slot],
                ctx=self.place.p,
            ).wait_send()

    def add(self, slot):
        part = self.first.at[slot]
        pltpu.make_async_copy(part, part, self.sem.at[1, slot]).wait()
        self.mine[slot] = self.mine[slot] + self.first[slot].astype(jnp.float32)

    def go(self, index, value, rank):
        self.out[index] = value.astype(jnp.bfloat16)
        self.turned(index, rank).start()
        self.started.append((index, rank))

    def turned(self, index, rank):
        return send(
            self.out.at[index], self.second.at[index], self.sem.at[0, 4 + index], self.sem.at[1, 4 + index], ctx=rank
        )

    def top(self, slot):
        return self.mine[slot, pl.ds(0, self.half), :]

    def low(self, slot):
        return self.mine[slot, pl.ds(self.half, self.half), :]

    def got(self, index):
        part = self.second.at[index]
        pltpu.make_async_copy(part, part, self.sem.at[1, 4 + index]).wait()
        return self.second[index].astype(jnp.float32)

    def across(self):
        self.add(3)
        self.go(1, self.top(3), self.place.x)
        self.go(3, self.low(3), self.place.y)

    def beside(self):
        self.add(1)
        self.go(0, self.top(1), self.place.x)
        self.add(2)
        self.go(2, self.low(2), self.place.y)

    def turn(self):
        self.go(4, self.top(2) + self.got(1), self.place.y)
        self.go(5, self.low(1) + self.got(3), self.place.x)

    def total(self, use):
        self.add(0)
        use(pl.ds(0, self.half), self.top(0) + self.got(0) + self.got(4))
        use(pl.ds(self.half, self.half), self.low(0) + self.got(2) + self.got(5))

    def finish(self):
        self.pushed()
        for index, rank in self.started:
            self.turned(index, rank).wait_send()


def flip(place, i):
    return place.me + (i % 2) * place.dp + ((i // 2) % 2) * place.dx + (i // 4) * place.dy


class HalfGather(Gather):
    sems = 16

    def __init__(self, place, own, out, sem):
        self.place, self.own, self.out, self.sem = place, own, out, sem
        self.half = out.shape[1]
        self.started = []
        self.met = False

    def part(self, rank, half):
        return self.out.at[2 * rank + half]

    def whole_block(self, index):
        return False

    def start(self):
        p = self.place
        halves = [self.own.at[pl.ds(h * self.half, self.half)] for h in range(2)]
        self.kept = [
            pltpu.make_async_copy(halves[h], self.part(p.me, h), self.sem.at[0, (13, 15)[h]]) for h in range(2)
        ]
        self.go(halves[0], self.part(p.me, 0), 0, p.x)
        self.go(halves[1], self.part(p.me, 1), 3, p.y)
        self.go(halves[0], self.part(p.me, 0), 6, p.p)
        self.go(halves[1], self.part(p.me, 1), 14, p.p)
        self.go(halves[1], self.part(p.me, 1), 1, p.x)
        self.go(halves[0], self.part(p.me, 0), 2, p.y)
        for copy in self.kept:
            copy.start()

    def first_partner(self):
        for h in range(2):
            self.arrived(self.place.p, h, (6, 14)[h])
        self.met = True

    def own_in(self):
        for copy in self.kept:
            copy.wait()

    def finish(self):
        self.sent()


def packed(block):
    rows = block.shape[0] // 2
    tail = jnp.concatenate([block[:, LANES:], jnp.zeros((2 * rows, 64), block.dtype)], axis=1)
    first = lax.broadcasted_iota(jnp.int32, (rows, LANES), 1) < 64
    return jnp.concatenate([block[:, :LANES], jnp.where(first, tail[:rows], pltpu.roll(tail[rows:], 64, 1))], axis=0)


def unpacked(block):
    rows = block.shape[0] // 3
    tail = block[2 * rows :].astype(jnp.float32)
    tails = jnp.concatenate([tail, pltpu.roll(tail, 64, 1)], axis=0)[:, :64].astype(block.dtype)
    return jnp.concatenate([block[: 2 * rows], tails], axis=1)


class PlaneReduce:
    def __init__(self, place, block, recv, sem):
        self.place, self.block, self.recv, self.sem = place, block, recv, sem

    def hop(self, ok, part, slot, target, first, wait):
        copy = send(
            self.block.at[part], self.recv.at[slot], self.sem.at[0, part], self.sem.at[1, slot], fsdp=target
        )

        @pl.when(ok)
        def _():
            if wait:
                copy.wait_send()
                return
            if not first:
                self.merge(part, part)
            copy.start()

    def merge(self, part, slot):
        piece = self.recv.at[slot]
        pltpu.make_async_copy(piece, piece, self.sem.at[1, slot]).wait()
        total = self.block[part].astype(jnp.float32) + self.recv[slot].astype(jnp.float32)
        self.block[part] = total.astype(jnp.bfloat16)

    def ends(self, i, wait=False):
        z = self.place.z
        low = z == 0
        part = jnp.where(low, 3 - i, i)
        slot = part if i < 2 else jnp.where(low, part, 4)
        self.hop(jnp.logical_or(low, z == 3), part, slot, jnp.where(low, 1, 2), True, wait)

    def inner(self, up, down, slot_up, slot_down, to_up, to_down, wait=False):
        z = self.place.z
        low = z == 1
        part = jnp.where(low, up, down)
        slot = jnp.where(low, slot_up, slot_down)
        self.hop(jnp.logical_or(low, z == 2), part, slot, jnp.where(low, to_up, to_down), False, wait)

    def start(self, wait=False):
        for i in range(3):
            self.ends(i, wait)

    def step1(self, wait=False):
        self.inner(3, 0, 3, 0, 2, 1, wait)

    def step2(self, wait=False):
        self.inner(2, 1, 2, 4, 2, 1, wait)
        self.inner(0, 3, 4, 3, 0, 3, wait)

    def total(self):
        z = self.place.z

        @pl.when(z > 0)
        def _():
            self.merge(z, z)

        @pl.when(z < 3)
        def _():
            self.merge(z, 4)

    def own(self):
        return self.block.at[self.place.z]

    def finish(self):
        self.start(True)
        self.step1(True)
        self.step2(True)


class Steps:
    def __init__(self, *steps):
        self.steps = list(steps)

    def next(self, count=1):
        for step in self.steps[:count]:
            step()
        self.steps = self.steps[count:]

    def rest(self):
        self.next(len(self.steps))


class OutGather(Gather):
    def __init__(self, place, own, out, sem):
        self.place, self.own, self.out, self.sem = place, own, out, sem
        self.half = out.shape[0] // 2
        self.started = []
        self.met = False

    def part(self, rank, half):
        return self.out.at[pl.ds(half * self.half, self.half), rank]

    def whole(self, rank):
        return self.out.at[:, rank]


def front_kernel(
    tok, pos, attn_own, ffn_own, qkv_own, gu_own, far_cos, far_sin, near, out_weight, down_weight, up,
    middle_grad, gain_grad, spots, gains, down_sum,
    hidden_o, qkv_o, down_o, q_o, k_o, v_o, att_o, lse_o, middle_o, turn_o, normed, agrad, low_all, gu_out, mcols,
    hidden, qkv_w, down_w, q_ref, k_ref, v_ref, att_ref, lse_ref, middle, turn_ref, mcols_send, up_low, spot, gain_own,
    wide_in, up_all, gul, gu_w, out_block, out_w, low_sorted, gain_all, spots_s, order_s, low,
    attended, own, mine, theirs, first, out, second, down_g, down_r,
    tok_sem, up_sem, spot_sem, gain_sem, qkv_sem, out_sem, outc_sem, gu_sem, down_sem, local_sem,
    low_sem, gather_sem, reduce_sem, agrad_sem, lows_sem, down_zs, mcols_sem,
):
    place = Place()
    n = place.n
    rows = tok.shape[0]
    half = rows // 2
    pairs = 8
    heads = rows
    length = n * rows
    width = tok.shape[1]
    out_own = out_weight.at[0, pl.ds(place.me * (out_weight.shape[1] // 8), out_weight.shape[1] // 8)]
    down_own = down_weight.at[0, pl.ds(place.me * (down_weight.shape[1] // 8), down_weight.shape[1] // 8)]
    spot[...] = jnp.broadcast_to(pos[0:1, 0:1], spot.shape)
    gain_own[pl.ds(0, 1), :] = attn_own[...].astype(jnp.float32)
    gain_own[pl.ds(1, 1), :] = ffn_own[...].astype(jnp.float32)
    fetch = pltpu.make_async_copy(up, middle_grad, local_sem.at[0])
    fetch.start()
    greet(place, planes=True)
    spans = Share(place, spot, spots, spot_sem)
    scales = PlaneShare(place, gain_own, gain_all, gain_sem)
    tokens = HalfGather(place, tok, wide_in, tok_sem)
    cots = Gather(place, up_low, up_all, up_sem)
    qkvs = PlaneGather(place, qkv_own, qkv_w, qkv_sem)
    outs = PlaneGather(place, out_own, out_block, out_sem)
    outc = OutGather(place, out_block, out_w, outc_sem)
    gus = PlaneGather(place, gu_own, gu_w, gu_sem)
    downs = PlaneGather(place, down_own, down_w, down_sem)
    given = []

    def give(source, target):
        copy = pltpu.make_async_copy(source, target, local_sem.at[5 + len(given)])
        copy.start()
        given.append(copy)

    tokens.start()
    qkvs.start()
    spans.start()
    scales.start()

    def turn_rows(at, carry):
        base = near[...]
        turn_ref[at] = base * far_cos[pl.ds(at, 1), :] + pltpu.roll(base, 64, 1) * far_sin[pl.ds(at, 1), :]
        return carry

    lax.fori_loop(0, 2 * pairs, turn_rows, 0)
    give(turn_ref, turn_o)
    fetch.wait()
    up_low[...] = middle_grad[...].astype(jnp.bfloat16)
    tokens.relay()
    qkvs.step(1)
    outs.start()
    qkvs.step(2)
    tokens.rest()
    cots.start()
    outs.step(1)
    downs.start()
    qkvs.step(3)
    tokens.partner()
    tokens.own_in()
    spans.finish()
    scales.finish()
    qkvs.keep.wait()
    table = pltpu.make_async_copy(spots, spots_s, local_sem.at[1])
    table.start()
    for g in range(2):
        gains[pl.ds(g, 1), :] = jnp.concatenate([gain_all[z, pl.ds(g, 1), :] for z in range(4)], axis=1)
    table.wait()
    early = [lax.div(spots_s[j, 0, 0], half) for j in range(pairs)]
    for t in range(pairs):
        at = 0
        for j in range(pairs):
            at = jnp.where(early[j] == t, j, at)
        order_s[t] = 2 * at
        order_s[2 * pairs - 1 - t] = 2 * at + 1
    cots.relay()

    def project(j, store):
        x = jnp.concatenate([wide_in[order_s[4 * j + i]] for i in range(4)], axis=0).astype(jnp.float32)
        factor = lax.rsqrt(jnp.mean(x * x, axis=-1, keepdims=True) + epsilon)
        scaled = (x * factor * gains[pl.ds(0, 1), :]).astype(jnp.bfloat16)
        store[pl.ds(2 * (j % 2), 2)] = scaled.reshape(2, rows, -1)
        proj = nn(scaled, qkv_w[...].reshape(-1, 3 * LANES))
        spread = spread_heads(proj)
        for piece in range(4):
            at = 4 * j + piece
            cosine, sine = wave(turn_ref[at])

            def turned(part):
                z = spread[part][piece * half : (piece + 1) * half]
                return (z * cosine + pltpu.roll(z, 64, 1) * sine).astype(jnp.bfloat16)

            base = (2 * j + piece // 2) * 4 * half + (piece % 2) * half
            q_ref[pl.ds(pl.multiple_of(base, half), half), :] = turned(0)
            q_ref[pl.ds(pl.multiple_of(base + 2 * half, half), half), :] = turned(1)
            k_ref[pl.ds(pl.multiple_of(at * half, half), half), :] = turned(2)
            v_ref[pl.ds(pl.multiple_of(at * half, half), half), :] = spread[3][piece * half : (piece + 1) * half].astype(jnp.bfloat16)

    def project_first(j, carry):
        project(j, theirs)
        return carry

    def project_second(j, carry):
        project(j, first)
        return carry

    lax.fori_loop(0, 2, project_first, 0)
    keep_first = pltpu.make_async_copy(theirs.at[pl.ds(0, 4)], normed.at[pl.ds(0, 4)], local_sem.at[2])
    keep_first.start()
    lax.fori_loop(2, 4, project_second, 0)
    keep_second = pltpu.make_async_copy(first, normed.at[pl.ds(4, 4)], local_sem.at[3])
    keep_second.start()
    give(q_ref, q_o)
    give(k_ref, k_o)
    give(v_ref, v_o)
    give(qkv_w, qkv_o)
    tokens.finish()
    outs.step(2)
    cots.rest()
    outs.step(3)
    outs.keep.wait()
    outc.start()

    def next_weights():
        downs.step(1)
        gus.start()

    steps = Steps(next_weights, lambda: None, outc.relay, lambda: downs.step(2))
    scaling = HEAD_DIM ** (-0.5)
    lane = lax.broadcasted_iota(jnp.int32, (half, LANES), 1)
    values_t = v_ref[...].astype(jnp.float32).T.astype(jnp.bfloat16)
    def attend_group(group):
        before = group * 4 * half

        def attend(place_of, carry):
            pair = 2 * group + place_of
            q = q_ref[pl.ds(pl.multiple_of(pair * 4 * half, 4 * half), 4 * half), :]
            scores = nt(k_ref[pl.ds(before, 4 * half), :], q) * scaling
            parts = [jnp.where(causal(2 * half, place_of), scores, -1e30)]
            if group:
                parts.append(nt(k_ref[pl.ds(0, before), :], q) * scaling)
            tops = [jnp.max(part, axis=0, keepdims=True) for part in parts]
            top = jnp.maximum(tops[0], tops[-1])
            parts = [jnp.exp(part - top) for part in parts]
            total = sum(jnp.sum(part, axis=0, keepdims=True) for part in parts)
            parts = [(part * (1.0 / total)).astype(jnp.bfloat16) for part in parts]
            lse_ref[pl.ds(pair, 1), :] = top + jnp.log(total)
            out_t = nn(values_t[:, before : before + 4 * half], parts[0])
            if group:
                out_t = out_t + nn(values_t[:, :before], parts[1])
            att_ref[pl.ds(pl.multiple_of(pair * LANES, LANES), LANES), :] = out_t
            result = out_t.T.astype(jnp.bfloat16).astype(jnp.float32)
            for part in range(2):
                left = result[part * half : (part + 1) * half]
                right = pltpu.roll(result[(2 + part) * half : (3 + part) * half], half, 1)
                low_sorted[2 * pair + part, :, 0:LANES] = jnp.where(lane < half, left, right).astype(jnp.bfloat16)
                low_sorted[2 * pair + part, :, LANES:] = right.astype(jnp.bfloat16)
            return carry

        lax.fori_loop(0, 2, attend, 0)

    for group in range(pairs // 2):
        attend_group(group)
        steps.next()
    give(att_ref, att_o)
    give(lse_ref, lse_o)
    for j in range(pairs):
        upper = low_sorted[early[j]]
        lower = low_sorted[2 * pairs - 1 - early[j]]
        low[j, pl.ds(0, half), :] = upper[:, :LANES]
        low[j, pl.ds(half, half), :] = lower[:, :LANES]
        tails = jnp.where(
            lane < 64, upper[:, LANES:].astype(jnp.float32), pltpu.roll(lower[:, LANES:].astype(jnp.float32), 64, 1)
        )
        low[j, pl.ds(2 * half, half), :] = tails.astype(jnp.bfloat16)
    keep_first.wait()
    keep_second.wait()
    moved = Exchange(place, low, attended, low_sem)
    moved.start()
    outc.rest()
    outc.partner()
    cots.partner()
    outc.keep.wait()
    moved.finish()
    middle[...] = tok[...].astype(jnp.float32)

    def out_project(q, carry):
        middle[...] += nn(unpacked(attended[q]), out_w[q // 2, pl.ds(4 * (q % 2), 4)].reshape(heads, -1))
        return carry

    lax.fori_loop(0, n, out_project, 0)
    give(middle, middle_o)
    gus.step(1)
    total = middle[...]
    factor = lax.rsqrt(jnp.mean(total * total, axis=-1, keepdims=True) + epsilon)
    own[...] = (total * factor * gains[pl.ds(1, 1), :]).astype(jnp.bfloat16)
    seconds = HalfGather(place, own, wide_in, gather_sem)
    seconds.start()
    seconds.relay()
    gus.step(2)
    seconds.rest()
    lows = Gather(place, low, low_all, lows_sem)
    lows.start()
    seconds.partner()
    downs.step(3)
    downs.keep.wait()
    give(down_w, down_o)
    cots.keep.wait()
    seconds.own_in()

    def early_grad(i, carry):
        rank = flip(place, i)
        at = pl.multiple_of((i % 2) * hidden.shape[2], LANES)
        mine[i // 2, :, pl.ds(at, hidden.shape[2])] = nt(up_all[rank], down_w[...].reshape(hidden.shape[2], -1))
        return carry

    lax.fori_loop(0, n, early_grad, 0)
    gus.step(3)
    gus.keep.wait()
    grads = Reduce(place, mine, theirs, first, out, second, reduce_sem)
    wide = hidden.shape[2]

    def block(i):
        rank = flip(place, i)
        gate_up = nn(wide_in[pl.ds(2 * rank, 2)].reshape(rows, -1), gu_w[...].reshape(-1, 2 * wide))
        gate, raised = gate_up[:, :wide], gate_up[:, wide:]
        sigmoid = 1.0 / (1.0 + jnp.exp(-gate))
        silu = gate * sigmoid
        hidden[rank] = (silu * raised).astype(jnp.bfloat16)
        hidden_grad = mine[i // 2, :, pl.ds(pl.multiple_of((i % 2) * wide, LANES), wide)]
        gul[rank, :, pl.ds(0, wide)] = (hidden_grad * raised * sigmoid * (1.0 + gate * (1.0 - sigmoid))).astype(jnp.bfloat16)
        gul[rank, :, pl.ds(wide, wide)] = (hidden_grad * silu).astype(jnp.bfloat16)
        return nt(gul[rank], gu_w[...].reshape(-1, 2 * wide))

    def block_at(t, carry):
        k = lax.rem(t // 2 + 1, 4)
        value = block(2 * k + 1 - t % 2)

        odd = t % 2
        theirs[k * (1 - odd) + 4 * odd] = value.astype(jnp.bfloat16)
        mine[k * odd + 4 * (1 - odd)] = value

        @pl.when(t % 2 == 0)
        def _():
            grads.push(k)

        @pl.when(t == 2)
        def _():
            lows.relay()

        @pl.when(t == 4)
        def _():
            grads.beside()

        @pl.when(t == 5)
        def _():
            lows.rest()

        @pl.when(t == 6)
        def _():
            grads.across()

        return carry

    lax.fori_loop(0, 8, block_at, 0)
    give(hidden, hidden_o)
    down_z = PlaneReduce(place, down_g, down_r, down_zs)
    piece = down_g.shape[1]

    def down_block(t, carry):
        left = hidden[:, :, pl.ds(pl.multiple_of(t * piece, piece), piece)].reshape(length, piece)
        down_g[t] = tn(left, up_all[...].reshape(length, width)).astype(jnp.bfloat16)
        return carry

    lax.fori_loop(0, 4, down_block, 0)
    down_z.start()
    grads.turn()
    seconds.finish()
    gain_grad[...] = jnp.zeros_like(gain_grad)

    def norm_back(part, second_grad):
        x = middle[part, :]
        factor = lax.rsqrt(jnp.mean(x * x, axis=-1, keepdims=True) + epsilon)
        unit = x * factor
        gain_grad[...] += jnp.sum(second_grad * unit, axis=0, keepdims=True)
        scaled = second_grad * gains[pl.ds(1, 1), :]
        inner = jnp.mean(scaled * unit, axis=-1, keepdims=True)
        grad = middle_grad[part, :] + factor * (scaled - unit * inner)
        middle_grad[part, :] = grad
        own[part, :] = grad.astype(jnp.bfloat16)

    gus.finish(kept=True)
    shard = gu_w.shape[1]

    def gu_block(t, carry):
        left = wide_in[:, :, pl.ds(pl.multiple_of(t * shard, shard), shard)].reshape(length, shard)
        gu_w[t] = tn(left, gul[...].reshape(length, 2 * wide)).astype(jnp.bfloat16)
        return carry

    lax.fori_loop(0, 4, gu_block, 0)
    give(gu_w, gu_out)
    down_z.step1()
    grads.total(norm_back)

    def head_grads(q, carry):
        weight = out_w[q // 2, pl.ds(4 * (q % 2), 4)].reshape(heads, -1)
        attended[q] = packed(nt(own[...], weight)).astype(jnp.bfloat16)
        return carry

    lax.fori_loop(0, n, head_grads, 0)
    heads_back = Exchange(place, attended, agrad, agrad_sem)
    heads_back.start()
    for q in range(8):
        mcols_send[q] = packed(own[:, q * heads : (q + 1) * heads].astype(jnp.float32)).astype(jnp.bfloat16)
    columns = Exchange(place, mcols_send, mcols, mcols_sem)
    columns.start()
    down_z.step2()
    lows.partner()
    heads_back.finish()
    down_z.total()
    down_sum[...] = down_g[place.z]
    for move in (qkvs, outs, downs, cots, outc):
        move.finish(kept=True)
    lows.finish()
    columns.finish()
    for copy in given:
        copy.wait()
    grads.finish()
    down_z.finish()


def front_moves(tok, pos, attn_own, ffn_own, qkv_own, gu_own, far_cos, far_sin, near, out_weight, down_weight, up):
    n, planes = lax.axis_size("ctx"), lax.axis_size("fsdp")
    rows, width = tok.shape
    length = n * rows
    bf, f32 = jnp.bfloat16, jnp.float32
    shape = jax.ShapeDtypeStruct
    out_own = shape((out_weight.shape[1] // n, width), bf)
    down_own = shape((down_weight.shape[1] // n, width), bf)
    spot = shape((8, LANES), jnp.int32)
    gain_own = shape((8, attn_own.shape[1]), f32)
    wide = planes * down_own.shape[0]
    dma = pltpu.SemaphoreType.DMA
    pairs = length // 192
    halves = pltpu.VMEM((6, rows // 2, width), bf)
    quads = pltpu.VMEM((4, rows, width), bf)
    small = (n, 3 * rows // 2, LANES)
    all_of = lambda x: shape((planes,) + x.shape, x.dtype)
    gathered = lambda x: pltpu.VMEM((planes,) + x.shape, x.dtype)
    ring = dma((2, Gather.sems))
    half_ring = dma((2, HalfGather.sems))
    line = dma((3, planes))
    swap = dma((2, n))
    kept = (
        shape((n, rows, wide), bf), all_of(qkv_own), all_of(down_own),
        shape((2 * length, LANES), bf), shape((length, LANES), bf), shape((length, LANES), bf),
        shape((pairs * LANES, 384), f32), shape((pairs, 384), f32), shape((rows, width), f32),
        shape((2 * n, rows // 2, LANES), f32),
    )
    return pl.pallas_call(
        front_kernel,
        out_shape=(
            shape((rows, width), f32), shape((1, width), f32), shape((n,) + spot.shape, spot.dtype), shape((2, width), f32),
            shape(down_own.shape, bf),
        ) + kept + (shape((n, rows, width), bf), shape(small, bf), shape((n,) + small, bf), all_of(gu_own), shape(small, bf)),
        in_specs=vm(9) + anywhere(3),
        out_specs=vm(5) + anywhere(15),
        scratch_shapes=[pltpu.VMEM(x.shape, x.dtype) for x in kept] + [
            pltpu.VMEM(small, bf), pltpu.VMEM((rows, width), bf), pltpu.VMEM(spot.shape, jnp.int32), pltpu.VMEM(gain_own.shape, f32),
            pltpu.VMEM((2 * n, rows // 2, width), bf), pltpu.VMEM((n, rows, width), bf), pltpu.VMEM((n, rows, 2 * wide), bf),
            gathered(gu_own), gathered(out_own), pltpu.VMEM((planes, n) + out_own.shape, bf),
            pltpu.VMEM((16, 96, 2 * LANES), bf), gathered(gain_own), pltpu.SMEM((n,) + spot.shape, jnp.int32),
            pltpu.SMEM((2 * n,), jnp.int32), pltpu.VMEM(small, bf),
            pltpu.VMEM(small, bf), pltpu.VMEM((rows, width), bf),
            pltpu.VMEM((5, rows, width), f32), pltpu.VMEM((5, rows, width), bf), quads, halves, halves,
            gathered(down_own), pltpu.VMEM((planes + 1,) + down_own.shape, bf),
            half_ring, ring, swap, dma((2, planes)), line, line, ring, line, line, dma((16,)),
            swap, half_ring, dma((2, Reduce.sems)), swap, ring, dma((2, planes + 1)), swap,
        ],
        compiler_params=pltpu.CompilerParams(collective_id=1, has_side_effects=True, vmem_limit_bytes=67043328),
        name="front_moves",
    )(tok, pos, attn_own, ffn_own, qkv_own, gu_own, far_cos, far_sin, near, out_weight, down_weight, up)


def back_moves_kernel(
    tok, gain, ffn_gain, down_sum, spots_i,
    gu_i, middle_grad_i, hidden_i, down_i, k_i, q_i, v_i, agrad_i, att_i, lse_i, turn_i, normed_i, middle_i, qkv_i, mcols_i, low_i,
    grad, result, attn_sum, ffn_sum, down_all, gu_all, out_all, qkv_all,
    spots_s, agrad_at, gu_g, hidden, down_w, k_ref, q_ref, v_ref, agrad, att_ref, lse_ref, turn_ref, normed_in, middle, qkv_w, mcols_in, low_in, out_g, qkv_g, gu_r, out_r, qkv_r,
    mine, theirs, first, out, second, dk_ref, dv_ref, pg_sorted, mcols,
    gain_sum, mine_gain, ctx_gain, plane_sum, plane_gain,
    free, local_sem, sum_sem, reduce_sem, gu_zs, out_zs, qkv_zs, down_cs, gu_cs, out_cs, qkv_cs,
    gain_sem, plane_sem,
):
    place = Place()
    n = place.n
    rows = tok.shape[0]
    half = rows // 2
    pairs = 8
    width = tok.shape[1]
    length = n * rows
    loads = [
        pltpu.make_async_copy(source, target, local_sem.at[at])
        for at, (source, target) in enumerate((
            (gu_i, gu_g), (hidden_i, hidden), (down_i, down_w), (k_i, k_ref), (q_i, q_ref), (v_i, v_ref),
            (agrad_i, agrad), (att_i, att_ref), (lse_i, lse_ref), (turn_i, turn_ref), (middle_i, middle),
            (normed_i, normed_in), (qkv_i, qkv_w), (mcols_i, mcols_in), (low_i, low_in), (middle_grad_i, grad),
        ))
    ]
    table = pltpu.make_async_copy(spots_i, spots_s, local_sem.at[16])
    table.start()
    for load in loads:
        load.start()
    greet(place, planes=True)
    table.wait()
    early = [lax.div(spots_s[j, 0, 0], half) for j in range(pairs)]
    holder = []
    for t in range(pairs):
        at = 0
        for j in range(pairs):
            at = jnp.where(early[j] == t, j, at)
        holder.append(at)
    gu_z = PlaneReduce(place, gu_g, gu_r, gu_zs)
    out_z = PlaneReduce(place, out_g, out_r, out_zs)
    qkv_z = PlaneReduce(place, qkv_g, qkv_r, qkv_zs)
    sums = Reduce(place, mine, theirs, first, out, second, sum_sem)
    downs = Gather(place, down_sum, down_all, down_cs)
    gus = Gather(place, gu_z.own(), gu_all, gu_cs)
    loads[0].wait()
    gu_z.start()
    downs.start()
    loads[1].wait()
    loads[2].wait()

    def other(k, carry):
        theirs[k] = nn(hidden[flip(place, 2 * k + 1)], down_w[...].reshape(-1, width)).astype(jnp.bfloat16)
        sums.push(k)
        return carry

    def ours(k, carry):
        mine[k] = nn(hidden[flip(place, 2 * k)], down_w[...].reshape(-1, width))
        return carry

    lax.fori_loop(0, 4, other, 0)
    lax.fori_loop(0, 4, ours, 0)
    downs.relay()
    sums.across()
    sums.beside()
    for load in loads[3:11]:
        load.wait()

    def finish_rows(part, down_out):
        result[part, :] = (middle[part, :] + down_out).astype(jnp.bfloat16)

    def sums_done():
        sums.total(finish_rows)
        sums.finish()
        for rank in (place.p, place.x, place.y):
            pl.semaphore_signal(free, inc=1, device_id={"ctx": rank}, device_id_type=MESH)

    def columns_done():
        loads[13].wait()

        def unpack(q, carry):
            mcols[q] = unpacked(mcols_in[q])
            return carry

        lax.fori_loop(0, n, unpack, 0)

    steps = Steps(downs.rest, gu_z.step1, lambda: (downs.partner(), sums.turn()), columns_done)
    scaling = HEAD_DIM ** (-0.5)
    lane = lax.broadcasted_iota(jnp.int32, (half, LANES), 1)
    keys_t = k_ref[...].astype(jnp.float32).T.astype(jnp.bfloat16)
    ranks_s = agrad_at
    for t in range(pairs):
        ranks_s[t] = holder[t]
        ranks_s[2 * pairs - 1 - t] = holder[t]
    dk_ref[...] = jnp.zeros_like(dk_ref)
    dv_ref[...] = jnp.zeros_like(dv_ref)

    def back_group(group):
        before = group * 4 * half
        side = 0 if group < pairs // 4 else 1
        cuts = [(before, 4 * half)] + [(at, min(768, before - at)) for at in range(0, before, 768)]

        def back(place_of, carry):
            pair = 2 * group + place_of
            q = q_ref[pl.ds(pl.multiple_of(pair * 4 * half, 4 * half), 4 * half), :]
            firsts, seconds = [], []
            for part in range(2):
                piece_of = agrad[ranks_s[2 * pair + part]].astype(jnp.float32)
                left = piece_of[side * half : (side + 1) * half]
                tail = piece_of[2 * half :]
                right = tail if side == 0 else pltpu.roll(tail, 64, 1)
                firsts.append(jnp.where(lane < half, left, 0.0))
                seconds.append(
                    jnp.where(lane < half, pltpu.roll(jnp.where(lane < half, right, left), LANES - half, 1), 0.0)
                )
            grads = jnp.concatenate(firsts + seconds, axis=0)
            att_t = att_ref[pl.ds(pl.multiple_of(pair * LANES, LANES), LANES), :]
            delta = jnp.sum(grads.T * att_t, axis=0, keepdims=True)
            grads = grads.astype(jnp.bfloat16)
            dq_t = None
            for at, count in cuts:
                keys = pl.ds(at, count)
                weights = jnp.exp(
                    jnp.where(
                        causal(2 * half, place_of), nt(k_ref[keys, :], q) * scaling - lse_ref[pl.ds(pair, 1), :], -1e30
                    )
                    if at == before
                    else nt(k_ref[keys, :], q) * scaling - lse_ref[pl.ds(pair, 1), :]
                )
                dp = nt(v_ref[keys, :], grads)
                ds = (weights * (dp - delta)).astype(jnp.bfloat16)
                dk_ref[keys, :] += nn(ds, q) * scaling
                dv_ref[keys, :] += nn(weights.astype(jnp.bfloat16), grads)
                term = nn(keys_t[:, at : at + count], ds)
                dq_t = term if dq_t is None else dq_t + term
            dq = dq_t.T * scaling
            for part in range(2):
                cosine, sine = wave(turn_ref[2 * pair + part])
                turned = []
                for head in range(2):
                    z = dq[(2 * head + part) * half : (2 * head + part + 1) * half]
                    turned.append(close_halves(z * cosine - pltpu.roll(z, 64, 1) * sine))
                second_head = pltpu.roll(turned[1], 96, 1)
                pg_sorted[2 * pair + part, :, 0:LANES] = jnp.where(lane < 96, turned[0], second_head).astype(jnp.bfloat16)
                pg_sorted[2 * pair + part, :, LANES : 2 * LANES] = second_head.astype(jnp.bfloat16)
            return carry

        lax.fori_loop(0, 2, back, 0)

    for group in reversed(range(pairs // 2)):
        back_group(group)
        steps.next()
    for s in range(2 * pairs):
        spot = pl.ds(s * half, half)
        cosine, sine = wave(turn_ref[s])
        z = dk_ref[spot, :]
        key_head = pltpu.roll(close_halves(z * cosine - pltpu.roll(z, 64, 1) * sine), 64, 1)
        queries_too = pg_sorted[s, :, LANES : 2 * LANES].astype(jnp.float32)
        pg_sorted[s, :, LANES : 2 * LANES] = jnp.where(lane < 64, queries_too, key_head).astype(jnp.bfloat16)
        pg_sorted[s, :, 2 * LANES :] = jnp.where(lane < 32, key_head, pltpu.roll(dv_ref[spot, :], 32, 1)).astype(jnp.bfloat16)

    loads[11].wait()
    loads[12].wait()
    shard = gu_g.shape[1]

    def qkv_block(t, carry):
        left = normed_in[:, :, pl.ds(pl.multiple_of(t * shard, shard), shard)].reshape(length, shard)
        qkv_g[t] = tn(left, pg_sorted[...].reshape(length, 3 * LANES)).astype(jnp.bfloat16)
        return carry

    lax.fori_loop(0, 4, qkv_block, 0)
    qkv_z.start()
    sums_done()
    gu_z.step2()
    pl.semaphore_wait(free, 3)
    grads = Reduce(place, mine, theirs, first, out, second, reduce_sem)

    def chunk(i):
        at = lax.div(spots_s[flip(place, i), 0, 0], half)
        rows_of = jnp.concatenate([pg_sorted[at], pg_sorted[2 * pairs - 1 - at]], axis=0)
        return nt(rows_of, qkv_w[...].reshape(width, -1))

    def push(k, carry):
        theirs[k] = chunk(2 * k + 1).astype(jnp.bfloat16)
        grads.push(k)
        return carry

    def keep(k, carry):
        mine[k] = chunk(2 * k)
        return carry

    lax.fori_loop(0, 4, push, 0)
    lax.fori_loop(0, 4, keep, 0)
    grads.across()
    grads.beside()
    loads[14].wait()
    loads[15].wait()

    def out_block(src, carry):
        heads = low_in[src, :, pl.ds(0, rows), :].reshape(length, LANES)
        tails = low_in[src, :, pl.ds(rows, half), :].reshape(length // 2, LANES)
        upper = tn(heads, mcols[...].reshape(length, rows))
        from_a = tn(tails, mcols[:, pl.ds(0, half), :].reshape(length // 2, rows))
        from_b = tn(tails, mcols[:, pl.ds(half, half), :].reshape(length // 2, rows))
        at = pl.multiple_of((src % 2) * rows, rows)
        out_g[src // 2, pl.ds(at, LANES), :] = upper.astype(jnp.bfloat16)
        out_g[src // 2, pl.ds(pl.multiple_of(at + LANES, 64), 64), :] = (from_a[:64] + from_b[64:]).astype(jnp.bfloat16)
        return carry

    lax.fori_loop(0, 8, out_block, 0)
    out_z.start()
    grads.turn()
    gu_z.total()
    gus.start()
    gain_sum[...] = jnp.zeros_like(gain_sum)

    def norm_back(part, normed_grad):
        x = tok[part, :].astype(jnp.float32)
        factor = lax.rsqrt(jnp.mean(x * x, axis=-1, keepdims=True) + epsilon)
        unit = x * factor
        gain_sum[...] += jnp.sum(normed_grad * unit, axis=0, keepdims=True)
        scaled = normed_grad * gain[pl.ds(0, 1), :]
        inner = jnp.mean(scaled * unit, axis=-1, keepdims=True)
        grad[part, :] = grad[part, :] + factor * (scaled - unit * inner)

    qkv_z.step1()
    grads.total(norm_back)
    gain_grad = gain_sum[...]
    count = mine_gain.shape[0] // 2
    for at in range(count):
        mine_gain[pl.ds(at, 1), :] = gain_grad[:, at * shard : (at + 1) * shard]
        mine_gain[pl.ds(count + at, 1), :] = ffn_gain[:, at * shard : (at + 1) * shard]
    ctx_sum = Share(place, mine_gain, ctx_gain, gain_sem)
    ctx_sum.start()
    gus.relay()
    qkv_z.step2()
    out_z.step1()
    ctx_sum.finish()
    plane_sum[...] = jnp.sum(ctx_gain[...], axis=0)
    planes = PlaneShare(place, plane_sum, plane_gain, plane_sem)
    planes.start()
    out_z.step2()
    qkv_z.total()
    gus.rest()
    qkvs = Gather(place, qkv_z.own(), qkv_all, qkv_cs)
    qkvs.start()
    out_z.total()
    outs = Gather(place, out_z.own(), out_all, out_cs)
    qkvs.relay()
    outs.start()
    qkvs.rest()
    outs.relay()
    outs.rest()
    planes.finish()
    plane_sum[...] = jnp.sum(plane_gain[...], axis=0)
    attn_sum[...] = plane_sum[pl.ds(place.z, 1), :]
    ffn_sum[...] = plane_sum[pl.ds(count + place.z, 1), :]
    gus.partner()
    qkvs.partner()
    outs.partner()
    for move in (gu_z, out_z, qkv_z, downs, gus, outs, qkvs, grads):
        move.finish()


def back_moves(tok, gain, ffn_gain, down_sum, spots, *moved):
    n, planes = lax.axis_size("ctx"), lax.axis_size("fsdp")
    rows, width = tok.shape
    length = n * rows
    shard = width // planes
    bf, f32 = jnp.bfloat16, jnp.float32
    shape = jax.ShapeDtypeStruct
    dma = pltpu.SemaphoreType.DMA
    halves = pltpu.VMEM((6, rows // 2, width), bf)
    quads = pltpu.VMEM((4, rows, width), bf)
    small = (2 * planes, shard)
    parts = (moved[0].shape[1:], (shard, rows), (shard, 3 * LANES))
    ring = dma((2, Gather.sems))
    return pl.pallas_call(
        back_moves_kernel,
        out_shape=(shape((rows, width), f32), shape((rows, width), bf), shape((1, shard), f32), shape((1, shard), f32))
        + tuple(shape((n,) + part, bf) for part in (down_sum.shape,) + parts),
        in_specs=vm(4) + anywhere(1 + len(moved)),
        out_specs=vm(4) + anywhere(4),
        scratch_shapes=[pltpu.SMEM(spots.shape, jnp.int32), pltpu.SMEM((2 * n,), jnp.int32)] + [pltpu.VMEM(x.shape, x.dtype) for at, x in enumerate(moved) if at != 1]
        + [pltpu.VMEM((planes,) + part, bf) for part in parts[1:]]
        + [pltpu.VMEM((planes + 1,) + part, bf) for part in parts]
        + [
            pltpu.VMEM((4, rows, width), f32), quads, quads, halves, halves,
            pltpu.VMEM((length, LANES), f32), pltpu.VMEM((length, LANES), f32), pltpu.VMEM((16, 96, 3 * LANES), bf),
            pltpu.VMEM((n, rows, rows), bf),
            pltpu.VMEM((1, width), f32), pltpu.VMEM(small, f32), pltpu.VMEM((n,) + small, f32),
            pltpu.VMEM(small, f32), pltpu.VMEM((planes,) + small, f32),
            pltpu.SemaphoreType.REGULAR, dma((17,)), dma((2, Reduce.sems)), dma((2, Reduce.sems)),
            dma((2, 5)), dma((2, 5)), dma((2, 5)), ring, ring, ring, ring, dma((2, n)), dma((2, planes)),
        ],
        compiler_params=pltpu.CompilerParams(collective_id=6, has_side_effects=True, vmem_limit_bytes=67043328),
        name="back_moves",
    )(tok, gain, ffn_gain, down_sum, spots, *moved)


def pack_kernel(
    down, gu, out, qkv, grad, result, attn, ffn, down_o, gu_o, out_o, qkv_o, grad_o, result_o, attn_o, ffn_o
):
    devices, rows = gu.shape[0], gu.shape[1]
    f32 = jnp.float32
    lane = lax.broadcasted_iota(jnp.int32, (rows, LANES), 1)
    down_o[...] = down[0].astype(f32)
    grad_o[...] = grad[...]
    result_o[...] = result[...]
    attn_o[...] = attn[...]
    ffn_o[...] = ffn[...]
    tiles = gu_o.shape[0] // rows
    spans = gu.shape[2] // (2 * LANES)
    for r in range(0, rows, 16):
        pieces = [
            gu[c, pl.ds(r, 16), (s * spans + z) * LANES : (s * spans + z + 1) * LANES].astype(f32)
            for z in range(spans) for c in range(devices) for s in range(2)
        ]
        gu_o[pl.ds(r * tiles, 16 * tiles), :] = jnp.swapaxes(jnp.stack(pieces, axis=0), 0, 1).reshape(16 * tiles, LANES)

    def tile(c, at):
        return qkv[c, :, at * LANES : (at + 1) * LANES].astype(f32)

    def key_head(c):
        return jnp.where(lane < 64, pltpu.roll(tile(c, 1), 64, 1), pltpu.roll(tile(c, 2), 64, 1))

    def value_head(c):
        return pltpu.roll(tile(c, 2), 96, 1)

    def store(at, heads):
        second, third, fourth = pltpu.roll(heads[1], 96, 1), pltpu.roll(heads[2], 64, 1), pltpu.roll(heads[3], 32, 1)
        qkv_o[:, at : at + LANES] = jnp.where(lane < 96, heads[0], second)
        qkv_o[:, at + LANES : at + 2 * LANES] = jnp.where(lane < 64, second, third)
        qkv_o[:, at + 2 * LANES : at + 3 * LANES] = jnp.where(lane < 32, third, fourth)

    for c in range(0, devices, 2):
        at = c * 192
        turned = pltpu.roll(tile(c + 1, 0), 64, 1)
        qkv_o[:, at : at + LANES] = tile(c, 0)
        qkv_o[:, at + LANES : at + 2 * LANES] = jnp.where(lane < 64, tile(c, 1), turned)
        qkv_o[:, at + 2 * LANES : at + 3 * LANES] = jnp.where(lane < 64, turned, pltpu.roll(tile(c + 1, 1), 64, 1))
    for c in range(0, devices, 4):
        store(HEADS * HEAD_DIM + c * 96, [key_head(c + i) for i in range(4)])
        store((HEADS + KV_HEADS) * HEAD_DIM + c * 96, [value_head(c + i) for i in range(4)])
    for c in range(0, devices, 2):
        at = c * 192
        first = out[c].astype(f32)
        second = out[c + 1].astype(f32)
        tail = jnp.concatenate([first[:, LANES:], jnp.zeros((rows, 64), f32)], axis=1)
        next_tail = jnp.concatenate([second[:, LANES:], jnp.zeros((rows, 64), f32)], axis=1)
        turned = pltpu.roll(second[:, :LANES], 64, 1)
        out_o[:, at : at + LANES] = first[:, :LANES]
        out_o[:, at + LANES : at + 2 * LANES] = jnp.where(lane < 64, tail, turned)
        out_o[:, at + 2 * LANES : at + 3 * LANES] = jnp.where(lane < 64, turned, pltpu.roll(next_tail, 64, 1))


def pack(down, gu, out, qkv, grad, result, attn, ffn):
    n, shard = gu.shape[0], gu.shape[1]
    rows = shard // n
    width = down.shape[2]
    f32 = jnp.float32
    spec = pl.BlockSpec
    shape = jax.ShapeDtypeStruct
    tiles = n * gu.shape[2] // LANES
    quarter = grad.shape[0] // 4
    return pl.pallas_call(
        pack_kernel,
        grid=(n,),
        out_shape=(
            shape((n * down.shape[1], width), f32), shape((shard * tiles, LANES), f32), shape((shard, n * out.shape[2]), f32),
            shape((shard, (HEADS + 2 * KV_HEADS) * HEAD_DIM), f32), shape(grad.shape, f32), shape(result.shape, result.dtype), shape(attn.shape, f32), shape(ffn.shape, f32),
        ),
        in_specs=[
            spec((1,) + down.shape[1:], lambda i: (i, 0, 0)), spec((n, rows, gu.shape[2]), lambda i: (0, i, 0)),
            spec((n, rows, out.shape[2]), lambda i: (0, i, 0)), spec((n, rows, qkv.shape[2]), lambda i: (0, i, 0)),
            spec((quarter, width), lambda i: (i // 2, 0)), spec((quarter, width), lambda i: (i // 2, 0)),
            spec(attn.shape, lambda i: (0, 0)), spec(ffn.shape, lambda i: (0, 0)),
        ],
        out_specs=[
            spec((down.shape[1], width), lambda i: (i, 0)), spec((rows * tiles, LANES), lambda i: (i, 0)),
            spec((rows, n * out.shape[2]), lambda i: (i, 0)), spec((rows, (HEADS + 2 * KV_HEADS) * HEAD_DIM), lambda i: (i, 0)),
            spec((quarter, width), lambda i: (i // 2, 0)), spec((quarter, width), lambda i: (i // 2, 0)),
            spec(attn.shape, lambda i: (0, 0)), spec(ffn.shape, lambda i: (0, 0)),
        ],
        name="pack",
    )(down, gu, out, qkv, grad, result, attn, ffn)


def fast_body(
    tokens, positions, qkv_weight, out_weight, gate_up_weight, down_weight, attn_gain, ffn_gain, cotangent
):
    me = lax.axis_index("ctx")
    n = lax.axis_size("ctx")
    planes = lax.axis_size("fsdp")
    rows = tokens.shape[1]
    length = n * rows
    width = tokens.shape[2]
    wide = down_weight.shape[1] * planes
    own = wide // n
    piece = own // planes
    shard = qkv_weight.shape[1]
    query_width = HEADS * HEAD_DIM
    key_width = KV_HEADS * HEAD_DIM
    cut = lax.dynamic_slice_in_dim

    qkv = qkv_weight[0]
    q_part = cut(qkv, me * 2 * HEAD_DIM, 2 * HEAD_DIM, 1)
    k_part = cut(qkv, query_width + me * HEAD_DIM, HEAD_DIM, 1)
    v_part = cut(qkv, query_width + key_width + me * HEAD_DIM, HEAD_DIM, 1)
    qkv_own = jnp.concatenate([q_part, k_part, v_part], axis=1)
    pieces = [cut(gate_up_weight[0], at * (wide // planes) + me * piece, piece, 2) for at in range(planes)]
    gate_up_own = jnp.concatenate(pieces, axis=2).reshape(shard, 2 * own)
    (
        middle_grad, ffn_partial, spots, gains, down_sum, hidden, qkv_block, down_block, q, k, v, att, lse, middle,
        turns, normed, attended_grad, low_all, gate_up_grad, middle_cols,
    ) = front_moves(
        tokens[0], positions, attn_gain, ffn_gain, qkv_own, gate_up_own, *turn_parts(2 * n, rows // 2),
        out_weight, down_weight, cotangent[0],
    )
    stream_grad, result, attn_sum, ffn_sum, down_grad, gate_up_grad, out_grad, qkv_grad = back_moves(
        tokens[0], gains, ffn_partial, down_sum, spots,
        gate_up_grad, middle_grad, hidden, down_block, k, q, v, attended_grad, att, lse, turns, normed, middle,
        qkv_block, middle_cols, low_all,
    )
    down_grad, gate_up_grad, out_grad, qkv_grad, stream_grad, result, attn_sum, ffn_sum = pack(
        down_grad, gate_up_grad, out_grad, qkv_grad, stream_grad, result, attn_sum, ffn_sum
    )
    gate_up_grad = gate_up_grad.reshape(shard, wide // LANES, 2, LANES).transpose(0, 2, 1, 3).reshape(shard, 2, wide)
    return (
        result[None],
        stream_grad[None],
        qkv_grad[None],
        out_grad[None],
        gate_up_grad[None],
        down_grad[None],
        attn_sum,
        ffn_sum,
    )


def solution(mesh):
    split = mesh.shape["ctx"] == KV_HEADS and mesh.shape["fsdp"] == 4
    placed = (
        P("fsdp", "ctx", None),
        P("fsdp", "ctx"),
        P(None, "fsdp", None),
        P(None, "fsdp", None),
        P(None, "fsdp", None, None),
        P(None, "fsdp", None),
        P(None, "fsdp"),
        P(None, "fsdp"),
        P("fsdp", "ctx", None),
    )
    return jax.shard_map(
        fast_body if split else body,
        mesh=mesh,
        in_specs=placed,
        out_specs=(
            P("fsdp", "ctx", None),
            P("fsdp", "ctx", None),
            P(None, "fsdp", None),
            P(None, "fsdp", None),
            P(None, "fsdp", None, None),
            P(None, "fsdp", None),
            P(None, "fsdp"),
            P(None, "fsdp"),
        ),
        check_vma=False,
    )
```

```python
import jax
import jax.numpy as jnp
import numpy as np
from jax import lax
from jax.experimental import pallas as pl
from jax.experimental.pallas import tpu as pltpu
from jax.sharding import PartitionSpec as P

HEADS = 16
KV_HEADS = 8
HEAD_DIM = 96
LAYERS = 1


epsilon = 1e-05
rope_base = 100000.0


def angles(place):
    halfway = HEAD_DIM // 2
    frequency = rope_base ** (-(jnp.arange(halfway, dtype=jnp.float32) * 2.0 / HEAD_DIM))
    phases = place.astype(jnp.float32)[:, None] * frequency[None, :]
    phases = jnp.concatenate([phases, phases], axis=-1)
    return (jnp.cos(phases)[:, None, :], jnp.sin(phases)[:, None, :])


def rotate(vectors, cosine, sine):
    halfway = vectors.shape[-1] // 2
    turned = jnp.concatenate([-vectors[..., halfway:], vectors[..., :halfway]], axis=-1)
    return vectors * cosine + turned * sine


def rotate_back(grads, cosine, sine):
    halfway = grads.shape[-1] // 2
    scaled = grads * sine
    return grads * cosine + jnp.concatenate(
        [scaled[..., halfway:], -scaled[..., :halfway]], axis=-1
    )


def normalize(rows, gain):
    factor = lax.rsqrt(jnp.mean(rows * rows, axis=-1, keepdims=True) + epsilon)
    return (rows * factor * gain, factor)


def normalize_back(upstream, rows, factor, gain):
    unit_rows = rows * factor
    gain_grad = jnp.sum(upstream * unit_rows, axis=0)
    scaled = upstream * gain
    row_inner = jnp.mean(scaled * unit_rows, axis=-1, keepdims=True)
    return (factor * (scaled - unit_rows * row_inner), gain_grad)


def split_blocks(queries, keys_all, values_all, key_place):
    rows = queries.shape[0]
    half = rows // 2
    shards = key_place.shape[0] // rows
    key_blocks = keys_all.reshape(shards, 2, half, KV_HEADS, HEAD_DIM)
    value_blocks = values_all.reshape(shards, 2, half, KV_HEADS, HEAD_DIM)
    place_blocks = key_place.reshape(shards, 2, half)
    return (key_blocks, value_blocks, place_blocks)


def scores_of(queries, key_block, place_block, query_place):
    scaling = HEAD_DIM ** (-0.5)
    scores = (
        jnp.einsum("rkgd,skd->kgrs", queries, key_block, preferred_element_type=jnp.float32)
        * scaling
    )
    allowed = place_block[None, None, None, :] <= query_place[None, None, :, None]
    return (scores, allowed)


def reachable(place_block, query_place):
    return jnp.min(place_block) <= jnp.max(query_place)


def attention_forward(queries, keys_all, values_all, query_place, key_place):
    key_blocks, value_blocks, place_blocks = split_blocks(queries, keys_all, values_all, key_place)
    rows = queries.shape[0]
    half = rows // 2
    groups = HEADS // KV_HEADS
    query_spans = queries.reshape(2, half, KV_HEADS, groups, HEAD_DIM)
    place_spans = query_place.reshape(2, half)

    def sweep_max(carry, inputs):
        key_block, place_block = inputs
        updated_all = []
        for span in range(2):
            state = carry[span]
            for part in range(2):

                def live(current, span=span, part=part):
                    maximum, total = current
                    scores, allowed = scores_of(
                        query_spans[span], key_block[part], place_block[part], place_spans[span]
                    )
                    masked = jnp.where(allowed, scores, -1e30)
                    updated = jnp.maximum(maximum, jnp.max(masked, axis=-1))
                    weights_now = jnp.where(allowed, jnp.exp(masked - updated[..., None]), 0.0)
                    return (
                        updated,
                        total * jnp.exp(maximum - updated) + jnp.sum(weights_now, axis=-1),
                    )

                state = lax.cond(
                    reachable(place_block[part], place_spans[span]),
                    live,
                    lambda current: current,
                    state,
                )
            updated_all.append(state)
        return (tuple(updated_all), None)

    start_max = jnp.full((KV_HEADS, groups, half), -1e30, jnp.float32)
    start_total = jnp.zeros((KV_HEADS, groups, half), jnp.float32)
    start = ((start_max, start_total), (start_max, start_total))
    finals, unused = lax.scan(sweep_max, start, (key_blocks, place_blocks))
    logsum_spans = [finals[span][0] + jnp.log(finals[span][1]) for span in range(2)]

    def sweep_out(results, inputs):
        key_block, value_block, place_block = inputs
        updated_all = []
        for span in range(2):
            result = results[span]
            for part in range(2):

                def live(current, span=span, part=part):
                    scores, allowed = scores_of(
                        query_spans[span], key_block[part], place_block[part], place_spans[span]
                    )
                    softmax_rows = jnp.where(
                        allowed, jnp.exp(scores - logsum_spans[span][..., None]), 0.0
                    ).astype(jnp.bfloat16)
                    return current + jnp.einsum(
                        "kgrs,skd->rkgd",
                        softmax_rows,
                        value_block[part],
                        preferred_element_type=jnp.float32,
                    )

                result = lax.cond(
                    reachable(place_block[part], place_spans[span]),
                    live,
                    lambda current: current,
                    result,
                )
            updated_all.append(result)
        return (tuple(updated_all), None)

    start_out = jnp.zeros((half, KV_HEADS, groups, HEAD_DIM), jnp.float32)
    outs, unused_out = lax.scan(
        sweep_out, (start_out, start_out), (key_blocks, value_blocks, place_blocks)
    )
    logsum = jnp.concatenate(logsum_spans, axis=-1)
    attended = jnp.concatenate([outs[0], outs[1]], axis=0)
    return (logsum, attended)


def attention_backward(
    queries, keys_all, values_all, query_place, key_place, logsum, attended_grad, row_inner
):
    key_blocks, value_blocks, place_blocks = split_blocks(queries, keys_all, values_all, key_place)
    rows = queries.shape[0]
    half = rows // 2
    groups = HEADS // KV_HEADS
    scaling = HEAD_DIM ** (-0.5)
    query_spans = queries.reshape(2, half, KV_HEADS, groups, HEAD_DIM)
    place_spans = query_place.reshape(2, half)
    grad_spans = attended_grad.reshape(2, half, KV_HEADS, groups, HEAD_DIM)
    logsum_spans = logsum.reshape(KV_HEADS, groups, 2, half)
    inner_spans = row_inner.reshape(KV_HEADS, groups, 2, half)

    def sweep_back(query_grads, inputs):
        key_block, value_block, place_block = inputs
        query_grads = list(query_grads)
        key_parts = []
        value_parts = []
        for part in range(2):
            key_acc = jnp.zeros((half, KV_HEADS, HEAD_DIM), jnp.float32)
            value_acc = jnp.zeros((half, KV_HEADS, HEAD_DIM), jnp.float32)
            for span in range(2):

                def live(current, span=span, part=part):
                    query_grad, key_grad, value_grad = current
                    scores, allowed = scores_of(
                        query_spans[span], key_block[part], place_block[part], place_spans[span]
                    )
                    softmax_rows = jnp.where(
                        allowed, jnp.exp(scores - logsum_spans[:, :, span][..., None]), 0.0
                    )
                    rounded = softmax_rows.astype(jnp.bfloat16)
                    weight_grad = jnp.einsum(
                        "rkgd,skd->kgrs",
                        grad_spans[span],
                        value_block[part],
                        preferred_element_type=jnp.float32,
                    )
                    score_grad = (
                        softmax_rows * (weight_grad - inner_spans[:, :, span][..., None])
                    ).astype(jnp.bfloat16)
                    query_grad = (
                        query_grad
                        + jnp.einsum(
                            "kgrs,skd->rkgd",
                            score_grad,
                            key_block[part],
                            preferred_element_type=jnp.float32,
                        )
                        * scaling
                    )
                    key_grad = (
                        key_grad
                        + jnp.einsum(
                            "kgrs,rkgd->skd",
                            score_grad,
                            query_spans[span],
                            preferred_element_type=jnp.float32,
                        )
                        * scaling
                    )
                    value_grad = value_grad + jnp.einsum(
                        "kgrs,rkgd->skd",
                        rounded,
                        grad_spans[span],
                        preferred_element_type=jnp.float32,
                    )
                    return (query_grad, key_grad, value_grad)

                state = (query_grads[span], key_acc, value_acc)
                state = lax.cond(
                    reachable(place_block[part], place_spans[span]),
                    live,
                    lambda current: current,
                    state,
                )
                query_grads[span], key_acc, value_acc = state
            key_parts.append(key_acc)
            value_parts.append(value_acc)
        key_out = jnp.concatenate(key_parts, axis=0)
        value_out = jnp.concatenate(value_parts, axis=0)
        return (tuple(query_grads), (key_out, value_out))

    start_grad = jnp.zeros((half, KV_HEADS, groups, HEAD_DIM), jnp.float32)
    query_pair, (key_grads, value_grads) = lax.scan(
        sweep_back, (start_grad, start_grad), (key_blocks, value_blocks, place_blocks)
    )
    query_grad = jnp.concatenate([query_pair[0], query_pair[1]], axis=0)
    return (
        query_grad,
        key_grads.reshape(-1, KV_HEADS, HEAD_DIM),
        value_grads.reshape(-1, KV_HEADS, HEAD_DIM),
    )


def fetch_layer(qkv_weight, out_weight, gate_up_weight, down_weight, attn_gain, ffn_gain, layer_id):
    return (
        lax.all_gather(qkv_weight[layer_id], "fsdp", axis=0, tiled=True),
        lax.all_gather(out_weight[layer_id], "fsdp", axis=0, tiled=True),
        lax.all_gather(gate_up_weight[layer_id], "fsdp", axis=0, tiled=True),
        lax.all_gather(down_weight[layer_id], "fsdp", axis=0, tiled=True),
        lax.all_gather(attn_gain[layer_id], "fsdp", axis=0, tiled=True),
        lax.all_gather(ffn_gain[layer_id], "fsdp", axis=0, tiled=True),
    )


def fetch_again(qkv_weight, out_weight, gate_up_weight, down_weight, attn_gain, ffn_gain, layer_id):
    return (
        lax.all_gather(qkv_weight[layer_id], "fsdp", axis=0, tiled=True),
        lax.all_gather(out_weight[layer_id], "fsdp", axis=0, tiled=True),
        lax.all_gather(gate_up_weight[layer_id], "fsdp", axis=0, tiled=True),
        lax.all_gather(down_weight[layer_id], "fsdp", axis=0, tiled=True),
        lax.all_gather(attn_gain[layer_id], "fsdp", axis=0, tiled=True),
        lax.all_gather(ffn_gain[layer_id], "fsdp", axis=0, tiled=True),
    )


def forward_layer(stream, query_place, key_place, gathered):
    qkv_full, out_full, gate_up_full, down_full, attn_full, ffn_full = gathered
    rows = stream.shape[0]
    groups = HEADS // KV_HEADS
    query_width = HEADS * HEAD_DIM
    key_width = KV_HEADS * HEAD_DIM
    cosine, sine = angles(query_place)
    normed, first_factor = normalize(stream, attn_full.astype(jnp.float32))
    normed = normed.astype(jnp.bfloat16)
    projected = jnp.dot(normed, qkv_full, preferred_element_type=jnp.float32)
    queries = rotate(projected[:, :query_width].reshape(rows, HEADS, HEAD_DIM), cosine, sine)
    queries = queries.reshape(rows, KV_HEADS, groups, HEAD_DIM).astype(jnp.bfloat16)
    keys_local = rotate(
        projected[:, query_width : query_width + key_width].reshape(rows, KV_HEADS, HEAD_DIM),
        cosine,
        sine,
    ).astype(jnp.bfloat16)
    values_local = (
        projected[:, query_width + key_width :]
        .reshape(rows, KV_HEADS, HEAD_DIM)
        .astype(jnp.bfloat16)
    )
    keys_all, values_all = (
        lax.all_gather(keys_local, "ctx", axis=0, tiled=True),
        lax.all_gather(values_local, "ctx", axis=0, tiled=True),
    )
    logsum, attended = attention_forward(queries, keys_all, values_all, query_place, key_place)
    attended_low = attended.reshape(rows, query_width).astype(jnp.bfloat16)
    middle = stream + jnp.dot(attended_low, out_full, preferred_element_type=jnp.float32)
    second, second_factor = normalize(middle, ffn_full.astype(jnp.float32))
    second = second.astype(jnp.bfloat16)
    gate_up = jnp.einsum("rd,dcf->rcf", second, gate_up_full, preferred_element_type=jnp.float32)
    hidden = (jax.nn.silu(gate_up[:, 0]) * gate_up[:, 1]).astype(jnp.bfloat16)
    result = middle + jnp.dot(hidden, down_full, preferred_element_type=jnp.float32)
    stored = (
        stream,
        first_factor,
        normed,
        queries,
        keys_local,
        values_local,
        keys_all,
        values_all,
        logsum,
        attended,
        attended_low,
        middle,
        second_factor,
        second,
        gate_up,
        hidden,
    )
    return (result, stored)


def backward_layer(upstream, stored, gathered, query_place, key_place, keys_all, values_all):
    (
        stream,
        first_factor,
        normed,
        queries,
        keys_local,
        values_local,
        kept_keys,
        kept_values,
        logsum,
        attended,
        attended_low,
        middle,
        second_factor,
        second,
        gate_up,
        hidden,
    ) = stored
    qkv_full, out_full, gate_up_full, down_full, attn_full, ffn_full = gathered
    rows = stream.shape[0]
    groups = HEADS // KV_HEADS
    cosine, sine = angles(query_place)
    upstream_low = upstream.astype(jnp.bfloat16)
    hidden_grad = jnp.einsum(
        "rd,fd->rf", upstream_low, down_full, preferred_element_type=jnp.float32
    )
    gate_part = gate_up[:, 0]
    up_part = gate_up[:, 1]
    sigmoid = jax.nn.sigmoid(gate_part)
    gate_grad = hidden_grad * up_part * sigmoid * (1.0 + gate_part * (1.0 - sigmoid))
    up_grad = hidden_grad * gate_part * sigmoid
    gate_up_low = jnp.stack([gate_grad, up_grad], axis=1).astype(jnp.bfloat16)
    second_grad = jnp.einsum(
        "rcf,dcf->rd", gate_up_low, gate_up_full, preferred_element_type=jnp.float32
    )
    middle_grad, ffn_gain_grad = normalize_back(
        second_grad, middle, second_factor, ffn_full.astype(jnp.float32)
    )
    middle_grad = middle_grad + upstream
    middle_low = middle_grad.astype(jnp.bfloat16)
    attended_grad = jnp.einsum(
        "rd,od->ro", middle_low, out_full, preferred_element_type=jnp.float32
    )
    attended_grad = attended_grad.astype(jnp.bfloat16).reshape(rows, KV_HEADS, groups, HEAD_DIM)
    row_inner = jnp.einsum("rkgd,rkgd->kgr", attended_grad.astype(jnp.float32), attended)
    query_grad, key_grads, value_grads = attention_backward(
        queries, keys_all, values_all, query_place, key_place, logsum, attended_grad, row_inner
    )
    key_grad, value_grad = (
        lax.psum_scatter(key_grads, "ctx", scatter_dimension=0, tiled=True),
        lax.psum_scatter(value_grads, "ctx", scatter_dimension=0, tiled=True),
    )
    query_grad = rotate_back(query_grad.reshape(rows, HEADS, HEAD_DIM), cosine, sine)
    key_grad = rotate_back(key_grad, cosine, sine)
    projected_grad = jnp.concatenate(
        [query_grad.reshape(rows, -1), key_grad.reshape(rows, -1), value_grad.reshape(rows, -1)],
        axis=1,
    ).astype(jnp.bfloat16)
    normed_grad = jnp.einsum(
        "re,de->rd", projected_grad, qkv_full, preferred_element_type=jnp.float32
    )
    stream_grad, attn_gain_grad = normalize_back(
        normed_grad, stream, first_factor, attn_full.astype(jnp.float32)
    )
    stream_grad = stream_grad + middle_grad
    qkv_grad = jnp.einsum("rd,re->de", normed, projected_grad, preferred_element_type=jnp.float32)
    out_grad = jnp.einsum("ro,rd->od", attended_low, middle_low, preferred_element_type=jnp.float32)
    gate_up_grad = jnp.einsum(
        "rd,rcf->dcf", second, gate_up_low, preferred_element_type=jnp.float32
    )
    down_grad = jnp.einsum("rf,rd->fd", hidden, upstream_low, preferred_element_type=jnp.float32)
    sharded = (
        lax.psum_scatter(qkv_grad, "fsdp", scatter_dimension=0, tiled=True),
        lax.psum_scatter(out_grad, "fsdp", scatter_dimension=0, tiled=True),
        lax.psum_scatter(gate_up_grad, "fsdp", scatter_dimension=0, tiled=True),
        lax.psum_scatter(down_grad, "fsdp", scatter_dimension=0, tiled=True),
        lax.psum_scatter(attn_gain_grad, "fsdp", scatter_dimension=0, tiled=True),
        lax.psum_scatter(ffn_gain_grad, "fsdp", scatter_dimension=0, tiled=True),
    )
    totals = lax.psum(
        (sharded[0], sharded[1], sharded[2], sharded[3], sharded[4], sharded[5]), "ctx"
    )
    return (stream_grad, totals)


def body(
    tokens,
    positions,
    qkv_weight,
    out_weight,
    gate_up_weight,
    down_weight,
    attn_gain,
    ffn_gain,
    cotangent,
):
    query_place = positions[0]
    key_place = lax.all_gather(query_place, "ctx", axis=0, tiled=True)
    stream = tokens[0].astype(jnp.float32)
    gathered_list = []
    layer_id = 0
    gathered = fetch_layer(
        qkv_weight, out_weight, gate_up_weight, down_weight, attn_gain, ffn_gain, layer_id
    )
    stream, stored = forward_layer(stream, query_place, key_place, gathered)
    saved = [stored]
    gathered_list.append(gathered)
    activations = stream.astype(jnp.bfloat16)[None]
    upstream = cotangent[0]
    layer_grads = [None] * LAYERS
    for layer_id in reversed(range(LAYERS)):
        stored = saved[layer_id]
        gathered = fetch_again(
            qkv_weight, out_weight, gate_up_weight, down_weight, attn_gain, ffn_gain, layer_id
        )
        keys_all, values_all = (stored[6], stored[7])
        upstream, totals = backward_layer(
            upstream, stored, gathered, query_place, key_place, keys_all, values_all
        )
        layer_grads[layer_id] = totals
    outputs = [jnp.stack([entry[slot] for entry in layer_grads], axis=0) for slot in range(6)]
    return (
        activations,
        upstream[None],
        outputs[0],
        outputs[1],
        outputs[2],
        outputs[3],
        outputs[4],
        outputs[5],
    )


LANES = 128


def spread(heads):
    half = HEAD_DIM // 2
    pad = ((0, 0), (0, 0), (0, 64 - half))
    return jnp.concatenate([jnp.pad(heads[..., :half], pad), jnp.pad(heads[..., half:], pad)], axis=-1)


def gathered_spread(padded):
    half = HEAD_DIM // 2
    return jnp.concatenate([padded[..., :half], padded[..., 64 : 64 + half]], axis=-1)


def turn_parts(spans, rows):
    half = HEAD_DIM // 2
    frequency = rope_base ** (-(np.arange(half, dtype=np.float64) * 2.0 / HEAD_DIM))

    def waves(place):
        phases = place[:, None] * frequency[None, :]
        pad = ((0, 0), (0, 64 - half))
        return np.pad(np.cos(phases), pad), np.pad(np.sin(phases), pad)

    cosine, sine = waves(np.arange(spans) * float(rows))
    parts = (
        np.concatenate([cosine, cosine], axis=1), np.concatenate([-sine, sine], axis=1),
        np.concatenate(waves(np.arange(rows, dtype=np.float64)), axis=1),
    )
    return tuple(jnp.asarray(part, jnp.float32) for part in parts)


def spread_heads(proj):
    lane = lax.broadcasted_iota(jnp.int32, (proj.shape[0], LANES), 1)
    tiles = [proj[:, at * LANES : (at + 1) * LANES] for at in range(3)]

    def put(*pieces):
        out = jnp.zeros_like(tiles[0])
        for tile, source, target, count in pieces:
            shift = (target - source) % LANES
            moved = pltpu.roll(tiles[tile], shift, 1) if shift else tiles[tile]
            out = jnp.where(jnp.logical_and(lane >= target, lane < target + count), moved, out)
        return out

    return (
        put((0, 0, 0, 48), (0, 48, 64, 48)),
        put((0, 96, 0, 32), (1, 0, 32, 16), (1, 16, 64, 48)),
        put((1, 64, 0, 48), (1, 112, 64, 16), (2, 0, 80, 32)),
        put((2, 32, 0, 96)),
    )


def close_halves(head):
    lane = lax.broadcasted_iota(jnp.int32, head.shape, 1)
    return jnp.where(lane < HEAD_DIM // 2, head, pltpu.roll(head, LANES - 64 + HEAD_DIM // 2, 1))


def wave(rows):
    first = lax.broadcasted_iota(jnp.int32, rows.shape, 1) < 64
    other = pltpu.roll(rows, 64, 1)
    return jnp.where(first, rows, other), jnp.where(first, -other, rows)


def nt(left, right):
    return lax.dot_general(left, right, (((1,), (1,)), ((), ())), preferred_element_type=jnp.float32)


def nn(left, right):
    return lax.dot_general(left, right, (((1,), (0,)), ((), ())), preferred_element_type=jnp.float32)


def tn(left, right):
    return lax.dot_general(left, right, (((0,), (0,)), ((), ())), preferred_element_type=jnp.float32)


def causal(width, place):
    key_at = lax.broadcasted_iota(jnp.int32, (2 * width, 2 * width), 0)
    query_at = lax.broadcasted_iota(jnp.int32, (2 * width, 2 * width), 1)
    query_at = jnp.where(query_at >= width, query_at - width, query_at)
    return key_at <= query_at + place * width


def vm(count):
    return [pl.BlockSpec(memory_space=pltpu.VMEM)] * count


MESH = pl.DeviceIdType.MESH


class Place:
    def __init__(self):
        self.me = lax.axis_index("ctx")
        core, x, y = self.me % 2, (self.me // 2) % 2, self.me // 4
        self.dp, self.dx, self.dy = 1 - 2 * core, 2 - 4 * x, 4 - 8 * y
        self.p, self.x, self.y = self.me + self.dp, self.me + self.dx, self.me + self.dy
        self.d = self.x + self.dy
        self.z = lax.axis_index("fsdp")
        self.planes = lax.axis_size("fsdp")
        self.n = lax.axis_size("ctx")


def greet(place, ctx=True, planes=False):
    barrier = pltpu.get_barrier_semaphore()
    count = 0
    if ctx:
        for step in range(1, place.n):
            pl.semaphore_signal(
                barrier, inc=1, device_id={"ctx": lax.rem(place.me + step, place.n)}, device_id_type=MESH
            )
            count += 1
    if planes:
        for step in range(1, place.planes):
            pl.semaphore_signal(
                barrier, inc=1, device_id={"fsdp": lax.rem(place.z + step, place.planes)}, device_id_type=MESH
            )
            count += 1
    pl.semaphore_wait(barrier, count)


def send(source, target, send_sem, recv_sem, **where):
    return pltpu.make_async_remote_copy(
        src_ref=source, dst_ref=target, send_sem=send_sem, recv_sem=recv_sem,
        device_id=where, device_id_type=MESH,
    )


class Gather:
    sems = 14

    def __init__(self, place, own, out, sem):
        self.place, self.own, self.out, self.sem = place, own, out, sem
        self.half = out.shape[1] // 2
        self.started = []
        self.met = False

    def go(self, source, target, index, rank):
        send(source, target, self.sem.at[0, index], self.sem.at[1, index], ctx=rank).start()
        self.started.append(index)

    def whole_block(self, index):
        return index == 6

    def sent(self):
        p = self.place
        for index in self.started:
            part = self.whole(p.me) if self.whole_block(index) else self.part(p.me, 0)
            send(part, part, self.sem.at[0, index], self.sem.at[1, index], ctx=p.p).wait_send()

    def part(self, rank, half):
        return self.out.at[rank, pl.ds(half * self.half, self.half)]

    def whole(self, rank):
        return self.out.at[rank]

    def start(self):
        p = self.place
        keep = pltpu.make_async_copy(self.own, self.whole(p.me), self.sem.at[0, 13])
        keep.start()
        self.keep = keep
        halves = [self.own.at[pl.ds(h * self.half, self.half)] for h in range(2)]
        self.go(halves[0], self.part(p.me, 0), 0, p.x)
        self.go(halves[1], self.part(p.me, 1), 3, p.y)
        self.go(self.own, self.whole(p.me), 6, p.p)
        self.go(halves[1], self.part(p.me, 1), 1, p.x)
        self.go(halves[0], self.part(p.me, 0), 2, p.y)

    def arrived(self, rank, half, index):
        part = self.part(rank, half)
        pltpu.make_async_copy(part, part, self.sem.at[1, index]).wait()
        return part

    def relay(self):
        p = self.place
        part = self.arrived(p.x, 0, 0)
        self.go(part, part, 4, p.y)
        self.go(part, part, 7, p.p)
        part = self.arrived(p.y, 1, 3)
        self.go(part, part, 5, p.x)
        self.go(part, part, 10, p.p)

    def rest(self):
        p = self.place
        for rank, half, index, onward in ((p.x, 1, 1, 8), (p.y, 0, 2, 9), (p.d, 0, 4, 11), (p.d, 1, 5, 12)):
            part = self.arrived(rank, half, index)
            self.go(part, part, onward, p.p)

    def first_partner(self):
        part = self.whole(self.place.p)
        pltpu.make_async_copy(part, part, self.sem.at[1, 6]).wait()
        self.met = True

    def partner(self):
        p = self.place
        if not self.met:
            self.first_partner()
        for rank, half, index in (
            (p.x, 0, 7), (p.y, 1, 10), (p.x, 1, 8), (p.y, 0, 9), (p.d, 0, 11), (p.d, 1, 12),
        ):
            self.arrived(rank + p.dp, half, index)

    def finish(self, kept=False):
        if not kept:
            self.keep.wait()
        self.sent()


class PlaneGather:
    def __init__(self, place, own, out, sem):
        self.place, self.own, self.out, self.sem = place, own, out, sem

    def hop(self, step, up):
        p = self.place
        sign = 1 if up else -1
        source = p.z - sign * step
        target = p.z + sign
        ok = jnp.logical_and(
            jnp.logical_and(source >= 0, source < p.planes),
            jnp.logical_and(target >= 0, target < p.planes),
        )
        source = jnp.clip(source, 0, p.planes - 1)
        target = jnp.clip(target, 0, p.planes - 1)
        block = self.own if step == 0 else self.out.at[source]
        return ok, send(
            block, self.out.at[source], self.sem.at[0 if up else 1, source], self.sem.at[2, source], fsdp=target
        )

    def start(self):
        p = self.place
        self.keep = pltpu.make_async_copy(self.own, self.out.at[p.z], self.sem.at[2, p.z])
        self.keep.start()
        for up in (True, False):
            ok, copy = self.hop(0, up)
            pl.when(ok)(copy.start)

    def got(self, step, up):
        p = self.place
        source = p.z - step if up else p.z + step
        ok = jnp.logical_and(source >= 0, source < p.planes)
        source = jnp.clip(source, 0, p.planes - 1)
        part = self.out.at[source]
        return ok, pltpu.make_async_copy(part, part, self.sem.at[2, source])

    def step(self, number):
        for up in (True, False):
            ok, copy = self.got(number, up)
            pl.when(ok)(copy.wait)
            if number < self.place.planes - 1:
                ok, copy = self.hop(number, up)
                pl.when(ok)(copy.start)

    def finish(self, kept=False):
        if not kept:
            self.keep.wait()
        for number in range(self.place.planes - 1):
            for up in (True, False):
                ok, copy = self.hop(number, up)
                pl.when(ok)(copy.wait_send)


class Exchange:
    def __init__(self, place, blocks, out, sem):
        self.place, self.blocks, self.out, self.sem = place, blocks, out, sem

    def pick(self, rank):
        return self.blocks.at[rank]

    def copy(self, step):
        p = self.place
        rank = lax.rem(p.me + step, p.n)
        return send(self.pick(rank), self.out.at[p.me], self.sem.at[0, step], self.sem.at[1, step], ctx=rank)

    def start(self):
        p = self.place
        for step in range(1, p.n):
            self.copy(step).start()
        self.keep = pltpu.make_async_copy(self.pick(p.me), self.out.at[p.me], self.sem.at[0, 0])
        self.keep.start()

    def finish(self):
        p = self.place
        self.keep.wait()
        for step in range(1, p.n):
            self.copy(step).wait_send()
        for step in range(1, p.n):
            part = self.out.at[lax.rem(p.me + p.n - step, p.n)]
            pltpu.make_async_copy(part, part, self.sem.at[1, step]).wait()


class Share(Exchange):
    def pick(self, rank):
        return self.blocks


class PlaneShare:
    def __init__(self, place, block, out, sem):
        self.place, self.block, self.out, self.sem = place, block, out, sem

    def copy(self, step):
        p = self.place
        plane = lax.rem(p.z + step, p.planes)
        return send(self.block, self.out.at[p.z], self.sem.at[0, step], self.sem.at[1, step], fsdp=plane)

    def start(self):
        p = self.place
        for step in range(1, p.planes):
            self.copy(step).start()
        self.keep = pltpu.make_async_copy(self.block, self.out.at[p.z], self.sem.at[0, 0])
        self.keep.start()

    def finish(self):
        p = self.place
        self.keep.wait()
        for step in range(1, p.planes):
            self.copy(step).wait_send()
        for step in range(1, p.planes):
            part = self.out.at[lax.rem(p.z + p.planes - step, p.planes)]
            pltpu.make_async_copy(part, part, self.sem.at[1, step]).wait()


def anywhere(count):
    return [pl.BlockSpec(memory_space=pl.ANY)] * count


class Reduce:
    sems = 10

    def __init__(self, place, mine, theirs, first, out, second, sem):
        self.place, self.mine, self.theirs, self.first, self.out, self.second, self.sem = (
            place, mine, theirs, first, out, second, sem
        )
        self.half = out.shape[1]
        self.started = []

    def push(self, slot):
        copy = send(
            self.theirs.at[slot], self.first.at[slot], self.sem.at[0, slot], self.sem.at[1, slot], ctx=self.place.p
        )
        copy.start()
        return copy

    def pushed(self):
        for slot in range(4):
            send(
                self.theirs.at[slot], self.first.at[slot], self.sem.at[0, slot], self.sem.at[1, slot],
                ctx=self.place.p,
            ).wait_send()

    def add(self, slot):
        part = self.first.at[slot]
        pltpu.make_async_copy(part, part, self.sem.at[1, slot]).wait()
        self.mine[slot] = self.mine[slot] + self.first[slot].astype(jnp.float32)

    def go(self, index, value, rank):
        self.out[index] = value.astype(jnp.bfloat16)
        self.turned(index, rank).start()
        self.started.append((index, rank))

    def turned(self, index, rank):
        return send(
            self.out.at[index], self.second.at[index], self.sem.at[0, 4 + index], self.sem.at[1, 4 + index], ctx=rank
        )

    def top(self, slot):
        return self.mine[slot, pl.ds(0, self.half), :]

    def low(self, slot):
        return self.mine[slot, pl.ds(self.half, self.half), :]

    def got(self, index):
        part = self.second.at[index]
        pltpu.make_async_copy(part, part, self.sem.at[1, 4 + index]).wait()
        return self.second[index].astype(jnp.float32)

    def across(self):
        self.add(3)
        self.go(1, self.top(3), self.place.x)
        self.go(3, self.low(3), self.place.y)

    def beside(self):
        self.add(1)
        self.go(0, self.top(1), self.place.x)
        self.add(2)
        self.go(2, self.low(2), self.place.y)

    def turn(self):
        self.go(4, self.top(2) + self.got(1), self.place.y)
        self.go(5, self.low(1) + self.got(3), self.place.x)

    def total(self, use):
        self.add(0)
        use(pl.ds(0, self.half), self.top(0) + self.got(0) + self.got(4))
        use(pl.ds(self.half, self.half), self.low(0) + self.got(2) + self.got(5))

    def finish(self):
        self.pushed()
        for index, rank in self.started:
            self.turned(index, rank).wait_send()


def flip(place, i):
    return place.me + (i % 2) * place.dp + ((i // 2) % 2) * place.dx + (i // 4) * place.dy


class HalfGather(Gather):
    sems = 16

    def __init__(self, place, own, out, sem):
        self.place, self.own, self.out, self.sem = place, own, out, sem
        self.half = out.shape[1]
        self.started = []
        self.met = False

    def part(self, rank, half):
        return self.out.at[2 * rank + half]

    def whole_block(self, index):
        return False

    def start(self):
        p = self.place
        halves = [self.own.at[pl.ds(h * self.half, self.half)] for h in range(2)]
        self.kept = [
            pltpu.make_async_copy(halves[h], self.part(p.me, h), self.sem.at[0, (13, 15)[h]]) for h in range(2)
        ]
        self.go(halves[0], self.part(p.me, 0), 0, p.x)
        self.go(halves[1], self.part(p.me, 1), 3, p.y)
        self.go(halves[0], self.part(p.me, 0), 6, p.p)
        self.go(halves[1], self.part(p.me, 1), 14, p.p)
        self.go(halves[1], self.part(p.me, 1), 1, p.x)
        self.go(halves[0], self.part(p.me, 0), 2, p.y)
        for copy in self.kept:
            copy.start()

    def first_partner(self):
        for h in range(2):
            self.arrived(self.place.p, h, (6, 14)[h])
        self.met = True

    def own_in(self):
        for copy in self.kept:
            copy.wait()

    def finish(self):
        self.sent()


def packed(block):
    rows = block.shape[0] // 2
    tail = jnp.concatenate([block[:, LANES:], jnp.zeros((2 * rows, 64), block.dtype)], axis=1)
    first = lax.broadcasted_iota(jnp.int32, (rows, LANES), 1) < 64
    return jnp.concatenate([block[:, :LANES], jnp.where(first, tail[:rows], pltpu.roll(tail[rows:], 64, 1))], axis=0)


def unpacked(block):
    rows = block.shape[0] // 3
    tail = block[2 * rows :].astype(jnp.float32)
    tails = jnp.concatenate([tail, pltpu.roll(tail, 64, 1)], axis=0)[:, :64].astype(block.dtype)
    return jnp.concatenate([block[: 2 * rows], tails], axis=1)


class PlaneReduce:
    def __init__(self, place, block, recv, sem):
        self.place, self.block, self.recv, self.sem = place, block, recv, sem

    def hop(self, ok, part, slot, target, first, wait):
        copy = send(
            self.block.at[part], self.recv.at[slot], self.sem.at[0, part], self.sem.at[1, slot], fsdp=target
        )

        @pl.when(ok)
        def _():
            if wait:
                copy.wait_send()
                return
            if not first:
                self.merge(part, part)
            copy.start()

    def merge(self, part, slot):
        piece = self.recv.at[slot]
        pltpu.make_async_copy(piece, piece, self.sem.at[1, slot]).wait()
        total = self.block[part].astype(jnp.float32) + self.recv[slot].astype(jnp.float32)
        self.block[part] = total.astype(jnp.bfloat16)

    def ends(self, i, wait=False):
        z = self.place.z
        low = z == 0
        part = jnp.where(low, 3 - i, i)
        slot = part if i < 2 else jnp.where(low, part, 4)
        self.hop(jnp.logical_or(low, z == 3), part, slot, jnp.where(low, 1, 2), True, wait)

    def inner(self, up, down, slot_up, slot_down, to_up, to_down, wait=False):
        z = self.place.z
        low = z == 1
        part = jnp.where(low, up, down)
        slot = jnp.where(low, slot_up, slot_down)
        self.hop(jnp.logical_or(low, z == 2), part, slot, jnp.where(low, to_up, to_down), False, wait)

    def start(self, wait=False):
        for i in range(3):
            self.ends(i, wait)

    def step1(self, wait=False):
        self.inner(3, 0, 3, 0, 2, 1, wait)

    def step2(self, wait=False):
        self.inner(2, 1, 2, 4, 2, 1, wait)
        self.inner(0, 3, 4, 3, 0, 3, wait)

    def total(self):
        z = self.place.z

        @pl.when(z > 0)
        def _():
            self.merge(z, z)

        @pl.when(z < 3)
        def _():
            self.merge(z, 4)

    def own(self):
        return self.block.at[self.place.z]

    def finish(self):
        self.start(True)
        self.step1(True)
        self.step2(True)


class Steps:
    def __init__(self, *steps):
        self.steps = list(steps)

    def next(self, count=1):
        for step in self.steps[:count]:
            step()
        self.steps = self.steps[count:]

    def rest(self):
        self.next(len(self.steps))


class OutGather(Gather):
    def __init__(self, place, own, out, sem):
        self.place, self.own, self.out, self.sem = place, own, out, sem
        self.half = out.shape[0] // 2
        self.started = []
        self.met = False

    def part(self, rank, half):
        return self.out.at[pl.ds(half * self.half, self.half), rank]

    def whole(self, rank):
        return self.out.at[:, rank]


def front_kernel(
    tok, pos, attn_own, ffn_own, qkv_own, gu_own, far_cos, far_sin, near, out_weight, down_weight, up,
    middle_grad, gain_grad, spots, gains, down_sum,
    hidden_o, qkv_o, down_o, q_o, k_o, v_o, att_o, lse_o, middle_o, turn_o, normed, agrad, low_all, gu_out, mcols,
    hidden, qkv_w, down_w, q_ref, k_ref, v_ref, att_ref, lse_ref, middle, turn_ref, mcols_send, up_low, spot, gain_own,
    wide_in, up_all, gul, gu_w, out_block, out_w, low_sorted, gain_all, spots_s, order_s, low,
    attended, own, mine, theirs, first, out, second, down_g, down_r,
    tok_sem, up_sem, spot_sem, gain_sem, qkv_sem, out_sem, outc_sem, gu_sem, down_sem, local_sem,
    low_sem, gather_sem, reduce_sem, agrad_sem, lows_sem, down_zs, mcols_sem,
):
    place = Place()
    n = place.n
    rows = tok.shape[0]
    half = rows // 2
    pairs = 8
    heads = rows
    length = n * rows
    width = tok.shape[1]
    out_own = out_weight.at[0, pl.ds(place.me * (out_weight.shape[1] // 8), out_weight.shape[1] // 8)]
    down_own = down_weight.at[0, pl.ds(place.me * (down_weight.shape[1] // 8), down_weight.shape[1] // 8)]
    spot[...] = jnp.broadcast_to(pos[0:1, 0:1], spot.shape)
    gain_own[pl.ds(0, 1), :] = attn_own[...].astype(jnp.float32)
    gain_own[pl.ds(1, 1), :] = ffn_own[...].astype(jnp.float32)
    fetch = pltpu.make_async_copy(up, middle_grad, local_sem.at[0])
    fetch.start()
    greet(place, planes=True)
    spans = Share(place, spot, spots, spot_sem)
    scales = PlaneShare(place, gain_own, gain_all, gain_sem)
    tokens = HalfGather(place, tok, wide_in, tok_sem)
    cots = Gather(place, up_low, up_all, up_sem)
    qkvs = PlaneGather(place, qkv_own, qkv_w, qkv_sem)
    outs = PlaneGather(place, out_own, out_block, out_sem)
    outc = OutGather(place, out_block, out_w, outc_sem)
    gus = PlaneGather(place, gu_own, gu_w, gu_sem)
    downs = PlaneGather(place, down_own, down_w, down_sem)
    given = []

    def give(source, target):
        copy = pltpu.make_async_copy(source, target, local_sem.at[5 + len(given)])
        copy.start()
        given.append(copy)

    tokens.start()
    qkvs.start()
    spans.start()
    scales.start()

    def turn_rows(at, carry):
        base = near[...]
        turn_ref[at] = base * far_cos[pl.ds(at, 1), :] + pltpu.roll(base, 64, 1) * far_sin[pl.ds(at, 1), :]
        return carry

    lax.fori_loop(0, 2 * pairs, turn_rows, 0)
    give(turn_ref, turn_o)
    fetch.wait()
    up_low[...] = middle_grad[...].astype(jnp.bfloat16)
    tokens.relay()
    qkvs.step(1)
    outs.start()
    qkvs.step(2)
    tokens.rest()
    cots.start()
    outs.step(1)
    downs.start()
    qkvs.step(3)
    tokens.partner()
    tokens.own_in()
    spans.finish()
    scales.finish()
    qkvs.keep.wait()
    table = pltpu.make_async_copy(spots, spots_s, local_sem.at[1])
    table.start()
    for g in range(2):
        gains[pl.ds(g, 1), :] = jnp.concatenate([gain_all[z, pl.ds(g, 1), :] for z in range(4)], axis=1)
    table.wait()
    early = [lax.div(spots_s[j, 0, 0], half) for j in range(pairs)]
    for t in range(pairs):
        at = 0
        for j in range(pairs):
            at = jnp.where(early[j] == t, j, at)
        order_s[t] = 2 * at
        order_s[2 * pairs - 1 - t] = 2 * at + 1
    cots.relay()

    def project(j, store):
        x = jnp.concatenate([wide_in[order_s[4 * j + i]] for i in range(4)], axis=0).astype(jnp.float32)
        factor = lax.rsqrt(jnp.mean(x * x, axis=-1, keepdims=True) + epsilon)
        scaled = (x * factor * gains[pl.ds(0, 1), :]).astype(jnp.bfloat16)
        store[pl.ds(2 * (j % 2), 2)] = scaled.reshape(2, rows, -1)
        proj = nn(scaled, qkv_w[...].reshape(-1, 3 * LANES))
        spread = spread_heads(proj)
        for piece in range(4):
            at = 4 * j + piece
            cosine, sine = wave(turn_ref[at])

            def turned(part):
                z = spread[part][piece * half : (piece + 1) * half]
                return (z * cosine + pltpu.roll(z, 64, 1) * sine).astype(jnp.bfloat16)

            base = (2 * j + piece // 2) * 4 * half + (piece % 2) * half
            q_ref[pl.ds(pl.multiple_of(base, half), half), :] = turned(0)
            q_ref[pl.ds(pl.multiple_of(base + 2 * half, half), half), :] = turned(1)
            k_ref[pl.ds(pl.multiple_of(at * half, half), half), :] = turned(2)
            v_ref[pl.ds(pl.multiple_of(at * half, half), half), :] = spread[3][piece * half : (piece + 1) * half].astype(jnp.bfloat16)

    def project_first(j, carry):
        project(j, theirs)
        return carry

    def project_second(j, carry):
        project(j, first)
        return carry

    lax.fori_loop(0, 2, project_first, 0)
    keep_first = pltpu.make_async_copy(theirs.at[pl.ds(0, 4)], normed.at[pl.ds(0, 4)], local_sem.at[2])
    keep_first.start()
    lax.fori_loop(2, 4, project_second, 0)
    keep_second = pltpu.make_async_copy(first, normed.at[pl.ds(4, 4)], local_sem.at[3])
    keep_second.start()
    give(q_ref, q_o)
    give(k_ref, k_o)
    give(v_ref, v_o)
    give(qkv_w, qkv_o)
    tokens.finish()
    outs.step(2)
    cots.rest()
    outs.step(3)
    outs.keep.wait()
    outc.start()

    def next_weights():
        downs.step(1)
        gus.start()

    steps = Steps(next_weights, lambda: None, outc.relay, lambda: downs.step(2))
    scaling = HEAD_DIM ** (-0.5)
    lane = lax.broadcasted_iota(jnp.int32, (half, LANES), 1)
    values_t = v_ref[...].astype(jnp.float32).T.astype(jnp.bfloat16)
    def attend_group(group):
        before = group * 4 * half

        def attend(place_of, carry):
            pair = 2 * group + place_of
            q = q_ref[pl.ds(pl.multiple_of(pair * 4 * half, 4 * half), 4 * half), :]
            scores = nt(k_ref[pl.ds(before, 4 * half), :], q) * scaling
            parts = [jnp.where(causal(2 * half, place_of), scores, -1e30)]
            if group:
                parts.append(nt(k_ref[pl.ds(0, before), :], q) * scaling)
            tops = [jnp.max(part, axis=0, keepdims=True) for part in parts]
            top = jnp.maximum(tops[0], tops[-1])
            parts = [jnp.exp(part - top) for part in parts]
            total = sum(jnp.sum(part, axis=0, keepdims=True) for part in parts)
            parts = [(part * (1.0 / total)).astype(jnp.bfloat16) for part in parts]
            lse_ref[pl.ds(pair, 1), :] = top + jnp.log(total)
            out_t = nn(values_t[:, before : before + 4 * half], parts[0])
            if group:
                out_t = out_t + nn(values_t[:, :before], parts[1])
            att_ref[pl.ds(pl.multiple_of(pair * LANES, LANES), LANES), :] = out_t
            result = out_t.T.astype(jnp.bfloat16).astype(jnp.float32)
            for part in range(2):
                left = result[part * half : (part + 1) * half]
                right = pltpu.roll(result[(2 + part) * half : (3 + part) * half], half, 1)
                low_sorted[2 * pair + part, :, 0:LANES] = jnp.where(lane < half, left, right).astype(jnp.bfloat16)
                low_sorted[2 * pair + part, :, LANES:] = right.astype(jnp.bfloat16)
            return carry

        lax.fori_loop(0, 2, attend, 0)

    for group in range(pairs // 2):
        attend_group(group)
        steps.next()
    give(att_ref, att_o)
    give(lse_ref, lse_o)
    for j in range(pairs):
        upper = low_sorted[early[j]]
        lower = low_sorted[2 * pairs - 1 - early[j]]
        low[j, pl.ds(0, half), :] = upper[:, :LANES]
        low[j, pl.ds(half, half), :] = lower[:, :LANES]
        tails = jnp.where(
            lane < 64, upper[:, LANES:].astype(jnp.float32), pltpu.roll(lower[:, LANES:].astype(jnp.float32), 64, 1)
        )
        low[j, pl.ds(2 * half, half), :] = tails.astype(jnp.bfloat16)
    keep_first.wait()
    keep_second.wait()
    moved = Exchange(place, low, attended, low_sem)
    moved.start()
    outc.rest()
    outc.partner()
    cots.partner()
    outc.keep.wait()
    moved.finish()
    middle[...] = tok[...].astype(jnp.float32)

    def out_project(q, carry):
        middle[...] += nn(unpacked(attended[q]), out_w[q // 2, pl.ds(4 * (q % 2), 4)].reshape(heads, -1))
        return carry

    lax.fori_loop(0, n, out_project, 0)
    give(middle, middle_o)
    gus.step(1)
    total = middle[...]
    factor = lax.rsqrt(jnp.mean(total * total, axis=-1, keepdims=True) + epsilon)
    own[...] = (total * factor * gains[pl.ds(1, 1), :]).astype(jnp.bfloat16)
    seconds = HalfGather(place, own, wide_in, gather_sem)
    seconds.start()
    seconds.relay()
    gus.step(2)
    seconds.rest()
    lows = Gather(place, low, low_all, lows_sem)
    lows.start()
    seconds.partner()
    downs.step(3)
    downs.keep.wait()
    give(down_w, down_o)
    cots.keep.wait()
    seconds.own_in()

    def early_grad(i, carry):
        rank = flip(place, i)
        at = pl.multiple_of((i % 2) * hidden.shape[2], LANES)
        mine[i // 2, :, pl.ds(at, hidden.shape[2])] = nt(up_all[rank], down_w[...].reshape(hidden.shape[2], -1))
        return carry

    lax.fori_loop(0, n, early_grad, 0)
    gus.step(3)
    gus.keep.wait()
    grads = Reduce(place, mine, theirs, first, out, second, reduce_sem)
    wide = hidden.shape[2]

    def block(i):
        rank = flip(place, i)
        gate_up = nn(wide_in[pl.ds(2 * rank, 2)].reshape(rows, -1), gu_w[...].reshape(-1, 2 * wide))
        gate, raised = gate_up[:, :wide], gate_up[:, wide:]
        sigmoid = 1.0 / (1.0 + jnp.exp(-gate))
        silu = gate * sigmoid
        hidden[rank] = (silu * raised).astype(jnp.bfloat16)
        hidden_grad = mine[i // 2, :, pl.ds(pl.multiple_of((i % 2) * wide, LANES), wide)]
        gul[rank, :, pl.ds(0, wide)] = (hidden_grad * raised * sigmoid * (1.0 + gate * (1.0 - sigmoid))).astype(jnp.bfloat16)
        gul[rank, :, pl.ds(wide, wide)] = (hidden_grad * silu).astype(jnp.bfloat16)
        return nt(gul[rank], gu_w[...].reshape(-1, 2 * wide))

    def block_at(t, carry):
        k = lax.rem(t // 2 + 1, 4)
        value = block(2 * k + 1 - t % 2)

        odd = t % 2
        theirs[k * (1 - odd) + 4 * odd] = value.astype(jnp.bfloat16)
        mine[k * odd + 4 * (1 - odd)] = value

        @pl.when(t % 2 == 0)
        def _():
            grads.push(k)

        @pl.when(t == 2)
        def _():
            lows.relay()

        @pl.when(t == 4)
        def _():
            grads.beside()

        @pl.when(t == 5)
        def _():
            lows.rest()

        @pl.when(t == 6)
        def _():
            grads.across()

        return carry

    lax.fori_loop(0, 8, block_at, 0)
    give(hidden, hidden_o)
    down_z = PlaneReduce(place, down_g, down_r, down_zs)
    piece = down_g.shape[1]

    def down_block(t, carry):
        left = hidden[:, :, pl.ds(pl.multiple_of(t * piece, piece), piece)].reshape(length, piece)
        down_g[t] = tn(left, up_all[...].reshape(length, width)).astype(jnp.bfloat16)
        return carry

    lax.fori_loop(0, 4, down_block, 0)
    down_z.start()
    grads.turn()
    seconds.finish()
    gain_grad[...] = jnp.zeros_like(gain_grad)

    def norm_back(part, second_grad):
        x = middle[part, :]
        factor = lax.rsqrt(jnp.mean(x * x, axis=-1, keepdims=True) + epsilon)
        unit = x * factor
        gain_grad[...] += jnp.sum(second_grad * unit, axis=0, keepdims=True)
        scaled = second_grad * gains[pl.ds(1, 1), :]
        inner = jnp.mean(scaled * unit, axis=-1, keepdims=True)
        grad = middle_grad[part, :] + factor * (scaled - unit * inner)
        middle_grad[part, :] = grad
        own[part, :] = grad.astype(jnp.bfloat16)

    gus.finish(kept=True)
    shard = gu_w.shape[1]

    def gu_block(t, carry):
        left = wide_in[:, :, pl.ds(pl.multiple_of(t * shard, shard), shard)].reshape(length, shard)
        gu_w[t] = tn(left, gul[...].reshape(length, 2 * wide)).astype(jnp.bfloat16)
        return carry

    lax.fori_loop(0, 4, gu_block, 0)
    give(gu_w, gu_out)
    down_z.step1()
    grads.total(norm_back)

    def head_grads(q, carry):
        weight = out_w[q // 2, pl.ds(4 * (q % 2), 4)].reshape(heads, -1)
        attended[q] = packed(nt(own[...], weight)).astype(jnp.bfloat16)
        return carry

    lax.fori_loop(0, n, head_grads, 0)
    heads_back = Exchange(place, attended, agrad, agrad_sem)
    heads_back.start()
    for q in range(8):
        mcols_send[q] = packed(own[:, q * heads : (q + 1) * heads].astype(jnp.float32)).astype(jnp.bfloat16)
    columns = Exchange(place, mcols_send, mcols, mcols_sem)
    columns.start()
    down_z.step2()
    lows.partner()
    heads_back.finish()
    down_z.total()
    down_sum[...] = down_g[place.z]
    for move in (qkvs, outs, downs, cots, outc):
        move.finish(kept=True)
    lows.finish()
    columns.finish()
    for copy in given:
        copy.wait()
    grads.finish()
    down_z.finish()


def front_moves(tok, pos, attn_own, ffn_own, qkv_own, gu_own, far_cos, far_sin, near, out_weight, down_weight, up):
    n, planes = lax.axis_size("ctx"), lax.axis_size("fsdp")
    rows, width = tok.shape
    length = n * rows
    bf, f32 = jnp.bfloat16, jnp.float32
    shape = jax.ShapeDtypeStruct
    out_own = shape((out_weight.shape[1] // n, width), bf)
    down_own = shape((down_weight.shape[1] // n, width), bf)
    spot = shape((8, LANES), jnp.int32)
    gain_own = shape((8, attn_own.shape[1]), f32)
    wide = planes * down_own.shape[0]
    dma = pltpu.SemaphoreType.DMA
    pairs = length // 192
    halves = pltpu.VMEM((6, rows // 2, width), bf)
    quads = pltpu.VMEM((4, rows, width), bf)
    small = (n, 3 * rows // 2, LANES)
    all_of = lambda x: shape((planes,) + x.shape, x.dtype)
    gathered = lambda x: pltpu.VMEM((planes,) + x.shape, x.dtype)
    ring = dma((2, Gather.sems))
    half_ring = dma((2, HalfGather.sems))
    line = dma((3, planes))
    swap = dma((2, n))
    kept = (
        shape((n, rows, wide), bf), all_of(qkv_own), all_of(down_own),
        shape((2 * length, LANES), bf), shape((length, LANES), bf), shape((length, LANES), bf),
        shape((pairs * LANES, 384), f32), shape((pairs, 384), f32), shape((rows, width), f32),
        shape((2 * n, rows // 2, LANES), f32),
    )
    return pl.pallas_call(
        front_kernel,
        out_shape=(
            shape((rows, width), f32), shape((1, width), f32), shape((n,) + spot.shape, spot.dtype), shape((2, width), f32),
            shape(down_own.shape, bf),
        ) + kept + (shape((n, rows, width), bf), shape(small, bf), shape((n,) + small, bf), all_of(gu_own), shape(small, bf)),
        in_specs=vm(9) + anywhere(3),
        out_specs=vm(5) + anywhere(15),
        scratch_shapes=[pltpu.VMEM(x.shape, x.dtype) for x in kept] + [
            pltpu.VMEM(small, bf), pltpu.VMEM((rows, width), bf), pltpu.VMEM(spot.shape, jnp.int32), pltpu.VMEM(gain_own.shape, f32),
            pltpu.VMEM((2 * n, rows // 2, width), bf), pltpu.VMEM((n, rows, width), bf), pltpu.VMEM((n, rows, 2 * wide), bf),
            gathered(gu_own), gathered(out_own), pltpu.VMEM((planes, n) + out_own.shape, bf),
            pltpu.VMEM((16, 96, 2 * LANES), bf), gathered(gain_own), pltpu.SMEM((n,) + spot.shape, jnp.int32),
            pltpu.SMEM((2 * n,), jnp.int32), pltpu.VMEM(small, bf),
            pltpu.VMEM(small, bf), pltpu.VMEM((rows, width), bf),
            pltpu.VMEM((5, rows, width), f32), pltpu.VMEM((5, rows, width), bf), quads, halves, halves,
            gathered(down_own), pltpu.VMEM((planes + 1,) + down_own.shape, bf),
            half_ring, ring, swap, dma((2, planes)), line, line, ring, line, line, dma((16,)),
            swap, half_ring, dma((2, Reduce.sems)), swap, ring, dma((2, planes + 1)), swap,
        ],
        compiler_params=pltpu.CompilerParams(collective_id=1, has_side_effects=True, vmem_limit_bytes=67043328),
        name="front_moves",
    )(tok, pos, attn_own, ffn_own, qkv_own, gu_own, far_cos, far_sin, near, out_weight, down_weight, up)


def back_moves_kernel(
    tok, gain, ffn_gain, down_sum, spots_i,
    gu_i, middle_grad_i, hidden_i, down_i, k_i, q_i, v_i, agrad_i, att_i, lse_i, turn_i, normed_i, middle_i, qkv_i, mcols_i, low_i,
    grad, result, attn_sum, ffn_sum, down_all, gu_all, out_all, qkv_all,
    spots_s, agrad_at, gu_g, hidden, down_w, k_ref, q_ref, v_ref, agrad, att_ref, lse_ref, turn_ref, normed_in, middle, qkv_w, mcols_in, low_in, out_g, qkv_g, gu_r, out_r, qkv_r,
    mine, theirs, first, out, second, theirs2, first2, out2, second2, dk_ref, dv_ref, pg_sorted, mcols,
    gain_sum, mine_gain, ctx_gain, plane_sum, plane_gain,
    local_sem, sum_sem, reduce_sem, gu_zs, out_zs, qkv_zs, down_cs, gu_cs, out_cs, qkv_cs,
    gain_sem, plane_sem,
):
    place = Place()
    n = place.n
    rows = tok.shape[0]
    half = rows // 2
    pairs = 8
    width = tok.shape[1]
    length = n * rows
    loads = [
        pltpu.make_async_copy(source, target, local_sem.at[at])
        for at, (source, target) in enumerate((
            (gu_i, gu_g), (hidden_i, hidden), (down_i, down_w), (k_i, k_ref), (q_i, q_ref), (v_i, v_ref),
            (agrad_i, agrad), (att_i, att_ref), (lse_i, lse_ref), (turn_i, turn_ref), (middle_i, middle),
            (normed_i, normed_in), (qkv_i, qkv_w), (mcols_i, mcols_in), (low_i, low_in), (middle_grad_i, grad),
        ))
    ]
    table = pltpu.make_async_copy(spots_i, spots_s, local_sem.at[16])
    table.start()
    for load in loads:
        load.start()
    greet(place, planes=True)
    table.wait()
    early = [lax.div(spots_s[j, 0, 0], half) for j in range(pairs)]
    holder = []
    for t in range(pairs):
        at = 0
        for j in range(pairs):
            at = jnp.where(early[j] == t, j, at)
        holder.append(at)
    gu_z = PlaneReduce(place, gu_g, gu_r, gu_zs)
    out_z = PlaneReduce(place, out_g, out_r, out_zs)
    qkv_z = PlaneReduce(place, qkv_g, qkv_r, qkv_zs)
    sums = Reduce(place, mine, theirs, first, out, second, sum_sem)
    downs = Gather(place, down_sum, down_all, down_cs)
    gus = Gather(place, gu_z.own(), gu_all, gu_cs)
    loads[0].wait()
    gu_z.start()
    downs.start()
    loads[1].wait()
    loads[2].wait()

    def other(k, carry):
        theirs[k] = nn(hidden[flip(place, 2 * k + 1)], down_w[...].reshape(-1, width)).astype(jnp.bfloat16)
        sums.push(k)
        return carry

    def ours(k, carry):
        mine[k] = nn(hidden[flip(place, 2 * k)], down_w[...].reshape(-1, width))
        return carry

    lax.fori_loop(0, 4, other, 0)
    lax.fori_loop(0, 4, ours, 0)
    downs.relay()
    sums.across()
    sums.beside()
    for load in loads[3:11]:
        load.wait()

    def finish_rows(part, down_out):
        result[part, :] = (middle[part, :] + down_out).astype(jnp.bfloat16)

    def sums_done():
        sums.total(finish_rows)
        sums.finish()

    def columns_done():
        loads[13].wait()

        def unpack(q, carry):
            mcols[q] = unpacked(mcols_in[q])
            return carry

        lax.fori_loop(0, n, unpack, 0)

    steps = Steps(downs.rest, gu_z.step1, lambda: (downs.partner(), sums.turn()), columns_done)
    scaling = HEAD_DIM ** (-0.5)
    lane = lax.broadcasted_iota(jnp.int32, (half, LANES), 1)
    keys_t = k_ref[...].astype(jnp.float32).T.astype(jnp.bfloat16)
    ranks_s = agrad_at
    for t in range(pairs):
        ranks_s[t] = holder[t]
        ranks_s[2 * pairs - 1 - t] = holder[t]
    dk_ref[...] = jnp.zeros_like(dk_ref)
    dv_ref[...] = jnp.zeros_like(dv_ref)

    def back_group(group):
        before = group * 4 * half
        side = 0 if group < pairs // 4 else 1
        cuts = [(before, 4 * half)] + [(at, min(768, before - at)) for at in range(0, before, 768)]

        def back(place_of, carry):
            pair = 2 * group + place_of
            q = q_ref[pl.ds(pl.multiple_of(pair * 4 * half, 4 * half), 4 * half), :]
            firsts, seconds = [], []
            for part in range(2):
                piece_of = agrad[ranks_s[2 * pair + part]].astype(jnp.float32)
                left = piece_of[side * half : (side + 1) * half]
                tail = piece_of[2 * half :]
                right = tail if side == 0 else pltpu.roll(tail, 64, 1)
                firsts.append(jnp.where(lane < half, left, 0.0))
                seconds.append(
                    jnp.where(lane < half, pltpu.roll(jnp.where(lane < half, right, left), LANES - half, 1), 0.0)
                )
            grads = jnp.concatenate(firsts + seconds, axis=0)
            att_t = att_ref[pl.ds(pl.multiple_of(pair * LANES, LANES), LANES), :]
            delta = jnp.sum(grads.T * att_t, axis=0, keepdims=True)
            grads = grads.astype(jnp.bfloat16)
            dq_t = None
            for at, count in cuts:
                keys = pl.ds(at, count)
                weights = jnp.exp(
                    jnp.where(
                        causal(2 * half, place_of), nt(k_ref[keys, :], q) * scaling - lse_ref[pl.ds(pair, 1), :], -1e30
                    )
                    if at == before
                    else nt(k_ref[keys, :], q) * scaling - lse_ref[pl.ds(pair, 1), :]
                )
                dp = nt(v_ref[keys, :], grads)
                ds = (weights * (dp - delta)).astype(jnp.bfloat16)
                dk_ref[keys, :] += nn(ds, q) * scaling
                dv_ref[keys, :] += nn(weights.astype(jnp.bfloat16), grads)
                term = nn(keys_t[:, at : at + count], ds)
                dq_t = term if dq_t is None else dq_t + term
            dq = dq_t.T * scaling
            for part in range(2):
                cosine, sine = wave(turn_ref[2 * pair + part])
                turned = []
                for head in range(2):
                    z = dq[(2 * head + part) * half : (2 * head + part + 1) * half]
                    turned.append(close_halves(z * cosine - pltpu.roll(z, 64, 1) * sine))
                second_head = pltpu.roll(turned[1], 96, 1)
                pg_sorted[2 * pair + part, :, 0:LANES] = jnp.where(lane < 96, turned[0], second_head).astype(jnp.bfloat16)
                pg_sorted[2 * pair + part, :, LANES : 2 * LANES] = second_head.astype(jnp.bfloat16)
            return carry

        lax.fori_loop(0, 2, back, 0)

    for group in reversed(range(pairs // 2)):
        back_group(group)
        steps.next()
    for s in range(2 * pairs):
        spot = pl.ds(s * half, half)
        cosine, sine = wave(turn_ref[s])
        z = dk_ref[spot, :]
        key_head = pltpu.roll(close_halves(z * cosine - pltpu.roll(z, 64, 1) * sine), 64, 1)
        queries_too = pg_sorted[s, :, LANES : 2 * LANES].astype(jnp.float32)
        pg_sorted[s, :, LANES : 2 * LANES] = jnp.where(lane < 64, queries_too, key_head).astype(jnp.bfloat16)
        pg_sorted[s, :, 2 * LANES :] = jnp.where(lane < 32, key_head, pltpu.roll(dv_ref[spot, :], 32, 1)).astype(jnp.bfloat16)

    loads[11].wait()
    loads[12].wait()
    shard = gu_g.shape[1]

    def qkv_block(t, carry):
        left = normed_in[:, :, pl.ds(pl.multiple_of(t * shard, shard), shard)].reshape(length, shard)
        qkv_g[t] = tn(left, pg_sorted[...].reshape(length, 3 * LANES)).astype(jnp.bfloat16)
        return carry

    lax.fori_loop(0, 4, qkv_block, 0)
    qkv_z.start()
    grads = Reduce(place, mine, theirs2, first2, out2, second2, reduce_sem)

    def chunk(i):
        at = lax.div(spots_s[flip(place, i), 0, 0], half)
        rows_of = jnp.concatenate([pg_sorted[at], pg_sorted[2 * pairs - 1 - at]], axis=0)
        return nt(rows_of, qkv_w[...].reshape(width, -1))

    def push(k, carry):
        theirs2[k] = chunk(2 * k + 1).astype(jnp.bfloat16)
        grads.push(k)
        return carry

    def keep(k, carry):
        mine[k] = chunk(2 * k)
        return carry

    lax.fori_loop(0, 4, push, 0)
    sums_done()
    gu_z.step2()
    lax.fori_loop(0, 4, keep, 0)
    grads.across()
    grads.beside()
    loads[14].wait()
    loads[15].wait()

    def out_block(src, carry):
        heads = low_in[src, :, pl.ds(0, rows), :].reshape(length, LANES)
        tails = low_in[src, :, pl.ds(rows, half), :].reshape(length // 2, LANES)
        upper = tn(heads, mcols[...].reshape(length, rows))
        from_a = tn(tails, mcols[:, pl.ds(0, half), :].reshape(length // 2, rows))
        from_b = tn(tails, mcols[:, pl.ds(half, half), :].reshape(length // 2, rows))
        at = pl.multiple_of((src % 2) * rows, rows)
        out_g[src // 2, pl.ds(at, LANES), :] = upper.astype(jnp.bfloat16)
        out_g[src // 2, pl.ds(pl.multiple_of(at + LANES, 64), 64), :] = (from_a[:64] + from_b[64:]).astype(jnp.bfloat16)
        return carry

    lax.fori_loop(0, 8, out_block, 0)
    out_z.start()
    grads.turn()
    gu_z.total()
    gus.start()
    gain_sum[...] = jnp.zeros_like(gain_sum)

    def norm_back(part, normed_grad):
        x = tok[part, :].astype(jnp.float32)
        factor = lax.rsqrt(jnp.mean(x * x, axis=-1, keepdims=True) + epsilon)
        unit = x * factor
        gain_sum[...] += jnp.sum(normed_grad * unit, axis=0, keepdims=True)
        scaled = normed_grad * gain[pl.ds(0, 1), :]
        inner = jnp.mean(scaled * unit, axis=-1, keepdims=True)
        grad[part, :] = grad[part, :] + factor * (scaled - unit * inner)

    qkv_z.step1()
    grads.total(norm_back)
    gain_grad = gain_sum[...]
    count = mine_gain.shape[0] // 2
    for at in range(count):
        mine_gain[pl.ds(at, 1), :] = gain_grad[:, at * shard : (at + 1) * shard]
        mine_gain[pl.ds(count + at, 1), :] = ffn_gain[:, at * shard : (at + 1) * shard]
    ctx_sum = Share(place, mine_gain, ctx_gain, gain_sem)
    ctx_sum.start()
    gus.relay()
    qkv_z.step2()
    out_z.step1()
    ctx_sum.finish()
    plane_sum[...] = jnp.sum(ctx_gain[...], axis=0)
    planes = PlaneShare(place, plane_sum, plane_gain, plane_sem)
    planes.start()
    out_z.step2()
    qkv_z.total()
    gus.rest()
    qkvs = Gather(place, qkv_z.own(), qkv_all, qkv_cs)
    qkvs.start()
    out_z.total()
    outs = Gather(place, out_z.own(), out_all, out_cs)
    qkvs.relay()
    outs.start()
    qkvs.rest()
    outs.relay()
    outs.rest()
    planes.finish()
    plane_sum[...] = jnp.sum(plane_gain[...], axis=0)
    attn_sum[...] = plane_sum[pl.ds(place.z, 1), :]
    ffn_sum[...] = plane_sum[pl.ds(count + place.z, 1), :]
    gus.partner()
    qkvs.partner()
    outs.partner()
    for move in (gu_z, out_z, qkv_z, downs, gus, outs, qkvs, grads):
        move.finish()


def back_moves(tok, gain, ffn_gain, down_sum, spots, *moved):
    n, planes = lax.axis_size("ctx"), lax.axis_size("fsdp")
    rows, width = tok.shape
    length = n * rows
    shard = width // planes
    bf, f32 = jnp.bfloat16, jnp.float32
    shape = jax.ShapeDtypeStruct
    dma = pltpu.SemaphoreType.DMA
    halves = pltpu.VMEM((6, rows // 2, width), bf)
    quads = pltpu.VMEM((4, rows, width), bf)
    small = (2 * planes, shard)
    parts = (moved[0].shape[1:], (shard, rows), (shard, 3 * LANES))
    ring = dma((2, Gather.sems))
    return pl.pallas_call(
        back_moves_kernel,
        out_shape=(shape((rows, width), f32), shape((rows, width), bf), shape((1, shard), f32), shape((1, shard), f32))
        + tuple(shape((n,) + part, bf) for part in (down_sum.shape,) + parts),
        in_specs=vm(4) + anywhere(1 + len(moved)),
        out_specs=vm(4) + anywhere(4),
        scratch_shapes=[pltpu.SMEM(spots.shape, jnp.int32), pltpu.SMEM((2 * n,), jnp.int32)] + [pltpu.VMEM(x.shape, x.dtype) for at, x in enumerate(moved) if at != 1]
        + [pltpu.VMEM((planes,) + part, bf) for part in parts[1:]]
        + [pltpu.VMEM((planes + 1,) + part, bf) for part in parts]
        + [
            pltpu.VMEM((4, rows, width), f32), quads, quads, halves, halves, quads, quads, halves, halves,
            pltpu.VMEM((length, LANES), f32), pltpu.VMEM((length, LANES), f32), pltpu.VMEM((16, 96, 3 * LANES), bf),
            pltpu.VMEM((n, rows, rows), bf),
            pltpu.VMEM((1, width), f32), pltpu.VMEM(small, f32), pltpu.VMEM((n,) + small, f32),
            pltpu.VMEM(small, f32), pltpu.VMEM((planes,) + small, f32),
            dma((17,)), dma((2, Reduce.sems)), dma((2, Reduce.sems)),
            dma((2, 5)), dma((2, 5)), dma((2, 5)), ring, ring, ring, ring, dma((2, n)), dma((2, planes)),
        ],
        compiler_params=pltpu.CompilerParams(collective_id=6, has_side_effects=True, vmem_limit_bytes=67043328),
        name="back_moves",
    )(tok, gain, ffn_gain, down_sum, spots, *moved)


def pack_kernel(
    down, gu, out, qkv, grad, result, attn, ffn, down_o, gu_o, out_o, qkv_o, grad_o, result_o, attn_o, ffn_o
):
    devices, rows = gu.shape[0], gu.shape[1]
    f32 = jnp.float32
    lane = lax.broadcasted_iota(jnp.int32, (rows, LANES), 1)
    down_o[...] = down[0].astype(f32)
    grad_o[...] = grad[...]
    result_o[...] = result[...]
    attn_o[...] = attn[...]
    ffn_o[...] = ffn[...]
    tiles = gu_o.shape[0] // rows
    spans = gu.shape[2] // (2 * LANES)
    for r in range(0, rows, 16):
        pieces = [
            gu[c, pl.ds(r, 16), (s * spans + z) * LANES : (s * spans + z + 1) * LANES].astype(f32)
            for z in range(spans) for c in range(devices) for s in range(2)
        ]
        gu_o[pl.ds(r * tiles, 16 * tiles), :] = jnp.swapaxes(jnp.stack(pieces, axis=0), 0, 1).reshape(16 * tiles, LANES)

    def tile(c, at):
        return qkv[c, :, at * LANES : (at + 1) * LANES].astype(f32)

    def key_head(c):
        return jnp.where(lane < 64, pltpu.roll(tile(c, 1), 64, 1), pltpu.roll(tile(c, 2), 64, 1))

    def value_head(c):
        return pltpu.roll(tile(c, 2), 96, 1)

    def store(at, heads):
        second, third, fourth = pltpu.roll(heads[1], 96, 1), pltpu.roll(heads[2], 64, 1), pltpu.roll(heads[3], 32, 1)
        qkv_o[:, at : at + LANES] = jnp.where(lane < 96, heads[0], second)
        qkv_o[:, at + LANES : at + 2 * LANES] = jnp.where(lane < 64, second, third)
        qkv_o[:, at + 2 * LANES : at + 3 * LANES] = jnp.where(lane < 32, third, fourth)

    for c in range(0, devices, 2):
        at = c * 192
        turned = pltpu.roll(tile(c + 1, 0), 64, 1)
        qkv_o[:, at : at + LANES] = tile(c, 0)
        qkv_o[:, at + LANES : at + 2 * LANES] = jnp.where(lane < 64, tile(c, 1), turned)
        qkv_o[:, at + 2 * LANES : at + 3 * LANES] = jnp.where(lane < 64, turned, pltpu.roll(tile(c + 1, 1), 64, 1))
    for c in range(0, devices, 4):
        store(HEADS * HEAD_DIM + c * 96, [key_head(c + i) for i in range(4)])
        store((HEADS + KV_HEADS) * HEAD_DIM + c * 96, [value_head(c + i) for i in range(4)])
    for c in range(0, devices, 2):
        at = c * 192
        first = out[c].astype(f32)
        second = out[c + 1].astype(f32)
        tail = jnp.concatenate([first[:, LANES:], jnp.zeros((rows, 64), f32)], axis=1)
        next_tail = jnp.concatenate([second[:, LANES:], jnp.zeros((rows, 64), f32)], axis=1)
        turned = pltpu.roll(second[:, :LANES], 64, 1)
        out_o[:, at : at + LANES] = first[:, :LANES]
        out_o[:, at + LANES : at + 2 * LANES] = jnp.where(lane < 64, tail, turned)
        out_o[:, at + 2 * LANES : at + 3 * LANES] = jnp.where(lane < 64, turned, pltpu.roll(next_tail, 64, 1))


def pack(down, gu, out, qkv, grad, result, attn, ffn):
    n, shard = gu.shape[0], gu.shape[1]
    rows = shard // n
    width = down.shape[2]
    f32 = jnp.float32
    spec = pl.BlockSpec
    shape = jax.ShapeDtypeStruct
    tiles = n * gu.shape[2] // LANES
    quarter = grad.shape[0] // 4
    return pl.pallas_call(
        pack_kernel,
        grid=(n,),
        out_shape=(
            shape((n * down.shape[1], width), f32), shape((shard * tiles, LANES), f32), shape((shard, n * out.shape[2]), f32),
            shape((shard, (HEADS + 2 * KV_HEADS) * HEAD_DIM), f32), shape(grad.shape, f32), shape(result.shape, result.dtype), shape(attn.shape, f32), shape(ffn.shape, f32),
        ),
        in_specs=[
            spec((1,) + down.shape[1:], lambda i: (i, 0, 0)), spec((n, rows, gu.shape[2]), lambda i: (0, i, 0)),
            spec((n, rows, out.shape[2]), lambda i: (0, i, 0)), spec((n, rows, qkv.shape[2]), lambda i: (0, i, 0)),
            spec((quarter, width), lambda i: (i // 2, 0)), spec((quarter, width), lambda i: (i // 2, 0)),
            spec(attn.shape, lambda i: (0, 0)), spec(ffn.shape, lambda i: (0, 0)),
        ],
        out_specs=[
            spec((down.shape[1], width), lambda i: (i, 0)), spec((rows * tiles, LANES), lambda i: (i, 0)),
            spec((rows, n * out.shape[2]), lambda i: (i, 0)), spec((rows, (HEADS + 2 * KV_HEADS) * HEAD_DIM), lambda i: (i, 0)),
            spec((quarter, width), lambda i: (i // 2, 0)), spec((quarter, width), lambda i: (i // 2, 0)),
            spec(attn.shape, lambda i: (0, 0)), spec(ffn.shape, lambda i: (0, 0)),
        ],
        name="pack",
    )(down, gu, out, qkv, grad, result, attn, ffn)


def fast_body(
    tokens, positions, qkv_weight, out_weight, gate_up_weight, down_weight, attn_gain, ffn_gain, cotangent
):
    me = lax.axis_index("ctx")
    n = lax.axis_size("ctx")
    planes = lax.axis_size("fsdp")
    rows = tokens.shape[1]
    length = n * rows
    width = tokens.shape[2]
    wide = down_weight.shape[1] * planes
    own = wide // n
    piece = own // planes
    shard = qkv_weight.shape[1]
    query_width = HEADS * HEAD_DIM
    key_width = KV_HEADS * HEAD_DIM
    cut = lax.dynamic_slice_in_dim

    qkv = qkv_weight[0]
    q_part = cut(qkv, me * 2 * HEAD_DIM, 2 * HEAD_DIM, 1)
    k_part = cut(qkv, query_width + me * HEAD_DIM, HEAD_DIM, 1)
    v_part = cut(qkv, query_width + key_width + me * HEAD_DIM, HEAD_DIM, 1)
    qkv_own = jnp.concatenate([q_part, k_part, v_part], axis=1)
    pieces = [cut(gate_up_weight[0], at * (wide // planes) + me * piece, piece, 2) for at in range(planes)]
    gate_up_own = jnp.concatenate(pieces, axis=2).reshape(shard, 2 * own)
    (
        middle_grad, ffn_partial, spots, gains, down_sum, hidden, qkv_block, down_block, q, k, v, att, lse, middle,
        turns, normed, attended_grad, low_all, gate_up_grad, middle_cols,
    ) = front_moves(
        tokens[0], positions, attn_gain, ffn_gain, qkv_own, gate_up_own, *turn_parts(2 * n, rows // 2),
        out_weight, down_weight, cotangent[0],
    )
    stream_grad, result, attn_sum, ffn_sum, down_grad, gate_up_grad, out_grad, qkv_grad = back_moves(
        tokens[0], gains, ffn_partial, down_sum, spots,
        gate_up_grad, middle_grad, hidden, down_block, k, q, v, attended_grad, att, lse, turns, normed, middle,
        qkv_block, middle_cols, low_all,
    )
    down_grad, gate_up_grad, out_grad, qkv_grad, stream_grad, result, attn_sum, ffn_sum = pack(
        down_grad, gate_up_grad, out_grad, qkv_grad, stream_grad, result, attn_sum, ffn_sum
    )
    gate_up_grad = gate_up_grad.reshape(shard, wide // LANES, 2, LANES).transpose(0, 2, 1, 3).reshape(shard, 2, wide)
    return (
        result[None],
        stream_grad[None],
        qkv_grad[None],
        out_grad[None],
        gate_up_grad[None],
        down_grad[None],
        attn_sum,
        ffn_sum,
    )


def solution(mesh):
    split = mesh.shape["ctx"] == KV_HEADS and mesh.shape["fsdp"] == 4
    placed = (
        P("fsdp", "ctx", None),
        P("fsdp", "ctx"),
        P(None, "fsdp", None),
        P(None, "fsdp", None),
        P(None, "fsdp", None, None),
        P(None, "fsdp", None),
        P(None, "fsdp"),
        P(None, "fsdp"),
        P("fsdp", "ctx", None),
    )
    return jax.shard_map(
        fast_body if split else body,
        mesh=mesh,
        in_specs=placed,
        out_specs=(
            P("fsdp", "ctx", None),
            P("fsdp", "ctx", None),
            P(None, "fsdp", None),
            P(None, "fsdp", None),
            P(None, "fsdp", None, None),
            P(None, "fsdp", None),
            P(None, "fsdp"),
            P(None, "fsdp"),
        ),
        check_vma=False,
    )
```
